32 devices in a mesh: comp: 2 (over core), lat: 4 (over z), lon: 4 (over y, x).
Axes of the slice: x: 2, y: 2, z: 4, core: 2. Of those that a mesh axis runs over, the one named last changes fastest.
Arguments:
- fields: float32 [2, 7, 2048, 256], P('comp', None, ('lat', 'lon')), may hold values from -4 to 4, as said below
- block_owner: int32 [2048], P(('lat', 'lon')), may hold values from 0 to 2047, as said below
- ice_covered: int32 [2048], P(('lat', 'lon')), may hold values 0 or 1
- land_mask: int32 [2048, 256], P(('lat', 'lon')), may hold values 0 or 1
Outputs:
- coupled_out: float32 [2, 2, 2048, 256], P('comp', None, ('lat', 'lon'))
The draws below stay inside these ranges and needn't reach their ends.
Inputs may be any that keep to these rules, and one draw needn't show every extreme that they name: `block_owner`: every block id appears once. Slot d of lat+lon index o holds a block of the ice tile of index d, that is an id from d * 128 to d * 128 + 127. `fields`: ocean channels: winds within 4, currents within 1.5, tilts within 1, air density 0.9 to 1.3; ice channels: velocities within 1.5, mass 0.5 to 4, concentration 0.05 to 1, stresses within 1.5.
All inputs are finite; a program needn't handle non-finite values.
Results may differ from the reference program's by a relative error of at most 0.00002.
Values sent between devices are 32-bit elements.
A program may use at most 64 MiB of HBM per device.

```python
import jax
import jax.numpy as jnp

KB = 128
GX = 1
BY = 2
BX = 128
NSUB = 4
NBALL = 2048
CELLS = 256
N_LAT = 4
N_LON = 4


def clipped_normal(subkey, scale, limit):
    return jnp.clip(scale * jax.random.normal(subkey, (NBALL, CELLS), jnp.float32), -limit, limit)


def uniform_draw(subkey, low, high):
    return jax.random.uniform(subkey, (NBALL, CELLS), jnp.float32, low, high)


def draw_fields(key, part):
    subkeys = jax.random.split(jax.random.fold_in(key, 11), 14)
    wind = [clipped_normal(subkeys[0], 1.5, 4.0), clipped_normal(subkeys[1], 1.5, 4.0)]
    current = [clipped_normal(subkeys[2], 0.5, 1.5), clipped_normal(subkeys[3], 0.5, 1.5)]
    tilt = [clipped_normal(subkeys[4], 0.3, 1.0), clipped_normal(subkeys[5], 0.3, 1.0)]
    drift = [clipped_normal(subkeys[7], 0.5, 1.5), clipped_normal(subkeys[8], 0.5, 1.5)]
    concentration = uniform_draw(subkeys[10], 0.05, 1.0)
    stresses = [clipped_normal(subkeys[11], 0.5, 1.5), clipped_normal(subkeys[12], 0.5, 1.5), clipped_normal(subkeys[13], 0.5, 1.5)]
    density = uniform_draw(subkeys[6], 0.9, 1.3)
    ice_mass = jnp.exp(uniform_draw(subkeys[9], jnp.log(0.5), jnp.log(4.0)))
    ocean = jnp.stack(wind + current + tilt + [density])
    sea_ice = jnp.stack(drift + [ice_mass, concentration] + stresses)
    return jnp.stack([ocean, sea_ice]).astype(jnp.float32)


def draw_block_owner(key, part):
    devices = N_LAT * N_LON
    per_peer = KB // devices
    subkeys = jax.random.split(jax.random.fold_in(key, 5), devices)
    orders = jax.vmap(lambda subkey: jax.random.permutation(subkey, KB))(subkeys)
    ids = orders.astype(jnp.int32) + (jnp.arange(devices, dtype=jnp.int32) * KB)[:, None]
    ids = ids.reshape(devices, devices, per_peer).transpose(1, 0, 2)
    return ids.reshape(devices * KB).astype(jnp.int32)


def plant(array, key, smallest, largest):
    extent = array.shape
    place = [jax.random.randint(jax.random.fold_in(key, axis), (), 0, extent[axis]) for axis in range(len(extent))]
    array = array.at[tuple(place)].set(smallest)
    longest = extent.index(max(extent))
    place[longest] = (place[longest] + 1) % extent[longest]
    return array.at[tuple(place)].set(largest)


def setup_inputs(seed: int = 0) -> dict:
    streams_of = jax.random.split(jax.random.key(seed), 5)
    fields = draw_fields(jax.random.fold_in(streams_of[4], 71), 0)
    block_owner = draw_block_owner(jax.random.fold_in(streams_of[4], 71), 0)
    ice_covered = plant((jax.random.randint(streams_of[2], (NBALL,), 0, 4) < 3).astype(jnp.int32), jax.random.fold_in(streams_of[2], 1), 0, 1)
    land_mask = plant((jax.random.randint(streams_of[3], (NBALL, CELLS), 0, 8) < 1).astype(jnp.int32), jax.random.fold_in(streams_of[3], 1), 0, 1)
    return dict(fields=fields, block_owner=block_owner, ice_covered=ice_covered, land_mask=land_mask)


CD_ICE = 0.1
CW = 1.5
CSTAR = 2.0
ECC2 = 4.0
DMIN2 = 0.25
RELAX = 0.5
DTE = 0.5
CORIO = 0.3
MASS_FLOOR = 0.5
DRAG_FLOOR = 0.1

def air_stress(ocean):
    wind_x, wind_y, current_x, current_y, tilt_x, tilt_y, density = ocean
    speed_ice = jnp.sqrt(wind_x * wind_x + wind_y * wind_y + 1.0)
    scale_ice = density * CD_ICE * speed_ice
    rel_x = wind_x - current_x
    rel_y = wind_y - current_y
    speed_open = jnp.sqrt(rel_x * rel_x + rel_y * rel_y + 1.0)
    scale_open = density * (0.1 + 0.05 * speed_open) * speed_open
    outbound = jnp.stack([scale_ice * wind_x, scale_ice * wind_y, current_x, current_y, tilt_x, tilt_y])
    open_stress = jnp.stack([scale_open * rel_x, scale_open * rel_y])
    return (outbound, open_stress)

def prepare(ice_tile, forcing, active):
    ice_mass = ice_tile[2]
    concentration = ice_tile[3]
    strength = ice_mass * jnp.exp(CSTAR * (concentration - 1.0)) * active
    drag_base = CW * concentration * active
    push_x = active * (concentration * forcing[0] - ice_mass * forcing[4])
    push_y = active * (concentration * forcing[1] - ice_mass * forcing[5])
    return jnp.stack([strength, ice_mass, drag_base, push_x, push_y, forcing[2], forcing[3], active])

def subcycle(ice_state, statics):
    east_vel, north_vel, stress_one, stress_two, stress_three = ice_state
    strength = statics[0]
    east_base = east_vel[:-1, :-1]
    north_base = north_vel[:-1, :-1]
    strain_xx = east_vel[:-1, 1:] - east_base
    strain_yy = north_vel[1:, :-1] - north_base
    shear = east_vel[1:, :-1] - east_base + (north_vel[:-1, 1:] - north_base)
    divergence = strain_xx + strain_yy
    tension = strain_xx - strain_yy
    delta_norm = jnp.sqrt(divergence * divergence + (tension * tension + shear * shear) / ECC2 + DMIN2)
    viscosity = strength[:-1, :-1] / delta_norm
    stress_sum = (stress_one[:-1, :-1] + RELAX * viscosity * (divergence - delta_norm)) / (1.0 + RELAX)
    stress_diff = (stress_two[:-1, :-1] + RELAX * viscosity * tension / ECC2) / (1.0 + RELAX)
    stress_shear = (stress_three[:-1, :-1] + RELAX * viscosity * shear / (2.0 * ECC2)) / (1.0 + RELAX)
    stress_xx = 0.5 * (stress_sum + stress_diff)
    stress_yy = 0.5 * (stress_sum - stress_diff)
    force_x = stress_xx[1:, 1:] - stress_xx[1:, :-1] + (stress_shear[1:, 1:] - stress_shear[:-1, 1:])
    force_y = stress_shear[1:, 1:] - stress_shear[1:, :-1] + (stress_yy[1:, 1:] - stress_yy[:-1, 1:])
    trimmed = statics[:, 1:-1, 1:-1]
    strength, ice_mass, drag_base, push_x, push_y, current_x, current_y, active = trimmed
    east_old = east_vel[1:-1, 1:-1]
    north_old = north_vel[1:-1, 1:-1]
    diff_x = current_x - east_old
    diff_y = current_y - north_old
    drag_coef = drag_base * jnp.sqrt(diff_x * diff_x + diff_y * diff_y + DRAG_FLOOR)
    denominator = jnp.maximum(ice_mass, MASS_FLOOR) / DTE + drag_coef
    east_new = active * (ice_mass / DTE * east_old + force_x + push_x + drag_coef * current_x + CORIO * ice_mass * north_old) / denominator
    north_new = active * (ice_mass / DTE * north_old + force_y + push_y + drag_coef * current_y - CORIO * ice_mass * east_old) / denominator
    new_state = jnp.stack([east_new, north_new, stress_sum[1:, 1:], stress_diff[1:, 1:], stress_shear[1:, 1:]])
    return (new_state, trimmed)

def give_back(ice_state, statics):
    east_vel = ice_state[0]
    north_vel = ice_state[1]
    drag_base = statics[2]
    current_x = statics[5]
    current_y = statics[6]
    diff_x = east_vel - current_x
    diff_y = north_vel - current_y
    factor = drag_base * jnp.sqrt(diff_x * diff_x + diff_y * diff_y + DRAG_FLOOR)
    return jnp.stack([factor * diff_x, factor * diff_y, drag_base / CW])

def to_grid(blocks):
    channels = blocks.shape[0]
    arranged = blocks.reshape(channels, N_LAT, N_LON, KB // GX, GX, BY, BX)
    arranged = arranged.transpose(0, 1, 3, 5, 2, 4, 6)
    return arranged.reshape(channels, N_LAT * (KB // GX) * BY, N_LON * GX * BX)

def from_grid(values):
    channels = values.shape[0]
    arranged = values.reshape(channels, N_LAT, KB // GX, BY, N_LON, GX, BX)
    arranged = arranged.transpose(0, 1, 4, 2, 5, 3, 6)
    return arranged.reshape(channels, N_LAT * N_LON * KB, BY * BX)

def extend_grid(values, width):
    values = jnp.concatenate([values[..., -width:], values, values[..., :width]], axis=-1)
    return jnp.pad(values, ((0, 0), (width, width), (0, 0)))

def reference(fields, block_owner, ice_covered, land_mask):
    outbound, open_stress = air_stress(fields[0])
    geographic = jnp.zeros_like(outbound).at[:, block_owner].set(outbound)
    forcing = to_grid(geographic)
    ice_tile = to_grid(fields[1])
    covered = ice_covered.astype(jnp.float32)[:, None] * (1 - land_mask).astype(jnp.float32)
    active = to_grid(covered[None])[0]
    statics = prepare(ice_tile, forcing, active)
    ice_state = jnp.stack([ice_tile[0], ice_tile[1], ice_tile[4], ice_tile[5], ice_tile[6]])
    ice_state = extend_grid(ice_state, NSUB)
    statics = extend_grid(statics, NSUB)
    for repeat in range(NSUB):
        ice_state, statics = subcycle(ice_state, statics)
    returned = from_grid(give_back(ice_state, statics))
    received_back = returned[:, block_owner]
    ocean_out = received_back[:2] + (1.0 - received_back[2]) * open_stress
    ice_out = from_grid(ice_state[:2])
    return jnp.stack([ocean_out, ice_out])
```

```python
import functools

import jax
import jax.numpy as jnp
from jax import lax
from jax.experimental import pallas as pl
from jax.experimental.pallas import tpu as pltpu
from jax.sharding import PartitionSpec as P

GX = 1
BY = 2
BX = 128
NSUB = 4


CD_ICE = 0.1
CW = 1.5
CSTAR = 2.0
ECC2 = 4.0
DMIN2 = 0.25
RELAX = 0.5
DTE = 0.5
CORIO = 0.3
MASS_FLOOR = 0.5
DRAG_FLOOR = 0.1


def from_behind(x, axis, by):
    size = lax.axis_size(axis)
    pairs = [(i, i + by) for i in range(size) if 0 <= i + by < size]
    return lax.ppermute(x, axis, pairs)


def with_halo(x, sides, width, wrap):
    for axis, dim in sides:
        size, length = (lax.axis_size(axis), x.shape[dim])
        up = [(i, (i + 1) % size) for i in range(size if wrap else size - 1)]
        down = [(j, i) for i, j in up]
        last = lax.slice_in_dim(x, length - width, length, axis=dim)
        first = lax.slice_in_dim(x, 0, width, axis=dim)
        before = lax.ppermute(last, axis, up)
        after = lax.ppermute(first, axis, down)
        x = jnp.concatenate([before, x, after], axis=dim)
    return x


def air_stress(ocean):
    wind_x, wind_y, current_x, current_y, tilt_x, tilt_y, density = ocean
    speed_ice = jnp.sqrt(wind_x * wind_x + wind_y * wind_y + 1.0)
    scale_ice = density * CD_ICE * speed_ice
    rel_x = wind_x - current_x
    rel_y = wind_y - current_y
    speed_open = jnp.sqrt(rel_x * rel_x + rel_y * rel_y + 1.0)
    scale_open = density * (0.1 + 0.05 * speed_open) * speed_open
    outbound = jnp.stack(
        [scale_ice * wind_x, scale_ice * wind_y, current_x, current_y, tilt_x, tilt_y]
    )
    open_stress = jnp.stack([scale_open * rel_x, scale_open * rel_y])
    return (outbound, open_stress)


def prepare(ice_tile, forcing, active):
    ice_mass = ice_tile[2]
    concentration = ice_tile[3]
    strength = ice_mass * jnp.exp(CSTAR * (concentration - 1.0)) * active
    drag_base = CW * concentration * active
    push_x = active * (concentration * forcing[0] - ice_mass * forcing[4])
    push_y = active * (concentration * forcing[1] - ice_mass * forcing[5])
    return jnp.stack(
        [strength, ice_mass, drag_base, push_x, push_y, forcing[2], forcing[3], active]
    )


def subcycle(ice_state, statics):
    east_vel, north_vel, stress_one, stress_two, stress_three = ice_state
    strength = statics[0]
    east_base = east_vel[:-1, :-1]
    north_base = north_vel[:-1, :-1]
    strain_xx = east_vel[:-1, 1:] - east_base
    strain_yy = north_vel[1:, :-1] - north_base
    shear = east_vel[1:, :-1] - east_base + (north_vel[:-1, 1:] - north_base)
    divergence = strain_xx + strain_yy
    tension = strain_xx - strain_yy
    delta_norm = jnp.sqrt(
        divergence * divergence + (tension * tension + shear * shear) / ECC2 + DMIN2
    )
    viscosity = strength[:-1, :-1] / delta_norm
    stress_sum = (stress_one[:-1, :-1] + RELAX * viscosity * (divergence - delta_norm)) / (
        1.0 + RELAX
    )
    stress_diff = (stress_two[:-1, :-1] + RELAX * viscosity * tension / ECC2) / (1.0 + RELAX)
    stress_shear = (stress_three[:-1, :-1] + RELAX * viscosity * shear / (2.0 * ECC2)) / (
        1.0 + RELAX
    )
    stress_xx = 0.5 * (stress_sum + stress_diff)
    stress_yy = 0.5 * (stress_sum - stress_diff)
    force_x = (
        stress_xx[1:, 1:] - stress_xx[1:, :-1] + (stress_shear[1:, 1:] - stress_shear[:-1, 1:])
    )
    force_y = (
        stress_shear[1:, 1:] - stress_shear[1:, :-1] + (stress_yy[1:, 1:] - stress_yy[:-1, 1:])
    )
    trimmed = statics[:, 1:-1, 1:-1]
    strength, ice_mass, drag_base, push_x, push_y, current_x, current_y, active = trimmed
    east_old = east_vel[1:-1, 1:-1]
    north_old = north_vel[1:-1, 1:-1]
    diff_x = current_x - east_old
    diff_y = current_y - north_old
    drag_coef = drag_base * jnp.sqrt(diff_x * diff_x + diff_y * diff_y + DRAG_FLOOR)
    denominator = jnp.maximum(ice_mass, MASS_FLOOR) / DTE + drag_coef
    east_new = (
        active
        * (
            ice_mass / DTE * east_old
            + force_x
            + push_x
            + drag_coef * current_x
            + CORIO * ice_mass * north_old
        )
        / denominator
    )
    north_new = (
        active
        * (
            ice_mass / DTE * north_old
            + force_y
            + push_y
            + drag_coef * current_y
            - CORIO * ice_mass * east_old
        )
        / denominator
    )
    new_state = jnp.stack(
        [east_new, north_new, stress_sum[1:, 1:], stress_diff[1:, 1:], stress_shear[1:, 1:]]
    )
    return (new_state, trimmed)


def give_back(ice_state, statics):
    east_vel = ice_state[0]
    north_vel = ice_state[1]
    drag_base = statics[2]
    current_x = statics[5]
    current_y = statics[6]
    diff_x = east_vel - current_x
    diff_y = north_vel - current_y
    factor = drag_base * jnp.sqrt(diff_x * diff_x + diff_y * diff_y + DRAG_FLOOR)
    return jnp.stack([factor * diff_x, factor * diff_y, drag_base / CW])


def to_tile(blocks):
    channels, count, cells = blocks.shape
    arranged = blocks.reshape(channels, count // GX, GX, BY, BX).transpose(0, 1, 3, 2, 4)
    return arranged.reshape(channels, count // GX * BY, GX * BX)


def from_tile(values):
    channels, rows, columns = values.shape
    arranged = values.reshape(channels, rows // BY, BY, GX, BX).transpose(0, 1, 3, 2, 4)
    return arranged.reshape(channels, rows // BY * GX, BY * BX)


def per_device(fields, block_owner, ice_covered, land_mask):
    count = block_owner.shape[0]
    is_ocean = lax.axis_index("comp") == 0
    outbound, open_stress = air_stress(fields[0])
    owner_row = block_owner.reshape(1, count)
    crossed = from_behind(outbound, "comp", 1)
    received, anchor = (
        lax.all_to_all(crossed, ("lat", "lon"), split_axis=1, concat_axis=1, tiled=True),
        lax.all_to_all(owner_row, ("lat", "lon"), split_axis=1, concat_axis=1, tiled=True),
    )
    local_ids = anchor[0] % count
    position = jnp.zeros((count,), jnp.int32).at[local_ids].set(jnp.arange(count, dtype=jnp.int32))
    forcing = to_tile(received[:, position])
    ice_tile = to_tile(fields[0])
    covered = ice_covered.astype(jnp.float32)[:, None] * (1 - land_mask).astype(jnp.float32)
    active = to_tile(covered[None])[0]
    statics = prepare(ice_tile, forcing, active)
    ice_state = jnp.stack([ice_tile[0], ice_tile[1], ice_tile[4], ice_tile[5], ice_tile[6]])
    joined = jnp.concatenate([ice_state, statics], 0)
    joined = with_halo(joined, (("lon", 2),), NSUB, True)
    joined = with_halo(joined, (("lat", 1),), NSUB, False)
    ice_state = joined[:5]
    statics = joined[5:]
    for repeat in range(NSUB):
        ice_state, statics = subcycle(ice_state, statics)
    returned = from_tile(give_back(ice_state, statics))
    back_send = returned[:, local_ids]
    regrouped = lax.all_to_all(back_send, ("lat", "lon"), split_axis=1, concat_axis=1, tiled=True)
    received_back = from_behind(regrouped, "comp", -1)
    ocean_out = received_back[:2] + (1.0 - received_back[2]) * open_stress
    ice_out = from_tile(ice_state[:2])
    return jnp.where(is_ocean, ocean_out, ice_out)[None]


LEAD = 16
GROUP = 6
TILE = 8
MESH = pl.DeviceIdType.MESH
DIRECTIONS = [(a, b) for a in (-1, 0, 1) for b in (-1, 0, 1) if (a, b) != (0, 0)]
U, V, MASS, CONC, S1, S2, S12, ACTIVE, PUSH_X, PUSH_Y, CUR_X, CUR_Y = range(12)


def tile_loop(tiles, together, body):
    def step(k, carry):
        for j in range(together):
            body(k * together + j)
        return carry
    lax.fori_loop(0, tiles // together, step, 0)


def split_dot(one_hot, values, contract):
    total = None
    rest = values
    for piece in range(3):
        part = rest.astype(jnp.bfloat16)
        if piece < 2:
            rest = rest - part.astype(jnp.float32)
        term = lax.dot_general(
            one_hot, part, ((contract, (0,)), ((), ())), preferred_element_type=jnp.float32
        )
        total = term if total is None else total + term
    return total


def step_kernel(
    n_lat, n_lon,
    fields, owner, covered, land, out,
    surf, open_st, ret, ids, recv, grid, strength, dragb, forc, one_hot, back, land_v,
    pack_early, pack_mid, pack_late, got_early, got_mid, got_late,
    load_sem, ids_ssem, ids_rsem, fwd_ssem, fwd_rsem, ret_ssem, ret_rsem,
    early_ssem, early_rsem, mid_ssem, mid_rsem, late_ssem, late_rsem,
):
    comp = lax.axis_index("comp")
    lat = lax.axis_index("lat")
    lon = lax.axis_index("lon")
    peers = n_lat * n_lon
    me = lat * n_lon + lon
    count = owner.shape[1]
    per = count // peers
    width = BX
    barrier = pltpu.get_barrier_semaphore()

    def rows_of(peer):
        return pl.ds(pl.multiple_of(peer * per, per), per)

    def device(kind, peer):
        return (kind, peer // n_lon, peer % n_lon)

    def each_peer(body):
        def step(k, carry):
            body((me + k) % peers)
            return carry
        lax.fori_loop(0, peers, step, 0)

    def signal_peers(kind):
        each_peer(
            lambda p: pl.semaphore_signal(
                barrier, inc=1, device_id=device(kind, p), device_id_type=MESH
            )
        )

    def send_rows(kind, src, lo, num, dst, dlo, ssem, rsem):
        def body(p):
            pltpu.make_async_remote_copy(
                src_ref=src.at[pl.ds(lo, num), rows_of(p), :],
                dst_ref=dst.at[pl.ds(dlo, num), rows_of(me), :],
                send_sem=ssem, recv_sem=rsem,
                device_id=device(kind, p), device_id_type=MESH,
            ).start()
        each_peer(body)

    def wait_bytes(ref, sem):
        pltpu.make_async_copy(ref, ref, sem).wait()

    @pl.when(comp == 0)
    def _ocean():
        signal_peers(1)
        raw = pltpu.make_async_copy(fields.at[0, pl.ds(2, 4)], surf.at[pl.ds(2, 4)], load_sem.at[0])
        wind = pltpu.make_async_copy(fields.at[0, pl.ds(0, 2)], surf.at[pl.ds(0, 2)], load_sem.at[1])
        rho = pltpu.make_async_copy(fields.at[0, pl.ds(6, 1)], surf.at[pl.ds(6, 1)], load_sem.at[2])
        raw.start()
        wind.start()
        rho.start()
        pl.semaphore_wait(barrier, peers)

        def ids_out(p):
            pltpu.make_async_remote_copy(
                src_ref=owner, dst_ref=ids.at[me], send_sem=ids_ssem, recv_sem=ids_rsem,
                device_id=device(1, p), device_id_type=MESH,
            ).start()
        each_peer(ids_out)
        raw.wait()
        send_rows(1, surf, 2, 4, recv, 2, fwd_ssem.at[0], fwd_rsem.at[0])
        wind.wait()
        rho.wait()

        def stress(t):
            r = pl.ds(pl.multiple_of(t * TILE, TILE), TILE)
            wx, wy, density = surf[0, r, :], surf[1, r, :], surf[6, r, :]
            scale = density * CD_ICE * jnp.sqrt(wx * wx + wy * wy + 1.0)
            forc[0, r, :] = scale * wx
            forc[1, r, :] = scale * wy

        tile_loop(count // TILE, 2, stress)
        send_rows(1, forc, 0, 2, recv, 0, fwd_ssem.at[1], fwd_rsem.at[1])

        def open_water(t):
            r = pl.ds(pl.multiple_of(t * TILE, TILE), TILE)
            density = surf[6, r, :]
            rel_x = surf[0, r, :] - surf[2, r, :]
            rel_y = surf[1, r, :] - surf[3, r, :]
            speed = jnp.sqrt(rel_x * rel_x + rel_y * rel_y + 1.0)
            scale = density * (0.1 + 0.05 * speed) * speed
            open_st[0, r, :] = scale * rel_x
            open_st[1, r, :] = scale * rel_y

        tile_loop(count // TILE, 2, open_water)
        wait_bytes(ret.at[pl.ds(2, 1)], ret_rsem.at[0])
        wait_bytes(ret.at[pl.ds(0, 2)], ret_rsem.at[1])

        def finish(t):
            r = pl.ds(pl.multiple_of(t * TILE, TILE), TILE)
            water = 1.0 - ret[2, r, :]
            out[0, 0, r, :] = ret[0, r, :] + water * open_st[0, r, :]
            out[0, 1, r, :] = ret[1, r, :] + water * open_st[1, r, :]

        tile_loop(count // TILE, 2, finish)
        wait_bytes(ids, ids_ssem)
        wait_bytes(surf.at[pl.ds(2, 4)], fwd_ssem.at[0])
        wait_bytes(forc.at[pl.ds(0, 2)], fwd_ssem.at[1])

    @pl.when(comp == 1)
    def _ice():
        def inside(a):
            if a == 0:
                return lat >= 0
            return lat + a >= 0 if a < 0 else lat + a < n_lat

        signal_peers(0)
        first, last = LEAD, LEAD + count
        core = pl.ds(first, count)
        main, side = pl.ds(0, width), pl.ds(width, width)
        loads = [
            pltpu.make_async_copy(
                fields.at[0, :, :, pl.ds(y * width, width)],
                grid.at[pl.ds(0, 7), y, core, main],
                load_sem.at[y],
            )
            for y in range(2)
        ]
        loads.append(pltpu.make_async_copy(land, land_v, load_sem.at[2]))
        for load in loads:
            load.start()
        for c in range(12):
            for y in range(2):
                blank = jnp.zeros((LEAD, 2 * width), jnp.float32)
                grid[c, y, pl.ds(0, LEAD), :] = blank
                grid[c, y, pl.ds(last, LEAD), :] = blank
        for got in (got_early, got_mid, got_late):
            for d in range(2):
                got[d, pl.ds(0, TILE), :] = jnp.zeros((TILE, width), jnp.float32)
                got[d, pl.ds(TILE + count, TILE), :] = jnp.zeros((TILE, width), jnp.float32)

        for a, b in DIRECTIONS:
            @pl.when(inside(a))
            def _():
                pl.semaphore_signal(
                    barrier, inc=1, device_id=(1, lat + a, (lon + b + n_lon) % n_lon),
                    device_id_type=MESH,
                )
        walls = jnp.where(lat == 0, 3, 0) + jnp.where(lat == n_lat - 1, 3, 0)
        pl.semaphore_wait(barrier, peers + 8 - walls)
        for load in loads:
            load.wait()

        diag = lax.broadcasted_iota(jnp.int32, (count, count), 0) == lax.broadcasted_iota(
            jnp.int32, (count, count), 1
        )
        wet = jnp.sum(
            jnp.where(diag, covered[...].astype(jnp.float32), 0.0), axis=1, keepdims=True
        )
        sea = wet * (1 - land_v[...]).astype(jnp.float32)
        for y in range(2):
            grid[ACTIVE, y, core, main] = sea[:, y * width:(y + 1) * width]

        lane = lax.broadcasted_iota(jnp.int32, (TILE, width), 1)

        def pack(lo, num, packed):
            def body(t):
                r = pl.ds(pl.multiple_of(first + t * TILE, TILE), TILE)
                east = jnp.zeros((TILE, width), jnp.float32)
                west = east
                for c in range(num):
                    for y in range(2):
                        x = grid[lo + c, y, r, main]
                        slot = (c * 2 + y) * NSUB
                        mine = (lane >= slot) & (lane < slot + NSUB)
                        east = jnp.where(mine, pltpu.roll(x, (slot + NSUB) % width, 1), east)
                        west = jnp.where(mine, pltpu.roll(x, slot, 1) if slot else x, west)
                q = pl.ds(pl.multiple_of(t * TILE, TILE), TILE)
                packed[0, q, :] = east
                packed[1, q, :] = west
            tile_loop(count // TILE, 2, body)

        def halo(lo, num, packed, got, ssem, rsem, begin):
            for k, (a, b) in enumerate(DIRECTIONS):
                src_row = {-1: 0, 0: 0, 1: count - TILE}[a]
                dst_row = {-1: count, 0: 0, 1: -TILE}[a]
                rows = count if a == 0 else TILE
                if b == 0:
                    src = grid.at[pl.ds(lo, num), :, pl.ds(first + src_row, rows), main]
                    dst = grid.at[pl.ds(lo, num), :, pl.ds(first + dst_row, rows), main]
                else:
                    d = 0 if b > 0 else 1
                    src = packed.at[d, pl.ds(src_row, rows), :]
                    dst = got.at[d, pl.ds(TILE + dst_row, rows), :]
                copy = pltpu.make_async_remote_copy(
                    src_ref=src, dst_ref=dst, send_sem=ssem.at[k], recv_sem=rsem.at[k],
                    device_id=(1, lat + a, (lon + b + n_lon) % n_lon), device_id_type=MESH,
                )
                if begin:
                    @pl.when(inside(a))
                    def _():
                        copy.start()
                else:
                    @pl.when(inside(a))
                    def _():
                        copy.wait_send()

                    @pl.when(inside(-a))
                    def _():
                        copy.wait_recv()

        def side_of(got, slot, q):
            east = got[1, q, :]
            west = got[0, q, :]
            east = pltpu.roll(east, (width - slot) % width, 1) if slot else east
            west = pltpu.roll(west, width - NSUB - slot, 1)
            return jnp.where(
                lane < NSUB, east, jnp.where(lane >= width - NSUB, west, 0.0)
            )

        def unpack(lo, num, got, after):
            def body(t):
                q = pl.ds(pl.multiple_of(t * TILE, TILE), TILE)
                r = pl.ds(pl.multiple_of(first + (t - 1) * TILE, TILE), TILE)
                for c in range(num):
                    for y in range(2):
                        grid[lo + c, y, r, side] = side_of(got, (c * 2 + y) * NSUB, q)
                after(r)
            tile_loop(count // TILE + 2, 2, body)

        pack(0, 8, pack_early)
        halo(0, 8, pack_early, got_early, early_ssem, early_rsem, True)

        def ice_statics(r):
            for y in range(2):
                conc = grid[CONC, y, r, :]
                act = grid[ACTIVE, y, r, :]
                strength[y, r, :] = (
                    (RELAX / (1.0 + RELAX)) * grid[MASS, y, r, :] * jnp.exp(CSTAR * (conc - 1.0)) * act
                )
                dragb[y, r, :] = CW * conc * act

        wait_bytes(ids, ids_rsem)
        wanted = me * per
        row_lane = lax.broadcasted_iota(jnp.int32, (per, count), 1)
        row_sub = lax.broadcasted_iota(jnp.int32, (per, count), 0)
        mine = row_lane == row_sub + wanted
        blocks = lax.broadcasted_iota(jnp.int32, (per, count), 1).astype(jnp.float32)
        base = (me * count).astype(jnp.float32)
        for p in range(peers):
            owned = jnp.broadcast_to(ids[p], (per, count)).astype(jnp.float32)
            local = jnp.sum(jnp.where(mine, owned, 0.0), axis=1, keepdims=True) - base
            one_hot[pl.ds(p * per, per), :] = jnp.where(local == blocks, 1.0, 0.0)

        halo(0, 8, pack_early, got_early, early_ssem, early_rsem, False)
        unpack(0, 8, got_early, ice_statics)

        def east_of(x):
            return pltpu.roll(x, 2 * width - 1, 1)

        def west_of(x):
            return pltpu.roll(x, 1, 1)

        sub = lax.broadcasted_iota(jnp.int32, (TILE, 2 * width), 0)

        def next_row(x, after):
            return pltpu.roll(jnp.where(sub == 0, after, x), TILE - 1, 0)

        def last_row(x, before):
            return pltpu.roll(jnp.where(sub == TILE - 1, before, x), 1, 0)

        def sweep(g, new_stress, new_velocity):
            spots = [
                pl.ds(pl.multiple_of(first + (g * GROUP + j - 2) * TILE, TILE), TILE)
                for j in range(GROUP + 2)
            ]
            before, spots, after = spots[0], spots[1:-1], spots[-1]
            keep = 1.0 / (1.0 + RELAX)
            vels, stresses = [], []
            for r in spots:
                vels.append([(grid[U, y, r, :], grid[V, y, r, :]) for y in range(2)])
            if new_stress:
                follow = (grid[U, 0, after, :], grid[V, 0, after, :])
            for j, r in enumerate(spots):
                if not new_stress:
                    stresses.append(
                        [tuple(grid[c, y, r, :] for c in (S1, S2, S12)) for y in range(2)]
                    )
                    continue
                beyond = vels[j + 1][0] if j + 1 < GROUP else follow
                row = []
                for y in range(2):
                    u, v = vels[j][y]
                    if y == 0:
                        u_up, v_up = vels[j][1]
                    else:
                        u_up = next_row(vels[j][0][0], beyond[0])
                        v_up = next_row(vels[j][0][1], beyond[1])
                    sxx = east_of(u) - u
                    syy = v_up - v
                    shear = (u_up - u) + (east_of(v) - v)
                    div = sxx + syy
                    ten = sxx - syy
                    square = div * div + (ten * ten + shear * shear) * (1.0 / ECC2) + DMIN2
                    inverse = lax.rsqrt(square)
                    visc = strength[y, r, :] * inverse
                    s1 = grid[S1, y, r, :] * keep + visc * (div - square * inverse)
                    s2 = grid[S2, y, r, :] * keep + visc * ten * (1.0 / ECC2)
                    s12 = grid[S12, y, r, :] * keep + visc * shear * (0.5 / ECC2)
                    grid[S1, y, r, :] = s1
                    grid[S2, y, r, :] = s2
                    grid[S12, y, r, :] = s12
                    row.append((s1, s2, s12))
                stresses.append(row)
            if not new_velocity:
                return
            yy_before = 0.5 * (grid[S1, 1, before, :] - grid[S2, 1, before, :])
            cross_before = grid[S12, 1, before, :]
            for j, r in enumerate(spots):
                xx = [0.5 * (s1 + s2) for s1, s2, _ in stresses[j]]
                yy = [0.5 * (s1 - s2) for s1, s2, _ in stresses[j]]
                cross = [s12 for _, _, s12 in stresses[j]]
                yy_down = [last_row(yy[1], yy_before), yy[0]]
                cross_down = [last_row(cross[1], cross_before), cross[0]]
                yy_before, cross_before = yy[1], cross[1]
                for y in range(2):
                    u, v = vels[j][y]
                    force_x = xx[y] - west_of(xx[y]) + (cross[y] - cross_down[y])
                    force_y = cross[y] - west_of(cross[y]) + (yy[y] - yy_down[y])
                    mass = grid[MASS, y, r, :]
                    cx, cy = grid[CUR_X, y, r, :], grid[CUR_Y, y, r, :]
                    dx, dy = cx - u, cy - v
                    square = dx * dx + dy * dy + DRAG_FLOOR
                    drag = dragb[y, r, :] * (square * lax.rsqrt(square))
                    gain = grid[ACTIVE, y, r, :] / (
                        jnp.maximum(mass, MASS_FLOOR) * (1.0 / DTE) + drag
                    )
                    inertia = mass * (1.0 / DTE)
                    turn = CORIO * mass
                    grid[U, y, r, :] = gain * (
                        inertia * u + force_x + grid[PUSH_X, y, r, :] + drag * cx + turn * v
                    )
                    grid[V, y, r, :] = gain * (
                        inertia * v + force_y + grid[PUSH_Y, y, r, :] + drag * cy - turn * u
                    )

        groups = (count // TILE + 2) // GROUP

        def stress_only():
            tile_loop(groups, 1, lambda g: sweep(g, True, False))

        perm = one_hot[...].astype(jnp.bfloat16)
        stress_only()
        wait_bytes(recv.at[pl.ds(2, 4)], fwd_rsem.at[0])
        for c in range(2):
            both = split_dot(perm, recv[2 + c], (0,))
            for y in range(2):
                grid[CUR_X + c, y, core, main] = both[:, y * width:(y + 1) * width]
        pack(CUR_X, 2, pack_mid)
        halo(CUR_X, 2, pack_mid, got_mid, mid_ssem, mid_rsem, True)
        for c in range(2):
            both = split_dot(perm, recv[4 + c], (0,))
            for y in range(2):
                part = both[:, y * width:(y + 1) * width]
                grid[PUSH_X + c, y, core, main] = grid[MASS, y, core, main] * part
        wait_bytes(recv.at[pl.ds(0, 2)], fwd_rsem.at[1])
        for c in range(2):
            both = split_dot(perm, recv[c], (0,))
            for y in range(2):
                part = both[:, y * width:(y + 1) * width]
                grid[PUSH_X + c, y, core, main] = grid[ACTIVE, y, core, main] * (
                    grid[CONC, y, core, main] * part - grid[PUSH_X + c, y, core, main]
                )
        pack(PUSH_X, 2, pack_late)
        halo(PUSH_X, 2, pack_late, got_late, late_ssem, late_rsem, True)

        for y in range(2):
            share = grid[CONC, y, core, main] * grid[ACTIVE, y, core, main]
            back[2, :, pl.ds(y * width, width)] = split_dot(perm, share, (1,))
        send_rows(0, back, 2, 1, ret, 2, ret_ssem.at[0], ret_rsem.at[0])

        halo(CUR_X, 2, pack_mid, got_mid, mid_ssem, mid_rsem, False)
        unpack(CUR_X, 2, got_mid, lambda r: None)
        halo(PUSH_X, 2, pack_late, got_late, late_ssem, late_rsem, False)
        unpack(PUSH_X, 2, got_late, lambda r: None)
        tile_loop(groups, 1, lambda g: sweep(g, False, True))
        tile_loop((NSUB - 1) * groups, 1, lambda k: sweep(k % groups, True, True))

        def returned(t):
            q = pl.ds(pl.multiple_of(t * TILE, TILE), TILE)
            r = pl.ds(pl.multiple_of(first + t * TILE, TILE), TILE)
            for y in range(2):
                half = pl.ds(y * width, width)
                u, v = grid[U, y, r, main], grid[V, y, r, main]
                out[0, 0, q, half] = u
                out[0, 1, q, half] = v
                dx, dy = u - grid[CUR_X, y, r, main], v - grid[CUR_Y, y, r, main]
                drag = dragb[y, r, main] * jnp.sqrt(dx * dx + dy * dy + DRAG_FLOOR)
                forc[0, q, half] = drag * dx
                forc[1, q, half] = drag * dy

        tile_loop(count // TILE, 2, returned)
        for c in range(2):
            back[c] = split_dot(perm, forc[c], (1,))
        send_rows(0, back, 0, 2, ret, 0, ret_ssem.at[1], ret_rsem.at[1])
        wait_bytes(back.at[pl.ds(2, 1)], ret_ssem.at[0])
        wait_bytes(back.at[pl.ds(0, 2)], ret_ssem.at[1])


def per_device_kernel(n_lat, n_lon, fields, block_owner, ice_covered, land_mask):
    count, cells = land_mask.shape
    peers = n_lat * n_lon
    long = count + 2 * LEAD
    f32 = jnp.float32
    anywhere = pl.BlockSpec(memory_space=pl.ANY)
    in_vmem = pl.BlockSpec(memory_space=pltpu.VMEM)
    dma = pltpu.SemaphoreType.DMA
    return pl.pallas_call(
        functools.partial(step_kernel, n_lat, n_lon),
        out_shape=pltpu.VMEM((1, 2, count, cells), f32),
        in_specs=[anywhere, in_vmem, in_vmem, anywhere],
        out_specs=in_vmem,
        scratch_shapes=[
            pltpu.VMEM((7, count, cells), f32),
            pltpu.VMEM((2, count, cells), f32),
            pltpu.VMEM((3, count, cells), f32),
            pltpu.VMEM((peers, 1, count), jnp.int32),
            pltpu.VMEM((6, count, cells), f32),
            pltpu.VMEM((12, 2, long, 2 * BX), f32),
            pltpu.VMEM((2, long, 2 * BX), f32),
            pltpu.VMEM((2, long, 2 * BX), f32),
            pltpu.VMEM((6, count, cells), f32),
            pltpu.VMEM((count, count), f32),
            pltpu.VMEM((3, count, cells), f32),
            pltpu.VMEM((count, cells), jnp.int32),
            pltpu.VMEM((2, count, BX), f32),
            pltpu.VMEM((2, count, BX), f32),
            pltpu.VMEM((2, count, BX), f32),
            pltpu.VMEM((2, count + 2 * TILE, BX), f32),
            pltpu.VMEM((2, count + 2 * TILE, BX), f32),
            pltpu.VMEM((2, count + 2 * TILE, BX), f32),
            dma((3,)), dma, dma, dma((2,)), dma((2,)), dma((2,)), dma((2,)),
            dma((8,)), dma((8,)), dma((8,)), dma((8,)), dma((8,)), dma((8,)),
        ],
        compiler_params=pltpu.CompilerParams(
            collective_id=0, has_side_effects=True, vmem_limit_bytes=63 * 1024 * 1024
        ),
    )(fields, block_owner.reshape(1, count), ice_covered.reshape(1, count), land_mask)


def solution(mesh):
    placed = (
        P("comp", None, ("lat", "lon"), None),
        P(("lat", "lon")),
        P(("lat", "lon")),
        P(("lat", "lon"), None),
    )
    n_lat, n_lon = mesh.shape["lat"], mesh.shape["lon"]

    def body(fields, block_owner, ice_covered, land_mask):
        count = block_owner.shape[0]
        whole_tiles = count % (n_lat * n_lon * TILE) == 0 and count == BX
        if whole_tiles and n_lon > 2:
            return per_device_kernel(n_lat, n_lon, fields, block_owner, ice_covered, land_mask)
        return per_device(fields, block_owner, ice_covered, land_mask)

    return jax.shard_map(
        body,
        mesh=mesh,
        in_specs=placed,
        out_specs=P("comp", None, ("lat", "lon"), None),
        check_vma=False,
    )
```

```python
import functools

import jax
import jax.numpy as jnp
from jax import lax
from jax.experimental import pallas as pl
from jax.experimental.pallas import tpu as pltpu
from jax.sharding import PartitionSpec as P

GX = 1
BY = 2
BX = 128
NSUB = 4


CD_ICE = 0.1
CW = 1.5
CSTAR = 2.0
ECC2 = 4.0
DMIN2 = 0.25
RELAX = 0.5
DTE = 0.5
CORIO = 0.3
MASS_FLOOR = 0.5
DRAG_FLOOR = 0.1


def from_behind(x, axis, by):
    size = lax.axis_size(axis)
    pairs = [(i, i + by) for i in range(size) if 0 <= i + by < size]
    return lax.ppermute(x, axis, pairs)


def with_halo(x, sides, width, wrap):
    for axis, dim in sides:
        size, length = (lax.axis_size(axis), x.shape[dim])
        up = [(i, (i + 1) % size) for i in range(size if wrap else size - 1)]
        down = [(j, i) for i, j in up]
        last = lax.slice_in_dim(x, length - width, length, axis=dim)
        first = lax.slice_in_dim(x, 0, width, axis=dim)
        before = lax.ppermute(last, axis, up)
        after = lax.ppermute(first, axis, down)
        x = jnp.concatenate([before, x, after], axis=dim)
    return x


def air_stress(ocean):
    wind_x, wind_y, current_x, current_y, tilt_x, tilt_y, density = ocean
    speed_ice = jnp.sqrt(wind_x * wind_x + wind_y * wind_y + 1.0)
    scale_ice = density * CD_ICE * speed_ice
    rel_x = wind_x - current_x
    rel_y = wind_y - current_y
    speed_open = jnp.sqrt(rel_x * rel_x + rel_y * rel_y + 1.0)
    scale_open = density * (0.1 + 0.05 * speed_open) * speed_open
    outbound = jnp.stack(
        [scale_ice * wind_x, scale_ice * wind_y, current_x, current_y, tilt_x, tilt_y]
    )
    open_stress = jnp.stack([scale_open * rel_x, scale_open * rel_y])
    return (outbound, open_stress)


def prepare(ice_tile, forcing, active):
    ice_mass = ice_tile[2]
    concentration = ice_tile[3]
    strength = ice_mass * jnp.exp(CSTAR * (concentration - 1.0)) * active
    drag_base = CW * concentration * active
    push_x = active * (concentration * forcing[0] - ice_mass * forcing[4])
    push_y = active * (concentration * forcing[1] - ice_mass * forcing[5])
    return jnp.stack(
        [strength, ice_mass, drag_base, push_x, push_y, forcing[2], forcing[3], active]
    )


def subcycle(ice_state, statics):
    east_vel, north_vel, stress_one, stress_two, stress_three = ice_state
    strength = statics[0]
    east_base = east_vel[:-1, :-1]
    north_base = north_vel[:-1, :-1]
    strain_xx = east_vel[:-1, 1:] - east_base
    strain_yy = north_vel[1:, :-1] - north_base
    shear = east_vel[1:, :-1] - east_base + (north_vel[:-1, 1:] - north_base)
    divergence = strain_xx + strain_yy
    tension = strain_xx - strain_yy
    delta_norm = jnp.sqrt(
        divergence * divergence + (tension * tension + shear * shear) / ECC2 + DMIN2
    )
    viscosity = strength[:-1, :-1] / delta_norm
    stress_sum = (stress_one[:-1, :-1] + RELAX * viscosity * (divergence - delta_norm)) / (
        1.0 + RELAX
    )
    stress_diff = (stress_two[:-1, :-1] + RELAX * viscosity * tension / ECC2) / (1.0 + RELAX)
    stress_shear = (stress_three[:-1, :-1] + RELAX * viscosity * shear / (2.0 * ECC2)) / (
        1.0 + RELAX
    )
    stress_xx = 0.5 * (stress_sum + stress_diff)
    stress_yy = 0.5 * (stress_sum - stress_diff)
    force_x = (
        stress_xx[1:, 1:] - stress_xx[1:, :-1] + (stress_shear[1:, 1:] - stress_shear[:-1, 1:])
    )
    force_y = (
        stress_shear[1:, 1:] - stress_shear[1:, :-1] + (stress_yy[1:, 1:] - stress_yy[:-1, 1:])
    )
    trimmed = statics[:, 1:-1, 1:-1]
    strength, ice_mass, drag_base, push_x, push_y, current_x, current_y, active = trimmed
    east_old = east_vel[1:-1, 1:-1]
    north_old = north_vel[1:-1, 1:-1]
    diff_x = current_x - east_old
    diff_y = current_y - north_old
    drag_coef = drag_base * jnp.sqrt(diff_x * diff_x + diff_y * diff_y + DRAG_FLOOR)
    denominator = jnp.maximum(ice_mass, MASS_FLOOR) / DTE + drag_coef
    east_new = (
        active
        * (
            ice_mass / DTE * east_old
            + force_x
            + push_x
            + drag_coef * current_x
            + CORIO * ice_mass * north_old
        )
        / denominator
    )
    north_new = (
        active
        * (
            ice_mass / DTE * north_old
            + force_y
            + push_y
            + drag_coef * current_y
            - CORIO * ice_mass * east_old
        )
        / denominator
    )
    new_state = jnp.stack(
        [east_new, north_new, stress_sum[1:, 1:], stress_diff[1:, 1:], stress_shear[1:, 1:]]
    )
    return (new_state, trimmed)


def give_back(ice_state, statics):
    east_vel = ice_state[0]
    north_vel = ice_state[1]
    drag_base = statics[2]
    current_x = statics[5]
    current_y = statics[6]
    diff_x = east_vel - current_x
    diff_y = north_vel - current_y
    factor = drag_base * jnp.sqrt(diff_x * diff_x + diff_y * diff_y + DRAG_FLOOR)
    return jnp.stack([factor * diff_x, factor * diff_y, drag_base / CW])


def to_tile(blocks):
    channels, count, cells = blocks.shape
    arranged = blocks.reshape(channels, count // GX, GX, BY, BX).transpose(0, 1, 3, 2, 4)
    return arranged.reshape(channels, count // GX * BY, GX * BX)


def from_tile(values):
    channels, rows, columns = values.shape
    arranged = values.reshape(channels, rows // BY, BY, GX, BX).transpose(0, 1, 3, 2, 4)
    return arranged.reshape(channels, rows // BY * GX, BY * BX)


def per_device(fields, block_owner, ice_covered, land_mask):
    count = block_owner.shape[0]
    is_ocean = lax.axis_index("comp") == 0
    outbound, open_stress = air_stress(fields[0])
    owner_row = block_owner.reshape(1, count)
    crossed = from_behind(outbound, "comp", 1)
    received, anchor = (
        lax.all_to_all(crossed, ("lat", "lon"), split_axis=1, concat_axis=1, tiled=True),
        lax.all_to_all(owner_row, ("lat", "lon"), split_axis=1, concat_axis=1, tiled=True),
    )
    local_ids = anchor[0] % count
    position = jnp.zeros((count,), jnp.int32).at[local_ids].set(jnp.arange(count, dtype=jnp.int32))
    forcing = to_tile(received[:, position])
    ice_tile = to_tile(fields[0])
    covered = ice_covered.astype(jnp.float32)[:, None] * (1 - land_mask).astype(jnp.float32)
    active = to_tile(covered[None])[0]
    statics = prepare(ice_tile, forcing, active)
    ice_state = jnp.stack([ice_tile[0], ice_tile[1], ice_tile[4], ice_tile[5], ice_tile[6]])
    joined = jnp.concatenate([ice_state, statics], 0)
    joined = with_halo(joined, (("lon", 2),), NSUB, True)
    joined = with_halo(joined, (("lat", 1),), NSUB, False)
    ice_state = joined[:5]
    statics = joined[5:]
    for repeat in range(NSUB):
        ice_state, statics = subcycle(ice_state, statics)
    returned = from_tile(give_back(ice_state, statics))
    back_send = returned[:, local_ids]
    regrouped = lax.all_to_all(back_send, ("lat", "lon"), split_axis=1, concat_axis=1, tiled=True)
    received_back = from_behind(regrouped, "comp", -1)
    ocean_out = received_back[:2] + (1.0 - received_back[2]) * open_stress
    ice_out = from_tile(ice_state[:2])
    return jnp.where(is_ocean, ocean_out, ice_out)[None]


TILE = 8
GROUP = 8
MESH = pl.DeviceIdType.MESH
U, V, MASS, CONC, S1, S2, S12, ACTIVE, PUSH_X, PUSH_Y, CUR_X, CUR_Y, STRENGTH, DRAG = range(14)
SIDES = [(a, b) for b in (-1, 1) for a in (0, -1, 1)]
ALL_AROUND = [(-1, 0), (1, 0)] + SIDES
ROUNDS = ((U, 8), (CUR_X, 2), (PUSH_X, 2))
KEEP = 1.0 / (1.0 + RELAX)


def tile_loop(tiles, together, body):
    def step(k, carry):
        for j in range(together):
            body(k * together + j)
        return carry
    lax.fori_loop(0, tiles // together, step, 0)


def pieces(values, axis):
    parts = []
    rest = values
    for piece in range(3):
        part = rest.astype(jnp.bfloat16)
        if piece < 2:
            rest = rest - part.astype(jnp.float32)
        parts.append(part)
    return jnp.concatenate(parts, axis=axis)


def dot_rows(thrice, values):
    return lax.dot_general(
        thrice, pieces(values, 0), (((1,), (0,)), ((), ())), preferred_element_type=jnp.float32
    )


def dot_lanes(thrice, values):
    return lax.dot_general(
        thrice, pieces(values, 1), (((1,), (1,)), ((), ())), preferred_element_type=jnp.float32
    )


def new_stress(strength, s1, s2, s12, u, v, u_east, v_east, u_up, v_up):
    sxx = u_east - u
    syy = v_up - v
    shear = (u_up - u) + (v_east - v)
    div = sxx + syy
    ten = sxx - syy
    square = div * div + (ten * ten + shear * shear) * (1.0 / ECC2) + DMIN2
    inverse = lax.rsqrt(square)
    visc = strength * inverse
    s1 = s1 * KEEP + visc * (div - square * inverse)
    s2 = s2 * KEEP + visc * ten * (1.0 / ECC2)
    s12 = s12 * KEEP + visc * shear * (0.5 / ECC2)
    return s1, s2, s12


def new_velocity(get, u, v, force_x, force_y):
    mass, cx, cy = get(MASS), get(CUR_X), get(CUR_Y)
    dx, dy = cx - u, cy - v
    square = dx * dx + dy * dy + DRAG_FLOOR
    drag = get(DRAG) * (square * lax.rsqrt(square))
    gain = get(ACTIVE) / (jnp.maximum(mass, MASS_FLOOR) * (1.0 / DTE) + drag)
    inertia = mass * (1.0 / DTE)
    turn = CORIO * mass
    return (
        gain * (inertia * u + force_x + get(PUSH_X) + drag * cx + turn * v),
        gain * (inertia * v + force_y + get(PUSH_Y) + drag * cy - turn * u),
    )


def step_kernel(
    n_lat, n_lon,
    fields, owner_hbm, covered_hbm, land, out,
    surf, open_st, ret, owner, covered, ids, recv, forc, one_hot, back, land_v,
    main, edge, flank, flank_back, flank_vel,
    rows_out0, rows_out1, rows_out2, rows_got0, rows_got1, rows_got2,
    side_out0, side_out1, side_out2, side_got0, side_got1, side_got2,
    load_sem, ids_ssem, ids_rsem, fwd_ssem, fwd_rsem, ret_ssem, ret_rsem, halo_ssem, halo_rsem,
):
    comp = lax.axis_index("comp")
    lat = lax.axis_index("lat")
    lon = lax.axis_index("lon")
    peers = n_lat * n_lon
    me = lat * n_lon + lon
    count = owner.shape[1]
    per = count // peers
    width = BX
    barrier = pltpu.get_barrier_semaphore()
    rows_out = (rows_out0, rows_out1, rows_out2)
    rows_got = (rows_got0, rows_got1, rows_got2)
    side_out = (side_out0, side_out1, side_out2)
    side_got = (side_got0, side_got1, side_got2)

    def rows_of(peer):
        return pl.ds(pl.multiple_of(peer * per, per), per)

    def device(kind, peer):
        return (kind, peer // n_lon, peer % n_lon)

    def each_peer(body):
        def step(k, carry):
            body((me + k) % peers)
            return carry
        lax.fori_loop(0, peers, step, 0)

    def signal_peers(kind):
        each_peer(
            lambda p: pl.semaphore_signal(
                barrier, inc=1, device_id=device(kind, p), device_id_type=MESH
            )
        )

    def send_rows(kind, src, lo, num, dst, dlo, ssem, rsem):
        def body(p):
            pltpu.make_async_remote_copy(
                src_ref=src.at[pl.ds(lo, num), rows_of(p), :],
                dst_ref=dst.at[pl.ds(dlo, num), rows_of(me), :],
                send_sem=ssem, recv_sem=rsem,
                device_id=device(kind, p), device_id_type=MESH,
            ).start()
        each_peer(body)

    def wait_bytes(ref, sem):
        pltpu.make_async_copy(ref, ref, sem).wait()

    @pl.when(comp == 0)
    def _ocean():
        signal_peers(1)
        names = pltpu.make_async_copy(owner_hbm, owner, load_sem.at[3])
        raw = pltpu.make_async_copy(fields.at[0, pl.ds(2, 4)], surf.at[pl.ds(2, 4)], load_sem.at[0])
        wind = pltpu.make_async_copy(fields.at[0, pl.ds(0, 2)], surf.at[pl.ds(0, 2)], load_sem.at[1])
        rho = pltpu.make_async_copy(fields.at[0, pl.ds(6, 1)], surf.at[pl.ds(6, 1)], load_sem.at[2])
        names.start()
        raw.start()
        wind.start()
        rho.start()
        names.wait()
        with jax.named_scope("o_barrier"):
            pl.semaphore_wait(barrier, peers)

        def ids_out(p):
            pltpu.make_async_remote_copy(
                src_ref=owner, dst_ref=ids.at[me], send_sem=ids_ssem, recv_sem=ids_rsem,
                device_id=device(1, p), device_id_type=MESH,
            ).start()
        with jax.named_scope("o_send4"):
            each_peer(ids_out)
            raw.wait()
            send_rows(1, surf, 2, 4, recv, 2, fwd_ssem.at[0], fwd_rsem.at[0])
            wind.wait()
            rho.wait()

        def stress(t):
            r = pl.ds(pl.multiple_of(t * TILE, TILE), TILE)
            wx, wy, density = surf[0, r, :], surf[1, r, :], surf[6, r, :]
            scale = density * CD_ICE * jnp.sqrt(wx * wx + wy * wy + 1.0)
            forc[0, r, :] = scale * wx
            forc[1, r, :] = scale * wy

        with jax.named_scope("o_stress"):
            tile_loop(count // TILE, 2, stress)
            send_rows(1, forc, 0, 2, recv, 0, fwd_ssem.at[1], fwd_rsem.at[1])

        def open_water(t):
            r = pl.ds(pl.multiple_of(t * TILE, TILE), TILE)
            density = surf[6, r, :]
            rel_x = surf[0, r, :] - surf[2, r, :]
            rel_y = surf[1, r, :] - surf[3, r, :]
            speed = jnp.sqrt(rel_x * rel_x + rel_y * rel_y + 1.0)
            scale = density * (0.1 + 0.05 * speed) * speed
            open_st[0, r, :] = scale * rel_x
            open_st[1, r, :] = scale * rel_y

        tile_loop(count // TILE, 2, open_water)
        with jax.named_scope("o_waitret1"):
            wait_bytes(ret.at[pl.ds(2, 1)], ret_rsem.at[0])
        with jax.named_scope("o_waitret2"):
            wait_bytes(ret.at[pl.ds(0, 2)], ret_rsem.at[1])

        def finish(t):
            r = pl.ds(pl.multiple_of(t * TILE, TILE), TILE)
            water = 1.0 - ret[2, r, :]
            out[0, 0, r, :] = ret[0, r, :] + water * open_st[0, r, :]
            out[0, 1, r, :] = ret[1, r, :] + water * open_st[1, r, :]

        with jax.named_scope("o_finish"):
            tile_loop(count // TILE, 2, finish)
        wait_bytes(ids, ids_ssem)
        wait_bytes(surf.at[pl.ds(2, 4)], fwd_ssem.at[0])
        wait_bytes(forc.at[pl.ds(0, 2)], fwd_ssem.at[1])

    @pl.when(comp == 1)
    def _ice():
        def inside(a):
            if a == 0:
                return lat >= 0
            return lat + a >= 0 if a < 0 else lat + a < n_lat

        def around(a, b):
            return (1, lat + a, (lon + b + n_lon) % n_lon)

        signal_peers(0)
        for a, b in ALL_AROUND:
            @pl.when(inside(a))
            def _():
                pl.semaphore_signal(barrier, inc=1, device_id=around(a, b), device_id_type=MESH)
        loads = [
            pltpu.make_async_copy(
                fields.at[0, :, :, pl.ds(y * width, width)], main.at[pl.ds(0, 7), y], load_sem.at[y]
            )
            for y in range(2)
        ]
        loads.append(pltpu.make_async_copy(land, land_v, load_sem.at[2]))
        loads.append(pltpu.make_async_copy(covered_hbm, covered, load_sem.at[3]))
        for load in loads:
            load.start()

        tiles = count // TILE
        top, bottom = pl.ds(0, TILE), pl.ds(count - TILE, TILE)
        zero_tile = jnp.zeros((TILE, width), jnp.float32)
        for wall, which in ((lat == 0, 0), (lat == n_lat - 1, 1)):
            @pl.when(wall)
            def _():
                for e in range(3):
                    for k in range(rows_got[e].shape[1]):
                        rows_got[e][which, k] = zero_tile
                    for k in range(2):
                        side_got[e][2 * which, k] = zero_tile

        def clear(t):
            r = pl.ds(pl.multiple_of(t * TILE, TILE), TILE)
            for c in range(2):
                for y in range(2):
                    flank_back[c, y, r, :] = zero_tile
                    flank_vel[c, y, r, :] = zero_tile

        tile_loop(tiles, 2, clear)
        for load in loads:
            load.wait()
        diag = lax.broadcasted_iota(jnp.int32, (count, count), 0) == lax.broadcasted_iota(
            jnp.int32, (count, count), 1
        )
        wet = jnp.sum(
            jnp.where(diag, covered[...].astype(jnp.float32), 0.0), axis=1, keepdims=True
        )
        sea = wet * (1 - land_v[...]).astype(jnp.float32)
        for y in range(2):
            main[ACTIVE, y] = sea[:, y * width:(y + 1) * width]

        lane = lax.broadcasted_iota(jnp.int32, (TILE, width), 1)
        sub = lax.broadcasted_iota(jnp.int32, (TILE, width), 0)
        pick_row = lax.broadcasted_iota(jnp.int32, (2 * TILE, width), 0)
        pick_col = lax.broadcasted_iota(jnp.int32, (2 * TILE, width), 1)
        picked = jnp.where(pick_row < TILE, pick_row, pick_row + (width - 2 * TILE)) == pick_col
        picker = jnp.where(picked, 1.0, 0.0).astype(jnp.bfloat16)
        picker = jnp.concatenate([picker] * 3, axis=1)

        def pack(e):
            lo, num = ROUNDS[e]
            west, east = zero_tile, zero_tile
            for k in range(num // 2):
                ups, downs = zero_tile, zero_tile
                for i in range(4):
                    c, y = lo + 2 * k + i // 2, i % 2
                    head, foot = main[c, y, top, :], main[c, y, bottom, :]
                    here = (sub >= 2 * i) & (sub < 2 * i + 2)
                    ups = jnp.where(here, pltpu.roll(head, 2 * i, 0) if i else head, ups)
                    downs = jnp.where(here, pltpu.roll(foot, (2 * i + 2) % TILE, 0) if i < 3 else foot, downs)
                    ends = jnp.where(sub < NSUB, head, foot)
                    slot = (k * 4 + i) * NSUB
                    mine = (lane >= slot) & (lane < slot + NSUB)
                    west = jnp.where(mine, pltpu.roll(ends, slot, 1) if slot else ends, west)
                    east = jnp.where(mine, pltpu.roll(ends, (slot + NSUB) % width, 1), east)
                rows_out[e][0, k] = ups
                rows_out[e][1, k] = downs
            side_out[e][0] = west
            side_out[e][1] = east
            for c in range(lo, lo + num):
                for y in range(2):
                    across = dot_lanes(picker, main[c, y])
                    flank[c, y, pl.ds(TILE, TILE), :] = across[:TILE]
                    flank[c, y, pl.ds(2 * TILE, TILE), :] = across[TILE:]

        def halo(e, begin):
            lo, num = ROUNDS[e]
            moves = []
            for a in (-1, 1):
                k = 1 if a > 0 else 0
                moves.append((a, 0, rows_out[e].at[k], rows_got[e].at[1 - k]))
            for a, b in SIDES:
                k = 1 if b > 0 else 0
                moves.append((a, b, side_out[e].at[k], side_got[e].at[1 - a, 1 - k]))
            for b in (-1, 1):
                src, dst = (2 * TILE, 0) if b > 0 else (TILE, 3 * TILE)
                moves.append((
                    0, b,
                    flank.at[pl.ds(lo, num), :, pl.ds(src, TILE), :],
                    flank.at[pl.ds(lo, num), :, pl.ds(dst, TILE), :],
                ))
            for k, (a, b, src, dst) in enumerate(moves):
                copy = pltpu.make_async_remote_copy(
                    src_ref=src, dst_ref=dst,
                    send_sem=halo_ssem.at[e, k], recv_sem=halo_rsem.at[e, k],
                    device_id=around(a, b), device_id_type=MESH,
                )
                if begin:
                    @pl.when(inside(a))
                    def _():
                        copy.start()
                else:
                    @pl.when(inside(a))
                    def _():
                        copy.wait_send()

                    @pl.when(inside(-a))
                    def _():
                        copy.wait_recv()

        def unpack(e):
            lo, num = ROUNDS[e]
            got, side = rows_got[e], side_got[e]
            ends = []
            for k in range(2):
                far, near = side[0, k], side[1, k]
                ends.append(pltpu.roll(jnp.where(sub >= TILE - 2, far, near), 2, 0))
            for k in range(2):
                far, near = side[2, k], side[1, k]
                ends.append(pltpu.roll(jnp.where(sub < 2, far, near), TILE - 2, 0))
            for k in range(num // 2):
                for i in range(4):
                    c, y = lo + 2 * k + i // 2, i % 2
                    slot = (k * 4 + i) * NSUB
                    for strip in range(2):
                        own = main[c, y, top if strip == 0 else bottom, :]
                        beyond = got[strip, k]
                        if strip == 0:
                            beyond = pltpu.roll(beyond, (TILE - 2 * i) % TILE, 0) if i else beyond
                            body = jnp.where(sub < 2, beyond, pltpu.roll(own, 2, 0))
                        else:
                            beyond = pltpu.roll(beyond, TILE - 2 - 2 * i, 0) if i < 3 else beyond
                            body = jnp.where(sub >= TILE - 2, beyond, pltpu.roll(own, TILE - 2, 0))
                        from_west, from_east = ends[2 * strip], ends[2 * strip + 1]
                        from_east = pltpu.roll(from_east, width - slot, 1) if slot else from_east
                        from_west = pltpu.roll(from_west, width - NSUB - slot, 1)
                        edge[c, strip, y, :, pl.ds(0, width)] = body
                        edge[c, strip, y, :, pl.ds(width, width)] = jnp.where(
                            lane < NSUB, from_east, jnp.where(lane >= width - NSUB, from_west, 0.0)
                        )

        def derive(load, store):
            conc, act = load(CONC), load(ACTIVE)
            store(STRENGTH, (RELAX * KEEP) * load(MASS) * jnp.exp(CSTAR * (conc - 1.0)) * act)
            store(DRAG, CW * conc * act)

        def derive_main(t):
            r = pl.ds(pl.multiple_of(t * TILE, TILE), TILE)
            for y in range(2):
                def store(c, x):
                    main[c, y, r, :] = x
                derive(lambda c: main[c, y, r, :], store)

        def derive_edges():
            for y in range(2):
                for strip in range(2):
                    def store(c, x):
                        edge[c, strip, y] = x
                    derive(lambda c: edge[c, strip, y], store)

                def store(c, x):
                    flank[c, y] = x
                derive(lambda c: flank[c, y], store)

        def sweep_main(g, stress, velocity):
            spots = [
                pl.ds(pl.multiple_of((g * GROUP + j) * TILE, TILE), TILE) for j in range(GROUP)
            ]
            behind = pl.ds(pl.multiple_of(jnp.maximum(g * GROUP - 1, 0) * TILE, TILE), TILE)
            ahead = pl.ds(
                pl.multiple_of(jnp.minimum(g * GROUP + GROUP, tiles - 1) * TILE, TILE), TILE
            )
            vels = [[(main[U, y, r, :], main[V, y, r, :]) for y in range(2)] for r in spots]
            stresses = []
            if stress:
                follow = (main[U, 0, ahead, :], main[V, 0, ahead, :])
            for j, r in enumerate(spots):
                old = [tuple(main[c, y, r, :] for c in (S1, S2, S12)) for y in range(2)]
                if not stress:
                    stresses.append(old)
                    continue
                beyond = vels[j + 1][0] if j + 1 < GROUP else follow
                row = []
                for y in range(2):
                    u, v = vels[j][y]
                    if y == 0:
                        u_up, v_up = vels[j][1]
                    else:
                        u_up, v_up = (
                            pltpu.roll(jnp.where(sub == 0, after, x), TILE - 1, 0)
                            for x, after in zip(vels[j][0], beyond)
                        )
                    fresh = new_stress(
                        main[STRENGTH, y, r, :], *old[y], u, v,
                        pltpu.roll(u, width - 1, 1), pltpu.roll(v, width - 1, 1), u_up, v_up,
                    )
                    for c, x in zip((S1, S2, S12), fresh):
                        main[c, y, r, :] = x
                    row.append(fresh)
                stresses.append(row)
            if not velocity:
                return
            yy_before = 0.5 * (main[S1, 1, behind, :] - main[S2, 1, behind, :])
            cross_before = main[S12, 1, behind, :]
            for j, r in enumerate(spots):
                xx = [0.5 * (s1 + s2) for s1, s2, _ in stresses[j]]
                yy = [0.5 * (s1 - s2) for s1, s2, _ in stresses[j]]
                cross = [s12 for _, _, s12 in stresses[j]]
                yy_down, cross_down = (
                    [pltpu.roll(jnp.where(sub == TILE - 1, before, x[1]), 1, 0), x[0]]
                    for x, before in ((yy, yy_before), (cross, cross_before))
                )
                yy_before, cross_before = yy[1], cross[1]
                for y in range(2):
                    force_x = xx[y] - pltpu.roll(xx[y], 1, 1) + (cross[y] - cross_down[y])
                    force_y = cross[y] - pltpu.roll(cross[y], 1, 1) + (yy[y] - yy_down[y])
                    u, v = new_velocity(lambda c: main[c, y, r, :], *vels[j][y], force_x, force_y)
                    main[U, y, r, :] = u
                    main[V, y, r, :] = v

        def sweep_edge(stress, velocity):
            for strip in range(2):
                vels = [(edge[U, strip, y], edge[V, strip, y]) for y in range(2)]
                fresh = [tuple(edge[c, strip, y] for c in (S1, S2, S12)) for y in range(2)]
                if stress:
                    ups = [vels[1], tuple(pltpu.roll(x, TILE - 1, 0) for x in vels[0])]
                    for y in range(2):
                        east = [pltpu.roll(x, 2 * width - 1, 1) for x in vels[y]]
                        fresh[y] = new_stress(
                            edge[STRENGTH, strip, y], *fresh[y], *vels[y], *east, *ups[y]
                        )
                        for c, x in zip((S1, S2, S12), fresh[y]):
                            edge[c, strip, y] = x
                if not velocity:
                    continue
                xx = [0.5 * (s1 + s2) for s1, s2, _ in fresh]
                yy = [0.5 * (s1 - s2) for s1, s2, _ in fresh]
                cross = [s12 for _, _, s12 in fresh]
                yy_down, cross_down = ([pltpu.roll(x[1], 1, 0), x[0]] for x in (yy, cross))
                for y in range(2):
                    force_x = xx[y] - pltpu.roll(xx[y], 1, 1) + (cross[y] - cross_down[y])
                    force_y = cross[y] - pltpu.roll(cross[y], 1, 1) + (yy[y] - yy_down[y])
                    u, v = new_velocity(lambda c: edge[c, strip, y], *vels[y], force_x, force_y)
                    edge[U, strip, y] = u
                    edge[V, strip, y] = v

        def sweep_flank(stress, velocity):
            spots = [pl.ds(j * TILE, TILE) for j in range(4)]
            vels = [[(flank[U, y, r, :], flank[V, y, r, :]) for y in range(2)] for r in spots]
            fresh = [
                [tuple(flank[c, y, r, :] for c in (S1, S2, S12)) for y in range(2)] for r in spots
            ]
            if stress:
                for j, r in enumerate(spots):
                    for y in range(2):
                        after = vels[min(j + 1, 3)][y]
                        east = [
                            pltpu.roll(jnp.where(sub == 0, b, x), TILE - 1, 0)
                            for x, b in zip(vels[j][y], after)
                        ]
                        ups = vels[j][1] if y == 0 else [
                            pltpu.roll(x, width - 1, 1) for x in vels[j][0]
                        ]
                        fresh[j][y] = new_stress(
                            flank[STRENGTH, y, r, :], *fresh[j][y], *vels[j][y], *east, *ups
                        )
                        for c, x in zip((S1, S2, S12), fresh[j][y]):
                            flank[c, y, r, :] = x
            if not velocity:
                return
            xx = [[0.5 * (s1 + s2) for s1, s2, _ in row] for row in fresh]
            yy = [[0.5 * (s1 - s2) for s1, s2, _ in row] for row in fresh]
            cross = [[s12 for _, _, s12 in row] for row in fresh]

            def westward(x, j, y):
                before = x[max(j - 1, 0)][y]
                return pltpu.roll(jnp.where(sub == TILE - 1, before, x[j][y]), 1, 0)

            def downward(x, j, y):
                return x[j][0] if y == 1 else pltpu.roll(x[j][1], 1, 1)

            for j, r in enumerate(spots):
                for y in range(2):
                    force_x = xx[j][y] - westward(xx, j, y) + (cross[j][y] - downward(cross, j, y))
                    force_y = cross[j][y] - westward(cross, j, y) + (yy[j][y] - downward(yy, j, y))
                    u, v = new_velocity(lambda c: flank[c, y, r, :], *vels[j][y], force_x, force_y)
                    flank[U, y, r, :] = u
                    flank[V, y, r, :] = v

        walls = jnp.where(lat == 0, 3, 0) + jnp.where(lat == n_lat - 1, 3, 0)
        with jax.named_scope("i_barrier"):
            pl.semaphore_wait(barrier, peers + 8 - walls)
        with jax.named_scope("i_pack0"):
            pack(0)
            halo(0, True)
        tile_loop(tiles, 2, derive_main)

        with jax.named_scope("i_waitids"):
            wait_bytes(ids, ids_rsem)
        wanted = me * per
        row_lane = lax.broadcasted_iota(jnp.int32, (per, count), 1)
        row_sub = lax.broadcasted_iota(jnp.int32, (per, count), 0)
        mine = row_lane == row_sub + wanted
        blocks = lax.broadcasted_iota(jnp.int32, (per, count), 1).astype(jnp.float32)
        base = (me * count).astype(jnp.float32)
        for p in range(peers):
            owned = jnp.broadcast_to(ids[p], (per, count)).astype(jnp.float32)
            local = jnp.sum(jnp.where(mine, owned, 0.0), axis=1, keepdims=True) - base
            one_hot[pl.ds(p * per, per), :] = jnp.where(local == blocks, 1.0, 0.0)

        with jax.named_scope("i_waithalo0"):
            halo(0, False)
        with jax.named_scope("i_unpack0"):
            unpack(0)
            derive_edges()
        groups = tiles // GROUP
        with jax.named_scope("i_stress"):
            tile_loop(groups, 1, lambda g: sweep_main(g, True, False))
            sweep_edge(True, False)
            sweep_flank(True, False)
        by_slot = one_hot[...]
        to_slots = jnp.concatenate([by_slot.astype(jnp.bfloat16)] * 3, axis=1)
        to_blocks = jnp.concatenate([by_slot.T.astype(jnp.bfloat16)] * 3, axis=1)

        with jax.named_scope("i_waitf4"):
            wait_bytes(recv.at[pl.ds(2, 4)], fwd_rsem.at[0])
        for c in range(2):
            both = dot_rows(to_blocks, recv[2 + c])
            for y in range(2):
                main[CUR_X + c, y] = both[:, y * width:(y + 1) * width]
        with jax.named_scope("i_packmid"):
            pack(1)
            halo(1, True)
        for c in range(2):
            both = dot_rows(to_blocks, recv[4 + c])
            for y in range(2):
                main[PUSH_X + c, y] = main[MASS, y] * both[:, y * width:(y + 1) * width]
        for y in range(2):
            share = main[CONC, y] * main[ACTIVE, y]
            back[2, :, pl.ds(y * width, width)] = dot_rows(to_slots, share)
        send_rows(0, back, 2, 1, ret, 2, ret_ssem.at[0], ret_rsem.at[0])

        with jax.named_scope("i_waitf2"):
            wait_bytes(recv.at[pl.ds(0, 2)], fwd_rsem.at[1])
        with jax.named_scope("i_push"):
            for c in range(2):
                both = dot_rows(to_blocks, recv[c])
                for y in range(2):
                    main[PUSH_X + c, y] = main[ACTIVE, y] * (
                        main[CONC, y] * both[:, y * width:(y + 1) * width] - main[PUSH_X + c, y]
                    )
        with jax.named_scope("i_packlate"):
            pack(2)
            halo(2, True)

        with jax.named_scope("i_vel1"):
            tile_loop(groups, 1, lambda g: sweep_main(g, False, True))
        with jax.named_scope("i_sweeps"):
            tile_loop((NSUB - 1) * groups, 1, lambda k: sweep_main(k % groups, True, True))
        with jax.named_scope("i_waitmid"):
            halo(1, False)
        unpack(1)
        with jax.named_scope("i_waitlate"):
            halo(2, False)
        with jax.named_scope("i_edge"):
            unpack(2)
            sweep_edge(False, True)
            tile_loop(NSUB - 1, 1, lambda k: sweep_edge(True, True))
        with jax.named_scope("i_flank"):
            sweep_flank(False, True)
            tile_loop(NSUB - 1, 1, lambda k: sweep_flank(True, True))

        def leave(get, u, v):
            dx, dy = u - get(CUR_X), v - get(CUR_Y)
            drag = get(DRAG) * jnp.sqrt(dx * dx + dy * dy + DRAG_FLOOR)
            return drag * dx, drag * dy

        outer = (lane < NSUB) | (lane >= width - NSUB)

        with jax.named_scope("i_returned"):
            for y in range(2):
                for c in (U, V):
                    north = pltpu.roll(edge[c, 0, y, :, pl.ds(0, width)], TILE - 2, 0)
                    south = pltpu.roll(edge[c, 1, y, :, pl.ds(0, width)], 2, 0)
                    main[c, y, top, :] = jnp.where(sub < 2, north, main[c, y, top, :])
                    main[c, y, bottom, :] = jnp.where(sub >= TILE - 2, south, main[c, y, bottom, :])
                for j, far in ((1, 0), (2, count - TILE)):
                    r = pl.ds(j * TILE, TILE)
                    held = (lane >= 2) & (lane < count - 2)
                    held = held & ((sub < NSUB) if j == 1 else (sub >= TILE - NSUB))
                    u, v = flank[U, y, r, :], flank[V, y, r, :]
                    gone = leave(lambda c: flank[c, y, r, :], u, v)
                    for c in range(2):
                        flank_back[c, y, pl.ds(far, TILE), :] = jnp.where(held, gone[c], 0.0)
                        flank_vel[c, y, pl.ds(far, TILE), :] = jnp.where(held, (u, v)[c], 0.0)

            def returned(t):
                r = pl.ds(pl.multiple_of(t * TILE, TILE), TILE)
                block = sub + t * TILE
                theirs = outer & (block >= 2) & (block < count - 2)
                for y in range(2):
                    half = pl.ds(y * width, width)
                    u, v = main[U, y, r, :], main[V, y, r, :]
                    gone = leave(lambda c: main[c, y, r, :], u, v)
                    for c in range(2):
                        forc[c, r, half] = jnp.where(theirs, 0.0, gone[c])
                        out[0, c, r, half] = jnp.where(theirs, 0.0, (u, v)[c])

            tile_loop(tiles, 2, returned)
        with jax.named_scope("i_back"):
            for c in range(2):
                both = dot_rows(to_slots, forc[c])
                for y in range(2):
                    part = both[:, y * width:(y + 1) * width]
                    back[c, :, pl.ds(y * width, width)] = part + dot_lanes(to_slots, flank_back[c, y])
            send_rows(0, back, 0, 2, ret, 0, ret_ssem.at[1], ret_rsem.at[1])
        same = jnp.where(diag, 1.0, 0.0).astype(jnp.bfloat16)
        same = jnp.concatenate([same] * 3, axis=1)
        for c in range(2):
            for y in range(2):
                half = pl.ds(y * width, width)
                out[0, c, :, half] += dot_lanes(same, flank_vel[c, y])
        wait_bytes(back.at[pl.ds(2, 1)], ret_ssem.at[0])
        wait_bytes(back.at[pl.ds(0, 2)], ret_ssem.at[1])


def per_device_kernel(n_lat, n_lon, fields, block_owner, ice_covered, land_mask):
    count, cells = land_mask.shape
    peers = n_lat * n_lon
    f32 = jnp.float32
    anywhere = pl.BlockSpec(memory_space=pl.ANY)
    in_vmem = pl.BlockSpec(memory_space=pltpu.VMEM)
    dma = pltpu.SemaphoreType.DMA
    halos = [pltpu.VMEM((2, num // 2, TILE, BX), f32) for _, num in ROUNDS] * 2
    sides = [pltpu.VMEM((2, TILE, BX), f32) for _ in ROUNDS]
    sides += [pltpu.VMEM((3, 2, TILE, BX), f32) for _ in ROUNDS]
    return pl.pallas_call(
        functools.partial(step_kernel, n_lat, n_lon),
        out_shape=pltpu.VMEM((1, 2, count, cells), f32),
        in_specs=[anywhere, anywhere, anywhere, anywhere],
        out_specs=in_vmem,
        scratch_shapes=[
            pltpu.VMEM((7, count, cells), f32),
            pltpu.VMEM((2, count, cells), f32),
            pltpu.VMEM((3, count, cells), f32),
            pltpu.VMEM((1, count), jnp.int32),
            pltpu.VMEM((1, count), jnp.int32),
            pltpu.VMEM((peers, 1, count), jnp.int32),
            pltpu.VMEM((6, count, cells), f32),
            pltpu.VMEM((2, count, cells), f32),
            pltpu.VMEM((count, count), f32),
            pltpu.VMEM((3, count, cells), f32),
            pltpu.VMEM((count, cells), jnp.int32),
            pltpu.VMEM((14, 2, count, BX), f32),
            pltpu.VMEM((14, 2, 2, TILE, 2 * BX), f32),
            pltpu.VMEM((14, 2, 4 * TILE, BX), f32),
            pltpu.VMEM((2, 2, BX, count), f32),
            pltpu.VMEM((2, 2, BX, count), f32),
            *halos, *sides,
            dma((4,)), dma, dma, dma((2,)), dma((2,)), dma((2,)), dma((2,)),
            dma((3, 10)), dma((3, 10)),
        ],
        compiler_params=pltpu.CompilerParams(
            collective_id=0, has_side_effects=True, vmem_limit_bytes=63 * 1024 * 1024
        ),
    )(fields, block_owner.reshape(1, count), ice_covered.reshape(1, count), land_mask)


def solution(mesh):
    placed = (
        P("comp", None, ("lat", "lon"), None),
        P(("lat", "lon")),
        P(("lat", "lon")),
        P(("lat", "lon"), None),
    )
    n_lat, n_lon = mesh.shape["lat"], mesh.shape["lon"]

    def body(fields, block_owner, ice_covered, land_mask):
        count = block_owner.shape[0]
        whole_tiles = count % (n_lat * n_lon * TILE) == 0 and count == BX
        if whole_tiles and n_lon > 2:
            return per_device_kernel(n_lat, n_lon, fields, block_owner, ice_covered, land_mask)
        return per_device(fields, block_owner, ice_covered, land_mask)

    return jax.shard_map(
        body,
        mesh=mesh,
        in_specs=placed,
        out_specs=P("comp", None, ("lat", "lon"), None),
        check_vma=False,
    )
```

```python
import functools

import jax
import jax.numpy as jnp
from jax import lax
from jax.experimental import pallas as pl
from jax.experimental.pallas import tpu as pltpu
from jax.sharding import PartitionSpec as P

GX = 1
BY = 2
BX = 128
NSUB = 4


CD_ICE = 0.1
CW = 1.5
CSTAR = 2.0
ECC2 = 4.0
DMIN2 = 0.25
RELAX = 0.5
DTE = 0.5
CORIO = 0.3
MASS_FLOOR = 0.5
DRAG_FLOOR = 0.1


def from_behind(x, axis, by):
    size = lax.axis_size(axis)
    pairs = [(i, i + by) for i in range(size) if 0 <= i + by < size]
    return lax.ppermute(x, axis, pairs)


def with_halo(x, sides, width, wrap):
    for axis, dim in sides:
        size, length = (lax.axis_size(axis), x.shape[dim])
        up = [(i, (i + 1) % size) for i in range(size if wrap else size - 1)]
        down = [(j, i) for i, j in up]
        last = lax.slice_in_dim(x, length - width, length, axis=dim)
        first = lax.slice_in_dim(x, 0, width, axis=dim)
        before = lax.ppermute(last, axis, up)
        after = lax.ppermute(first, axis, down)
        x = jnp.concatenate([before, x, after], axis=dim)
    return x


def air_stress(ocean):
    wind_x, wind_y, current_x, current_y, tilt_x, tilt_y, density = ocean
    speed_ice = jnp.sqrt(wind_x * wind_x + wind_y * wind_y + 1.0)
    scale_ice = density * CD_ICE * speed_ice
    rel_x = wind_x - current_x
    rel_y = wind_y - current_y
    speed_open = jnp.sqrt(rel_x * rel_x + rel_y * rel_y + 1.0)
    scale_open = density * (0.1 + 0.05 * speed_open) * speed_open
    outbound = jnp.stack(
        [scale_ice * wind_x, scale_ice * wind_y, current_x, current_y, tilt_x, tilt_y]
    )
    open_stress = jnp.stack([scale_open * rel_x, scale_open * rel_y])
    return (outbound, open_stress)


def prepare(ice_tile, forcing, active):
    ice_mass = ice_tile[2]
    concentration = ice_tile[3]
    strength = ice_mass * jnp.exp(CSTAR * (concentration - 1.0)) * active
    drag_base = CW * concentration * active
    push_x = active * (concentration * forcing[0] - ice_mass * forcing[4])
    push_y = active * (concentration * forcing[1] - ice_mass * forcing[5])
    return jnp.stack(
        [strength, ice_mass, drag_base, push_x, push_y, forcing[2], forcing[3], active]
    )


def subcycle(ice_state, statics):
    east_vel, north_vel, stress_one, stress_two, stress_three = ice_state
    strength = statics[0]
    east_base = east_vel[:-1, :-1]
    north_base = north_vel[:-1, :-1]
    strain_xx = east_vel[:-1, 1:] - east_base
    strain_yy = north_vel[1:, :-1] - north_base
    shear = east_vel[1:, :-1] - east_base + (north_vel[:-1, 1:] - north_base)
    divergence = strain_xx + strain_yy
    tension = strain_xx - strain_yy
    delta_norm = jnp.sqrt(
        divergence * divergence + (tension * tension + shear * shear) / ECC2 + DMIN2
    )
    viscosity = strength[:-1, :-1] / delta_norm
    stress_sum = (stress_one[:-1, :-1] + RELAX * viscosity * (divergence - delta_norm)) / (
        1.0 + RELAX
    )
    stress_diff = (stress_two[:-1, :-1] + RELAX * viscosity * tension / ECC2) / (1.0 + RELAX)
    stress_shear = (stress_three[:-1, :-1] + RELAX * viscosity * shear / (2.0 * ECC2)) / (
        1.0 + RELAX
    )
    stress_xx = 0.5 * (stress_sum + stress_diff)
    stress_yy = 0.5 * (stress_sum - stress_diff)
    force_x = (
        stress_xx[1:, 1:] - stress_xx[1:, :-1] + (stress_shear[1:, 1:] - stress_shear[:-1, 1:])
    )
    force_y = (
        stress_shear[1:, 1:] - stress_shear[1:, :-1] + (stress_yy[1:, 1:] - stress_yy[:-1, 1:])
    )
    trimmed = statics[:, 1:-1, 1:-1]
    strength, ice_mass, drag_base, push_x, push_y, current_x, current_y, active = trimmed
    east_old = east_vel[1:-1, 1:-1]
    north_old = north_vel[1:-1, 1:-1]
    diff_x = current_x - east_old
    diff_y = current_y - north_old
    drag_coef = drag_base * jnp.sqrt(diff_x * diff_x + diff_y * diff_y + DRAG_FLOOR)
    denominator = jnp.maximum(ice_mass, MASS_FLOOR) / DTE + drag_coef
    east_new = (
        active
        * (
            ice_mass / DTE * east_old
            + force_x
            + push_x
            + drag_coef * current_x
            + CORIO * ice_mass * north_old
        )
        / denominator
    )
    north_new = (
        active
        * (
            ice_mass / DTE * north_old
            + force_y
            + push_y
            + drag_coef * current_y
            - CORIO * ice_mass * east_old
        )
        / denominator
    )
    new_state = jnp.stack(
        [east_new, north_new, stress_sum[1:, 1:], stress_diff[1:, 1:], stress_shear[1:, 1:]]
    )
    return (new_state, trimmed)


def give_back(ice_state, statics):
    east_vel = ice_state[0]
    north_vel = ice_state[1]
    drag_base = statics[2]
    current_x = statics[5]
    current_y = statics[6]
    diff_x = east_vel - current_x
    diff_y = north_vel - current_y
    factor = drag_base * jnp.sqrt(diff_x * diff_x + diff_y * diff_y + DRAG_FLOOR)
    return jnp.stack([factor * diff_x, factor * diff_y, drag_base / CW])


def to_tile(blocks):
    channels, count, cells = blocks.shape
    arranged = blocks.reshape(channels, count // GX, GX, BY, BX).transpose(0, 1, 3, 2, 4)
    return arranged.reshape(channels, count // GX * BY, GX * BX)


def from_tile(values):
    channels, rows, columns = values.shape
    arranged = values.reshape(channels, rows // BY, BY, GX, BX).transpose(0, 1, 3, 2, 4)
    return arranged.reshape(channels, rows // BY * GX, BY * BX)


def per_device(fields, block_owner, ice_covered, land_mask):
    count = block_owner.shape[0]
    is_ocean = lax.axis_index("comp") == 0
    outbound, open_stress = air_stress(fields[0])
    owner_row = block_owner.reshape(1, count)
    crossed = from_behind(outbound, "comp", 1)
    received, anchor = (
        lax.all_to_all(crossed, ("lat", "lon"), split_axis=1, concat_axis=1, tiled=True),
        lax.all_to_all(owner_row, ("lat", "lon"), split_axis=1, concat_axis=1, tiled=True),
    )
    local_ids = anchor[0] % count
    position = jnp.zeros((count,), jnp.int32).at[local_ids].set(jnp.arange(count, dtype=jnp.int32))
    forcing = to_tile(received[:, position])
    ice_tile = to_tile(fields[0])
    covered = ice_covered.astype(jnp.float32)[:, None] * (1 - land_mask).astype(jnp.float32)
    active = to_tile(covered[None])[0]
    statics = prepare(ice_tile, forcing, active)
    ice_state = jnp.stack([ice_tile[0], ice_tile[1], ice_tile[4], ice_tile[5], ice_tile[6]])
    joined = jnp.concatenate([ice_state, statics], 0)
    joined = with_halo(joined, (("lon", 2),), NSUB, True)
    joined = with_halo(joined, (("lat", 1),), NSUB, False)
    ice_state = joined[:5]
    statics = joined[5:]
    for repeat in range(NSUB):
        ice_state, statics = subcycle(ice_state, statics)
    returned = from_tile(give_back(ice_state, statics))
    back_send = returned[:, local_ids]
    regrouped = lax.all_to_all(back_send, ("lat", "lon"), split_axis=1, concat_axis=1, tiled=True)
    received_back = from_behind(regrouped, "comp", -1)
    ocean_out = received_back[:2] + (1.0 - received_back[2]) * open_stress
    ice_out = from_tile(ice_state[:2])
    return jnp.where(is_ocean, ocean_out, ice_out)[None]


TILE = 8
GROUP = 8
MESH = pl.DeviceIdType.MESH
U, V, MASS, CONC, S1, S2, S12, ACTIVE, PUSH_X, PUSH_Y, CUR_X, CUR_Y, STRENGTH, DRAG = range(14)
SIDES = [(a, b) for b in (-1, 1) for a in (0, -1, 1)]
ALL_AROUND = [(-1, 0), (1, 0)] + SIDES
ROUNDS = ((U, 8), (CUR_X, 2), (PUSH_X, 2))
KEEP = 1.0 / (1.0 + RELAX)


def tile_loop(tiles, together, body):
    def step(k, carry):
        for j in range(together):
            body(k * together + j)
        return carry
    lax.fori_loop(0, tiles // together, step, 0)


def pieces(values, axis):
    parts = []
    rest = values
    for piece in range(3):
        part = rest.astype(jnp.bfloat16)
        if piece < 2:
            rest = rest - part.astype(jnp.float32)
        parts.append(part)
    return jnp.concatenate(parts, axis=axis)


def dot_rows(thrice, values):
    return lax.dot_general(
        thrice, pieces(values, 0), (((1,), (0,)), ((), ())), preferred_element_type=jnp.float32
    )


def dot_lanes(thrice, values):
    return lax.dot_general(
        thrice, pieces(values, 1), (((1,), (1,)), ((), ())), preferred_element_type=jnp.float32
    )


def new_stress(strength, s1, s2, s12, u, v, u_east, v_east, u_up, v_up):
    sxx = u_east - u
    syy = v_up - v
    shear = (u_up - u) + (v_east - v)
    div = sxx + syy
    ten = sxx - syy
    square = div * div + (ten * ten + shear * shear) * (1.0 / ECC2) + DMIN2
    inverse = lax.rsqrt(square)
    visc = strength * inverse
    s1 = s1 * KEEP + visc * (div - square * inverse)
    s2 = s2 * KEEP + visc * ten * (1.0 / ECC2)
    s12 = s12 * KEEP + visc * shear * (0.5 / ECC2)
    return s1, s2, s12


def new_velocity(get, u, v, force_x, force_y):
    mass, cx, cy = get(MASS), get(CUR_X), get(CUR_Y)
    dx, dy = cx - u, cy - v
    square = dx * dx + dy * dy + DRAG_FLOOR
    drag = get(DRAG) * (square * lax.rsqrt(square))
    gain = get(ACTIVE) / (jnp.maximum(mass, MASS_FLOOR) * (1.0 / DTE) + drag)
    inertia = mass * (1.0 / DTE)
    turn = CORIO * mass
    return (
        gain * (inertia * u + force_x + get(PUSH_X) + drag * cx + turn * v),
        gain * (inertia * v + force_y + get(PUSH_Y) + drag * cy - turn * u),
    )


def step_kernel(
    n_lat, n_lon,
    fields, owner_hbm, covered_hbm, land, ret, here,
    surf, stay, owner, covered, ids, recv, forc, one_hot, back, land_v,
    main, edge, flank, flank_back, flank_vel,
    rows_out0, rows_out1, rows_out2, rows_got0, rows_got1, rows_got2,
    side_out0, side_out1, side_out2, side_got0, side_got1, side_got2,
    load_sem, ids_ssem, ids_rsem, fwd_ssem, fwd_rsem, ret_ssem, ret_rsem, halo_ssem, halo_rsem,
):
    comp = lax.axis_index("comp")
    lat = lax.axis_index("lat")
    lon = lax.axis_index("lon")
    peers = n_lat * n_lon
    me = lat * n_lon + lon
    count = owner.shape[1]
    per = count // peers
    width = BX
    barrier = pltpu.get_barrier_semaphore()
    rows_out = (rows_out0, rows_out1, rows_out2)
    rows_got = (rows_got0, rows_got1, rows_got2)
    side_out = (side_out0, side_out1, side_out2)
    side_got = (side_got0, side_got1, side_got2)

    def rows_of(peer):
        return pl.ds(pl.multiple_of(peer * per, per), per)

    def device(kind, peer):
        return (kind, peer // n_lon, peer % n_lon)

    def each_peer(body):
        beyond = jnp.where(lat < n_lat // 2, n_lat // 2, 0)

        def step(k, carry):
            body((beyond + k // n_lon) % n_lat * n_lon + (lon + k) % n_lon)
            return carry
        lax.fori_loop(0, peers, step, 0)

    def signal_peers(kind):
        each_peer(
            lambda p: pl.semaphore_signal(
                barrier, inc=1, device_id=device(kind, p), device_id_type=MESH
            )
        )

    def send_rows(kind, src, lo, num, dst, dlo, ssem, rsem):
        def body(p):
            pltpu.make_async_remote_copy(
                src_ref=src.at[pl.ds(lo, num), rows_of(p), :],
                dst_ref=dst.at[pl.ds(dlo, num), rows_of(me), :],
                send_sem=ssem, recv_sem=rsem,
                device_id=device(kind, p), device_id_type=MESH,
            ).start()
        each_peer(body)

    def wait_bytes(ref, sem):
        pltpu.make_async_copy(ref, ref, sem).wait()

    def keep_here():
        copy = pltpu.make_async_copy(stay, here, load_sem.at[4])
        copy.start()
        copy.wait()

    @pl.when(comp == 0)
    def _ocean():
        signal_peers(1)
        names = pltpu.make_async_copy(owner_hbm, owner, load_sem.at[3])
        raw = pltpu.make_async_copy(fields.at[0, pl.ds(2, 4)], surf.at[pl.ds(2, 4)], load_sem.at[0])
        wind = pltpu.make_async_copy(fields.at[0, pl.ds(0, 2)], surf.at[pl.ds(0, 2)], load_sem.at[1])
        rho = pltpu.make_async_copy(fields.at[0, pl.ds(6, 1)], surf.at[pl.ds(6, 1)], load_sem.at[2])
        names.start()
        raw.start()
        wind.start()
        rho.start()
        names.wait()
        with jax.named_scope("o_barrier"):
            pl.semaphore_wait(barrier, peers)

        def ids_out(p):
            pltpu.make_async_remote_copy(
                src_ref=owner, dst_ref=ids.at[me], send_sem=ids_ssem, recv_sem=ids_rsem,
                device_id=device(1, p), device_id_type=MESH,
            ).start()
        with jax.named_scope("o_send4"):
            each_peer(ids_out)
            raw.wait()
            send_rows(1, surf, 2, 4, recv, 2, fwd_ssem.at[0], fwd_rsem.at[0])
            wind.wait()
            rho.wait()

        def stress(t):
            r = pl.ds(pl.multiple_of(t * TILE, TILE), TILE)
            wx, wy, density = surf[0, r, :], surf[1, r, :], surf[6, r, :]
            scale = density * CD_ICE * jnp.sqrt(wx * wx + wy * wy + 1.0)
            forc[0, r, :] = scale * wx
            forc[1, r, :] = scale * wy

        with jax.named_scope("o_stress"):
            tile_loop(count // TILE, 2, stress)
            send_rows(1, forc, 0, 2, recv, 0, fwd_ssem.at[1], fwd_rsem.at[1])

        def open_water(t):
            r = pl.ds(pl.multiple_of(t * TILE, TILE), TILE)
            density = surf[6, r, :]
            rel_x = surf[0, r, :] - surf[2, r, :]
            rel_y = surf[1, r, :] - surf[3, r, :]
            speed = jnp.sqrt(rel_x * rel_x + rel_y * rel_y + 1.0)
            scale = density * (0.1 + 0.05 * speed) * speed
            stay[0, r, :] = scale * rel_x
            stay[1, r, :] = scale * rel_y

        tile_loop(count // TILE, 2, open_water)
        keep_here()
        with jax.named_scope("o_waitret1"):
            wait_bytes(ret.at[pl.ds(2, 1)], ret_rsem.at[0])
        with jax.named_scope("o_waitret2"):
            wait_bytes(ret.at[pl.ds(0, 2)], ret_rsem.at[1])

        wait_bytes(ids, ids_ssem)
        wait_bytes(surf.at[pl.ds(2, 4)], fwd_ssem.at[0])
        wait_bytes(forc.at[pl.ds(0, 2)], fwd_ssem.at[1])

    @pl.when(comp == 1)
    def _ice():
        def inside(a):
            if a == 0:
                return lat >= 0
            return lat + a >= 0 if a < 0 else lat + a < n_lat

        def around(a, b):
            return (1, lat + a, (lon + b + n_lon) % n_lon)

        signal_peers(0)
        for a, b in ALL_AROUND:
            @pl.when(inside(a))
            def _():
                pl.semaphore_signal(barrier, inc=1, device_id=around(a, b), device_id_type=MESH)
        loads = [
            pltpu.make_async_copy(
                fields.at[0, :, :, pl.ds(y * width, width)], main.at[pl.ds(0, 7), y], load_sem.at[y]
            )
            for y in range(2)
        ]
        loads.append(pltpu.make_async_copy(land, land_v, load_sem.at[2]))
        loads.append(pltpu.make_async_copy(covered_hbm, covered, load_sem.at[3]))
        for load in loads:
            load.start()

        tiles = count // TILE
        top, bottom = pl.ds(0, TILE), pl.ds(count - TILE, TILE)
        zero_tile = jnp.zeros((TILE, width), jnp.float32)
        for wall, which in ((lat == 0, 0), (lat == n_lat - 1, 1)):
            @pl.when(wall)
            def _():
                for e in range(3):
                    for k in range(rows_got[e].shape[1]):
                        rows_got[e][which, k] = zero_tile
                    for k in range(2):
                        side_got[e][2 * which, k] = zero_tile

        def clear(t):
            r = pl.ds(pl.multiple_of(t * TILE, TILE), TILE)
            for c in range(2):
                for y in range(2):
                    flank_back[c, y, r, :] = zero_tile
                    flank_vel[c, y, r, :] = zero_tile

        tile_loop(tiles, 2, clear)
        for load in loads:
            load.wait()
        diag = lax.broadcasted_iota(jnp.int32, (count, count), 0) == lax.broadcasted_iota(
            jnp.int32, (count, count), 1
        )
        wet = jnp.sum(
            jnp.where(diag, covered[...].astype(jnp.float32), 0.0), axis=1, keepdims=True
        )
        sea = wet * (1 - land_v[...]).astype(jnp.float32)
        for y in range(2):
            main[ACTIVE, y] = sea[:, y * width:(y + 1) * width]

        lane = lax.broadcasted_iota(jnp.int32, (TILE, width), 1)
        sub = lax.broadcasted_iota(jnp.int32, (TILE, width), 0)
        pick_row = lax.broadcasted_iota(jnp.int32, (2 * TILE, width), 0)
        pick_col = lax.broadcasted_iota(jnp.int32, (2 * TILE, width), 1)
        picked = jnp.where(pick_row < TILE, pick_row, pick_row + (width - 2 * TILE)) == pick_col
        picker = jnp.where(picked, 1.0, 0.0).astype(jnp.bfloat16)
        picker = jnp.concatenate([picker] * 3, axis=1)

        def pack(e):
            lo, num = ROUNDS[e]
            west, east = zero_tile, zero_tile
            for k in range(num // 2):
                ups, downs = zero_tile, zero_tile
                for i in range(4):
                    c, y = lo + 2 * k + i // 2, i % 2
                    head, foot = main[c, y, top, :], main[c, y, bottom, :]
                    here = (sub >= 2 * i) & (sub < 2 * i + 2)
                    ups = jnp.where(here, pltpu.roll(head, 2 * i, 0) if i else head, ups)
                    downs = jnp.where(here, pltpu.roll(foot, (2 * i + 2) % TILE, 0) if i < 3 else foot, downs)
                    ends = jnp.where(sub < NSUB, head, foot)
                    slot = (k * 4 + i) * NSUB
                    mine = (lane >= slot) & (lane < slot + NSUB)
                    west = jnp.where(mine, pltpu.roll(ends, slot, 1) if slot else ends, west)
                    east = jnp.where(mine, pltpu.roll(ends, (slot + NSUB) % width, 1), east)
                rows_out[e][0, k] = ups
                rows_out[e][1, k] = downs
            side_out[e][0] = west
            side_out[e][1] = east
            for c in range(lo, lo + num):
                for y in range(2):
                    across = dot_lanes(picker, main[c, y])
                    flank[c, y, pl.ds(TILE, TILE), :] = across[:TILE]
                    flank[c, y, pl.ds(2 * TILE, TILE), :] = across[TILE:]

        def halo(e, begin):
            lo, num = ROUNDS[e]
            moves = []
            for a in (-1, 1):
                k = 1 if a > 0 else 0
                moves.append((a, 0, rows_out[e].at[k], rows_got[e].at[1 - k]))
            for a, b in SIDES:
                k = 1 if b > 0 else 0
                moves.append((a, b, side_out[e].at[k], side_got[e].at[1 - a, 1 - k]))
            for b in (-1, 1):
                src, dst = (2 * TILE, 0) if b > 0 else (TILE, 3 * TILE)
                moves.append((
                    0, b,
                    flank.at[pl.ds(lo, num), :, pl.ds(src, TILE), :],
                    flank.at[pl.ds(lo, num), :, pl.ds(dst, TILE), :],
                ))
            for k, (a, b, src, dst) in enumerate(moves):
                copy = pltpu.make_async_remote_copy(
                    src_ref=src, dst_ref=dst,
                    send_sem=halo_ssem.at[e, k], recv_sem=halo_rsem.at[e, k],
                    device_id=around(a, b), device_id_type=MESH,
                )
                if begin:
                    @pl.when(inside(a))
                    def _():
                        copy.start()
                else:
                    @pl.when(inside(a))
                    def _():
                        copy.wait_send()

                    @pl.when(inside(-a))
                    def _():
                        copy.wait_recv()

        def unpack(e):
            lo, num = ROUNDS[e]
            got, side = rows_got[e], side_got[e]
            ends = []
            for k in range(2):
                far, near = side[0, k], side[1, k]
                ends.append(pltpu.roll(jnp.where(sub >= TILE - 2, far, near), 2, 0))
            for k in range(2):
                far, near = side[2, k], side[1, k]
                ends.append(pltpu.roll(jnp.where(sub < 2, far, near), TILE - 2, 0))
            for k in range(num // 2):
                for i in range(4):
                    c, y = lo + 2 * k + i // 2, i % 2
                    slot = (k * 4 + i) * NSUB
                    for strip in range(2):
                        own = main[c, y, top if strip == 0 else bottom, :]
                        beyond = got[strip, k]
                        if strip == 0:
                            beyond = pltpu.roll(beyond, (TILE - 2 * i) % TILE, 0) if i else beyond
                            body = jnp.where(sub < 2, beyond, pltpu.roll(own, 2, 0))
                        else:
                            beyond = pltpu.roll(beyond, TILE - 2 - 2 * i, 0) if i < 3 else beyond
                            body = jnp.where(sub >= TILE - 2, beyond, pltpu.roll(own, TILE - 2, 0))
                        from_west, from_east = ends[2 * strip], ends[2 * strip + 1]
                        from_east = pltpu.roll(from_east, width - slot, 1) if slot else from_east
                        from_west = pltpu.roll(from_west, width - NSUB - slot, 1)
                        edge[c, strip, y, :, pl.ds(0, width)] = body
                        edge[c, strip, y, :, pl.ds(width, width)] = jnp.where(
                            lane < NSUB, from_east, jnp.where(lane >= width - NSUB, from_west, 0.0)
                        )

        def derive(load, store):
            conc, act = load(CONC), load(ACTIVE)
            store(STRENGTH, (RELAX * KEEP) * load(MASS) * jnp.exp(CSTAR * (conc - 1.0)) * act)
            store(DRAG, CW * conc * act)

        def derive_main(t):
            r = pl.ds(pl.multiple_of(t * TILE, TILE), TILE)
            for y in range(2):
                def store(c, x):
                    main[c, y, r, :] = x
                derive(lambda c: main[c, y, r, :], store)

        def derive_edges():
            for y in range(2):
                for strip in range(2):
                    def store(c, x):
                        edge[c, strip, y] = x
                    derive(lambda c: edge[c, strip, y], store)

                def store(c, x):
                    flank[c, y] = x
                derive(lambda c: flank[c, y], store)

        def sweep_main(g, stress, velocity):
            spots = [
                pl.ds(pl.multiple_of((g * GROUP + j) * TILE, TILE), TILE) for j in range(GROUP)
            ]
            behind = pl.ds(pl.multiple_of(jnp.maximum(g * GROUP - 1, 0) * TILE, TILE), TILE)
            ahead = pl.ds(
                pl.multiple_of(jnp.minimum(g * GROUP + GROUP, tiles - 1) * TILE, TILE), TILE
            )
            vels = [[(main[U, y, r, :], main[V, y, r, :]) for y in range(2)] for r in spots]
            stresses = []
            if stress:
                follow = (main[U, 0, ahead, :], main[V, 0, ahead, :])
            for j, r in enumerate(spots):
                old = [tuple(main[c, y, r, :] for c in (S1, S2, S12)) for y in range(2)]
                if not stress:
                    stresses.append(old)
                    continue
                beyond = vels[j + 1][0] if j + 1 < GROUP else follow
                row = []
                for y in range(2):
                    u, v = vels[j][y]
                    if y == 0:
                        u_up, v_up = vels[j][1]
                    else:
                        u_up, v_up = (
                            pltpu.roll(jnp.where(sub == 0, after, x), TILE - 1, 0)
                            for x, after in zip(vels[j][0], beyond)
                        )
                    fresh = new_stress(
                        main[STRENGTH, y, r, :], *old[y], u, v,
                        pltpu.roll(u, width - 1, 1), pltpu.roll(v, width - 1, 1), u_up, v_up,
                    )
                    for c, x in zip((S1, S2, S12), fresh):
                        main[c, y, r, :] = x
                    row.append(fresh)
                stresses.append(row)
            if not velocity:
                return
            yy_before = 0.5 * (main[S1, 1, behind, :] - main[S2, 1, behind, :])
            cross_before = main[S12, 1, behind, :]
            for j, r in enumerate(spots):
                xx = [0.5 * (s1 + s2) for s1, s2, _ in stresses[j]]
                yy = [0.5 * (s1 - s2) for s1, s2, _ in stresses[j]]
                cross = [s12 for _, _, s12 in stresses[j]]
                yy_down, cross_down = (
                    [pltpu.roll(jnp.where(sub == TILE - 1, before, x[1]), 1, 0), x[0]]
                    for x, before in ((yy, yy_before), (cross, cross_before))
                )
                yy_before, cross_before = yy[1], cross[1]
                for y in range(2):
                    force_x = xx[y] - pltpu.roll(xx[y], 1, 1) + (cross[y] - cross_down[y])
                    force_y = cross[y] - pltpu.roll(cross[y], 1, 1) + (yy[y] - yy_down[y])
                    u, v = new_velocity(lambda c: main[c, y, r, :], *vels[j][y], force_x, force_y)
                    main[U, y, r, :] = u
                    main[V, y, r, :] = v

        def sweep_edge(stress, velocity):
            for strip in range(2):
                vels = [(edge[U, strip, y], edge[V, strip, y]) for y in range(2)]
                fresh = [tuple(edge[c, strip, y] for c in (S1, S2, S12)) for y in range(2)]
                if stress:
                    ups = [vels[1], tuple(pltpu.roll(x, TILE - 1, 0) for x in vels[0])]
                    for y in range(2):
                        east = [pltpu.roll(x, 2 * width - 1, 1) for x in vels[y]]
                        fresh[y] = new_stress(
                            edge[STRENGTH, strip, y], *fresh[y], *vels[y], *east, *ups[y]
                        )
                        for c, x in zip((S1, S2, S12), fresh[y]):
                            edge[c, strip, y] = x
                if not velocity:
                    continue
                xx = [0.5 * (s1 + s2) for s1, s2, _ in fresh]
                yy = [0.5 * (s1 - s2) for s1, s2, _ in fresh]
                cross = [s12 for _, _, s12 in fresh]
                yy_down, cross_down = ([pltpu.roll(x[1], 1, 0), x[0]] for x in (yy, cross))
                for y in range(2):
                    force_x = xx[y] - pltpu.roll(xx[y], 1, 1) + (cross[y] - cross_down[y])
                    force_y = cross[y] - pltpu.roll(cross[y], 1, 1) + (yy[y] - yy_down[y])
                    u, v = new_velocity(lambda c: edge[c, strip, y], *vels[y], force_x, force_y)
                    edge[U, strip, y] = u
                    edge[V, strip, y] = v

        def sweep_flank(stress, velocity):
            spots = [pl.ds(j * TILE, TILE) for j in range(4)]
            vels = [[(flank[U, y, r, :], flank[V, y, r, :]) for y in range(2)] for r in spots]
            fresh = [
                [tuple(flank[c, y, r, :] for c in (S1, S2, S12)) for y in range(2)] for r in spots
            ]
            if stress:
                for j, r in enumerate(spots):
                    for y in range(2):
                        after = vels[min(j + 1, 3)][y]
                        east = [
                            pltpu.roll(jnp.where(sub == 0, b, x), TILE - 1, 0)
                            for x, b in zip(vels[j][y], after)
                        ]
                        ups = vels[j][1] if y == 0 else [
                            pltpu.roll(x, width - 1, 1) for x in vels[j][0]
                        ]
                        fresh[j][y] = new_stress(
                            flank[STRENGTH, y, r, :], *fresh[j][y], *vels[j][y], *east, *ups
                        )
                        for c, x in zip((S1, S2, S12), fresh[j][y]):
                            flank[c, y, r, :] = x
            if not velocity:
                return
            xx = [[0.5 * (s1 + s2) for s1, s2, _ in row] for row in fresh]
            yy = [[0.5 * (s1 - s2) for s1, s2, _ in row] for row in fresh]
            cross = [[s12 for _, _, s12 in row] for row in fresh]

            def westward(x, j, y):
                before = x[max(j - 1, 0)][y]
                return pltpu.roll(jnp.where(sub == TILE - 1, before, x[j][y]), 1, 0)

            def downward(x, j, y):
                return x[j][0] if y == 1 else pltpu.roll(x[j][1], 1, 1)

            for j, r in enumerate(spots):
                for y in range(2):
                    force_x = xx[j][y] - westward(xx, j, y) + (cross[j][y] - downward(cross, j, y))
                    force_y = cross[j][y] - westward(cross, j, y) + (yy[j][y] - downward(yy, j, y))
                    u, v = new_velocity(lambda c: flank[c, y, r, :], *vels[j][y], force_x, force_y)
                    flank[U, y, r, :] = u
                    flank[V, y, r, :] = v

        walls = jnp.where(lat == 0, 3, 0) + jnp.where(lat == n_lat - 1, 3, 0)
        with jax.named_scope("i_barrier"):
            pl.semaphore_wait(barrier, peers + 8 - walls)
        with jax.named_scope("i_pack0"):
            pack(0)
            halo(0, True)
        tile_loop(tiles, 2, derive_main)

        with jax.named_scope("i_waitids"):
            wait_bytes(ids, ids_rsem)
        wanted = me * per
        row_lane = lax.broadcasted_iota(jnp.int32, (per, count), 1)
        row_sub = lax.broadcasted_iota(jnp.int32, (per, count), 0)
        mine = row_lane == row_sub + wanted
        blocks = lax.broadcasted_iota(jnp.int32, (per, count), 1).astype(jnp.float32)
        base = (me * count).astype(jnp.float32)
        for p in range(peers):
            owned = jnp.broadcast_to(ids[p], (per, count)).astype(jnp.float32)
            local = jnp.sum(jnp.where(mine, owned, 0.0), axis=1, keepdims=True) - base
            one_hot[pl.ds(p * per, per), :] = jnp.where(local == blocks, 1.0, 0.0)

        with jax.named_scope("i_waithalo0"):
            halo(0, False)
        with jax.named_scope("i_unpack0"):
            unpack(0)
            derive_edges()
        groups = tiles // GROUP
        with jax.named_scope("i_stress"):
            tile_loop(groups, 1, lambda g: sweep_main(g, True, False))
            sweep_edge(True, False)
            sweep_flank(True, False)
        by_slot = one_hot[...]
        to_slots = jnp.concatenate([by_slot.astype(jnp.bfloat16)] * 3, axis=1)
        to_blocks = jnp.concatenate([by_slot.T.astype(jnp.bfloat16)] * 3, axis=1)

        with jax.named_scope("i_waitf4"):
            wait_bytes(recv.at[pl.ds(2, 4)], fwd_rsem.at[0])
        for c in range(2):
            both = dot_rows(to_blocks, recv[2 + c])
            for y in range(2):
                main[CUR_X + c, y] = both[:, y * width:(y + 1) * width]
        with jax.named_scope("i_packmid"):
            pack(1)
            halo(1, True)
        for c in range(2):
            both = dot_rows(to_blocks, recv[4 + c])
            for y in range(2):
                main[PUSH_X + c, y] = main[MASS, y] * both[:, y * width:(y + 1) * width]
        for y in range(2):
            share = main[CONC, y] * main[ACTIVE, y]
            back[2, :, pl.ds(y * width, width)] = dot_rows(to_slots, share)

        with jax.named_scope("i_waitf2"):
            wait_bytes(recv.at[pl.ds(0, 2)], fwd_rsem.at[1])
        with jax.named_scope("i_push"):
            for c in range(2):
                both = dot_rows(to_blocks, recv[c])
                for y in range(2):
                    main[PUSH_X + c, y] = main[ACTIVE, y] * (
                        main[CONC, y] * both[:, y * width:(y + 1) * width] - main[PUSH_X + c, y]
                    )
        with jax.named_scope("i_packlate"):
            pack(2)
            halo(2, True)

        with jax.named_scope("i_vel1"):
            tile_loop(groups, 1, lambda g: sweep_main(g, False, True))
        with jax.named_scope("i_sweeps"):
            tile_loop((NSUB - 1) * groups, 1, lambda k: sweep_main(k % groups, True, True))
        send_rows(0, back, 2, 1, ret, 2, ret_ssem.at[0], ret_rsem.at[0])
        with jax.named_scope("i_waitmid"):
            halo(1, False)
        unpack(1)
        with jax.named_scope("i_waitlate"):
            halo(2, False)
        def sweep_strips(stress, velocity):
            sweep_flank(stress, velocity)
            sweep_edge(stress, velocity)

        with jax.named_scope("i_edge"):
            unpack(2)
            sweep_strips(False, True)
            tile_loop(NSUB - 1, 1, lambda k: sweep_strips(True, True))

        def leave(get, u, v):
            dx, dy = u - get(CUR_X), v - get(CUR_Y)
            drag = get(DRAG) * jnp.sqrt(dx * dx + dy * dy + DRAG_FLOOR)
            return drag * dx, drag * dy

        outer = (lane < NSUB) | (lane >= width - NSUB)

        with jax.named_scope("i_returned"):
            for y in range(2):
                for c in (U, V):
                    north = pltpu.roll(edge[c, 0, y, :, pl.ds(0, width)], TILE - 2, 0)
                    south = pltpu.roll(edge[c, 1, y, :, pl.ds(0, width)], 2, 0)
                    main[c, y, top, :] = jnp.where(sub < 2, north, main[c, y, top, :])
                    main[c, y, bottom, :] = jnp.where(sub >= TILE - 2, south, main[c, y, bottom, :])
                for j, far in ((1, 0), (2, count - TILE)):
                    r = pl.ds(j * TILE, TILE)
                    held = (lane >= 2) & (lane < count - 2)
                    held = held & ((sub < NSUB) if j == 1 else (sub >= TILE - NSUB))
                    u, v = flank[U, y, r, :], flank[V, y, r, :]
                    gone = leave(lambda c: flank[c, y, r, :], u, v)
                    for c in range(2):
                        flank_back[c, y, pl.ds(far, TILE), :] = jnp.where(held, gone[c], 0.0)
                        flank_vel[c, y, pl.ds(far, TILE), :] = jnp.where(held, (u, v)[c], 0.0)

            def returned(t):
                r = pl.ds(pl.multiple_of(t * TILE, TILE), TILE)
                block = sub + t * TILE
                theirs = outer & (block >= 2) & (block < count - 2)
                for y in range(2):
                    half = pl.ds(y * width, width)
                    u, v = main[U, y, r, :], main[V, y, r, :]
                    gone = leave(lambda c: main[c, y, r, :], u, v)
                    for c in range(2):
                        forc[c, r, half] = jnp.where(theirs, 0.0, gone[c])
                        stay[c, r, half] = jnp.where(theirs, 0.0, (u, v)[c])

            tile_loop(tiles, 2, returned)
        with jax.named_scope("i_back"):
            for c in range(2):
                both = dot_rows(to_slots, forc[c])
                for y in range(2):
                    part = both[:, y * width:(y + 1) * width]
                    back[c, :, pl.ds(y * width, width)] = part + dot_lanes(to_slots, flank_back[c, y])
            send_rows(0, back, 0, 2, ret, 0, ret_ssem.at[1], ret_rsem.at[1])
        same = jnp.where(diag, 1.0, 0.0).astype(jnp.bfloat16)
        same = jnp.concatenate([same] * 3, axis=1)
        for c in range(2):
            for y in range(2):
                half = pl.ds(y * width, width)
                stay[c, :, half] += dot_lanes(same, flank_vel[c, y])
        keep_here()
        wait_bytes(back.at[pl.ds(2, 1)], ret_ssem.at[0])
        wait_bytes(back.at[pl.ds(0, 2)], ret_ssem.at[1])


def per_device_kernel(n_lat, n_lon, fields, block_owner, ice_covered, land_mask):
    count, cells = land_mask.shape
    peers = n_lat * n_lon
    f32 = jnp.float32
    anywhere = pl.BlockSpec(memory_space=pl.ANY)
    dma = pltpu.SemaphoreType.DMA
    halos = [pltpu.VMEM((2, num // 2, TILE, BX), f32) for _, num in ROUNDS] * 2
    sides = [pltpu.VMEM((2, TILE, BX), f32) for _ in ROUNDS]
    sides += [pltpu.VMEM((3, 2, TILE, BX), f32) for _ in ROUNDS]
    ret, here = pl.pallas_call(
        functools.partial(step_kernel, n_lat, n_lon),
        out_shape=(pltpu.VMEM((3, count, cells), f32), pltpu.VMEM((2, count, cells), f32)),
        in_specs=[anywhere, anywhere, anywhere, anywhere],
        out_specs=(anywhere, anywhere),
        scratch_shapes=[
            pltpu.VMEM((7, count, cells), f32),
            pltpu.VMEM((2, count, cells), f32),
            pltpu.VMEM((1, count), jnp.int32),
            pltpu.VMEM((1, count), jnp.int32),
            pltpu.VMEM((peers, 1, count), jnp.int32),
            pltpu.VMEM((6, count, cells), f32),
            pltpu.VMEM((2, count, cells), f32),
            pltpu.VMEM((count, count), f32),
            pltpu.VMEM((3, count, cells), f32),
            pltpu.VMEM((count, cells), jnp.int32),
            pltpu.VMEM((14, 2, count, BX), f32),
            pltpu.VMEM((14, 2, 2, TILE, 2 * BX), f32),
            pltpu.VMEM((14, 2, 4 * TILE, BX), f32),
            pltpu.VMEM((2, 2, BX, count), f32),
            pltpu.VMEM((2, 2, BX, count), f32),
            *halos, *sides,
            dma((5,)), dma, dma, dma((2,)), dma((2,)), dma((2,)), dma((2,)),
            dma((3, 10)), dma((3, 10)),
        ],
        compiler_params=pltpu.CompilerParams(
            collective_id=0, has_side_effects=True, vmem_limit_bytes=63 * 1024 * 1024
        ),
    )(fields, block_owner.reshape(1, count), ice_covered.reshape(1, count), land_mask)
    is_ocean = lax.axis_index("comp") == 0
    return jnp.where(is_ocean, ret[:2] + (1.0 - ret[2]) * here, here)[None]


def solution(mesh):
    placed = (
        P("comp", None, ("lat", "lon"), None),
        P(("lat", "lon")),
        P(("lat", "lon")),
        P(("lat", "lon"), None),
    )
    n_lat, n_lon = mesh.shape["lat"], mesh.shape["lon"]

    def body(fields, block_owner, ice_covered, land_mask):
        count = block_owner.shape[0]
        whole_tiles = count % (n_lat * n_lon * TILE) == 0 and count == BX
        if whole_tiles and n_lon > 2:
            return per_device_kernel(n_lat, n_lon, fields, block_owner, ice_covered, land_mask)
        return per_device(fields, block_owner, ice_covered, land_mask)

    return jax.shard_map(
        body,
        mesh=mesh,
        in_specs=placed,
        out_specs=P("comp", None, ("lat", "lon"), None),
        check_vma=False,
    )
```

```python
import functools

import jax
import jax.numpy as jnp
from jax import lax
from jax.experimental import pallas as pl
from jax.experimental.pallas import tpu as pltpu
from jax.sharding import PartitionSpec as P

GX = 1
BY = 2
BX = 128
NSUB = 4


CD_ICE = 0.1
CW = 1.5
CSTAR = 2.0
ECC2 = 4.0
DMIN2 = 0.25
RELAX = 0.5
DTE = 0.5
CORIO = 0.3
MASS_FLOOR = 0.5
DRAG_FLOOR = 0.1


def from_behind(x, axis, by):
    size = lax.axis_size(axis)
    pairs = [(i, i + by) for i in range(size) if 0 <= i + by < size]
    return lax.ppermute(x, axis, pairs)


def with_halo(x, sides, width, wrap):
    for axis, dim in sides:
        size, length = (lax.axis_size(axis), x.shape[dim])
        up = [(i, (i + 1) % size) for i in range(size if wrap else size - 1)]
        down = [(j, i) for i, j in up]
        last = lax.slice_in_dim(x, length - width, length, axis=dim)
        first = lax.slice_in_dim(x, 0, width, axis=dim)
        before = lax.ppermute(last, axis, up)
        after = lax.ppermute(first, axis, down)
        x = jnp.concatenate([before, x, after], axis=dim)
    return x


def air_stress(ocean):
    wind_x, wind_y, current_x, current_y, tilt_x, tilt_y, density = ocean
    speed_ice = jnp.sqrt(wind_x * wind_x + wind_y * wind_y + 1.0)
    scale_ice = density * CD_ICE * speed_ice
    rel_x = wind_x - current_x
    rel_y = wind_y - current_y
    speed_open = jnp.sqrt(rel_x * rel_x + rel_y * rel_y + 1.0)
    scale_open = density * (0.1 + 0.05 * speed_open) * speed_open
    outbound = jnp.stack(
        [scale_ice * wind_x, scale_ice * wind_y, current_x, current_y, tilt_x, tilt_y]
    )
    open_stress = jnp.stack([scale_open * rel_x, scale_open * rel_y])
    return (outbound, open_stress)


def prepare(ice_tile, forcing, active):
    ice_mass = ice_tile[2]
    concentration = ice_tile[3]
    strength = ice_mass * jnp.exp(CSTAR * (concentration - 1.0)) * active
    drag_base = CW * concentration * active
    push_x = active * (concentration * forcing[0] - ice_mass * forcing[4])
    push_y = active * (concentration * forcing[1] - ice_mass * forcing[5])
    return jnp.stack(
        [strength, ice_mass, drag_base, push_x, push_y, forcing[2], forcing[3], active]
    )


def subcycle(ice_state, statics):
    east_vel, north_vel, stress_one, stress_two, stress_three = ice_state
    strength = statics[0]
    east_base = east_vel[:-1, :-1]
    north_base = north_vel[:-1, :-1]
    strain_xx = east_vel[:-1, 1:] - east_base
    strain_yy = north_vel[1:, :-1] - north_base
    shear = east_vel[1:, :-1] - east_base + (north_vel[:-1, 1:] - north_base)
    divergence = strain_xx + strain_yy
    tension = strain_xx - strain_yy
    delta_norm = jnp.sqrt(
        divergence * divergence + (tension * tension + shear * shear) / ECC2 + DMIN2
    )
    viscosity = strength[:-1, :-1] / delta_norm
    stress_sum = (stress_one[:-1, :-1] + RELAX * viscosity * (divergence - delta_norm)) / (
        1.0 + RELAX
    )
    stress_diff = (stress_two[:-1, :-1] + RELAX * viscosity * tension / ECC2) / (1.0 + RELAX)
    stress_shear = (stress_three[:-1, :-1] + RELAX * viscosity * shear / (2.0 * ECC2)) / (
        1.0 + RELAX
    )
    stress_xx = 0.5 * (stress_sum + stress_diff)
    stress_yy = 0.5 * (stress_sum - stress_diff)
    force_x = (
        stress_xx[1:, 1:] - stress_xx[1:, :-1] + (stress_shear[1:, 1:] - stress_shear[:-1, 1:])
    )
    force_y = (
        stress_shear[1:, 1:] - stress_shear[1:, :-1] + (stress_yy[1:, 1:] - stress_yy[:-1, 1:])
    )
    trimmed = statics[:, 1:-1, 1:-1]
    strength, ice_mass, drag_base, push_x, push_y, current_x, current_y, active = trimmed
    east_old = east_vel[1:-1, 1:-1]
    north_old = north_vel[1:-1, 1:-1]
    diff_x = current_x - east_old
    diff_y = current_y - north_old
    drag_coef = drag_base * jnp.sqrt(diff_x * diff_x + diff_y * diff_y + DRAG_FLOOR)
    denominator = jnp.maximum(ice_mass, MASS_FLOOR) / DTE + drag_coef
    east_new = (
        active
        * (
            ice_mass / DTE * east_old
            + force_x
            + push_x
            + drag_coef * current_x
            + CORIO * ice_mass * north_old
        )
        / denominator
    )
    north_new = (
        active
        * (
            ice_mass / DTE * north_old
            + force_y
            + push_y
            + drag_coef * current_y
            - CORIO * ice_mass * east_old
        )
        / denominator
    )
    new_state = jnp.stack(
        [east_new, north_new, stress_sum[1:, 1:], stress_diff[1:, 1:], stress_shear[1:, 1:]]
    )
    return (new_state, trimmed)


def give_back(ice_state, statics):
    east_vel = ice_state[0]
    north_vel = ice_state[1]
    drag_base = statics[2]
    current_x = statics[5]
    current_y = statics[6]
    diff_x = east_vel - current_x
    diff_y = north_vel - current_y
    factor = drag_base * jnp.sqrt(diff_x * diff_x + diff_y * diff_y + DRAG_FLOOR)
    return jnp.stack([factor * diff_x, factor * diff_y, drag_base / CW])


def to_tile(blocks):
    channels, count, cells = blocks.shape
    arranged = blocks.reshape(channels, count // GX, GX, BY, BX).transpose(0, 1, 3, 2, 4)
    return arranged.reshape(channels, count // GX * BY, GX * BX)


def from_tile(values):
    channels, rows, columns = values.shape
    arranged = values.reshape(channels, rows // BY, BY, GX, BX).transpose(0, 1, 3, 2, 4)
    return arranged.reshape(channels, rows // BY * GX, BY * BX)


def per_device(fields, block_owner, ice_covered, land_mask):
    count = block_owner.shape[0]
    is_ocean = lax.axis_index("comp") == 0
    outbound, open_stress = air_stress(fields[0])
    owner_row = block_owner.reshape(1, count)
    crossed = from_behind(outbound, "comp", 1)
    received, anchor = (
        lax.all_to_all(crossed, ("lat", "lon"), split_axis=1, concat_axis=1, tiled=True),
        lax.all_to_all(owner_row, ("lat", "lon"), split_axis=1, concat_axis=1, tiled=True),
    )
    local_ids = anchor[0] % count
    position = jnp.zeros((count,), jnp.int32).at[local_ids].set(jnp.arange(count, dtype=jnp.int32))
    forcing = to_tile(received[:, position])
    ice_tile = to_tile(fields[0])
    covered = ice_covered.astype(jnp.float32)[:, None] * (1 - land_mask).astype(jnp.float32)
    active = to_tile(covered[None])[0]
    statics = prepare(ice_tile, forcing, active)
    ice_state = jnp.stack([ice_tile[0], ice_tile[1], ice_tile[4], ice_tile[5], ice_tile[6]])
    joined = jnp.concatenate([ice_state, statics], 0)
    joined = with_halo(joined, (("lon", 2),), NSUB, True)
    joined = with_halo(joined, (("lat", 1),), NSUB, False)
    ice_state = joined[:5]
    statics = joined[5:]
    for repeat in range(NSUB):
        ice_state, statics = subcycle(ice_state, statics)
    returned = from_tile(give_back(ice_state, statics))
    back_send = returned[:, local_ids]
    regrouped = lax.all_to_all(back_send, ("lat", "lon"), split_axis=1, concat_axis=1, tiled=True)
    received_back = from_behind(regrouped, "comp", -1)
    ocean_out = received_back[:2] + (1.0 - received_back[2]) * open_stress
    ice_out = from_tile(ice_state[:2])
    return jnp.where(is_ocean, ocean_out, ice_out)[None]


TILE = 8
GROUP = 8
MESH = pl.DeviceIdType.MESH
U, V, MASS, CONC, S1, S2, S12, ACTIVE, PUSH_X, PUSH_Y, CUR_X, CUR_Y, STRENGTH, DRAG = range(14)
SIDES = [(a, b) for b in (-1, 1) for a in (-1, 1, 0)]
ALL_AROUND = [(-1, 0), (1, 0)] + SIDES
ROUNDS = ((U, 8), (CUR_X, 2), (PUSH_X, 2))
KEEP = 1.0 / (1.0 + RELAX)


def tile_loop(tiles, together, body):
    def step(k, carry):
        for j in range(together):
            body(k * together + j)
        return carry
    lax.fori_loop(0, tiles // together, step, 0)


def pieces(values, axis):
    high = values.astype(jnp.bfloat16)
    low = (values - high.astype(jnp.float32)).astype(jnp.bfloat16)
    return jnp.concatenate([high, low], axis=axis)


def dot_rows(twice, values):
    return lax.dot_general(
        twice, pieces(values, 0), (((1,), (0,)), ((), ())), preferred_element_type=jnp.float32
    )


def dot_lanes(twice, values):
    return lax.dot_general(
        twice, pieces(values, 1), (((1,), (1,)), ((), ())), preferred_element_type=jnp.float32
    )


def new_stress(strength, s1, s2, s12, u, v, u_east, v_east, u_up, v_up):
    sxx = u_east - u
    syy = v_up - v
    shear = (u_up - u) + (v_east - v)
    div = sxx + syy
    ten = sxx - syy
    square = div * div + (ten * ten + shear * shear) * (1.0 / ECC2) + DMIN2
    inverse = lax.rsqrt(square)
    visc = strength * inverse
    s1 = s1 * KEEP + visc * (div - square * inverse)
    s2 = s2 * KEEP + visc * ten * (1.0 / ECC2)
    s12 = s12 * KEEP + visc * shear * (0.5 / ECC2)
    return s1, s2, s12


def new_velocity(get, u, v, force_x, force_y):
    mass, cx, cy = get(MASS), get(CUR_X), get(CUR_Y)
    dx, dy = cx - u, cy - v
    square = dx * dx + dy * dy + DRAG_FLOOR
    drag = get(DRAG) * (square * lax.rsqrt(square))
    gain = get(ACTIVE) / (jnp.maximum(mass, MASS_FLOOR) * (1.0 / DTE) + drag)
    inertia = mass * (1.0 / DTE)
    turn = CORIO * mass
    return (
        gain * (inertia * u + force_x + get(PUSH_X) + drag * cx + turn * v),
        gain * (inertia * v + force_y + get(PUSH_Y) + drag * cy - turn * u),
    )


def step_kernel(
    n_lat, n_lon,
    fields, owner_hbm, covered_hbm, land, out,
    surf, open_st, ret, owner, covered, ids, recv, forc, one_hot, back, land_v,
    main, edge, flank, flank_back, flank_vel, ends,
    rows_out0, rows_out1, rows_out2, rows_got0, rows_got1, rows_got2,
    side_out0, side_out1, side_out2, side_got0, side_got1, side_got2,
    load_sem, ids_ssem, ids_rsem, fwd_ssem, fwd_rsem, ret_ssem, ret_rsem,
    early_ssem, early_rsem, mid_rsem, late_rsem, later_ssem,
):
    comp = lax.axis_index("comp")
    lat = lax.axis_index("lat")
    lon = lax.axis_index("lon")
    peers = n_lat * n_lon
    me = lat * n_lon + lon
    count = owner.shape[1]
    per = count // peers
    width = BX
    barrier = pltpu.get_barrier_semaphore()
    rows_out = (rows_out0, rows_out1, rows_out2)
    rows_got = (rows_got0, rows_got1, rows_got2)
    side_out = (side_out0, side_out1, side_out2)
    side_got = (side_got0, side_got1, side_got2)

    def rows_of(peer):
        return pl.ds(pl.multiple_of(peer * per, per), per)

    planes = [(jnp.where(lat < n_lat // 2, n_lat // 2, 0) + j) % n_lat for j in range(n_lat)]
    places = [(lon + i) % n_lon for i in range(n_lon)]

    def each_peer(body, part=None):
        chosen = {None: planes, 0: planes[:n_lat // 2], 1: planes[n_lat // 2:]}[part]
        for plane in chosen:
            for place in places:
                body(plane * n_lon + place, plane, place)

    def signal_peers(kind):
        each_peer(
            lambda p, plane, place: pl.semaphore_signal(
                barrier, inc=1, device_id=(kind, plane, place), device_id_type=MESH
            )
        )

    def send_rows(kind, src, lo, num, dst, dlo, ssem, rsem, part=None):
        def body(p, plane, place):
            pltpu.make_async_remote_copy(
                src_ref=src.at[pl.ds(lo, num), rows_of(p), :],
                dst_ref=dst.at[pl.ds(dlo, num), rows_of(me), :],
                send_sem=ssem, recv_sem=rsem,
                device_id=(kind, plane, place), device_id_type=MESH,
            ).start()
        each_peer(body, part)

    def wait_bytes(ref, sem):
        pltpu.make_async_copy(ref, ref, sem).wait()

    def wait_tiles(num, sem):
        wait_bytes(main.at[0, 0, pl.ds(0, num * TILE), :], sem)

    @pl.when(comp == 0)
    def _ocean():
        signal_peers(1)
        names = pltpu.make_async_copy(owner_hbm, owner, load_sem.at[3])
        raw = pltpu.make_async_copy(fields.at[0, pl.ds(2, 4)], surf.at[pl.ds(2, 4)], load_sem.at[0])
        wind = pltpu.make_async_copy(fields.at[0, pl.ds(0, 2)], surf.at[pl.ds(0, 2)], load_sem.at[1])
        rho = pltpu.make_async_copy(fields.at[0, pl.ds(6, 1)], surf.at[pl.ds(6, 1)], load_sem.at[2])
        names.start()
        raw.start()
        wind.start()
        rho.start()
        names.wait()
        with jax.named_scope("o_barrier"):
            pl.semaphore_wait(barrier, peers)

        def ids_out(p, plane, place):
            pltpu.make_async_remote_copy(
                src_ref=owner, dst_ref=ids.at[me], send_sem=ids_ssem, recv_sem=ids_rsem,
                device_id=(1, plane, place), device_id_type=MESH,
            ).start()
        with jax.named_scope("o_send4"):
            each_peer(ids_out)
            raw.wait()
            send_rows(1, surf, 2, 4, recv, 2, fwd_ssem.at[0], fwd_rsem.at[0], 0)
            wind.wait()
            rho.wait()

        def stress(t):
            r = pl.ds(pl.multiple_of(t * TILE, TILE), TILE)
            wx, wy, density = surf[0, r, :], surf[1, r, :], surf[6, r, :]
            scale = density * CD_ICE * jnp.sqrt(wx * wx + wy * wy + 1.0)
            forc[0, r, :] = scale * wx
            forc[1, r, :] = scale * wy

        with jax.named_scope("o_stress"):
            tile_loop(count // TILE, 4, stress)
            send_rows(1, forc, 0, 2, recv, 0, fwd_ssem.at[1], fwd_rsem.at[1], 0)
            send_rows(1, surf, 2, 4, recv, 2, fwd_ssem.at[0], fwd_rsem.at[0], 1)
            send_rows(1, forc, 0, 2, recv, 0, fwd_ssem.at[1], fwd_rsem.at[1], 1)

        def open_water(t):
            r = pl.ds(pl.multiple_of(t * TILE, TILE), TILE)
            density = surf[6, r, :]
            rel_x = surf[0, r, :] - surf[2, r, :]
            rel_y = surf[1, r, :] - surf[3, r, :]
            speed = jnp.sqrt(rel_x * rel_x + rel_y * rel_y + 1.0)
            scale = density * (0.1 + 0.05 * speed) * speed
            open_st[0, r, :] = scale * rel_x
            open_st[1, r, :] = scale * rel_y

        tile_loop(count // TILE, 2, open_water)
        with jax.named_scope("o_waitret1"):
            wait_bytes(ret.at[pl.ds(2, 1)], ret_rsem.at[0])

        def water(t):
            r = pl.ds(pl.multiple_of(t * TILE, TILE), TILE)
            share = 1.0 - ret[2, r, :]
            for c in range(2):
                open_st[c, r, :] = share * open_st[c, r, :]

        tile_loop(count // TILE, 4, water)
        with jax.named_scope("o_waitret2"):
            wait_bytes(ret.at[pl.ds(0, 2)], ret_rsem.at[1])

        def finish(t):
            r = pl.ds(pl.multiple_of(t * TILE, TILE), TILE)
            for c in range(2):
                out[0, c, r, :] = ret[c, r, :] + open_st[c, r, :]

        tile_loop(count // TILE, 4, finish)
        wait_bytes(ids, ids_ssem)
        wait_bytes(surf.at[pl.ds(2, 4)], fwd_ssem.at[0])
        wait_bytes(forc.at[pl.ds(0, 2)], fwd_ssem.at[1])

    @pl.when(comp == 1)
    def _ice():
        def inside(a):
            if a == 0:
                return lat >= 0
            return lat + a >= 0 if a < 0 else lat + a < n_lat

        def around(a, b):
            return (1, lat + a, (lon + b + n_lon) % n_lon)

        signal_peers(0)
        for a, b in ALL_AROUND:
            @pl.when(inside(a))
            def _():
                pl.semaphore_signal(barrier, inc=1, device_id=around(a, b), device_id_type=MESH)
        loads = [
            pltpu.make_async_copy(
                fields.at[0, :, :, pl.ds(y * width, width)], main.at[pl.ds(0, 7), y], load_sem.at[y]
            )
            for y in range(2)
        ]
        loads.append(pltpu.make_async_copy(land, land_v, load_sem.at[2]))
        loads.append(pltpu.make_async_copy(covered_hbm, covered, load_sem.at[3]))
        for load in loads:
            load.start()

        tiles = count // TILE
        top, bottom = pl.ds(0, TILE), pl.ds(count - TILE, TILE)
        zero_tile = jnp.zeros((TILE, width), jnp.float32)
        for wall, which in ((lat == 0, 0), (lat == n_lat - 1, 1)):
            @pl.when(wall)
            def _():
                for e in range(3):
                    for k in range(rows_got[e].shape[1]):
                        rows_got[e][which, k] = zero_tile
                    for k in range(2):
                        side_got[e][2 * which, k] = zero_tile

        def clear(t):
            r = pl.ds(pl.multiple_of(t * TILE, TILE), TILE)
            for c in range(2):
                for y in range(2):
                    flank_vel[c, y, r, :] = zero_tile
            flank_back[r, :] = zero_tile

        tile_loop(tiles, 2, clear)
        for load in loads:
            load.wait()
        diag = lax.broadcasted_iota(jnp.int32, (count, count), 0) == lax.broadcasted_iota(
            jnp.int32, (count, count), 1
        )
        wet = jnp.sum(
            jnp.where(diag, covered[...].astype(jnp.float32), 0.0), axis=1, keepdims=True
        )
        sea = wet * (1 - land_v[...]).astype(jnp.float32)
        for y in range(2):
            main[ACTIVE, y] = sea[:, y * width:(y + 1) * width]

        lane = lax.broadcasted_iota(jnp.int32, (TILE, width), 1)
        sub = lax.broadcasted_iota(jnp.int32, (TILE, width), 0)
        pick_row = lax.broadcasted_iota(jnp.int32, (2 * TILE, width), 0)
        pick_col = lax.broadcasted_iota(jnp.int32, (2 * TILE, width), 1)
        picked = jnp.where(pick_row < TILE, pick_row, pick_row + (width - 2 * TILE)) == pick_col
        picker = jnp.where(picked, 1.0, 0.0).astype(jnp.bfloat16)
        picker = jnp.concatenate([picker] * 2, axis=1)

        def pack_rows(e):
            lo, num = ROUNDS[e]
            for k in range(num // 2):
                ups, downs = zero_tile, zero_tile
                for i in range(4):
                    c, y = lo + 2 * k + i // 2, i % 2
                    head, foot = main[c, y, top, :], main[c, y, bottom, :]
                    here = (sub >= 2 * i) & (sub < 2 * i + 2)
                    ups = jnp.where(here, pltpu.roll(head, 2 * i, 0) if i else head, ups)
                    downs = jnp.where(here, pltpu.roll(foot, (2 * i + 2) % TILE, 0) if i < 3 else foot, downs)
                rows_out[e][0, k] = ups
                rows_out[e][1, k] = downs

        def pack_sides(e):
            lo, num = ROUNDS[e]
            west, east = zero_tile, zero_tile
            for i in range(2 * num):
                c, y = lo + i // 2, i % 2
                ends = jnp.where(sub < NSUB, main[c, y, top, :], main[c, y, bottom, :])
                slot = i * NSUB
                mine = (lane >= slot) & (lane < slot + NSUB)
                west = jnp.where(mine, pltpu.roll(ends, slot, 1) if slot else ends, west)
                east = jnp.where(mine, pltpu.roll(ends, (slot + NSUB) % width, 1), east)
            side_out[e][0] = west
            side_out[e][1] = east

        def pack_flank(e):
            lo, num = ROUNDS[e]
            for c in range(lo, lo + num):
                for y in range(2):
                    across = dot_lanes(picker, main[c, y])
                    flank[c, y, pl.ds(TILE, TILE), :] = across[:TILE]
                    flank[c, y, pl.ds(2 * TILE, TILE), :] = across[TILE:]

        def push_on(e, a, b, src, dst, lane_of_sem, recv_lane):
            sems = (early_rsem, mid_rsem, late_rsem)[e]
            sent = early_ssem if e == 0 else later_ssem

            @pl.when(inside(a))
            def _():
                pltpu.make_async_remote_copy(
                    src_ref=src, dst_ref=dst,
                    send_sem=sent.at[lane_of_sem], recv_sem=sems.at[recv_lane],
                    device_id=around(a, b), device_id_type=MESH,
                ).start()

        def send_ends(e):
            for a in (-1, 1):
                k = 1 if a > 0 else 0
                push_on(e, a, 0, rows_out[e].at[k], rows_got[e].at[1 - k], k, 1 - k)

        def send_sides(e):
            for a, b in SIDES:
                k = 1 if b > 0 else 0
                group = {0: 2, -1: 0, 1: 1}[a]
                land_in = {0: 2, -1: 1, 1: 0}[a] + (4 if e == 2 and a != 0 else 0)
                push_on(e, a, b, side_out[e].at[k], side_got[e].at[1 - a, 1 - k], group, land_in)

        def send_flank(e):
            lo, num = ROUNDS[e]
            for b in (-1, 1):
                src, dst = (2 * TILE, 0) if b > 0 else (TILE, 3 * TILE)
                push_on(
                    e, 0, b,
                    flank.at[pl.ds(lo, num), :, pl.ds(src, TILE), :],
                    flank.at[pl.ds(lo, num), :, pl.ds(dst, TILE), :], 3, 3,
                )

        def when_inside(a, num, sem):
            @pl.when(inside(a))
            def _():
                wait_tiles(num, sem)

        def unpack_rows(e):
            lo, num = ROUNDS[e]
            got = rows_got[e]
            for k in range(num // 2):
                for i in range(4):
                    c, y = lo + 2 * k + i // 2, i % 2
                    north = pltpu.roll(got[0, k], (TILE - 2 * i) % TILE, 0) if i else got[0, k]
                    south = pltpu.roll(got[1, k], TILE - 2 - 2 * i, 0) if i < 3 else got[1, k]
                    head, foot = main[c, y, top, :], main[c, y, bottom, :]
                    edge[c, 0, y, :, pl.ds(0, width)] = jnp.where(
                        sub < 2, north, pltpu.roll(head, 2, 0)
                    )
                    edge[c, 1, y, :, pl.ds(0, width)] = jnp.where(
                        sub >= TILE - 2, south, pltpu.roll(foot, TILE - 2, 0)
                    )

        def unpack_sides(e):
            lo, num = ROUNDS[e]
            side = side_got[e]
            ends = []
            for k in range(2):
                far, near = side[0, k], side[1, k]
                ends.append(pltpu.roll(jnp.where(sub >= TILE - 2, far, near), 2, 0))
            for k in range(2):
                far, near = side[2, k], side[1, k]
                ends.append(pltpu.roll(jnp.where(sub < 2, far, near), TILE - 2, 0))
            for i in range(2 * num):
                c, y = lo + i // 2, i % 2
                slot = i * NSUB
                for strip in range(2):
                    from_west, from_east = ends[2 * strip], ends[2 * strip + 1]
                    from_east = pltpu.roll(from_east, width - slot, 1) if slot else from_east
                    from_west = pltpu.roll(from_west, width - NSUB - slot, 1)
                    edge[c, strip, y, :, pl.ds(width, width)] = jnp.where(
                        lane < NSUB, from_east, jnp.where(lane >= width - NSUB, from_west, 0.0)
                    )

        def derive(load, store):
            conc, act = load(CONC), load(ACTIVE)
            store(STRENGTH, (RELAX * KEEP) * load(MASS) * jnp.exp(CSTAR * (conc - 1.0)) * act)
            store(DRAG, CW * conc * act)

        def derive_main(t):
            r = pl.ds(pl.multiple_of(t * TILE, TILE), TILE)
            for y in range(2):
                def store(c, x):
                    main[c, y, r, :] = x
                derive(lambda c: main[c, y, r, :], store)

        def derive_edges():
            for y in range(2):
                for strip in range(2):
                    def store(c, x):
                        edge[c, strip, y] = x
                    derive(lambda c: edge[c, strip, y], store)

                def store(c, x):
                    flank[c, y] = x
                derive(lambda c: flank[c, y], store)

        def sweep_main(g, stress, velocity):
            spots = [
                pl.ds(pl.multiple_of((g * GROUP + j) * TILE, TILE), TILE) for j in range(GROUP)
            ]
            behind = pl.ds(pl.multiple_of(jnp.maximum(g * GROUP - 1, 0) * TILE, TILE), TILE)
            ahead = pl.ds(
                pl.multiple_of(jnp.minimum(g * GROUP + GROUP, tiles - 1) * TILE, TILE), TILE
            )
            vels = [[(main[U, y, r, :], main[V, y, r, :]) for y in range(2)] for r in spots]
            stresses = []
            if stress:
                follow = (main[U, 0, ahead, :], main[V, 0, ahead, :])
            for j, r in enumerate(spots):
                old = [tuple(main[c, y, r, :] for c in (S1, S2, S12)) for y in range(2)]
                if not stress:
                    stresses.append(old)
                    continue
                beyond = vels[j + 1][0] if j + 1 < GROUP else follow
                row = []
                for y in range(2):
                    u, v = vels[j][y]
                    if y == 0:
                        u_up, v_up = vels[j][1]
                    else:
                        u_up, v_up = (
                            pltpu.roll(jnp.where(sub == 0, after, x), TILE - 1, 0)
                            for x, after in zip(vels[j][0], beyond)
                        )
                    fresh = new_stress(
                        main[STRENGTH, y, r, :], *old[y], u, v,
                        pltpu.roll(u, width - 1, 1), pltpu.roll(v, width - 1, 1), u_up, v_up,
                    )
                    for c, x in zip((S1, S2, S12), fresh):
                        main[c, y, r, :] = x
                    row.append(fresh)
                stresses.append(row)
            if not velocity:
                return
            yy_before = 0.5 * (main[S1, 1, behind, :] - main[S2, 1, behind, :])
            cross_before = main[S12, 1, behind, :]
            for j, r in enumerate(spots):
                xx = [0.5 * (s1 + s2) for s1, s2, _ in stresses[j]]
                yy = [0.5 * (s1 - s2) for s1, s2, _ in stresses[j]]
                cross = [s12 for _, _, s12 in stresses[j]]
                yy_down, cross_down = (
                    [pltpu.roll(jnp.where(sub == TILE - 1, before, x[1]), 1, 0), x[0]]
                    for x, before in ((yy, yy_before), (cross, cross_before))
                )
                yy_before, cross_before = yy[1], cross[1]
                for y in range(2):
                    force_x = xx[y] - pltpu.roll(xx[y], 1, 1) + (cross[y] - cross_down[y])
                    force_y = cross[y] - pltpu.roll(cross[y], 1, 1) + (yy[y] - yy_down[y])
                    u, v = new_velocity(lambda c: main[c, y, r, :], *vels[j][y], force_x, force_y)
                    main[U, y, r, :] = u
                    main[V, y, r, :] = v

        def sweep_edge(stress, velocity):
            lanes = 2 * width

            for strip in range(2):
                vels = [(edge[U, strip, y], edge[V, strip, y]) for y in range(2)]
                fresh = [tuple(edge[c, strip, y] for c in (S1, S2, S12)) for y in range(2)]
                if stress:
                    ups = [vels[1], tuple(pltpu.roll(x, TILE - 1, 0) for x in vels[0])]
                    for y in range(2):
                        east = [pltpu.roll(x, lanes - 1, 1) for x in vels[y]]
                        fresh[y] = new_stress(
                            edge[STRENGTH, strip, y], *fresh[y], *vels[y], *east, *ups[y]
                        )
                        for c, x in zip((S1, S2, S12), fresh[y]):
                            edge[c, strip, y] = x
                if not velocity:
                    continue
                xx = [0.5 * (s1 + s2) for s1, s2, _ in fresh]
                yy = [0.5 * (s1 - s2) for s1, s2, _ in fresh]
                cross = [s12 for _, _, s12 in fresh]
                yy_down, cross_down = ([pltpu.roll(x[1], 1, 0), x[0]] for x in (yy, cross))
                for y in range(2):
                    force_x = xx[y] - pltpu.roll(xx[y], 1, 1) + (cross[y] - cross_down[y])
                    force_y = cross[y] - pltpu.roll(cross[y], 1, 1) + (yy[y] - yy_down[y])
                    u, v = new_velocity(lambda c: edge[c, strip, y], *vels[y], force_x, force_y)
                    edge[U, strip, y] = u
                    edge[V, strip, y] = v

        def sweep_flank(stress, velocity):
            spots = [pl.ds(j * TILE, TILE) for j in range(4)]
            vels = [[(flank[U, y, r, :], flank[V, y, r, :]) for y in range(2)] for r in spots]
            fresh = [
                [tuple(flank[c, y, r, :] for c in (S1, S2, S12)) for y in range(2)] for r in spots
            ]
            if stress:
                for j, r in enumerate(spots):
                    for y in range(2):
                        after = vels[min(j + 1, 3)][y]
                        east = [
                            pltpu.roll(jnp.where(sub == 0, b, x), TILE - 1, 0)
                            for x, b in zip(vels[j][y], after)
                        ]
                        ups = vels[j][1] if y == 0 else [
                            pltpu.roll(x, width - 1, 1) for x in vels[j][0]
                        ]
                        fresh[j][y] = new_stress(
                            flank[STRENGTH, y, r, :], *fresh[j][y], *vels[j][y], *east, *ups
                        )
                        for c, x in zip((S1, S2, S12), fresh[j][y]):
                            flank[c, y, r, :] = x
            if not velocity:
                return
            xx = [[0.5 * (s1 + s2) for s1, s2, _ in row] for row in fresh]
            yy = [[0.5 * (s1 - s2) for s1, s2, _ in row] for row in fresh]
            cross = [[s12 for _, _, s12 in row] for row in fresh]

            def westward(x, j, y):
                before = x[max(j - 1, 0)][y]
                return pltpu.roll(jnp.where(sub == TILE - 1, before, x[j][y]), 1, 0)

            def downward(x, j, y):
                return x[j][0] if y == 1 else pltpu.roll(x[j][1], 1, 1)

            for j, r in enumerate(spots):
                for y in range(2):
                    force_x = xx[j][y] - westward(xx, j, y) + (cross[j][y] - downward(cross, j, y))
                    force_y = cross[j][y] - westward(cross, j, y) + (yy[j][y] - downward(yy, j, y))
                    u, v = new_velocity(lambda c: flank[c, y, r, :], *vels[j][y], force_x, force_y)
                    flank[U, y, r, :] = u
                    flank[V, y, r, :] = v

        walls = jnp.where(lat == 0, 3, 0) + jnp.where(lat == n_lat - 1, 3, 0)
        with jax.named_scope("i_barrier"):
            pl.semaphore_wait(barrier, peers + 8 - walls)
        with jax.named_scope("i_pack0"):
            pack_rows(0)
            pack_sides(0)
            send_ends(0)
            send_sides(0)
            pack_flank(0)
            send_flank(0)
        tile_loop(tiles, 2, derive_main)

        with jax.named_scope("i_waitids"):
            wait_bytes(ids, ids_rsem)
        wanted = me * per
        row_lane = lax.broadcasted_iota(jnp.int32, (per, count), 1)
        row_sub = lax.broadcasted_iota(jnp.int32, (per, count), 0)
        mine = row_lane == row_sub + wanted
        blocks = lax.broadcasted_iota(jnp.int32, (per, count), 1).astype(jnp.float32)
        base = (me * count).astype(jnp.float32)
        for p in range(peers):
            owned = jnp.broadcast_to(ids[p], (per, count)).astype(jnp.float32)
            local = jnp.sum(jnp.where(mine, owned, 0.0), axis=1, keepdims=True) - base
            one_hot[pl.ds(p * per, per), :] = jnp.where(local == blocks, 1.0, 0.0)

        with jax.named_scope("i_waithalo0"):
            for sems in (early_ssem, early_rsem):
                when_inside(-1, 6, sems.at[0])
                when_inside(1, 6, sems.at[1])
                wait_tiles(2, sems.at[2])
                wait_bytes(main.at[0], sems.at[3])
        with jax.named_scope("i_unpack0"):
            unpack_rows(0)
            unpack_sides(0)
            derive_edges()
        groups = tiles // GROUP
        with jax.named_scope("i_stress"):
            tile_loop(groups, 1, lambda g: sweep_main(g, True, False))
            sweep_edge(True, False)
            sweep_flank(True, False)
        by_slot = one_hot[...]
        to_slots = jnp.concatenate([by_slot.astype(jnp.bfloat16)] * 2, axis=1)
        to_ends = jnp.concatenate([by_slot[:, :TILE], by_slot[:, count - TILE:]] * 2, axis=1)
        to_ends = to_ends.astype(jnp.bfloat16)
        by_block = by_slot.T.astype(jnp.bfloat16)
        to_blocks = jnp.concatenate([by_block] * 2, axis=1)
        columns = jnp.concatenate([by_block] * 2, axis=0)

        with jax.named_scope("i_waitf4"):
            wait_bytes(recv.at[pl.ds(2, 4)], fwd_rsem.at[0])
        for c in range(2):
            both = dot_rows(to_blocks, recv[2 + c])
            for y in range(2):
                main[CUR_X + c, y] = both[:, y * width:(y + 1) * width]
        with jax.named_scope("i_packmid"):
            pack_rows(1)
            pack_sides(1)
            send_ends(1)
            send_sides(1)
            pack_flank(1)
            send_flank(1)
        for c in range(2):
            both = dot_rows(to_blocks, recv[4 + c])
            for y in range(2):
                main[PUSH_X + c, y] = main[MASS, y] * both[:, y * width:(y + 1) * width]
        for y in range(2):
            share = main[CONC, y] * main[ACTIVE, y]
            back[2, :, pl.ds(y * width, width)] = dot_rows(to_slots, share)

        with jax.named_scope("i_waitf2"):
            wait_bytes(recv.at[pl.ds(0, 2)], fwd_rsem.at[1])
        with jax.named_scope("i_push"):
            for c in range(2):
                both = dot_rows(to_blocks, recv[c])
                for y in range(2):
                    main[PUSH_X + c, y] = main[ACTIVE, y] * (
                        main[CONC, y] * both[:, y * width:(y + 1) * width] - main[PUSH_X + c, y]
                    )
        with jax.named_scope("i_packlate"):
            pack_rows(2)
            send_ends(2)
            pack_sides(2)
            send_sides(2)
            pack_flank(2)
            send_flank(2)

        def leave(get, u, v):
            dx, dy = u - get(CUR_X), v - get(CUR_Y)
            drag = get(DRAG) * jnp.sqrt(dx * dx + dy * dy + DRAG_FLOOR)
            return drag * dx, drag * dy

        outer = (lane < NSUB) | (lane >= width - NSUB)

        with jax.named_scope("i_vel1"):
            tile_loop(groups, 1, lambda g: sweep_main(g, False, True))
        with jax.named_scope("i_sweeps"):
            tile_loop((NSUB - 1) * groups, 1, lambda k: sweep_main(k % groups, True, True))
        send_rows(0, back, 2, 1, ret, 2, ret_ssem.at[0], ret_rsem.at[0])

        def returned(t):
            r = pl.ds(pl.multiple_of(t * TILE, TILE), TILE)
            block = sub + t * TILE
            theirs = outer | (block < 2) | (block >= count - 2)
            for y in range(2):
                half = pl.ds(y * width, width)
                u, v = main[U, y, r, :], main[V, y, r, :]
                gone = leave(lambda c: main[c, y, r, :], u, v)
                for c in range(2):
                    forc[c, r, half] = jnp.where(theirs, 0.0, gone[c])

        with jax.named_scope("i_back"):
            tile_loop(tiles, 4, returned)
            for c in range(2):
                back[c] = dot_rows(to_slots, forc[c])
        with jax.named_scope("i_waitmid"):
            when_inside(1, 3, mid_rsem.at[1])
            when_inside(-1, 3, mid_rsem.at[0])
            wait_tiles(2, mid_rsem.at[2])
            wait_tiles(8, mid_rsem.at[3])
        unpack_rows(1)
        unpack_sides(1)
        with jax.named_scope("i_waitrows"):
            when_inside(-1, 1, late_rsem.at[0])
            when_inside(1, 1, late_rsem.at[1])
        unpack_rows(2)
        with jax.named_scope("i_waitlate"):
            wait_tiles(2, late_rsem.at[2])
            when_inside(-1, 2, late_rsem.at[4])
            when_inside(1, 2, late_rsem.at[5])
            wait_tiles(8, late_rsem.at[3])

        def sweep_strips(stress, velocity):
            sweep_flank(stress, velocity)
            sweep_edge(stress, velocity)

        with jax.named_scope("i_edge"):
            unpack_sides(2)
            sweep_strips(False, True)
            tile_loop(NSUB - 1, 1, lambda k: sweep_strips(True, True))

        with jax.named_scope("i_fix"):
            for y in range(2):
                for j, far in ((1, 0), (2, count - TILE)):
                    r = pl.ds(j * TILE, TILE)
                    held = (lane >= 2) & (lane < count - 2)
                    held = held & ((sub < NSUB) if j == 1 else (sub >= TILE - NSUB))
                    u, v = flank[U, y, r, :], flank[V, y, r, :]
                    gone = leave(lambda c: flank[c, y, r, :], u, v)
                    for c in range(2):
                        slot = (c * 2 + y) * 2 * TILE + (TILE if j == 1 else 0)
                        flank_back[pl.ds(slot, TILE), :] = jnp.where(held, gone[c], 0.0)
                        flank_vel[c, y, pl.ds(far, TILE), :] = jnp.where(held, (u, v)[c], 0.0)
                for strip in range(2):
                    def get(c):
                        return edge[c, strip, y, :, pl.ds(0, width)]
                    gone = leave(get, get(U), get(V))
                    held = (sub < 2) if strip == 0 else (sub >= TILE - 2)
                    for c in range(2):
                        moved = pltpu.roll(gone[c], TILE - 2 if strip == 0 else 2, 0)
                        ends[c, pl.ds(strip * TILE, TILE), pl.ds(y * width, width)] = jnp.where(
                            held, moved, 0.0
                        )
            across = lax.dot_general(
                pieces(flank_back[...], 1), columns,
                (((1,), (0,)), ((), ())), preferred_element_type=jnp.float32,
            ).T
            for c in range(2):
                rest = dot_rows(to_ends, ends[c])
                for y in range(2):
                    slot = (c * 2 + y) * 2 * TILE
                    for t in range(tiles):
                        r, half = pl.ds(t * TILE, TILE), pl.ds(y * width, width)
                        moved = pltpu.roll(across[t * TILE:(t + 1) * TILE], width - TILE - slot, 1)
                        back[c, r, half] += jnp.where(outer, moved, 0.0) + (
                            rest[t * TILE:(t + 1) * TILE, y * width:(y + 1) * width]
                        )
            send_rows(0, back, 0, 2, ret, 0, ret_ssem.at[1], ret_rsem.at[1])

        same = jnp.where(diag, 1.0, 0.0).astype(jnp.bfloat16)
        same = jnp.concatenate([same] * 2, axis=1)
        for y in range(2):
            for c in range(2):
                half = pl.ds(y * width, width)
                for strip, r in ((0, top), (1, bottom)):
                    end = pltpu.roll(
                        edge[c, strip, y, :, pl.ds(0, width)], TILE - 2 if strip == 0 else 2, 0
                    )
                    held = (sub < 2) if strip == 0 else (sub >= TILE - 2)
                    main[c, y, r, :] = jnp.where(held, end, main[c, y, r, :])
                other = dot_lanes(same, flank_vel[c, y])
                row = lax.broadcasted_iota(jnp.int32, (count, width), 0)
                column = lax.broadcasted_iota(jnp.int32, (count, width), 1)
                theirs = (row >= 2) & (row < count - 2)
                theirs = theirs & ((column < NSUB) | (column >= width - NSUB))
                out[0, c, :, half] = jnp.where(theirs, other, main[c, y])
        wait_bytes(back.at[pl.ds(2, 1)], ret_ssem.at[0])
        wait_bytes(back.at[pl.ds(0, 2)], ret_ssem.at[1])
        when_inside(-1, 6, later_ssem.at[0])
        when_inside(1, 6, later_ssem.at[1])
        wait_tiles(4, later_ssem.at[2])
        wait_tiles(16, later_ssem.at[3])


def per_device_kernel(n_lat, n_lon, fields, block_owner, ice_covered, land_mask):
    count, cells = land_mask.shape
    peers = n_lat * n_lon
    f32 = jnp.float32
    anywhere = pl.BlockSpec(memory_space=pl.ANY)
    dma = pltpu.SemaphoreType.DMA
    halos = [pltpu.VMEM((2, num // 2, TILE, BX), f32) for _, num in ROUNDS] * 2
    sides = [pltpu.VMEM((2, TILE, BX), f32) for _ in ROUNDS]
    sides += [pltpu.VMEM((3, 2, TILE, BX), f32) for _ in ROUNDS]
    return pl.pallas_call(
        functools.partial(step_kernel, n_lat, n_lon),
        out_shape=pltpu.VMEM((1, 2, count, cells), f32),
        in_specs=[anywhere, anywhere, anywhere, anywhere],
        out_specs=pl.BlockSpec(memory_space=pltpu.VMEM),
        scratch_shapes=[
            pltpu.VMEM((7, count, cells), f32),
            pltpu.VMEM((2, count, cells), f32),
            pltpu.VMEM((3, count, cells), f32),
            pltpu.VMEM((1, count), jnp.int32),
            pltpu.VMEM((1, count), jnp.int32),
            pltpu.VMEM((peers, 1, count), jnp.int32),
            pltpu.VMEM((6, count, cells), f32),
            pltpu.VMEM((2, count, cells), f32),
            pltpu.VMEM((count, count), f32),
            pltpu.VMEM((3, count, cells), f32),
            pltpu.VMEM((count, cells), jnp.int32),
            pltpu.VMEM((14, 2, count, BX), f32),
            pltpu.VMEM((14, 2, 2, TILE, 2 * BX), f32),
            pltpu.VMEM((14, 2, 4 * TILE, BX), f32),
            pltpu.VMEM((BX, count), f32),
            pltpu.VMEM((2, 2, BX, count), f32),
            pltpu.VMEM((2, 2 * TILE, cells), f32),
            *halos, *sides,
            dma((4,)), dma, dma, dma((2,)), dma((2,)), dma((2,)), dma((2,)),
            dma((4,)), dma((4,)), dma((4,)), dma((6,)), dma((4,)),
        ],
        compiler_params=pltpu.CompilerParams(
            collective_id=0, has_side_effects=True, vmem_limit_bytes=63 * 1024 * 1024
        ),
    )(fields, block_owner.reshape(1, count), ice_covered.reshape(1, count), land_mask)


def solution(mesh):
    placed = (
        P("comp", None, ("lat", "lon"), None),
        P(("lat", "lon")),
        P(("lat", "lon")),
        P(("lat", "lon"), None),
    )
    n_lat, n_lon = mesh.shape["lat"], mesh.shape["lon"]

    def body(fields, block_owner, ice_covered, land_mask):
        count = block_owner.shape[0]
        whole_tiles = count % (n_lat * n_lon * TILE) == 0 and count == BX
        if whole_tiles and n_lon > 2:
            return per_device_kernel(n_lat, n_lon, fields, block_owner, ice_covered, land_mask)
        return per_device(fields, block_owner, ice_covered, land_mask)

    return jax.shard_map(
        body,
        mesh=mesh,
        in_specs=placed,
        out_specs=P("comp", None, ("lat", "lon"), None),
        check_vma=False,
    )
```

```python
import functools

import jax
import jax.numpy as jnp
from jax import lax
from jax.experimental import pallas as pl
from jax.experimental.pallas import tpu as pltpu
from jax.sharding import PartitionSpec as P

GX = 1
BY = 2
BX = 128
NSUB = 4


CD_ICE = 0.1
CW = 1.5
CSTAR = 2.0
ECC2 = 4.0
DMIN2 = 0.25
RELAX = 0.5
DTE = 0.5
CORIO = 0.3
MASS_FLOOR = 0.5
DRAG_FLOOR = 0.1


def from_behind(x, axis, by):
    size = lax.axis_size(axis)
    pairs = [(i, i + by) for i in range(size) if 0 <= i + by < size]
    return lax.ppermute(x, axis, pairs)


def with_halo(x, sides, width, wrap):
    for axis, dim in sides:
        size, length = (lax.axis_size(axis), x.shape[dim])
        up = [(i, (i + 1) % size) for i in range(size if wrap else size - 1)]
        down = [(j, i) for i, j in up]
        last = lax.slice_in_dim(x, length - width, length, axis=dim)
        first = lax.slice_in_dim(x, 0, width, axis=dim)
        before = lax.ppermute(last, axis, up)
        after = lax.ppermute(first, axis, down)
        x = jnp.concatenate([before, x, after], axis=dim)
    return x


def air_stress(ocean):
    wind_x, wind_y, current_x, current_y, tilt_x, tilt_y, density = ocean
    speed_ice = jnp.sqrt(wind_x * wind_x + wind_y * wind_y + 1.0)
    scale_ice = density * CD_ICE * speed_ice
    rel_x = wind_x - current_x
    rel_y = wind_y - current_y
    speed_open = jnp.sqrt(rel_x * rel_x + rel_y * rel_y + 1.0)
    scale_open = density * (0.1 + 0.05 * speed_open) * speed_open
    outbound = jnp.stack(
        [scale_ice * wind_x, scale_ice * wind_y, current_x, current_y, tilt_x, tilt_y]
    )
    open_stress = jnp.stack([scale_open * rel_x, scale_open * rel_y])
    return (outbound, open_stress)


def prepare(ice_tile, forcing, active):
    ice_mass = ice_tile[2]
    concentration = ice_tile[3]
    strength = ice_mass * jnp.exp(CSTAR * (concentration - 1.0)) * active
    drag_base = CW * concentration * active
    push_x = active * (concentration * forcing[0] - ice_mass * forcing[4])
    push_y = active * (concentration * forcing[1] - ice_mass * forcing[5])
    return jnp.stack(
        [strength, ice_mass, drag_base, push_x, push_y, forcing[2], forcing[3], active]
    )


def subcycle(ice_state, statics):
    east_vel, north_vel, stress_one, stress_two, stress_three = ice_state
    strength = statics[0]
    east_base = east_vel[:-1, :-1]
    north_base = north_vel[:-1, :-1]
    strain_xx = east_vel[:-1, 1:] - east_base
    strain_yy = north_vel[1:, :-1] - north_base
    shear = east_vel[1:, :-1] - east_base + (north_vel[:-1, 1:] - north_base)
    divergence = strain_xx + strain_yy
    tension = strain_xx - strain_yy
    delta_norm = jnp.sqrt(
        divergence * divergence + (tension * tension + shear * shear) / ECC2 + DMIN2
    )
    viscosity = strength[:-1, :-1] / delta_norm
    stress_sum = (stress_one[:-1, :-1] + RELAX * viscosity * (divergence - delta_norm)) / (
        1.0 + RELAX
    )
    stress_diff = (stress_two[:-1, :-1] + RELAX * viscosity * tension / ECC2) / (1.0 + RELAX)
    stress_shear = (stress_three[:-1, :-1] + RELAX * viscosity * shear / (2.0 * ECC2)) / (
        1.0 + RELAX
    )
    stress_xx = 0.5 * (stress_sum + stress_diff)
    stress_yy = 0.5 * (stress_sum - stress_diff)
    force_x = (
        stress_xx[1:, 1:] - stress_xx[1:, :-1] + (stress_shear[1:, 1:] - stress_shear[:-1, 1:])
    )
    force_y = (
        stress_shear[1:, 1:] - stress_shear[1:, :-1] + (stress_yy[1:, 1:] - stress_yy[:-1, 1:])
    )
    trimmed = statics[:, 1:-1, 1:-1]
    strength, ice_mass, drag_base, push_x, push_y, current_x, current_y, active = trimmed
    east_old = east_vel[1:-1, 1:-1]
    north_old = north_vel[1:-1, 1:-1]
    diff_x = current_x - east_old
    diff_y = current_y - north_old
    drag_coef = drag_base * jnp.sqrt(diff_x * diff_x + diff_y * diff_y + DRAG_FLOOR)
    denominator = jnp.maximum(ice_mass, MASS_FLOOR) / DTE + drag_coef
    east_new = (
        active
        * (
            ice_mass / DTE * east_old
            + force_x
            + push_x
            + drag_coef * current_x
            + CORIO * ice_mass * north_old
        )
        / denominator
    )
    north_new = (
        active
        * (
            ice_mass / DTE * north_old
            + force_y
            + push_y
            + drag_coef * current_y
            - CORIO * ice_mass * east_old
        )
        / denominator
    )
    new_state = jnp.stack(
        [east_new, north_new, stress_sum[1:, 1:], stress_diff[1:, 1:], stress_shear[1:, 1:]]
    )
    return (new_state, trimmed)


def give_back(ice_state, statics):
    east_vel = ice_state[0]
    north_vel = ice_state[1]
    drag_base = statics[2]
    current_x = statics[5]
    current_y = statics[6]
    diff_x = east_vel - current_x
    diff_y = north_vel - current_y
    factor = drag_base * jnp.sqrt(diff_x * diff_x + diff_y * diff_y + DRAG_FLOOR)
    return jnp.stack([factor * diff_x, factor * diff_y, drag_base / CW])


def to_tile(blocks):
    channels, count, cells = blocks.shape
    arranged = blocks.reshape(channels, count // GX, GX, BY, BX).transpose(0, 1, 3, 2, 4)
    return arranged.reshape(channels, count // GX * BY, GX * BX)


def from_tile(values):
    channels, rows, columns = values.shape
    arranged = values.reshape(channels, rows // BY, BY, GX, BX).transpose(0, 1, 3, 2, 4)
    return arranged.reshape(channels, rows // BY * GX, BY * BX)


def per_device(fields, block_owner, ice_covered, land_mask):
    count = block_owner.shape[0]
    is_ocean = lax.axis_index("comp") == 0
    outbound, open_stress = air_stress(fields[0])
    owner_row = block_owner.reshape(1, count)
    crossed = from_behind(outbound, "comp", 1)
    received, anchor = (
        lax.all_to_all(crossed, ("lat", "lon"), split_axis=1, concat_axis=1, tiled=True),
        lax.all_to_all(owner_row, ("lat", "lon"), split_axis=1, concat_axis=1, tiled=True),
    )
    local_ids = anchor[0] % count
    position = jnp.zeros((count,), jnp.int32).at[local_ids].set(jnp.arange(count, dtype=jnp.int32))
    forcing = to_tile(received[:, position])
    ice_tile = to_tile(fields[0])
    covered = ice_covered.astype(jnp.float32)[:, None] * (1 - land_mask).astype(jnp.float32)
    active = to_tile(covered[None])[0]
    statics = prepare(ice_tile, forcing, active)
    ice_state = jnp.stack([ice_tile[0], ice_tile[1], ice_tile[4], ice_tile[5], ice_tile[6]])
    joined = jnp.concatenate([ice_state, statics], 0)
    joined = with_halo(joined, (("lon", 2),), NSUB, True)
    joined = with_halo(joined, (("lat", 1),), NSUB, False)
    ice_state = joined[:5]
    statics = joined[5:]
    for repeat in range(NSUB):
        ice_state, statics = subcycle(ice_state, statics)
    returned = from_tile(give_back(ice_state, statics))
    back_send = returned[:, local_ids]
    regrouped = lax.all_to_all(back_send, ("lat", "lon"), split_axis=1, concat_axis=1, tiled=True)
    received_back = from_behind(regrouped, "comp", -1)
    ocean_out = received_back[:2] + (1.0 - received_back[2]) * open_stress
    ice_out = from_tile(ice_state[:2])
    return jnp.where(is_ocean, ocean_out, ice_out)[None]


TILE = 8
GROUP = 8
MESH = pl.DeviceIdType.MESH
U, V, MASS, CONC, S1, S2, S12, ACTIVE, PUSH_X, PUSH_Y, CUR_X, CUR_Y, STRENGTH, DRAG = range(14)
SIDES = [(a, b) for b in (-1, 1) for a in (-1, 1, 0)]
ROUNDS = ((U, 8), (CUR_X, 2), (PUSH_X, 2))
KEEP = 1.0 / (1.0 + RELAX)


def tile_loop(tiles, together, body):
    def step(k, carry):
        for j in range(together):
            body(k * together + j)
        return carry
    lax.fori_loop(0, tiles // together, step, 0)


def pieces(values, axis):
    high = values.astype(jnp.bfloat16)
    low = (values - high.astype(jnp.float32)).astype(jnp.bfloat16)
    return jnp.concatenate([high, low], axis=axis)


def dot_rows(twice, values):
    return lax.dot_general(
        twice, pieces(values, 0), (((1,), (0,)), ((), ())), preferred_element_type=jnp.float32
    )


def dot_lanes(twice, values):
    return lax.dot_general(
        twice, pieces(values, 1), (((1,), (1,)), ((), ())), preferred_element_type=jnp.float32
    )


def new_stress(strength, s1, s2, s12, u, v, u_east, v_east, u_up, v_up):
    sxx = u_east - u
    syy = v_up - v
    shear = (u_up - u) + (v_east - v)
    div = sxx + syy
    ten = sxx - syy
    square = div * div + (ten * ten + shear * shear) * (1.0 / ECC2) + DMIN2
    inverse = lax.rsqrt(square)
    visc = strength * inverse
    s1 = s1 * KEEP + visc * (div - square * inverse)
    s2 = s2 * KEEP + visc * ten * (1.0 / ECC2)
    s12 = s12 * KEEP + visc * shear * (0.5 / ECC2)
    return s1, s2, s12


def new_velocity(get, u, v, force_x, force_y):
    mass, cx, cy = get(MASS), get(CUR_X), get(CUR_Y)
    dx, dy = cx - u, cy - v
    square = dx * dx + dy * dy + DRAG_FLOOR
    drag = get(DRAG) * (square * lax.rsqrt(square))
    gain = get(ACTIVE) / (jnp.maximum(mass, MASS_FLOOR) * (1.0 / DTE) + drag)
    inertia = mass * (1.0 / DTE)
    turn = CORIO * mass
    return (
        gain * (inertia * u + force_x + get(PUSH_X) + drag * cx + turn * v),
        gain * (inertia * v + force_y + get(PUSH_Y) + drag * cy - turn * u),
    )


def step_kernel(
    n_lat, n_lon,
    fields, owner_hbm, covered_hbm, land, out,
    surf, open_st, ret, owner, covered, ids, recv, forc, one_hot, back, land_v,
    main, edge, flank, flank_back, flank_vel, ends,
    rows_out0, rows_out1, rows_out2, rows_got0, rows_got1, rows_got2,
    side_out0, side_out1, side_out2, side_got0, side_got1, side_got2,
    load_sem, ids_ssem, ids_rsem, fwd_ssem, fwd_rsem, ret_ssem, ret_rsem,
    early_ssem, early_rsem, mid_rsem, late_rsem, later_ssem, ready,
):
    comp = lax.axis_index("comp")
    lat = lax.axis_index("lat")
    lon = lax.axis_index("lon")
    peers = n_lat * n_lon
    me = lat * n_lon + lon
    count = owner.shape[1]
    per = count // peers
    width = BX
    barrier = pltpu.get_barrier_semaphore()
    rows_out = (rows_out0, rows_out1, rows_out2)
    rows_got = (rows_got0, rows_got1, rows_got2)
    side_out = (side_out0, side_out1, side_out2)
    side_got = (side_got0, side_got1, side_got2)

    def rows_of(peer):
        return pl.ds(pl.multiple_of(peer * per, per), per)

    planes = [(jnp.where(lat < n_lat // 2, n_lat // 2, 0) + j) % n_lat for j in range(n_lat)]
    places = [(lon + i) % n_lon for i in range(n_lon)]

    half_lat = n_lat // 2
    groups_of = {
        "all": ((planes, places),),
        "column": ((planes[:half_lat], places[:1]),),
        "beyond": ((planes[:half_lat], places[1:]),),
        "near": ((planes[half_lat:], places),),
    }

    def each_peer(body, part="all"):
        for chosen, along in groups_of[part]:
            for plane in chosen:
                for place in along:
                    body(plane * n_lon + place, plane, place)

    def signal_peers(kind, part="all"):
        each_peer(
            lambda p, plane, place: pl.semaphore_signal(
                barrier, inc=1, device_id=(kind, plane, place), device_id_type=MESH
            ),
            part,
        )

    def send_rows(kind, src, lo, num, dst, dlo, ssem, rsem, part="all"):
        def body(p, plane, place):
            pltpu.make_async_remote_copy(
                src_ref=src.at[pl.ds(lo, num), rows_of(p), :],
                dst_ref=dst.at[pl.ds(dlo, num), rows_of(me), :],
                send_sem=ssem, recv_sem=rsem,
                device_id=(kind, plane, place), device_id_type=MESH,
            ).start()
        each_peer(body, part)

    def wait_bytes(ref, sem):
        pltpu.make_async_copy(ref, ref, sem).wait()

    def wait_tiles(num, sem):
        wait_bytes(main.at[0, 0, pl.ds(0, num * TILE), :], sem)

    @pl.when(comp == 0)
    def _ocean():
        signal_peers(1)
        names = pltpu.make_async_copy(owner_hbm, owner, load_sem.at[3])
        raw = pltpu.make_async_copy(fields.at[0, pl.ds(2, 4)], surf.at[pl.ds(2, 4)], load_sem.at[0])
        wind = pltpu.make_async_copy(fields.at[0, pl.ds(0, 2)], surf.at[pl.ds(0, 2)], load_sem.at[1])
        rho = pltpu.make_async_copy(fields.at[0, pl.ds(6, 1)], surf.at[pl.ds(6, 1)], load_sem.at[2])
        names.start()
        raw.start()
        wind.start()
        rho.start()
        names.wait()
        with jax.named_scope("o_barrier"):
            pl.semaphore_wait(barrier, half_lat)

        def ids_out(p, plane, place):
            pltpu.make_async_remote_copy(
                src_ref=owner, dst_ref=ids.at[me], send_sem=ids_ssem, recv_sem=ids_rsem,
                device_id=(1, plane, place), device_id_type=MESH,
            ).start()

        def send_four(part):
            send_rows(1, surf, 2, 4, recv, 2, fwd_ssem.at[0], fwd_rsem.at[0], part)

        def send_two(part):
            send_rows(1, forc, 0, 2, recv, 0, fwd_ssem.at[1], fwd_rsem.at[1], part)

        with jax.named_scope("o_send4"):
            raw.wait()
            send_four("column")
            wind.wait()
            rho.wait()

        def stress(t):
            r = pl.ds(pl.multiple_of(t * TILE, TILE), TILE)
            wx, wy, density = surf[0, r, :], surf[1, r, :], surf[6, r, :]
            scale = density * CD_ICE * jnp.sqrt(wx * wx + wy * wy + 1.0)
            forc[0, r, :] = scale * wx
            forc[1, r, :] = scale * wy

        with jax.named_scope("o_stress"):
            tile_loop(count // TILE, 4, stress)
            send_two("column")
        with jax.named_scope("o_ready"):
            pl.semaphore_wait(ready, 1)
        with jax.named_scope("o_rest"):
            each_peer(ids_out)
            send_four("beyond")
            send_two("beyond")
            send_four("near")
            send_two("near")

        def open_water(t):
            r = pl.ds(pl.multiple_of(t * TILE, TILE), TILE)
            density = surf[6, r, :]
            rel_x = surf[0, r, :] - surf[2, r, :]
            rel_y = surf[1, r, :] - surf[3, r, :]
            speed = jnp.sqrt(rel_x * rel_x + rel_y * rel_y + 1.0)
            scale = density * (0.1 + 0.05 * speed) * speed
            open_st[0, r, :] = scale * rel_x
            open_st[1, r, :] = scale * rel_y

        tile_loop(count // TILE, 2, open_water)
        with jax.named_scope("o_waitret1"):
            wait_bytes(ret.at[pl.ds(2, 1)], ret_rsem.at[0])

        def water(t):
            r = pl.ds(pl.multiple_of(t * TILE, TILE), TILE)
            share = 1.0 - ret[2, r, :]
            for c in range(2):
                open_st[c, r, :] = share * open_st[c, r, :]

        tile_loop(count // TILE, 4, water)
        with jax.named_scope("o_waitret2"):
            wait_bytes(ret.at[pl.ds(0, 2)], ret_rsem.at[1])

        def finish(t):
            r = pl.ds(pl.multiple_of(t * TILE, TILE), TILE)
            for c in range(2):
                out[0, c, r, :] = ret[c, r, :] + open_st[c, r, :]

        tile_loop(count // TILE, 4, finish)
        wait_bytes(ids, ids_ssem)
        wait_bytes(surf.at[pl.ds(2, 4)], fwd_ssem.at[0])
        wait_bytes(forc.at[pl.ds(0, 2)], fwd_ssem.at[1])

    @pl.when(comp == 1)
    def _ice():
        def inside(a):
            if a == 0:
                return lat >= 0
            return lat + a >= 0 if a < 0 else lat + a < n_lat

        def around(a, b):
            return (1, lat + a, (lon + b + n_lon) % n_lon)

        signal_peers(0, "column")
        for a in range(n_lat):
            for b in range(n_lon):
                if a or b:
                    pl.semaphore_signal(
                        barrier, inc=1, device_id=(1, (lat + a) % n_lat, (lon + b) % n_lon),
                        device_id_type=MESH,
                    )
        loads = [
            pltpu.make_async_copy(
                fields.at[0, :, :, pl.ds(y * width, width)], main.at[pl.ds(0, 7), y], load_sem.at[y]
            )
            for y in range(2)
        ]
        loads.append(pltpu.make_async_copy(land, land_v, load_sem.at[2]))
        loads.append(pltpu.make_async_copy(covered_hbm, covered, load_sem.at[3]))
        for load in loads:
            load.start()
        with jax.named_scope("i_barrier"):
            pl.semaphore_wait(barrier, 2 * peers - 1)
            pl.semaphore_signal(ready, inc=1, device_id=(0, lat, lon), device_id_type=MESH)

        tiles = count // TILE
        top, bottom = pl.ds(0, TILE), pl.ds(count - TILE, TILE)
        zero_tile = jnp.zeros((TILE, width), jnp.float32)
        for wall, which in ((lat == 0, 0), (lat == n_lat - 1, 1)):
            @pl.when(wall)
            def _():
                for e in range(3):
                    for k in range(rows_got[e].shape[1]):
                        rows_got[e][which, k] = zero_tile
                    for k in range(2):
                        side_got[e][2 * which, k] = zero_tile

        def clear(t):
            r = pl.ds(pl.multiple_of(t * TILE, TILE), TILE)
            for c in range(2):
                for y in range(2):
                    flank_vel[c, y, r, :] = zero_tile
            flank_back[r, :] = zero_tile

        tile_loop(tiles, 2, clear)
        for load in loads:
            load.wait()
        diag = lax.broadcasted_iota(jnp.int32, (count, count), 0) == lax.broadcasted_iota(
            jnp.int32, (count, count), 1
        )
        wet = jnp.sum(
            jnp.where(diag, covered[...].astype(jnp.float32), 0.0), axis=1, keepdims=True
        )
        sea = wet * (1 - land_v[...]).astype(jnp.float32)
        for y in range(2):
            main[ACTIVE, y] = sea[:, y * width:(y + 1) * width]

        lane = lax.broadcasted_iota(jnp.int32, (TILE, width), 1)
        sub = lax.broadcasted_iota(jnp.int32, (TILE, width), 0)
        pick_row = lax.broadcasted_iota(jnp.int32, (2 * TILE, width), 0)
        pick_col = lax.broadcasted_iota(jnp.int32, (2 * TILE, width), 1)
        picked = jnp.where(pick_row < TILE, pick_row, pick_row + (width - 2 * TILE)) == pick_col
        picker = jnp.where(picked, 1.0, 0.0).astype(jnp.bfloat16)
        picker = jnp.concatenate([picker] * 2, axis=1)

        def pack_rows(e):
            lo, num = ROUNDS[e]
            for k in range(num // 2):
                ups, downs = zero_tile, zero_tile
                for i in range(4):
                    c, y = lo + 2 * k + i // 2, i % 2
                    head, foot = main[c, y, top, :], main[c, y, bottom, :]
                    here = (sub >= 2 * i) & (sub < 2 * i + 2)
                    ups = jnp.where(here, pltpu.roll(head, 2 * i, 0) if i else head, ups)
                    downs = jnp.where(here, pltpu.roll(foot, (2 * i + 2) % TILE, 0) if i < 3 else foot, downs)
                rows_out[e][0, k] = ups
                rows_out[e][1, k] = downs

        def pack_sides(e):
            lo, num = ROUNDS[e]
            west, east = zero_tile, zero_tile
            for i in range(2 * num):
                c, y = lo + i // 2, i % 2
                ends = jnp.where(sub < NSUB, main[c, y, top, :], main[c, y, bottom, :])
                slot = i * NSUB
                mine = (lane >= slot) & (lane < slot + NSUB)
                west = jnp.where(mine, pltpu.roll(ends, slot, 1) if slot else ends, west)
                east = jnp.where(mine, pltpu.roll(ends, (slot + NSUB) % width, 1), east)
            side_out[e][0] = west
            side_out[e][1] = east

        def pack_flank(e):
            lo, num = ROUNDS[e]
            for c in range(lo, lo + num):
                for y in range(2):
                    across = dot_lanes(picker, main[c, y])
                    flank[c, y, pl.ds(TILE, TILE), :] = across[:TILE]
                    flank[c, y, pl.ds(2 * TILE, TILE), :] = across[TILE:]

        def push_on(e, a, b, src, dst, lane_of_sem, recv_lane):
            sems = (early_rsem, mid_rsem, late_rsem)[e]
            sent = early_ssem if e == 0 else later_ssem

            @pl.when(inside(a))
            def _():
                pltpu.make_async_remote_copy(
                    src_ref=src, dst_ref=dst,
                    send_sem=sent.at[lane_of_sem], recv_sem=sems.at[recv_lane],
                    device_id=around(a, b), device_id_type=MESH,
                ).start()

        def send_ends(e):
            for a in (-1, 1):
                k = 1 if a > 0 else 0
                push_on(e, a, 0, rows_out[e].at[k], rows_got[e].at[1 - k], k, 1 - k)

        def send_sides(e):
            for a, b in SIDES:
                k = 1 if b > 0 else 0
                group = {0: 2, -1: 0, 1: 1}[a]
                land_in = {0: 2, -1: 1, 1: 0}[a] + (4 if e == 2 and a != 0 else 0)
                push_on(e, a, b, side_out[e].at[k], side_got[e].at[1 - a, 1 - k], group, land_in)

        def send_flank(e):
            lo, num = ROUNDS[e]
            for b in (-1, 1):
                src, dst = (2 * TILE, 0) if b > 0 else (TILE, 3 * TILE)
                push_on(
                    e, 0, b,
                    flank.at[pl.ds(lo, num), :, pl.ds(src, TILE), :],
                    flank.at[pl.ds(lo, num), :, pl.ds(dst, TILE), :], 3, 3,
                )

        def when_inside(a, num, sem):
            @pl.when(inside(a))
            def _():
                wait_tiles(num, sem)

        def unpack_rows(e):
            lo, num = ROUNDS[e]
            got = rows_got[e]
            for k in range(num // 2):
                for i in range(4):
                    c, y = lo + 2 * k + i // 2, i % 2
                    north = pltpu.roll(got[0, k], (TILE - 2 * i) % TILE, 0) if i else got[0, k]
                    south = pltpu.roll(got[1, k], TILE - 2 - 2 * i, 0) if i < 3 else got[1, k]
                    head, foot = main[c, y, top, :], main[c, y, bottom, :]
                    edge[c, 0, y, :, pl.ds(0, width)] = jnp.where(
                        sub < 2, north, pltpu.roll(head, 2, 0)
                    )
                    edge[c, 1, y, :, pl.ds(0, width)] = jnp.where(
                        sub >= TILE - 2, south, pltpu.roll(foot, TILE - 2, 0)
                    )

        def unpack_sides(e):
            lo, num = ROUNDS[e]
            side = side_got[e]
            ends = []
            for k in range(2):
                far, near = side[0, k], side[1, k]
                ends.append(pltpu.roll(jnp.where(sub >= TILE - 2, far, near), 2, 0))
            for k in range(2):
                far, near = side[2, k], side[1, k]
                ends.append(pltpu.roll(jnp.where(sub < 2, far, near), TILE - 2, 0))
            for i in range(2 * num):
                c, y = lo + i // 2, i % 2
                slot = i * NSUB
                for strip in range(2):
                    from_west, from_east = ends[2 * strip], ends[2 * strip + 1]
                    from_east = pltpu.roll(from_east, width - slot, 1) if slot else from_east
                    from_west = pltpu.roll(from_west, width - NSUB - slot, 1)
                    edge[c, strip, y, :, pl.ds(width, width)] = jnp.where(
                        lane < NSUB, from_east, jnp.where(lane >= width - NSUB, from_west, 0.0)
                    )

        def derive(load, store):
            conc, act = load(CONC), load(ACTIVE)
            store(STRENGTH, (RELAX * KEEP) * load(MASS) * jnp.exp(CSTAR * (conc - 1.0)) * act)
            store(DRAG, CW * conc * act)

        def derive_main(t):
            r = pl.ds(pl.multiple_of(t * TILE, TILE), TILE)
            for y in range(2):
                def store(c, x):
                    main[c, y, r, :] = x
                derive(lambda c: main[c, y, r, :], store)

        def derive_edges():
            for y in range(2):
                for strip in range(2):
                    def store(c, x):
                        edge[c, strip, y] = x
                    derive(lambda c: edge[c, strip, y], store)

                def store(c, x):
                    flank[c, y] = x
                derive(lambda c: flank[c, y], store)

        def sweep_main(g, stress, velocity):
            spots = [
                pl.ds(pl.multiple_of((g * GROUP + j) * TILE, TILE), TILE) for j in range(GROUP)
            ]
            behind = pl.ds(pl.multiple_of(jnp.maximum(g * GROUP - 1, 0) * TILE, TILE), TILE)
            ahead = pl.ds(
                pl.multiple_of(jnp.minimum(g * GROUP + GROUP, tiles - 1) * TILE, TILE), TILE
            )
            vels = [[(main[U, y, r, :], main[V, y, r, :]) for y in range(2)] for r in spots]
            stresses = []
            if stress:
                follow = (main[U, 0, ahead, :], main[V, 0, ahead, :])
            for j, r in enumerate(spots):
                old = [tuple(main[c, y, r, :] for c in (S1, S2, S12)) for y in range(2)]
                if not stress:
                    stresses.append(old)
                    continue
                beyond = vels[j + 1][0] if j + 1 < GROUP else follow
                row = []
                for y in range(2):
                    u, v = vels[j][y]
                    if y == 0:
                        u_up, v_up = vels[j][1]
                    else:
                        u_up, v_up = (
                            pltpu.roll(jnp.where(sub == 0, after, x), TILE - 1, 0)
                            for x, after in zip(vels[j][0], beyond)
                        )
                    fresh = new_stress(
                        main[STRENGTH, y, r, :], *old[y], u, v,
                        pltpu.roll(u, width - 1, 1), pltpu.roll(v, width - 1, 1), u_up, v_up,
                    )
                    for c, x in zip((S1, S2, S12), fresh):
                        main[c, y, r, :] = x
                    row.append(fresh)
                stresses.append(row)
            if not velocity:
                return
            yy_before = 0.5 * (main[S1, 1, behind, :] - main[S2, 1, behind, :])
            cross_before = main[S12, 1, behind, :]
            for j, r in enumerate(spots):
                xx = [0.5 * (s1 + s2) for s1, s2, _ in stresses[j]]
                yy = [0.5 * (s1 - s2) for s1, s2, _ in stresses[j]]
                cross = [s12 for _, _, s12 in stresses[j]]
                yy_down, cross_down = (
                    [pltpu.roll(jnp.where(sub == TILE - 1, before, x[1]), 1, 0), x[0]]
                    for x, before in ((yy, yy_before), (cross, cross_before))
                )
                yy_before, cross_before = yy[1], cross[1]
                for y in range(2):
                    force_x = xx[y] - pltpu.roll(xx[y], 1, 1) + (cross[y] - cross_down[y])
                    force_y = cross[y] - pltpu.roll(cross[y], 1, 1) + (yy[y] - yy_down[y])
                    u, v = new_velocity(lambda c: main[c, y, r, :], *vels[j][y], force_x, force_y)
                    main[U, y, r, :] = u
                    main[V, y, r, :] = v

        def sweep_edge(stress, velocity):
            lanes = 2 * width

            for strip in range(2):
                vels = [(edge[U, strip, y], edge[V, strip, y]) for y in range(2)]
                fresh = [tuple(edge[c, strip, y] for c in (S1, S2, S12)) for y in range(2)]
                if stress:
                    ups = [vels[1], tuple(pltpu.roll(x, TILE - 1, 0) for x in vels[0])]
                    for y in range(2):
                        east = [pltpu.roll(x, lanes - 1, 1) for x in vels[y]]
                        fresh[y] = new_stress(
                            edge[STRENGTH, strip, y], *fresh[y], *vels[y], *east, *ups[y]
                        )
                        for c, x in zip((S1, S2, S12), fresh[y]):
                            edge[c, strip, y] = x
                if not velocity:
                    continue
                xx = [0.5 * (s1 + s2) for s1, s2, _ in fresh]
                yy = [0.5 * (s1 - s2) for s1, s2, _ in fresh]
                cross = [s12 for _, _, s12 in fresh]
                yy_down, cross_down = ([pltpu.roll(x[1], 1, 0), x[0]] for x in (yy, cross))
                for y in range(2):
                    force_x = xx[y] - pltpu.roll(xx[y], 1, 1) + (cross[y] - cross_down[y])
                    force_y = cross[y] - pltpu.roll(cross[y], 1, 1) + (yy[y] - yy_down[y])
                    u, v = new_velocity(lambda c: edge[c, strip, y], *vels[y], force_x, force_y)
                    edge[U, strip, y] = u
                    edge[V, strip, y] = v

        def sweep_flank(stress, velocity):
            spots = [pl.ds(j * TILE, TILE) for j in range(4)]
            vels = [[(flank[U, y, r, :], flank[V, y, r, :]) for y in range(2)] for r in spots]
            fresh = [
                [tuple(flank[c, y, r, :] for c in (S1, S2, S12)) for y in range(2)] for r in spots
            ]
            if stress:
                for j, r in enumerate(spots):
                    for y in range(2):
                        after = vels[min(j + 1, 3)][y]
                        east = [
                            pltpu.roll(jnp.where(sub == 0, b, x), TILE - 1, 0)
                            for x, b in zip(vels[j][y], after)
                        ]
                        ups = vels[j][1] if y == 0 else [
                            pltpu.roll(x, width - 1, 1) for x in vels[j][0]
                        ]
                        fresh[j][y] = new_stress(
                            flank[STRENGTH, y, r, :], *fresh[j][y], *vels[j][y], *east, *ups
                        )
                        for c, x in zip((S1, S2, S12), fresh[j][y]):
                            flank[c, y, r, :] = x
            if not velocity:
                return
            xx = [[0.5 * (s1 + s2) for s1, s2, _ in row] for row in fresh]
            yy = [[0.5 * (s1 - s2) for s1, s2, _ in row] for row in fresh]
            cross = [[s12 for _, _, s12 in row] for row in fresh]

            def westward(x, j, y):
                before = x[max(j - 1, 0)][y]
                return pltpu.roll(jnp.where(sub == TILE - 1, before, x[j][y]), 1, 0)

            def downward(x, j, y):
                return x[j][0] if y == 1 else pltpu.roll(x[j][1], 1, 1)

            for j, r in enumerate(spots):
                for y in range(2):
                    force_x = xx[j][y] - westward(xx, j, y) + (cross[j][y] - downward(cross, j, y))
                    force_y = cross[j][y] - westward(cross, j, y) + (yy[j][y] - downward(yy, j, y))
                    u, v = new_velocity(lambda c: flank[c, y, r, :], *vels[j][y], force_x, force_y)
                    flank[U, y, r, :] = u
                    flank[V, y, r, :] = v

        with jax.named_scope("i_pack0"):
            pack_rows(0)
            pack_sides(0)
            send_ends(0)
            send_sides(0)
            pack_flank(0)
            send_flank(0)
        tile_loop(tiles, 2, derive_main)

        with jax.named_scope("i_waitids"):
            wait_bytes(ids, ids_rsem)
        wanted = me * per
        row_lane = lax.broadcasted_iota(jnp.int32, (per, count), 1)
        row_sub = lax.broadcasted_iota(jnp.int32, (per, count), 0)
        mine = row_lane == row_sub + wanted
        blocks = lax.broadcasted_iota(jnp.int32, (per, count), 1).astype(jnp.float32)
        base = (me * count).astype(jnp.float32)
        for p in range(peers):
            owned = jnp.broadcast_to(ids[p], (per, count)).astype(jnp.float32)
            local = jnp.sum(jnp.where(mine, owned, 0.0), axis=1, keepdims=True) - base
            one_hot[pl.ds(p * per, per), :] = jnp.where(local == blocks, 1.0, 0.0)

        with jax.named_scope("i_waithalo0"):
            for sems in (early_ssem, early_rsem):
                when_inside(-1, 6, sems.at[0])
                when_inside(1, 6, sems.at[1])
                wait_tiles(2, sems.at[2])
                wait_bytes(main.at[0], sems.at[3])
        with jax.named_scope("i_unpack0"):
            unpack_rows(0)
            unpack_sides(0)
            derive_edges()
        groups = tiles // GROUP
        with jax.named_scope("i_stress"):
            tile_loop(groups, 1, lambda g: sweep_main(g, True, False))
            sweep_edge(True, False)
            sweep_flank(True, False)
        by_slot = one_hot[...]
        to_slots = jnp.concatenate([by_slot.astype(jnp.bfloat16)] * 2, axis=1)
        to_ends = jnp.concatenate([by_slot[:, :TILE], by_slot[:, count - TILE:]] * 2, axis=1)
        to_ends = to_ends.astype(jnp.bfloat16)
        by_block = by_slot.T.astype(jnp.bfloat16)
        to_blocks = jnp.concatenate([by_block] * 2, axis=1)
        columns = jnp.concatenate([by_block] * 2, axis=0)

        with jax.named_scope("i_waitf4"):
            wait_bytes(recv.at[pl.ds(2, 4)], fwd_rsem.at[0])
        for c in range(2):
            both = dot_rows(to_blocks, recv[2 + c])
            for y in range(2):
                main[CUR_X + c, y] = both[:, y * width:(y + 1) * width]
        with jax.named_scope("i_packmid"):
            pack_rows(1)
            pack_sides(1)
            send_ends(1)
            send_sides(1)
            pack_flank(1)
            send_flank(1)
        for c in range(2):
            both = dot_rows(to_blocks, recv[4 + c])
            for y in range(2):
                main[PUSH_X + c, y] = main[MASS, y] * both[:, y * width:(y + 1) * width]
        for y in range(2):
            share = main[CONC, y] * main[ACTIVE, y]
            back[2, :, pl.ds(y * width, width)] = dot_rows(to_slots, share)

        with jax.named_scope("i_waitf2"):
            wait_bytes(recv.at[pl.ds(0, 2)], fwd_rsem.at[1])
        with jax.named_scope("i_push"):
            for c in range(2):
                both = dot_rows(to_blocks, recv[c])
                for y in range(2):
                    main[PUSH_X + c, y] = main[ACTIVE, y] * (
                        main[CONC, y] * both[:, y * width:(y + 1) * width] - main[PUSH_X + c, y]
                    )
        with jax.named_scope("i_packlate"):
            pack_rows(2)
            send_ends(2)
            pack_sides(2)
            send_sides(2)
            pack_flank(2)
            send_flank(2)

        def leave(get, u, v):
            dx, dy = u - get(CUR_X), v - get(CUR_Y)
            drag = get(DRAG) * jnp.sqrt(dx * dx + dy * dy + DRAG_FLOOR)
            return drag * dx, drag * dy

        outer = (lane < NSUB) | (lane >= width - NSUB)

        with jax.named_scope("i_vel1"):
            tile_loop(groups, 1, lambda g: sweep_main(g, False, True))
        with jax.named_scope("i_sweeps"):
            tile_loop((NSUB - 1) * groups, 1, lambda k: sweep_main(k % groups, True, True))
        send_rows(0, back, 2, 1, ret, 2, ret_ssem.at[0], ret_rsem.at[0])

        def returned(t):
            r = pl.ds(pl.multiple_of(t * TILE, TILE), TILE)
            block = sub + t * TILE
            theirs = outer | (block < 2) | (block >= count - 2)
            for y in range(2):
                half = pl.ds(y * width, width)
                u, v = main[U, y, r, :], main[V, y, r, :]
                gone = leave(lambda c: main[c, y, r, :], u, v)
                for c in range(2):
                    forc[c, r, half] = jnp.where(theirs, 0.0, gone[c])

        with jax.named_scope("i_back"):
            tile_loop(tiles, 4, returned)
            for c in range(2):
                back[c] = dot_rows(to_slots, forc[c])
        with jax.named_scope("i_waitmid"):
            when_inside(1, 3, mid_rsem.at[1])
            when_inside(-1, 3, mid_rsem.at[0])
            wait_tiles(2, mid_rsem.at[2])
            wait_tiles(8, mid_rsem.at[3])
        unpack_rows(1)
        unpack_sides(1)
        with jax.named_scope("i_waitrows"):
            when_inside(-1, 1, late_rsem.at[0])
            when_inside(1, 1, late_rsem.at[1])
        unpack_rows(2)
        with jax.named_scope("i_waitlate"):
            wait_tiles(2, late_rsem.at[2])
            when_inside(-1, 2, late_rsem.at[4])
            when_inside(1, 2, late_rsem.at[5])
            wait_tiles(8, late_rsem.at[3])

        def sweep_strips(stress, velocity):
            sweep_flank(stress, velocity)
            sweep_edge(stress, velocity)

        with jax.named_scope("i_edge"):
            unpack_sides(2)
            sweep_strips(False, True)
            tile_loop(NSUB - 1, 1, lambda k: sweep_strips(True, True))

        with jax.named_scope("i_fix"):
            for y in range(2):
                for j, far in ((1, 0), (2, count - TILE)):
                    r = pl.ds(j * TILE, TILE)
                    held = (lane >= 2) & (lane < count - 2)
                    held = held & ((sub < NSUB) if j == 1 else (sub >= TILE - NSUB))
                    u, v = flank[U, y, r, :], flank[V, y, r, :]
                    gone = leave(lambda c: flank[c, y, r, :], u, v)
                    for c in range(2):
                        slot = (c * 2 + y) * 2 * TILE + (TILE if j == 1 else 0)
                        flank_back[pl.ds(slot, TILE), :] = jnp.where(held, gone[c], 0.0)
                        flank_vel[c, y, pl.ds(far, TILE), :] = jnp.where(held, (u, v)[c], 0.0)
                for strip in range(2):
                    def get(c):
                        return edge[c, strip, y, :, pl.ds(0, width)]
                    gone = leave(get, get(U), get(V))
                    held = (sub < 2) if strip == 0 else (sub >= TILE - 2)
                    for c in range(2):
                        moved = pltpu.roll(gone[c], TILE - 2 if strip == 0 else 2, 0)
                        ends[c, pl.ds(strip * TILE, TILE), pl.ds(y * width, width)] = jnp.where(
                            held, moved, 0.0
                        )
            across = lax.dot_general(
                pieces(flank_back[...], 1), columns,
                (((1,), (0,)), ((), ())), preferred_element_type=jnp.float32,
            ).T
            for c in range(2):
                rest = dot_rows(to_ends, ends[c])
                for y in range(2):
                    slot = (c * 2 + y) * 2 * TILE
                    for t in range(tiles):
                        r, half = pl.ds(t * TILE, TILE), pl.ds(y * width, width)
                        moved = pltpu.roll(across[t * TILE:(t + 1) * TILE], width - TILE - slot, 1)
                        back[c, r, half] += jnp.where(outer, moved, 0.0) + (
                            rest[t * TILE:(t + 1) * TILE, y * width:(y + 1) * width]
                        )
            send_rows(0, back, 0, 2, ret, 0, ret_ssem.at[1], ret_rsem.at[1])

        same = jnp.where(diag, 1.0, 0.0).astype(jnp.bfloat16)
        same = jnp.concatenate([same] * 2, axis=1)
        for y in range(2):
            for c in range(2):
                half = pl.ds(y * width, width)
                for strip, r in ((0, top), (1, bottom)):
                    end = pltpu.roll(
                        edge[c, strip, y, :, pl.ds(0, width)], TILE - 2 if strip == 0 else 2, 0
                    )
                    held = (sub < 2) if strip == 0 else (sub >= TILE - 2)
                    main[c, y, r, :] = jnp.where(held, end, main[c, y, r, :])
                other = dot_lanes(same, flank_vel[c, y])
                row = lax.broadcasted_iota(jnp.int32, (count, width), 0)
                column = lax.broadcasted_iota(jnp.int32, (count, width), 1)
                theirs = (row >= 2) & (row < count - 2)
                theirs = theirs & ((column < NSUB) | (column >= width - NSUB))
                out[0, c, :, half] = jnp.where(theirs, other, main[c, y])
        wait_bytes(back.at[pl.ds(2, 1)], ret_ssem.at[0])
        wait_bytes(back.at[pl.ds(0, 2)], ret_ssem.at[1])
        when_inside(-1, 6, later_ssem.at[0])
        when_inside(1, 6, later_ssem.at[1])
        wait_tiles(4, later_ssem.at[2])
        wait_tiles(16, later_ssem.at[3])


def per_device_kernel(n_lat, n_lon, fields, block_owner, ice_covered, land_mask):
    count, cells = land_mask.shape
    peers = n_lat * n_lon
    f32 = jnp.float32
    anywhere = pl.BlockSpec(memory_space=pl.ANY)
    dma = pltpu.SemaphoreType.DMA
    halos = [pltpu.VMEM((2, num // 2, TILE, BX), f32) for _, num in ROUNDS] * 2
    sides = [pltpu.VMEM((2, TILE, BX), f32) for _ in ROUNDS]
    sides += [pltpu.VMEM((3, 2, TILE, BX), f32) for _ in ROUNDS]
    return pl.pallas_call(
        functools.partial(step_kernel, n_lat, n_lon),
        out_shape=pltpu.VMEM((1, 2, count, cells), f32),
        in_specs=[anywhere, anywhere, anywhere, anywhere],
        out_specs=pl.BlockSpec(memory_space=pltpu.VMEM),
        scratch_shapes=[
            pltpu.VMEM((7, count, cells), f32),
            pltpu.VMEM((2, count, cells), f32),
            pltpu.VMEM((3, count, cells), f32),
            pltpu.VMEM((1, count), jnp.int32),
            pltpu.VMEM((1, count), jnp.int32),
            pltpu.VMEM((peers, 1, count), jnp.int32),
            pltpu.VMEM((6, count, cells), f32),
            pltpu.VMEM((2, count, cells), f32),
            pltpu.VMEM((count, count), f32),
            pltpu.VMEM((3, count, cells), f32),
            pltpu.VMEM((count, cells), jnp.int32),
            pltpu.VMEM((14, 2, count, BX), f32),
            pltpu.VMEM((14, 2, 2, TILE, 2 * BX), f32),
            pltpu.VMEM((14, 2, 4 * TILE, BX), f32),
            pltpu.VMEM((BX, count), f32),
            pltpu.VMEM((2, 2, BX, count), f32),
            pltpu.VMEM((2, 2 * TILE, cells), f32),
            *halos, *sides,
            dma((4,)), dma, dma, dma((2,)), dma((2,)), dma((2,)), dma((2,)),
            dma((4,)), dma((4,)), dma((4,)), dma((6,)), dma((4,)),
            pltpu.SemaphoreType.REGULAR,
        ],
        compiler_params=pltpu.CompilerParams(
            collective_id=0, has_side_effects=True, vmem_limit_bytes=63 * 1024 * 1024
        ),
    )(fields, block_owner.reshape(1, count), ice_covered.reshape(1, count), land_mask)


def solution(mesh):
    placed = (
        P("comp", None, ("lat", "lon"), None),
        P(("lat", "lon")),
        P(("lat", "lon")),
        P(("lat", "lon"), None),
    )
    n_lat, n_lon = mesh.shape["lat"], mesh.shape["lon"]

    def body(fields, block_owner, ice_covered, land_mask):
        count = block_owner.shape[0]
        whole_tiles = count % (n_lat * n_lon * TILE) == 0 and count == BX
        if whole_tiles and n_lon > 2:
            return per_device_kernel(n_lat, n_lon, fields, block_owner, ice_covered, land_mask)
        return per_device(fields, block_owner, ice_covered, land_mask)

    return jax.shard_map(
        body,
        mesh=mesh,
        in_specs=placed,
        out_specs=P("comp", None, ("lat", "lon"), None),
        check_vma=False,
    )
```

```python
import functools

import jax
import jax.numpy as jnp
from jax import lax
from jax.experimental import pallas as pl
from jax.experimental.pallas import tpu as pltpu
from jax.sharding import PartitionSpec as P

GX = 1
BY = 2
BX = 128
NSUB = 4


CD_ICE = 0.1
CW = 1.5
CSTAR = 2.0
ECC2 = 4.0
DMIN2 = 0.25
RELAX = 0.5
DTE = 0.5
CORIO = 0.3
MASS_FLOOR = 0.5
DRAG_FLOOR = 0.1


def from_behind(x, axis, by):
    size = lax.axis_size(axis)
    pairs = [(i, i + by) for i in range(size) if 0 <= i + by < size]
    return lax.ppermute(x, axis, pairs)


def with_halo(x, sides, width, wrap):
    for axis, dim in sides:
        size, length = (lax.axis_size(axis), x.shape[dim])
        up = [(i, (i + 1) % size) for i in range(size if wrap else size - 1)]
        down = [(j, i) for i, j in up]
        last = lax.slice_in_dim(x, length - width, length, axis=dim)
        first = lax.slice_in_dim(x, 0, width, axis=dim)
        before = lax.ppermute(last, axis, up)
        after = lax.ppermute(first, axis, down)
        x = jnp.concatenate([before, x, after], axis=dim)
    return x


def air_stress(ocean):
    wind_x, wind_y, current_x, current_y, tilt_x, tilt_y, density = ocean
    speed_ice = jnp.sqrt(wind_x * wind_x + wind_y * wind_y + 1.0)
    scale_ice = density * CD_ICE * speed_ice
    rel_x = wind_x - current_x
    rel_y = wind_y - current_y
    speed_open = jnp.sqrt(rel_x * rel_x + rel_y * rel_y + 1.0)
    scale_open = density * (0.1 + 0.05 * speed_open) * speed_open
    outbound = jnp.stack(
        [scale_ice * wind_x, scale_ice * wind_y, current_x, current_y, tilt_x, tilt_y]
    )
    open_stress = jnp.stack([scale_open * rel_x, scale_open * rel_y])
    return (outbound, open_stress)


def prepare(ice_tile, forcing, active):
    ice_mass = ice_tile[2]
    concentration = ice_tile[3]
    strength = ice_mass * jnp.exp(CSTAR * (concentration - 1.0)) * active
    drag_base = CW * concentration * active
    push_x = active * (concentration * forcing[0] - ice_mass * forcing[4])
    push_y = active * (concentration * forcing[1] - ice_mass * forcing[5])
    return jnp.stack(
        [strength, ice_mass, drag_base, push_x, push_y, forcing[2], forcing[3], active]
    )


def subcycle(ice_state, statics):
    east_vel, north_vel, stress_one, stress_two, stress_three = ice_state
    strength = statics[0]
    east_base = east_vel[:-1, :-1]
    north_base = north_vel[:-1, :-1]
    strain_xx = east_vel[:-1, 1:] - east_base
    strain_yy = north_vel[1:, :-1] - north_base
    shear = east_vel[1:, :-1] - east_base + (north_vel[:-1, 1:] - north_base)
    divergence = strain_xx + strain_yy
    tension = strain_xx - strain_yy
    delta_norm = jnp.sqrt(
        divergence * divergence + (tension * tension + shear * shear) / ECC2 + DMIN2
    )
    viscosity = strength[:-1, :-1] / delta_norm
    stress_sum = (stress_one[:-1, :-1] + RELAX * viscosity * (divergence - delta_norm)) / (
        1.0 + RELAX
    )
    stress_diff = (stress_two[:-1, :-1] + RELAX * viscosity * tension / ECC2) / (1.0 + RELAX)
    stress_shear = (stress_three[:-1, :-1] + RELAX * viscosity * shear / (2.0 * ECC2)) / (
        1.0 + RELAX
    )
    stress_xx = 0.5 * (stress_sum + stress_diff)
    stress_yy = 0.5 * (stress_sum - stress_diff)
    force_x = (
        stress_xx[1:, 1:] - stress_xx[1:, :-1] + (stress_shear[1:, 1:] - stress_shear[:-1, 1:])
    )
    force_y = (
        stress_shear[1:, 1:] - stress_shear[1:, :-1] + (stress_yy[1:, 1:] - stress_yy[:-1, 1:])
    )
    trimmed = statics[:, 1:-1, 1:-1]
    strength, ice_mass, drag_base, push_x, push_y, current_x, current_y, active = trimmed
    east_old = east_vel[1:-1, 1:-1]
    north_old = north_vel[1:-1, 1:-1]
    diff_x = current_x - east_old
    diff_y = current_y - north_old
    drag_coef = drag_base * jnp.sqrt(diff_x * diff_x + diff_y * diff_y + DRAG_FLOOR)
    denominator = jnp.maximum(ice_mass, MASS_FLOOR) / DTE + drag_coef
    east_new = (
        active
        * (
            ice_mass / DTE * east_old
            + force_x
            + push_x
            + drag_coef * current_x
            + CORIO * ice_mass * north_old
        )
        / denominator
    )
    north_new = (
        active
        * (
            ice_mass / DTE * north_old
            + force_y
            + push_y
            + drag_coef * current_y
            - CORIO * ice_mass * east_old
        )
        / denominator
    )
    new_state = jnp.stack(
        [east_new, north_new, stress_sum[1:, 1:], stress_diff[1:, 1:], stress_shear[1:, 1:]]
    )
    return (new_state, trimmed)


def give_back(ice_state, statics):
    east_vel = ice_state[0]
    north_vel = ice_state[1]
    drag_base = statics[2]
    current_x = statics[5]
    current_y = statics[6]
    diff_x = east_vel - current_x
    diff_y = north_vel - current_y
    factor = drag_base * jnp.sqrt(diff_x * diff_x + diff_y * diff_y + DRAG_FLOOR)
    return jnp.stack([factor * diff_x, factor * diff_y, drag_base / CW])


def to_tile(blocks):
    channels, count, cells = blocks.shape
    arranged = blocks.reshape(channels, count // GX, GX, BY, BX).transpose(0, 1, 3, 2, 4)
    return arranged.reshape(channels, count // GX * BY, GX * BX)


def from_tile(values):
    channels, rows, columns = values.shape
    arranged = values.reshape(channels, rows // BY, BY, GX, BX).transpose(0, 1, 3, 2, 4)
    return arranged.reshape(channels, rows // BY * GX, BY * BX)


def per_device(fields, block_owner, ice_covered, land_mask):
    count = block_owner.shape[0]
    is_ocean = lax.axis_index("comp") == 0
    outbound, open_stress = air_stress(fields[0])
    owner_row = block_owner.reshape(1, count)
    crossed = from_behind(outbound, "comp", 1)
    received, anchor = (
        lax.all_to_all(crossed, ("lat", "lon"), split_axis=1, concat_axis=1, tiled=True),
        lax.all_to_all(owner_row, ("lat", "lon"), split_axis=1, concat_axis=1, tiled=True),
    )
    local_ids = anchor[0] % count
    position = jnp.zeros((count,), jnp.int32).at[local_ids].set(jnp.arange(count, dtype=jnp.int32))
    forcing = to_tile(received[:, position])
    ice_tile = to_tile(fields[0])
    covered = ice_covered.astype(jnp.float32)[:, None] * (1 - land_mask).astype(jnp.float32)
    active = to_tile(covered[None])[0]
    statics = prepare(ice_tile, forcing, active)
    ice_state = jnp.stack([ice_tile[0], ice_tile[1], ice_tile[4], ice_tile[5], ice_tile[6]])
    joined = jnp.concatenate([ice_state, statics], 0)
    joined = with_halo(joined, (("lon", 2),), NSUB, True)
    joined = with_halo(joined, (("lat", 1),), NSUB, False)
    ice_state = joined[:5]
    statics = joined[5:]
    for repeat in range(NSUB):
        ice_state, statics = subcycle(ice_state, statics)
    returned = from_tile(give_back(ice_state, statics))
    back_send = returned[:, local_ids]
    regrouped = lax.all_to_all(back_send, ("lat", "lon"), split_axis=1, concat_axis=1, tiled=True)
    received_back = from_behind(regrouped, "comp", -1)
    ocean_out = received_back[:2] + (1.0 - received_back[2]) * open_stress
    ice_out = from_tile(ice_state[:2])
    return jnp.where(is_ocean, ocean_out, ice_out)[None]


TILE = 8
GROUP = 8
MESH = pl.DeviceIdType.MESH
U, V, MASS, CONC, S1, S2, S12, ACTIVE, PUSH_X, PUSH_Y, CUR_X, CUR_Y, STRENGTH, DRAG = range(14)
SIDES = [(a, b) for b in (-1, 1) for a in (-1, 1, 0)]
ROUNDS = ((U, 8), (CUR_X, 2), (PUSH_X, 2))
KEEP = 1.0 / (1.0 + RELAX)


def tile_loop(tiles, together, body):
    def step(k, carry):
        for j in range(together):
            body(k * together + j)
        return carry
    lax.fori_loop(0, tiles // together, step, 0)


def pieces(values, axis):
    high = values.astype(jnp.bfloat16)
    low = (values - high.astype(jnp.float32)).astype(jnp.bfloat16)
    return jnp.concatenate([high, low], axis=axis)


def dot_rows(twice, values):
    return lax.dot_general(
        twice, pieces(values, 0), (((1,), (0,)), ((), ())), preferred_element_type=jnp.float32
    )


def dot_lanes(twice, values):
    return lax.dot_general(
        twice, pieces(values, 1), (((1,), (1,)), ((), ())), preferred_element_type=jnp.float32
    )


def new_stress(strength, s1, s2, s12, u, v, u_east, v_east, u_up, v_up):
    sxx = u_east - u
    syy = v_up - v
    shear = (u_up - u) + (v_east - v)
    div = sxx + syy
    ten = sxx - syy
    square = div * div + (ten * ten + shear * shear) * (1.0 / ECC2) + DMIN2
    inverse = lax.rsqrt(square)
    visc = strength * inverse
    s1 = s1 * KEEP + visc * (div - square * inverse)
    s2 = s2 * KEEP + visc * ten * (1.0 / ECC2)
    s12 = s12 * KEEP + visc * shear * (0.5 / ECC2)
    return s1, s2, s12


def new_velocity(get, u, v, force_x, force_y):
    mass, cx, cy = get(MASS), get(CUR_X), get(CUR_Y)
    dx, dy = cx - u, cy - v
    square = dx * dx + dy * dy + DRAG_FLOOR
    drag = get(DRAG) * (square * lax.rsqrt(square))
    gain = get(ACTIVE) / (jnp.maximum(mass, MASS_FLOOR) * (1.0 / DTE) + drag)
    inertia = mass * (1.0 / DTE)
    turn = CORIO * mass
    return (
        gain * (inertia * u + force_x + get(PUSH_X) + drag * cx + turn * v),
        gain * (inertia * v + force_y + get(PUSH_Y) + drag * cy - turn * u),
    )


def step_kernel(
    n_lat, n_lon,
    fields, owner_hbm, covered_hbm, land, out,
    surf, open_st, ret, owner, covered, ids, recv, forc, one_hot, back, land_v,
    main, edge, flank, flank_back, flank_vel, ends,
    rows_out0, rows_out1, rows_out2, rows_got0, rows_got1, rows_got2,
    side_out0, side_out1, side_out2, side_got0, side_got1, side_got2,
    load_sem, ids_ssem, ids_rsem, fwd_ssem, fwd_rsem, ret_ssem, ret_rsem,
    halo_ssem, early_rsem, later_rsem, ready,
):
    comp = lax.axis_index("comp")
    lat = lax.axis_index("lat")
    lon = lax.axis_index("lon")
    peers = n_lat * n_lon
    me = lat * n_lon + lon
    count = owner.shape[1]
    per = count // peers
    width = BX
    barrier = pltpu.get_barrier_semaphore()
    rows_out = (rows_out0, rows_out1, rows_out2)
    rows_got = (rows_got0, rows_got1, rows_got2)
    side_out = (side_out0, side_out1, side_out2)
    side_got = (side_got0, side_got1, side_got2)

    def rows_of(peer):
        return pl.ds(pl.multiple_of(peer * per, per), per)

    planes = [jnp.where(lat < n_lat // 2, n_lat - 1 - j, j) for j in range(n_lat)]
    places = [(lon + i) % n_lon for i in range(n_lon)]

    half_lat = n_lat // 2
    groups_of = {
        "all": ((planes, places),),
        "column": ((planes[:half_lat], places[:1]),),
        "beyond": ((planes[:half_lat], places[1:]),),
        "near": ((planes[half_lat:], places),),
    }

    def each_peer(body, part="all"):
        for chosen, along in groups_of[part]:
            for plane in chosen:
                for place in along:
                    body(plane * n_lon + place, plane, place)

    def signal_peers(kind, part="all"):
        each_peer(
            lambda p, plane, place: pl.semaphore_signal(
                barrier, inc=1, device_id=(kind, plane, place), device_id_type=MESH
            ),
            part,
        )

    def send_rows(kind, src, lo, num, dst, dlo, ssem, rsem, part="all"):
        def body(p, plane, place):
            pltpu.make_async_remote_copy(
                src_ref=src.at[pl.ds(lo, num), rows_of(p), :],
                dst_ref=dst.at[pl.ds(dlo, num), rows_of(me), :],
                send_sem=ssem, recv_sem=rsem,
                device_id=(kind, plane, place), device_id_type=MESH,
            ).start()
        each_peer(body, part)

    def wait_bytes(ref, sem):
        pltpu.make_async_copy(ref, ref, sem).wait()

    def wait_tiles(num, sem):
        wait_bytes(main.at[0, 0, pl.ds(0, num * TILE), :], sem)

    @pl.when(comp == 0)
    def _ocean():
        signal_peers(1)
        raw = pltpu.make_async_copy(fields.at[0, pl.ds(2, 4)], surf.at[pl.ds(2, 4)], load_sem.at[0])
        wind = pltpu.make_async_copy(fields.at[0, pl.ds(0, 2)], surf.at[pl.ds(0, 2)], load_sem.at[1])
        rho = pltpu.make_async_copy(fields.at[0, pl.ds(6, 1)], surf.at[pl.ds(6, 1)], load_sem.at[2])
        raw.start()
        wind.start()
        rho.start()
        with jax.named_scope("o_barrier"):
            pl.semaphore_wait(barrier, half_lat)

        def send_four(part):
            send_rows(1, surf, 2, 4, recv, 2, fwd_ssem, fwd_rsem.at[0], part)

        def send_two(part):
            send_rows(1, forc, 0, 2, recv, 0, fwd_ssem, fwd_rsem.at[1], part)

        with jax.named_scope("o_send4"):
            raw.wait()
            send_four("column")
            wind.wait()
            rho.wait()

        def stress(t):
            r = pl.ds(pl.multiple_of(t * TILE, TILE), TILE)
            wx, wy, density = surf[0, r, :], surf[1, r, :], surf[6, r, :]
            scale = density * CD_ICE * jnp.sqrt(wx * wx + wy * wy + 1.0)
            forc[0, r, :] = scale * wx
            forc[1, r, :] = scale * wy

        with jax.named_scope("o_stress"):
            tile_loop(count // TILE, 4, stress)
            send_two("column")
        with jax.named_scope("o_ready"):
            pl.semaphore_wait(ready, 1)
        with jax.named_scope("o_rest"):
            send_four("beyond")
            send_two("beyond")
            send_four("near")
            send_two("near")

        def open_water(t):
            r = pl.ds(pl.multiple_of(t * TILE, TILE), TILE)
            density = surf[6, r, :]
            rel_x = surf[0, r, :] - surf[2, r, :]
            rel_y = surf[1, r, :] - surf[3, r, :]
            speed = jnp.sqrt(rel_x * rel_x + rel_y * rel_y + 1.0)
            scale = density * (0.1 + 0.05 * speed) * speed
            open_st[0, r, :] = scale * rel_x
            open_st[1, r, :] = scale * rel_y

        tile_loop(count // TILE, 2, open_water)
        with jax.named_scope("o_waitret1"):
            wait_bytes(ret.at[pl.ds(2, 1)], ret_rsem.at[0])

        def water(t):
            r = pl.ds(pl.multiple_of(t * TILE, TILE), TILE)
            share = 1.0 - ret[2, r, :]
            for c in range(2):
                open_st[c, r, :] = share * open_st[c, r, :]

        tile_loop(count // TILE, 4, water)
        with jax.named_scope("o_waitret2"):
            wait_bytes(ret.at[pl.ds(0, 2)], ret_rsem.at[1])

        def finish(t):
            r = pl.ds(pl.multiple_of(t * TILE, TILE), TILE)
            for c in range(2):
                out[0, c, r, :] = ret[c, r, :] + open_st[c, r, :]

        tile_loop(count // TILE, 4, finish)
        wait_bytes(surf.at[pl.ds(0, 6)], fwd_ssem)

    @pl.when(comp == 1)
    def _ice():
        def inside(a):
            if a == 0:
                return lat >= 0
            return lat + a >= 0 if a < 0 else lat + a < n_lat

        def around(a, b):
            return (1, lat + a, (lon + b + n_lon) % n_lon)

        signal_peers(0, "column")
        for a in range(n_lat):
            for b in range(n_lon):
                if a or b:
                    pl.semaphore_signal(
                        barrier, inc=1, device_id=(1, (lat + a) % n_lat, (lon + b) % n_lon),
                        device_id_type=MESH,
                    )
        loads = [
            pltpu.make_async_copy(
                fields.at[0, :, :, pl.ds(y * width, width)], main.at[pl.ds(0, 7), y], load_sem.at[y]
            )
            for y in range(2)
        ]
        loads.append(pltpu.make_async_copy(land, land_v, load_sem.at[2]))
        loads.append(pltpu.make_async_copy(covered_hbm, covered, load_sem.at[3]))
        names = pltpu.make_async_copy(owner_hbm, owner, load_sem.at[4])
        names.start()
        for load in loads:
            load.start()
        with jax.named_scope("i_barrier"):
            pl.semaphore_wait(barrier, 2 * peers - 1)
            pl.semaphore_signal(ready, inc=1, device_id=(0, lat, lon), device_id_type=MESH)
            names.wait()
            for a in range(n_lat):
                for b in range(n_lon):
                    if a or b:
                        pltpu.make_async_remote_copy(
                            src_ref=owner, dst_ref=ids.at[me], send_sem=ids_ssem, recv_sem=ids_rsem,
                            device_id=(1, (lat + a) % n_lat, (lon + b) % n_lon),
                            device_id_type=MESH,
                        ).start()
        ids[me] = owner[...]

        tiles = count // TILE
        top, bottom = pl.ds(0, TILE), pl.ds(count - TILE, TILE)
        zero_tile = jnp.zeros((TILE, width), jnp.float32)
        for wall, which in ((lat == 0, 0), (lat == n_lat - 1, 1)):
            @pl.when(wall)
            def _():
                for e in range(3):
                    for k in range(rows_got[e].shape[1]):
                        rows_got[e][which, k] = zero_tile
                    for k in range(2):
                        side_got[e][2 * which, k] = zero_tile

        def clear(t):
            r = pl.ds(pl.multiple_of(t * TILE, TILE), TILE)
            for c in range(2):
                for y in range(2):
                    flank_vel[c, y, r, :] = zero_tile
            flank_back[r, :] = zero_tile

        tile_loop(tiles, 2, clear)
        for load in loads:
            load.wait()
        diag = lax.broadcasted_iota(jnp.int32, (count, count), 0) == lax.broadcasted_iota(
            jnp.int32, (count, count), 1
        )
        wet = jnp.sum(
            jnp.where(diag, covered[...].astype(jnp.float32), 0.0), axis=1, keepdims=True
        )
        sea = wet * (1 - land_v[...]).astype(jnp.float32)
        for y in range(2):
            main[ACTIVE, y] = sea[:, y * width:(y + 1) * width]

        lane = lax.broadcasted_iota(jnp.int32, (TILE, width), 1)
        sub = lax.broadcasted_iota(jnp.int32, (TILE, width), 0)
        pick_row = lax.broadcasted_iota(jnp.int32, (2 * TILE, width), 0)
        pick_col = lax.broadcasted_iota(jnp.int32, (2 * TILE, width), 1)
        picked = jnp.where(pick_row < TILE, pick_row, pick_row + (width - 2 * TILE)) == pick_col
        picker = jnp.where(picked, 1.0, 0.0).astype(jnp.bfloat16)
        picker = jnp.concatenate([picker] * 2, axis=1)

        def pack_rows(e):
            lo, num = ROUNDS[e]
            for k in range(num // 2):
                ups, downs = zero_tile, zero_tile
                for i in range(4):
                    c, y = lo + 2 * k + i // 2, i % 2
                    head, foot = main[c, y, top, :], main[c, y, bottom, :]
                    here = (sub >= 2 * i) & (sub < 2 * i + 2)
                    ups = jnp.where(here, pltpu.roll(head, 2 * i, 0) if i else head, ups)
                    downs = jnp.where(here, pltpu.roll(foot, (2 * i + 2) % TILE, 0) if i < 3 else foot, downs)
                rows_out[e][0, k] = ups
                rows_out[e][1, k] = downs

        def pack_sides(e):
            lo, num = ROUNDS[e]
            west, east = zero_tile, zero_tile
            for i in range(2 * num):
                c, y = lo + i // 2, i % 2
                ends = jnp.where(sub < NSUB, main[c, y, top, :], main[c, y, bottom, :])
                slot = i * NSUB
                mine = (lane >= slot) & (lane < slot + NSUB)
                west = jnp.where(mine, pltpu.roll(ends, slot, 1) if slot else ends, west)
                east = jnp.where(mine, pltpu.roll(ends, (slot + NSUB) % width, 1), east)
            side_out[e][0] = west
            side_out[e][1] = east

        def pack_flank(e):
            lo, num = ROUNDS[e]
            for c in range(lo, lo + num):
                for y in range(2):
                    across = dot_lanes(picker, main[c, y])
                    flank[c, y, pl.ds(TILE, TILE), :] = across[:TILE]
                    flank[c, y, pl.ds(2 * TILE, TILE), :] = across[TILE:]

        def push_on(e, a, b, src, dst, lane_of_sem, recv_lane):
            sems = early_rsem if e == 0 else later_rsem

            @pl.when(inside(a))
            def _():
                pltpu.make_async_remote_copy(
                    src_ref=src, dst_ref=dst,
                    send_sem=halo_ssem.at[lane_of_sem], recv_sem=sems.at[recv_lane],
                    device_id=around(a, b), device_id_type=MESH,
                ).start()

        def send_ends(e):
            for a in (-1, 1):
                k = 1 if a > 0 else 0
                push_on(e, a, 0, rows_out[e].at[k], rows_got[e].at[1 - k], k, 1 - k)

        def send_sides(e):
            for a, b in SIDES:
                k = 1 if b > 0 else 0
                group = {0: 2, -1: 0, 1: 1}[a]
                land_in = {0: 2, -1: 1, 1: 0}[a]
                push_on(e, a, b, side_out[e].at[k], side_got[e].at[1 - a, 1 - k], group, land_in)

        def send_flank(e):
            lo, num = ROUNDS[e]
            for b in (-1, 1):
                src, dst = (2 * TILE, 0) if b > 0 else (TILE, 3 * TILE)
                push_on(
                    e, 0, b,
                    flank.at[pl.ds(lo, num), :, pl.ds(src, TILE), :],
                    flank.at[pl.ds(lo, num), :, pl.ds(dst, TILE), :], 3, 3,
                )

        def when_inside(a, num, sem):
            @pl.when(inside(a))
            def _():
                wait_tiles(num, sem)

        def unpack_rows(e):
            lo, num = ROUNDS[e]
            got = rows_got[e]
            for k in range(num // 2):
                for i in range(4):
                    c, y = lo + 2 * k + i // 2, i % 2
                    north = pltpu.roll(got[0, k], (TILE - 2 * i) % TILE, 0) if i else got[0, k]
                    south = pltpu.roll(got[1, k], TILE - 2 - 2 * i, 0) if i < 3 else got[1, k]
                    head, foot = main[c, y, top, :], main[c, y, bottom, :]
                    edge[c, 0, y, :, pl.ds(0, width)] = jnp.where(
                        sub < 2, north, pltpu.roll(head, 2, 0)
                    )
                    edge[c, 1, y, :, pl.ds(0, width)] = jnp.where(
                        sub >= TILE - 2, south, pltpu.roll(foot, TILE - 2, 0)
                    )

        def unpack_sides(e):
            lo, num = ROUNDS[e]
            side = side_got[e]
            ends = []
            for k in range(2):
                far, near = side[0, k], side[1, k]
                ends.append(pltpu.roll(jnp.where(sub >= TILE - 2, far, near), 2, 0))
            for k in range(2):
                far, near = side[2, k], side[1, k]
                ends.append(pltpu.roll(jnp.where(sub < 2, far, near), TILE - 2, 0))
            for i in range(2 * num):
                c, y = lo + i // 2, i % 2
                slot = i * NSUB
                for strip in range(2):
                    from_west, from_east = ends[2 * strip], ends[2 * strip + 1]
                    from_east = pltpu.roll(from_east, width - slot, 1) if slot else from_east
                    from_west = pltpu.roll(from_west, width - NSUB - slot, 1)
                    edge[c, strip, y, :, pl.ds(width, width)] = jnp.where(
                        lane < NSUB, from_east, jnp.where(lane >= width - NSUB, from_west, 0.0)
                    )

        def derive(load, store):
            conc, act = load(CONC), load(ACTIVE)
            store(STRENGTH, (RELAX * KEEP) * load(MASS) * jnp.exp(CSTAR * (conc - 1.0)) * act)
            store(DRAG, CW * conc * act)

        def derive_main(t):
            r = pl.ds(pl.multiple_of(t * TILE, TILE), TILE)
            for y in range(2):
                def store(c, x):
                    main[c, y, r, :] = x
                derive(lambda c: main[c, y, r, :], store)

        def derive_edges():
            for y in range(2):
                for strip in range(2):
                    def store(c, x):
                        edge[c, strip, y] = x
                    derive(lambda c: edge[c, strip, y], store)

                def store(c, x):
                    flank[c, y] = x
                derive(lambda c: flank[c, y], store)

        def sweep_main(g, stress, velocity):
            spots = [
                pl.ds(pl.multiple_of((g * GROUP + j) * TILE, TILE), TILE) for j in range(GROUP)
            ]
            behind = pl.ds(pl.multiple_of(jnp.maximum(g * GROUP - 1, 0) * TILE, TILE), TILE)
            ahead = pl.ds(
                pl.multiple_of(jnp.minimum(g * GROUP + GROUP, tiles - 1) * TILE, TILE), TILE
            )
            vels = [[(main[U, y, r, :], main[V, y, r, :]) for y in range(2)] for r in spots]
            stresses = []
            if stress:
                follow = (main[U, 0, ahead, :], main[V, 0, ahead, :])
            for j, r in enumerate(spots):
                old = [tuple(main[c, y, r, :] for c in (S1, S2, S12)) for y in range(2)]
                if not stress:
                    stresses.append(old)
                    continue
                beyond = vels[j + 1][0] if j + 1 < GROUP else follow
                row = []
                for y in range(2):
                    u, v = vels[j][y]
                    if y == 0:
                        u_up, v_up = vels[j][1]
                    else:
                        u_up, v_up = (
                            pltpu.roll(jnp.where(sub == 0, after, x), TILE - 1, 0)
                            for x, after in zip(vels[j][0], beyond)
                        )
                    fresh = new_stress(
                        main[STRENGTH, y, r, :], *old[y], u, v,
                        pltpu.roll(u, width - 1, 1), pltpu.roll(v, width - 1, 1), u_up, v_up,
                    )
                    for c, x in zip((S1, S2, S12), fresh):
                        main[c, y, r, :] = x
                    row.append(fresh)
                stresses.append(row)
            if not velocity:
                return
            yy_before = 0.5 * (main[S1, 1, behind, :] - main[S2, 1, behind, :])
            cross_before = main[S12, 1, behind, :]
            for j, r in enumerate(spots):
                xx = [0.5 * (s1 + s2) for s1, s2, _ in stresses[j]]
                yy = [0.5 * (s1 - s2) for s1, s2, _ in stresses[j]]
                cross = [s12 for _, _, s12 in stresses[j]]
                yy_down, cross_down = (
                    [pltpu.roll(jnp.where(sub == TILE - 1, before, x[1]), 1, 0), x[0]]
                    for x, before in ((yy, yy_before), (cross, cross_before))
                )
                yy_before, cross_before = yy[1], cross[1]
                for y in range(2):
                    force_x = xx[y] - pltpu.roll(xx[y], 1, 1) + (cross[y] - cross_down[y])
                    force_y = cross[y] - pltpu.roll(cross[y], 1, 1) + (yy[y] - yy_down[y])
                    u, v = new_velocity(lambda c: main[c, y, r, :], *vels[j][y], force_x, force_y)
                    main[U, y, r, :] = u
                    main[V, y, r, :] = v

        def sweep_edge(stress, velocity):
            lanes = 2 * width

            for strip in range(2):
                vels = [(edge[U, strip, y], edge[V, strip, y]) for y in range(2)]
                fresh = [tuple(edge[c, strip, y] for c in (S1, S2, S12)) for y in range(2)]
                if stress:
                    ups = [vels[1], tuple(pltpu.roll(x, TILE - 1, 0) for x in vels[0])]
                    for y in range(2):
                        east = [pltpu.roll(x, lanes - 1, 1) for x in vels[y]]
                        fresh[y] = new_stress(
                            edge[STRENGTH, strip, y], *fresh[y], *vels[y], *east, *ups[y]
                        )
                        for c, x in zip((S1, S2, S12), fresh[y]):
                            edge[c, strip, y] = x
                if not velocity:
                    continue
                xx = [0.5 * (s1 + s2) for s1, s2, _ in fresh]
                yy = [0.5 * (s1 - s2) for s1, s2, _ in fresh]
                cross = [s12 for _, _, s12 in fresh]
                yy_down, cross_down = ([pltpu.roll(x[1], 1, 0), x[0]] for x in (yy, cross))
                for y in range(2):
                    force_x = xx[y] - pltpu.roll(xx[y], 1, 1) + (cross[y] - cross_down[y])
                    force_y = cross[y] - pltpu.roll(cross[y], 1, 1) + (yy[y] - yy_down[y])
                    u, v = new_velocity(lambda c: edge[c, strip, y], *vels[y], force_x, force_y)
                    edge[U, strip, y] = u
                    edge[V, strip, y] = v

        def sweep_flank(stress, velocity):
            spots = [pl.ds(j * TILE, TILE) for j in range(4)]
            vels = [[(flank[U, y, r, :], flank[V, y, r, :]) for y in range(2)] for r in spots]
            fresh = [
                [tuple(flank[c, y, r, :] for c in (S1, S2, S12)) for y in range(2)] for r in spots
            ]
            if stress:
                for j, r in enumerate(spots):
                    for y in range(2):
                        after = vels[min(j + 1, 3)][y]
                        east = [
                            pltpu.roll(jnp.where(sub == 0, b, x), TILE - 1, 0)
                            for x, b in zip(vels[j][y], after)
                        ]
                        ups = vels[j][1] if y == 0 else [
                            pltpu.roll(x, width - 1, 1) for x in vels[j][0]
                        ]
                        fresh[j][y] = new_stress(
                            flank[STRENGTH, y, r, :], *fresh[j][y], *vels[j][y], *east, *ups
                        )
                        for c, x in zip((S1, S2, S12), fresh[j][y]):
                            flank[c, y, r, :] = x
            if not velocity:
                return
            xx = [[0.5 * (s1 + s2) for s1, s2, _ in row] for row in fresh]
            yy = [[0.5 * (s1 - s2) for s1, s2, _ in row] for row in fresh]
            cross = [[s12 for _, _, s12 in row] for row in fresh]

            def westward(x, j, y):
                before = x[max(j - 1, 0)][y]
                return pltpu.roll(jnp.where(sub == TILE - 1, before, x[j][y]), 1, 0)

            def downward(x, j, y):
                return x[j][0] if y == 1 else pltpu.roll(x[j][1], 1, 1)

            for j, r in enumerate(spots):
                for y in range(2):
                    force_x = xx[j][y] - westward(xx, j, y) + (cross[j][y] - downward(cross, j, y))
                    force_y = cross[j][y] - westward(cross, j, y) + (yy[j][y] - downward(yy, j, y))
                    u, v = new_velocity(lambda c: flank[c, y, r, :], *vels[j][y], force_x, force_y)
                    flank[U, y, r, :] = u
                    flank[V, y, r, :] = v

        with jax.named_scope("i_pack0"):
            pack_rows(0)
            pack_sides(0)
            send_ends(0)
            send_sides(0)
            pack_flank(0)
            send_flank(0)
        tile_loop(tiles, 2, derive_main)

        with jax.named_scope("i_waitids"):
            wait_bytes(ids.at[pl.ds(0, peers - 1)], ids_rsem)
        wanted = me * per
        row_lane = lax.broadcasted_iota(jnp.int32, (per, count), 1)
        row_sub = lax.broadcasted_iota(jnp.int32, (per, count), 0)
        mine = row_lane == row_sub + wanted
        blocks = lax.broadcasted_iota(jnp.int32, (per, count), 1).astype(jnp.float32)
        base = (me * count).astype(jnp.float32)
        for p in range(peers):
            owned = jnp.broadcast_to(ids[p], (per, count)).astype(jnp.float32)
            local = jnp.sum(jnp.where(mine, owned, 0.0), axis=1, keepdims=True) - base
            one_hot[pl.ds(p * per, per), :] = jnp.where(local == blocks, 1.0, 0.0)

        with jax.named_scope("i_waithalo0"):
            for sems in (halo_ssem, early_rsem):
                when_inside(-1, 6, sems.at[0])
                when_inside(1, 6, sems.at[1])
                wait_tiles(2, sems.at[2])
                wait_bytes(main.at[0], sems.at[3])
        with jax.named_scope("i_unpack0"):
            unpack_rows(0)
            unpack_sides(0)
            derive_edges()
        groups = tiles // GROUP
        with jax.named_scope("i_stress"):
            tile_loop(groups, 1, lambda g: sweep_main(g, True, False))
            sweep_edge(True, False)
            sweep_flank(True, False)
        by_slot = one_hot[...]
        to_slots = jnp.concatenate([by_slot.astype(jnp.bfloat16)] * 2, axis=1)
        to_ends = jnp.concatenate([by_slot[:, :TILE], by_slot[:, count - TILE:]] * 2, axis=1)
        to_ends = to_ends.astype(jnp.bfloat16)
        by_block = by_slot.T.astype(jnp.bfloat16)
        to_blocks = jnp.concatenate([by_block] * 2, axis=1)
        columns = jnp.concatenate([by_block] * 2, axis=0)

        with jax.named_scope("i_waitf4"):
            wait_bytes(recv.at[pl.ds(2, 4)], fwd_rsem.at[0])
        for c in range(2):
            both = dot_rows(to_blocks, recv[2 + c])
            for y in range(2):
                main[CUR_X + c, y] = both[:, y * width:(y + 1) * width]
        with jax.named_scope("i_packmid"):
            pack_rows(1)
            pack_sides(1)
            send_ends(1)
            send_sides(1)
            pack_flank(1)
            send_flank(1)
        for c in range(2):
            both = dot_rows(to_blocks, recv[4 + c])
            for y in range(2):
                main[PUSH_X + c, y] = main[MASS, y] * both[:, y * width:(y + 1) * width]
        for y in range(2):
            share = main[CONC, y] * main[ACTIVE, y]
            back[2, :, pl.ds(y * width, width)] = dot_rows(to_slots, share)

        with jax.named_scope("i_waitf2"):
            wait_bytes(recv.at[pl.ds(0, 2)], fwd_rsem.at[1])
        with jax.named_scope("i_push"):
            for c in range(2):
                both = dot_rows(to_blocks, recv[c])
                for y in range(2):
                    main[PUSH_X + c, y] = main[ACTIVE, y] * (
                        main[CONC, y] * both[:, y * width:(y + 1) * width] - main[PUSH_X + c, y]
                    )
        with jax.named_scope("i_packlate"):
            pack_sides(2)
            send_sides(2)
            pack_flank(2)
            send_flank(2)
            pack_rows(2)
            send_ends(2)

        def leave(get, u, v):
            dx, dy = u - get(CUR_X), v - get(CUR_Y)
            drag = get(DRAG) * jnp.sqrt(dx * dx + dy * dy + DRAG_FLOOR)
            return drag * dx, drag * dy

        outer = (lane < NSUB) | (lane >= width - NSUB)

        with jax.named_scope("i_vel1"):
            tile_loop(groups, 1, lambda g: sweep_main(g, False, True))
        with jax.named_scope("i_sweeps"):
            tile_loop((NSUB - 1) * groups, 1, lambda k: sweep_main(k % groups, True, True))
        send_rows(0, back, 2, 1, ret, 2, ret_ssem, ret_rsem.at[0])

        def returned(t):
            r = pl.ds(pl.multiple_of(t * TILE, TILE), TILE)
            block = sub + t * TILE
            theirs = outer | (block < 2) | (block >= count - 2)
            for y in range(2):
                half = pl.ds(y * width, width)
                u, v = main[U, y, r, :], main[V, y, r, :]
                gone = leave(lambda c: main[c, y, r, :], u, v)
                for c in range(2):
                    forc[c, r, half] = jnp.where(theirs, 0.0, gone[c])

        with jax.named_scope("i_back"):
            tile_loop(tiles, 4, returned)
            for c in range(2):
                back[c] = dot_rows(to_slots, forc[c])
        with jax.named_scope("i_waitlate"):
            when_inside(-1, 6, later_rsem.at[0])
            when_inside(1, 6, later_rsem.at[1])
            wait_tiles(4, later_rsem.at[2])
            wait_tiles(16, later_rsem.at[3])

        def sweep_strips(stress, velocity):
            sweep_flank(stress, velocity)
            sweep_edge(stress, velocity)

        with jax.named_scope("i_edge"):
            for e in (1, 2):
                unpack_rows(e)
                unpack_sides(e)
            sweep_strips(False, True)
            for _ in range(NSUB - 1):
                sweep_strips(True, True)

        with jax.named_scope("i_fix"):
            for y in range(2):
                for j, far in ((1, 0), (2, count - TILE)):
                    r = pl.ds(j * TILE, TILE)
                    held = (lane >= 2) & (lane < count - 2)
                    held = held & ((sub < NSUB) if j == 1 else (sub >= TILE - NSUB))
                    u, v = flank[U, y, r, :], flank[V, y, r, :]
                    gone = leave(lambda c: flank[c, y, r, :], u, v)
                    for c in range(2):
                        slot = (c * 2 + y) * 2 * TILE + (TILE if j == 1 else 0)
                        flank_back[pl.ds(slot, TILE), :] = jnp.where(held, gone[c], 0.0)
                        flank_vel[c, y, pl.ds(far, TILE), :] = jnp.where(held, (u, v)[c], 0.0)
                for strip in range(2):
                    def get(c):
                        return edge[c, strip, y, :, pl.ds(0, width)]
                    gone = leave(get, get(U), get(V))
                    held = (sub < 2) if strip == 0 else (sub >= TILE - 2)
                    for c in range(2):
                        moved = pltpu.roll(gone[c], TILE - 2 if strip == 0 else 2, 0)
                        ends[c, pl.ds(strip * TILE, TILE), pl.ds(y * width, width)] = jnp.where(
                            held, moved, 0.0
                        )
            across = lax.dot_general(
                pieces(flank_back[...], 1), columns,
                (((1,), (0,)), ((), ())), preferred_element_type=jnp.float32,
            ).T
            for c in range(2):
                rest = dot_rows(to_ends, ends[c])
                for y in range(2):
                    slot = (c * 2 + y) * 2 * TILE
                    for t in range(tiles):
                        r, half = pl.ds(t * TILE, TILE), pl.ds(y * width, width)
                        moved = pltpu.roll(across[t * TILE:(t + 1) * TILE], width - TILE - slot, 1)
                        back[c, r, half] += jnp.where(outer, moved, 0.0) + (
                            rest[t * TILE:(t + 1) * TILE, y * width:(y + 1) * width]
                        )
            send_rows(0, back, 0, 2, ret, 0, ret_ssem, ret_rsem.at[1])

        same = jnp.where(diag, 1.0, 0.0).astype(jnp.bfloat16)
        same = jnp.concatenate([same] * 2, axis=1)
        for y in range(2):
            for c in range(2):
                half = pl.ds(y * width, width)
                for strip, r in ((0, top), (1, bottom)):
                    end = pltpu.roll(
                        edge[c, strip, y, :, pl.ds(0, width)], TILE - 2 if strip == 0 else 2, 0
                    )
                    held = (sub < 2) if strip == 0 else (sub >= TILE - 2)
                    main[c, y, r, :] = jnp.where(held, end, main[c, y, r, :])
                other = dot_lanes(same, flank_vel[c, y])
                row = lax.broadcasted_iota(jnp.int32, (count, width), 0)
                column = lax.broadcasted_iota(jnp.int32, (count, width), 1)
                theirs = (row >= 2) & (row < count - 2)
                theirs = theirs & ((column < NSUB) | (column >= width - NSUB))
                out[0, c, :, half] = jnp.where(theirs, other, main[c, y])
        wait_bytes(ids.at[pl.ds(0, peers - 1)], ids_ssem)
        wait_bytes(back, ret_ssem)
        when_inside(-1, 6, halo_ssem.at[0])
        when_inside(1, 6, halo_ssem.at[1])
        wait_tiles(4, halo_ssem.at[2])
        wait_tiles(16, halo_ssem.at[3])


def per_device_kernel(n_lat, n_lon, fields, block_owner, ice_covered, land_mask):
    count, cells = land_mask.shape
    peers = n_lat * n_lon
    f32 = jnp.float32
    anywhere = pl.BlockSpec(memory_space=pl.ANY)
    dma = pltpu.SemaphoreType.DMA
    halos = [pltpu.VMEM((2, num // 2, TILE, BX), f32) for _, num in ROUNDS] * 2
    sides = [pltpu.VMEM((2, TILE, BX), f32) for _ in ROUNDS]
    sides += [pltpu.VMEM((3, 2, TILE, BX), f32) for _ in ROUNDS]
    return pl.pallas_call(
        functools.partial(step_kernel, n_lat, n_lon),
        out_shape=pltpu.VMEM((1, 2, count, cells), f32),
        in_specs=[anywhere, anywhere, anywhere, anywhere],
        out_specs=pl.BlockSpec(memory_space=pltpu.VMEM),
        scratch_shapes=[
            pltpu.VMEM((7, count, cells), f32),
            pltpu.VMEM((2, count, cells), f32),
            pltpu.VMEM((3, count, cells), f32),
            pltpu.VMEM((1, count), jnp.int32),
            pltpu.VMEM((1, count), jnp.int32),
            pltpu.VMEM((peers, 1, count), jnp.int32),
            pltpu.VMEM((6, count, cells), f32),
            pltpu.VMEM((2, count, cells), f32),
            pltpu.VMEM((count, count), f32),
            pltpu.VMEM((3, count, cells), f32),
            pltpu.VMEM((count, cells), jnp.int32),
            pltpu.VMEM((14, 2, count, BX), f32),
            pltpu.VMEM((14, 2, 2, TILE, 2 * BX), f32),
            pltpu.VMEM((14, 2, 4 * TILE, BX), f32),
            pltpu.VMEM((BX, count), f32),
            pltpu.VMEM((2, 2, BX, count), f32),
            pltpu.VMEM((2, 2 * TILE, cells), f32),
            *halos, *sides,
            dma((5,)), dma, dma, dma, dma((2,)), dma, dma((2,)),
            dma((4,)), dma((4,)), dma((4,)),
            pltpu.SemaphoreType.REGULAR,
        ],
        compiler_params=pltpu.CompilerParams(
            collective_id=0, has_side_effects=True, vmem_limit_bytes=63 * 1024 * 1024
        ),
    )(fields, block_owner.reshape(1, count), ice_covered.reshape(1, count), land_mask)


def solution(mesh):
    placed = (
        P("comp", None, ("lat", "lon"), None),
        P(("lat", "lon")),
        P(("lat", "lon")),
        P(("lat", "lon"), None),
    )
    n_lat, n_lon = mesh.shape["lat"], mesh.shape["lon"]

    def body(fields, block_owner, ice_covered, land_mask):
        count = block_owner.shape[0]
        whole_tiles = count % (n_lat * n_lon * TILE) == 0 and count == BX
        if whole_tiles and n_lon > 2:
            return per_device_kernel(n_lat, n_lon, fields, block_owner, ice_covered, land_mask)
        return per_device(fields, block_owner, ice_covered, land_mask)

    return jax.shard_map(
        body,
        mesh=mesh,
        in_specs=placed,
        out_specs=P("comp", None, ("lat", "lon"), None),
        check_vma=False,
    )
```

```python
import functools

import jax
import jax.numpy as jnp
from jax import lax
from jax.experimental import pallas as pl
from jax.experimental.pallas import tpu as pltpu
from jax.sharding import PartitionSpec as P

GX = 1
BY = 2
BX = 128
NSUB = 4


CD_ICE = 0.1
CW = 1.5
CSTAR = 2.0
ECC2 = 4.0
DMIN2 = 0.25
RELAX = 0.5
DTE = 0.5
CORIO = 0.3
MASS_FLOOR = 0.5
DRAG_FLOOR = 0.1


def from_behind(x, axis, by):
    size = lax.axis_size(axis)
    pairs = [(i, i + by) for i in range(size) if 0 <= i + by < size]
    return lax.ppermute(x, axis, pairs)


def with_halo(x, sides, width, wrap):
    for axis, dim in sides:
        size, length = (lax.axis_size(axis), x.shape[dim])
        up = [(i, (i + 1) % size) for i in range(size if wrap else size - 1)]
        down = [(j, i) for i, j in up]
        last = lax.slice_in_dim(x, length - width, length, axis=dim)
        first = lax.slice_in_dim(x, 0, width, axis=dim)
        before = lax.ppermute(last, axis, up)
        after = lax.ppermute(first, axis, down)
        x = jnp.concatenate([before, x, after], axis=dim)
    return x


def air_stress(ocean):
    wind_x, wind_y, current_x, current_y, tilt_x, tilt_y, density = ocean
    speed_ice = jnp.sqrt(wind_x * wind_x + wind_y * wind_y + 1.0)
    scale_ice = density * CD_ICE * speed_ice
    rel_x = wind_x - current_x
    rel_y = wind_y - current_y
    speed_open = jnp.sqrt(rel_x * rel_x + rel_y * rel_y + 1.0)
    scale_open = density * (0.1 + 0.05 * speed_open) * speed_open
    outbound = jnp.stack(
        [scale_ice * wind_x, scale_ice * wind_y, current_x, current_y, tilt_x, tilt_y]
    )
    open_stress = jnp.stack([scale_open * rel_x, scale_open * rel_y])
    return (outbound, open_stress)


def prepare(ice_tile, forcing, active):
    ice_mass = ice_tile[2]
    concentration = ice_tile[3]
    strength = ice_mass * jnp.exp(CSTAR * (concentration - 1.0)) * active
    drag_base = CW * concentration * active
    push_x = active * (concentration * forcing[0] - ice_mass * forcing[4])
    push_y = active * (concentration * forcing[1] - ice_mass * forcing[5])
    return jnp.stack(
        [strength, ice_mass, drag_base, push_x, push_y, forcing[2], forcing[3], active]
    )


def subcycle(ice_state, statics):
    east_vel, north_vel, stress_one, stress_two, stress_three = ice_state
    strength = statics[0]
    east_base = east_vel[:-1, :-1]
    north_base = north_vel[:-1, :-1]
    strain_xx = east_vel[:-1, 1:] - east_base
    strain_yy = north_vel[1:, :-1] - north_base
    shear = east_vel[1:, :-1] - east_base + (north_vel[:-1, 1:] - north_base)
    divergence = strain_xx + strain_yy
    tension = strain_xx - strain_yy
    delta_norm = jnp.sqrt(
        divergence * divergence + (tension * tension + shear * shear) / ECC2 + DMIN2
    )
    viscosity = strength[:-1, :-1] / delta_norm
    stress_sum = (stress_one[:-1, :-1] + RELAX * viscosity * (divergence - delta_norm)) / (
        1.0 + RELAX
    )
    stress_diff = (stress_two[:-1, :-1] + RELAX * viscosity * tension / ECC2) / (1.0 + RELAX)
    stress_shear = (stress_three[:-1, :-1] + RELAX * viscosity * shear / (2.0 * ECC2)) / (
        1.0 + RELAX
    )
    stress_xx = 0.5 * (stress_sum + stress_diff)
    stress_yy = 0.5 * (stress_sum - stress_diff)
    force_x = (
        stress_xx[1:, 1:] - stress_xx[1:, :-1] + (stress_shear[1:, 1:] - stress_shear[:-1, 1:])
    )
    force_y = (
        stress_shear[1:, 1:] - stress_shear[1:, :-1] + (stress_yy[1:, 1:] - stress_yy[:-1, 1:])
    )
    trimmed = statics[:, 1:-1, 1:-1]
    strength, ice_mass, drag_base, push_x, push_y, current_x, current_y, active = trimmed
    east_old = east_vel[1:-1, 1:-1]
    north_old = north_vel[1:-1, 1:-1]
    diff_x = current_x - east_old
    diff_y = current_y - north_old
    drag_coef = drag_base * jnp.sqrt(diff_x * diff_x + diff_y * diff_y + DRAG_FLOOR)
    denominator = jnp.maximum(ice_mass, MASS_FLOOR) / DTE + drag_coef
    east_new = (
        active
        * (
            ice_mass / DTE * east_old
            + force_x
            + push_x
            + drag_coef * current_x
            + CORIO * ice_mass * north_old
        )
        / denominator
    )
    north_new = (
        active
        * (
            ice_mass / DTE * north_old
            + force_y
            + push_y
            + drag_coef * current_y
            - CORIO * ice_mass * east_old
        )
        / denominator
    )
    new_state = jnp.stack(
        [east_new, north_new, stress_sum[1:, 1:], stress_diff[1:, 1:], stress_shear[1:, 1:]]
    )
    return (new_state, trimmed)


def give_back(ice_state, statics):
    east_vel = ice_state[0]
    north_vel = ice_state[1]
    drag_base = statics[2]
    current_x = statics[5]
    current_y = statics[6]
    diff_x = east_vel - current_x
    diff_y = north_vel - current_y
    factor = drag_base * jnp.sqrt(diff_x * diff_x + diff_y * diff_y + DRAG_FLOOR)
    return jnp.stack([factor * diff_x, factor * diff_y, drag_base / CW])


def to_tile(blocks):
    channels, count, cells = blocks.shape
    arranged = blocks.reshape(channels, count // GX, GX, BY, BX).transpose(0, 1, 3, 2, 4)
    return arranged.reshape(channels, count // GX * BY, GX * BX)


def from_tile(values):
    channels, rows, columns = values.shape
    arranged = values.reshape(channels, rows // BY, BY, GX, BX).transpose(0, 1, 3, 2, 4)
    return arranged.reshape(channels, rows // BY * GX, BY * BX)


def per_device(fields, block_owner, ice_covered, land_mask):
    count = block_owner.shape[0]
    is_ocean = lax.axis_index("comp") == 0
    outbound, open_stress = air_stress(fields[0])
    owner_row = block_owner.reshape(1, count)
    crossed = from_behind(outbound, "comp", 1)
    received, anchor = (
        lax.all_to_all(crossed, ("lat", "lon"), split_axis=1, concat_axis=1, tiled=True),
        lax.all_to_all(owner_row, ("lat", "lon"), split_axis=1, concat_axis=1, tiled=True),
    )
    local_ids = anchor[0] % count
    position = jnp.zeros((count,), jnp.int32).at[local_ids].set(jnp.arange(count, dtype=jnp.int32))
    forcing = to_tile(received[:, position])
    ice_tile = to_tile(fields[0])
    covered = ice_covered.astype(jnp.float32)[:, None] * (1 - land_mask).astype(jnp.float32)
    active = to_tile(covered[None])[0]
    statics = prepare(ice_tile, forcing, active)
    ice_state = jnp.stack([ice_tile[0], ice_tile[1], ice_tile[4], ice_tile[5], ice_tile[6]])
    joined = jnp.concatenate([ice_state, statics], 0)
    joined = with_halo(joined, (("lon", 2),), NSUB, True)
    joined = with_halo(joined, (("lat", 1),), NSUB, False)
    ice_state = joined[:5]
    statics = joined[5:]
    for repeat in range(NSUB):
        ice_state, statics = subcycle(ice_state, statics)
    returned = from_tile(give_back(ice_state, statics))
    back_send = returned[:, local_ids]
    regrouped = lax.all_to_all(back_send, ("lat", "lon"), split_axis=1, concat_axis=1, tiled=True)
    received_back = from_behind(regrouped, "comp", -1)
    ocean_out = received_back[:2] + (1.0 - received_back[2]) * open_stress
    ice_out = from_tile(ice_state[:2])
    return jnp.where(is_ocean, ocean_out, ice_out)[None]


TILE = 8
GROUP = 8
MESH = pl.DeviceIdType.MESH
U, V, MASS, CONC, S1, S2, S12, ACTIVE, PUSH_X, PUSH_Y, CUR_X, CUR_Y, STRENGTH, DRAG = range(14)
SIDES = [(a, b) for b in (-1, 1) for a in (-1, 1, 0)]
ROUNDS = ((U, 8), (CUR_X, 2), (PUSH_X, 2))
KEEP = 1.0 / (1.0 + RELAX)


def tile_loop(tiles, together, body):
    def step(k, carry):
        for j in range(together):
            body(k * together + j)
        return carry
    lax.fori_loop(0, tiles // together, step, 0)


def pieces(values, axis):
    high = values.astype(jnp.bfloat16)
    low = (values - high.astype(jnp.float32)).astype(jnp.bfloat16)
    return jnp.concatenate([high, low], axis=axis)


def dot_rows(twice, values):
    return lax.dot_general(
        twice, pieces(values, 0), (((1,), (0,)), ((), ())), preferred_element_type=jnp.float32
    )


def dot_lanes(twice, values):
    return lax.dot_general(
        twice, pieces(values, 1), (((1,), (1,)), ((), ())), preferred_element_type=jnp.float32
    )


def new_stress(strength, s1, s2, s12, u, v, u_east, v_east, u_up, v_up):
    sxx = u_east - u
    syy = v_up - v
    shear = (u_up - u) + (v_east - v)
    div = sxx + syy
    ten = sxx - syy
    square = div * div + (ten * ten + shear * shear) * (1.0 / ECC2) + DMIN2
    inverse = lax.rsqrt(square)
    visc = strength * inverse
    s1 = s1 * KEEP + visc * (div - square * inverse)
    s2 = s2 * KEEP + visc * ten * (1.0 / ECC2)
    s12 = s12 * KEEP + visc * shear * (0.5 / ECC2)
    return s1, s2, s12


def new_velocity(get, u, v, force_x, force_y):
    mass, cx, cy = get(MASS), get(CUR_X), get(CUR_Y)
    dx, dy = cx - u, cy - v
    square = dx * dx + dy * dy + DRAG_FLOOR
    drag = get(DRAG) * (square * lax.rsqrt(square))
    gain = get(ACTIVE) / (jnp.maximum(mass, MASS_FLOOR) * (1.0 / DTE) + drag)
    inertia = mass * (1.0 / DTE)
    turn = CORIO * mass
    return (
        gain * (inertia * u + force_x + get(PUSH_X) + drag * cx + turn * v),
        gain * (inertia * v + force_y + get(PUSH_Y) + drag * cy - turn * u),
    )


def step_kernel(
    n_lat, n_lon,
    fields, owner_hbm, covered_hbm, land, out,
    surf, open_st, ret, owner, covered, ids, recv, forc, one_hot, back, land_v,
    main, edge, flank, flank_back, flank_vel, ends, near_push,
    rows_out0, rows_out1, rows_out2, rows_got0, rows_got1, rows_got2,
    side_out0, side_out1, side_out2, side_got0, side_got1, side_got2,
    bulk_ssem, bulk_rsem, ids_ssem, ids_rsem, halo_ssem, early_rsem, mid_rsem, late_rsem, ready,
):
    comp = lax.axis_index("comp")
    lat = lax.axis_index("lat")
    lon = lax.axis_index("lon")
    peers = n_lat * n_lon
    me = lat * n_lon + lon
    count = owner.shape[1]
    per = count // peers
    width = BX
    barrier = pltpu.get_barrier_semaphore()
    rows_out = (rows_out0, rows_out1, rows_out2)
    rows_got = (rows_got0, rows_got1, rows_got2)
    side_out = (side_out0, side_out1, side_out2)
    side_got = (side_got0, side_got1, side_got2)

    def rows_of(peer):
        return pl.ds(pl.multiple_of(peer * per, per), per)

    planes = [jnp.where(lat < n_lat // 2, n_lat - 1 - j, j) for j in range(n_lat)]
    places = [(lon + i) % n_lon for i in range(n_lon)]

    half_lat = n_lat // 2
    groups_of = {
        "all": ((planes, places),),
        "column": ((planes[:half_lat], places[:1]),),
        "beyond": ((planes[:half_lat], places[1:]),),
        "near": ((planes[half_lat:], places),),
    }

    def each_peer(body, part="all"):
        for chosen, along in groups_of[part]:
            for plane in chosen:
                for place in along:
                    body(plane * n_lon + place, plane, place)

    def home_first(body):
        body(0, 0, 0)
        for plane in range(n_lat):
            for place in places:
                if plane:
                    body(plane * n_lon + place, plane, place)
                else:
                    @pl.when(place > 0)
                    def _():
                        body(place, 0, place)

    def signal_peers(kind, part="all"):
        each_peer(
            lambda p, plane, place: pl.semaphore_signal(
                barrier, inc=1, device_id=(kind, plane, place), device_id_type=MESH
            ),
            part,
        )

    def send_rows(kind, src, lo, num, dst, dlo, ssem, rsem, part="all"):
        def body(p, plane, place):
            pltpu.make_async_remote_copy(
                src_ref=src.at[pl.ds(lo, num), rows_of(p), :],
                dst_ref=dst.at[pl.ds(dlo, num), rows_of(me), :],
                send_sem=ssem, recv_sem=rsem,
                device_id=(kind, plane, place), device_id_type=MESH,
            ).start()
        home_first(body) if part == "home" else each_peer(body, part)

    def wait_bytes(ref, sem):
        pltpu.make_async_copy(ref, ref, sem).wait()

    def wait_tiles(num, sem):
        wait_bytes(main.at[0, 0, pl.ds(0, num * TILE), :], sem)

    @pl.when(comp == 0)
    def _ocean():
        signal_peers(1)
        raw = pltpu.make_async_copy(fields.at[0, pl.ds(2, 4)], surf.at[pl.ds(2, 4)], halo_ssem.at[0])
        wind = pltpu.make_async_copy(fields.at[0, pl.ds(0, 2)], surf.at[pl.ds(0, 2)], halo_ssem.at[1])
        rho = pltpu.make_async_copy(fields.at[0, pl.ds(6, 1)], surf.at[pl.ds(6, 1)], halo_ssem.at[2])
        raw.start()
        wind.start()
        rho.start()
        with jax.named_scope("o_barrier"):
            pl.semaphore_wait(barrier, half_lat)

        def send_four(part):
            send_rows(1, surf, 2, 4, recv, 2, bulk_ssem, bulk_rsem.at[0], part)

        def send_two(part):
            send_rows(1, forc, 0, 2, recv, 0, bulk_ssem, bulk_rsem.at[1], part)

        with jax.named_scope("o_send4"):
            raw.wait()
            send_four("column")
            wind.wait()
            rho.wait()

        def stress(t):
            r = pl.ds(pl.multiple_of(t * TILE, TILE), TILE)
            wx, wy, density = surf[0, r, :], surf[1, r, :], surf[6, r, :]
            scale = density * CD_ICE * jnp.sqrt(wx * wx + wy * wy + 1.0)
            forc[0, r, :] = scale * wx
            forc[1, r, :] = scale * wy

        with jax.named_scope("o_stress"):
            tile_loop(count // TILE, 4, stress)
            send_two("column")
        with jax.named_scope("o_ready"):
            pl.semaphore_wait(ready, 1)
        with jax.named_scope("o_rest"):
            send_four("beyond")
            send_two("beyond")
            send_four("near")
            send_two("near")

        def open_water(t):
            r = pl.ds(pl.multiple_of(t * TILE, TILE), TILE)
            density = surf[6, r, :]
            rel_x = surf[0, r, :] - surf[2, r, :]
            rel_y = surf[1, r, :] - surf[3, r, :]
            speed = jnp.sqrt(rel_x * rel_x + rel_y * rel_y + 1.0)
            scale = density * (0.1 + 0.05 * speed) * speed
            open_st[0, r, :] = scale * rel_x
            open_st[1, r, :] = scale * rel_y

        tile_loop(count // TILE, 2, open_water)
        with jax.named_scope("o_waitret1"):
            wait_bytes(ret.at[pl.ds(2, 1)], bulk_rsem.at[0])

        def water(t):
            r = pl.ds(pl.multiple_of(t * TILE, TILE), TILE)
            share = 1.0 - ret[2, r, :]
            for c in range(2):
                open_st[c, r, :] = share * open_st[c, r, :]

        tile_loop(count // TILE, 4, water)
        with jax.named_scope("o_waitret2"):
            wait_bytes(ret.at[pl.ds(0, 2)], bulk_rsem.at[1])

        def finish(t):
            r = pl.ds(pl.multiple_of(t * TILE, TILE), TILE)
            for c in range(2):
                out[0, c, r, :] = ret[c, r, :] + open_st[c, r, :]

        tile_loop(count // TILE, 4, finish)
        wait_bytes(surf.at[pl.ds(0, 6)], bulk_ssem)

    @pl.when(comp == 1)
    def _ice():
        def inside(a):
            if a == 0:
                return lat >= 0
            return lat + a >= 0 if a < 0 else lat + a < n_lat

        def around(a, b):
            return (1, lat + a, (lon + b + n_lon) % n_lon)

        signal_peers(0, "column")
        for a in range(n_lat):
            for b in range(n_lon):
                if a or b:
                    pl.semaphore_signal(
                        barrier, inc=1, device_id=(1, (lat + a) % n_lat, (lon + b) % n_lon),
                        device_id_type=MESH,
                    )
        for y in range(2):
            pltpu.make_async_copy(
                fields.at[0, :, :, pl.ds(y * width, width)], main.at[pl.ds(0, 7), y], halo_ssem.at[0]
            ).start()
        loads = [
            pltpu.make_async_copy(land, land_v, halo_ssem.at[1]),
            pltpu.make_async_copy(covered_hbm, covered, halo_ssem.at[2]),
        ]
        names = pltpu.make_async_copy(owner_hbm, owner, halo_ssem.at[3])
        names.start()
        for load in loads:
            load.start()
        with jax.named_scope("i_barrier"):
            pl.semaphore_wait(barrier, 2 * peers - 1)
            pl.semaphore_signal(ready, inc=1, device_id=(0, lat, lon), device_id_type=MESH)
            names.wait()
            for a in range(n_lat):
                for b in range(n_lon):
                    if a or b:
                        pltpu.make_async_remote_copy(
                            src_ref=owner, dst_ref=ids.at[me], send_sem=ids_ssem, recv_sem=ids_rsem,
                            device_id=(1, (lat + a) % n_lat, (lon + b) % n_lon),
                            device_id_type=MESH,
                        ).start()
        ids[me] = owner[...]

        tiles = count // TILE
        top, bottom = pl.ds(0, TILE), pl.ds(count - TILE, TILE)
        zero_tile = jnp.zeros((TILE, width), jnp.float32)
        for wall, which in ((lat == 0, 0), (lat == n_lat - 1, 1)):
            @pl.when(wall)
            def _():
                for e in range(3):
                    for k in range(rows_got[e].shape[1]):
                        rows_got[e][which, k] = zero_tile
                    for k in range(2):
                        side_got[e][2 * which, k] = zero_tile

        def clear(t):
            r = pl.ds(pl.multiple_of(t * TILE, TILE), TILE)
            for c in range(2):
                for y in range(2):
                    flank_vel[c, y, r, :] = zero_tile
            flank_back[r, :] = zero_tile

        tile_loop(tiles, 2, clear)
        wait_bytes(main.at[pl.ds(0, 7)], halo_ssem.at[0])
        for load in loads:
            load.wait()
        diag = lax.broadcasted_iota(jnp.int32, (count, count), 0) == lax.broadcasted_iota(
            jnp.int32, (count, count), 1
        )
        wet = jnp.sum(
            jnp.where(diag, covered[...].astype(jnp.float32), 0.0), axis=1, keepdims=True
        )
        sea = wet * (1 - land_v[...]).astype(jnp.float32)
        for y in range(2):
            main[ACTIVE, y] = sea[:, y * width:(y + 1) * width]

        lane = lax.broadcasted_iota(jnp.int32, (TILE, width), 1)
        sub = lax.broadcasted_iota(jnp.int32, (TILE, width), 0)
        pick_row = lax.broadcasted_iota(jnp.int32, (2 * TILE, width), 0)
        pick_col = lax.broadcasted_iota(jnp.int32, (2 * TILE, width), 1)
        picked = jnp.where(pick_row < TILE, pick_row, pick_row + (width - 2 * TILE)) == pick_col
        picker = jnp.where(picked, 1.0, 0.0).astype(jnp.bfloat16)
        picker = jnp.concatenate([picker] * 2, axis=1)

        def end_of(e, c, y, k):
            if e == 2:
                return near_push[c - PUSH_X, y, k]
            return main[c, y, (top, bottom)[k], :]

        def pack_rows(e):
            lo, num = ROUNDS[e]
            for k in range(num // 2):
                ups, downs = zero_tile, zero_tile
                for i in range(4):
                    c, y = lo + 2 * k + i // 2, i % 2
                    head, foot = end_of(e, c, y, 0), end_of(e, c, y, 1)
                    here = (sub >= 2 * i) & (sub < 2 * i + 2)
                    ups = jnp.where(here, pltpu.roll(head, 2 * i, 0) if i else head, ups)
                    downs = jnp.where(here, pltpu.roll(foot, (2 * i + 2) % TILE, 0) if i < 3 else foot, downs)
                rows_out[e][0, k] = ups
                rows_out[e][1, k] = downs

        def pack_sides(e):
            lo, num = ROUNDS[e]
            west, east = zero_tile, zero_tile
            for i in range(2 * num):
                c, y = lo + i // 2, i % 2
                ends = jnp.where(sub < NSUB, end_of(e, c, y, 0), end_of(e, c, y, 1))
                slot = i * NSUB
                mine = (lane >= slot) & (lane < slot + NSUB)
                west = jnp.where(mine, pltpu.roll(ends, slot, 1) if slot else ends, west)
                east = jnp.where(mine, pltpu.roll(ends, (slot + NSUB) % width, 1), east)
            side_out[e][0] = west
            side_out[e][1] = east

        def pack_flank(e):
            lo, num = ROUNDS[e]
            for c in range(lo, lo + num):
                for y in range(2):
                    across = dot_lanes(picker, main[c, y])
                    flank[c, y, pl.ds(TILE, TILE), :] = across[:TILE]
                    flank[c, y, pl.ds(2 * TILE, TILE), :] = across[TILE:]

        def push_on(e, a, b, src, dst, lane_of_sem, recv_lane):
            sems = (early_rsem, mid_rsem, late_rsem)[e]

            @pl.when(inside(a))
            def _():
                pltpu.make_async_remote_copy(
                    src_ref=src, dst_ref=dst,
                    send_sem=halo_ssem.at[lane_of_sem], recv_sem=sems.at[recv_lane],
                    device_id=around(a, b), device_id_type=MESH,
                ).start()

        def send_ends(e):
            for a in (-1, 1):
                k = 1 if a > 0 else 0
                push_on(e, a, 0, rows_out[e].at[k], rows_got[e].at[1 - k], k, 1 - k)

        def send_sides(e):
            for a, b in SIDES:
                k = 1 if b > 0 else 0
                group = {0: 2, -1: 0, 1: 1}[a]
                land_in = {0: 2, -1: 1, 1: 0}[a]
                push_on(e, a, b, side_out[e].at[k], side_got[e].at[1 - a, 1 - k], group, land_in)

        def send_flank(e):
            lo, num = ROUNDS[e]
            for b in (-1, 1):
                src, dst = (2 * TILE, 0) if b > 0 else (TILE, 3 * TILE)
                push_on(
                    e, 0, b,
                    flank.at[pl.ds(lo, num), :, pl.ds(src, TILE), :],
                    flank.at[pl.ds(lo, num), :, pl.ds(dst, TILE), :], 3, 3,
                )

        def when_inside(a, num, sem):
            @pl.when(inside(a))
            def _():
                wait_tiles(num, sem)

        def unpack_rows(e):
            lo, num = ROUNDS[e]
            got = rows_got[e]
            for k in range(num // 2):
                for i in range(4):
                    c, y = lo + 2 * k + i // 2, i % 2
                    north = pltpu.roll(got[0, k], (TILE - 2 * i) % TILE, 0) if i else got[0, k]
                    south = pltpu.roll(got[1, k], TILE - 2 - 2 * i, 0) if i < 3 else got[1, k]
                    head, foot = main[c, y, top, :], main[c, y, bottom, :]
                    edge[c, 0, y, :, pl.ds(0, width)] = jnp.where(
                        sub < 2, north, pltpu.roll(head, 2, 0)
                    )
                    edge[c, 1, y, :, pl.ds(0, width)] = jnp.where(
                        sub >= TILE - 2, south, pltpu.roll(foot, TILE - 2, 0)
                    )

        def unpack_sides(e):
            lo, num = ROUNDS[e]
            side = side_got[e]
            ends = []
            for k in range(2):
                far, near = side[0, k], side[1, k]
                ends.append(pltpu.roll(jnp.where(sub >= TILE - 2, far, near), 2, 0))
            for k in range(2):
                far, near = side[2, k], side[1, k]
                ends.append(pltpu.roll(jnp.where(sub < 2, far, near), TILE - 2, 0))
            for i in range(2 * num):
                c, y = lo + i // 2, i % 2
                slot = i * NSUB
                for strip in range(2):
                    from_west, from_east = ends[2 * strip], ends[2 * strip + 1]
                    from_east = pltpu.roll(from_east, width - slot, 1) if slot else from_east
                    from_west = pltpu.roll(from_west, width - NSUB - slot, 1)
                    edge[c, strip, y, :, pl.ds(width, width)] = jnp.where(
                        lane < NSUB, from_east, jnp.where(lane >= width - NSUB, from_west, 0.0)
                    )

        def derive(load, store):
            conc, act = load(CONC), load(ACTIVE)
            store(STRENGTH, (RELAX * KEEP) * load(MASS) * jnp.exp(CSTAR * (conc - 1.0)) * act)
            store(DRAG, CW * conc * act)

        def derive_main(t):
            r = pl.ds(pl.multiple_of(t * TILE, TILE), TILE)
            for y in range(2):
                def store(c, x):
                    main[c, y, r, :] = x
                derive(lambda c: main[c, y, r, :], store)

        def derive_edges():
            for y in range(2):
                for strip in range(2):
                    def store(c, x):
                        edge[c, strip, y] = x
                    derive(lambda c: edge[c, strip, y], store)

                def store(c, x):
                    flank[c, y] = x
                derive(lambda c: flank[c, y], store)

        def sweep_main(g, stress, velocity):
            spots = [
                pl.ds(pl.multiple_of((g * GROUP + j) * TILE, TILE), TILE) for j in range(GROUP)
            ]
            behind = pl.ds(pl.multiple_of(jnp.maximum(g * GROUP - 1, 0) * TILE, TILE), TILE)
            ahead = pl.ds(
                pl.multiple_of(jnp.minimum(g * GROUP + GROUP, tiles - 1) * TILE, TILE), TILE
            )
            vels = [[(main[U, y, r, :], main[V, y, r, :]) for y in range(2)] for r in spots]
            stresses = []
            if stress:
                follow = (main[U, 0, ahead, :], main[V, 0, ahead, :])
            for j, r in enumerate(spots):
                old = [tuple(main[c, y, r, :] for c in (S1, S2, S12)) for y in range(2)]
                if not stress:
                    stresses.append(old)
                    continue
                beyond = vels[j + 1][0] if j + 1 < GROUP else follow
                row = []
                for y in range(2):
                    u, v = vels[j][y]
                    if y == 0:
                        u_up, v_up = vels[j][1]
                    else:
                        u_up, v_up = (
                            pltpu.roll(jnp.where(sub == 0, after, x), TILE - 1, 0)
                            for x, after in zip(vels[j][0], beyond)
                        )
                    fresh = new_stress(
                        main[STRENGTH, y, r, :], *old[y], u, v,
                        pltpu.roll(u, width - 1, 1), pltpu.roll(v, width - 1, 1), u_up, v_up,
                    )
                    for c, x in zip((S1, S2, S12), fresh):
                        main[c, y, r, :] = x
                    row.append(fresh)
                stresses.append(row)
            if not velocity:
                return
            yy_before = 0.5 * (main[S1, 1, behind, :] - main[S2, 1, behind, :])
            cross_before = main[S12, 1, behind, :]
            for j, r in enumerate(spots):
                xx = [0.5 * (s1 + s2) for s1, s2, _ in stresses[j]]
                yy = [0.5 * (s1 - s2) for s1, s2, _ in stresses[j]]
                cross = [s12 for _, _, s12 in stresses[j]]
                yy_down, cross_down = (
                    [pltpu.roll(jnp.where(sub == TILE - 1, before, x[1]), 1, 0), x[0]]
                    for x, before in ((yy, yy_before), (cross, cross_before))
                )
                yy_before, cross_before = yy[1], cross[1]
                for y in range(2):
                    force_x = xx[y] - pltpu.roll(xx[y], 1, 1) + (cross[y] - cross_down[y])
                    force_y = cross[y] - pltpu.roll(cross[y], 1, 1) + (yy[y] - yy_down[y])
                    u, v = new_velocity(lambda c: main[c, y, r, :], *vels[j][y], force_x, force_y)
                    main[U, y, r, :] = u
                    main[V, y, r, :] = v

        def sweep_edge(stress, velocity):
            lanes = 2 * width

            for strip in range(2):
                vels = [(edge[U, strip, y], edge[V, strip, y]) for y in range(2)]
                fresh = [tuple(edge[c, strip, y] for c in (S1, S2, S12)) for y in range(2)]
                if stress:
                    ups = [vels[1], tuple(pltpu.roll(x, TILE - 1, 0) for x in vels[0])]
                    for y in range(2):
                        east = [pltpu.roll(x, lanes - 1, 1) for x in vels[y]]
                        fresh[y] = new_stress(
                            edge[STRENGTH, strip, y], *fresh[y], *vels[y], *east, *ups[y]
                        )
                        for c, x in zip((S1, S2, S12), fresh[y]):
                            edge[c, strip, y] = x
                if not velocity:
                    continue
                xx = [0.5 * (s1 + s2) for s1, s2, _ in fresh]
                yy = [0.5 * (s1 - s2) for s1, s2, _ in fresh]
                cross = [s12 for _, _, s12 in fresh]
                yy_down, cross_down = ([pltpu.roll(x[1], 1, 0), x[0]] for x in (yy, cross))
                for y in range(2):
                    force_x = xx[y] - pltpu.roll(xx[y], 1, 1) + (cross[y] - cross_down[y])
                    force_y = cross[y] - pltpu.roll(cross[y], 1, 1) + (yy[y] - yy_down[y])
                    u, v = new_velocity(lambda c: edge[c, strip, y], *vels[y], force_x, force_y)
                    edge[U, strip, y] = u
                    edge[V, strip, y] = v

        def sweep_flank(stress, velocity):
            spots = [pl.ds(j * TILE, TILE) for j in range(4)]
            vels = [[(flank[U, y, r, :], flank[V, y, r, :]) for y in range(2)] for r in spots]
            fresh = [
                [tuple(flank[c, y, r, :] for c in (S1, S2, S12)) for y in range(2)] for r in spots
            ]
            if stress:
                for j, r in enumerate(spots):
                    for y in range(2):
                        after = vels[min(j + 1, 3)][y]
                        east = [
                            pltpu.roll(jnp.where(sub == 0, b, x), TILE - 1, 0)
                            for x, b in zip(vels[j][y], after)
                        ]
                        ups = vels[j][1] if y == 0 else [
                            pltpu.roll(x, width - 1, 1) for x in vels[j][0]
                        ]
                        fresh[j][y] = new_stress(
                            flank[STRENGTH, y, r, :], *fresh[j][y], *vels[j][y], *east, *ups
                        )
                        for c, x in zip((S1, S2, S12), fresh[j][y]):
                            flank[c, y, r, :] = x
            if not velocity:
                return
            xx = [[0.5 * (s1 + s2) for s1, s2, _ in row] for row in fresh]
            yy = [[0.5 * (s1 - s2) for s1, s2, _ in row] for row in fresh]
            cross = [[s12 for _, _, s12 in row] for row in fresh]

            def westward(x, j, y):
                before = x[max(j - 1, 0)][y]
                return pltpu.roll(jnp.where(sub == TILE - 1, before, x[j][y]), 1, 0)

            def downward(x, j, y):
                return x[j][0] if y == 1 else pltpu.roll(x[j][1], 1, 1)

            for j, r in enumerate(spots):
                for y in range(2):
                    force_x = xx[j][y] - westward(xx, j, y) + (cross[j][y] - downward(cross, j, y))
                    force_y = cross[j][y] - westward(cross, j, y) + (yy[j][y] - downward(yy, j, y))
                    u, v = new_velocity(lambda c: flank[c, y, r, :], *vels[j][y], force_x, force_y)
                    flank[U, y, r, :] = u
                    flank[V, y, r, :] = v

        with jax.named_scope("i_pack0"):
            pack_rows(0)
            pack_sides(0)
            send_ends(0)
            send_sides(0)
            pack_flank(0)
            send_flank(0)
        tile_loop(tiles, 2, derive_main)

        with jax.named_scope("i_waitids"):
            wait_bytes(ids.at[pl.ds(0, peers - 1)], ids_rsem)
        wanted = me * per
        row_lane = lax.broadcasted_iota(jnp.int32, (per, count), 1)
        row_sub = lax.broadcasted_iota(jnp.int32, (per, count), 0)
        mine = row_lane == row_sub + wanted
        blocks = lax.broadcasted_iota(jnp.int32, (per, count), 1).astype(jnp.float32)
        base = (me * count).astype(jnp.float32)
        for p in range(peers):
            owned = jnp.broadcast_to(ids[p], (per, count)).astype(jnp.float32)
            local = jnp.sum(jnp.where(mine, owned, 0.0), axis=1, keepdims=True) - base
            one_hot[pl.ds(p * per, per), :] = jnp.where(local == blocks, 1.0, 0.0)

        with jax.named_scope("i_waithalo0"):
            for sems in (halo_ssem, early_rsem):
                when_inside(-1, 6, sems.at[0])
                when_inside(1, 6, sems.at[1])
                wait_tiles(2, sems.at[2])
                wait_bytes(main.at[0], sems.at[3])
        with jax.named_scope("i_unpack0"):
            unpack_rows(0)
            unpack_sides(0)
            derive_edges()
        groups = tiles // GROUP
        with jax.named_scope("i_stress"):
            tile_loop(groups, 1, lambda g: sweep_main(g, True, False))
            sweep_edge(True, False)
            sweep_flank(True, False)
        by_slot = one_hot[...]
        to_slots = jnp.concatenate([by_slot.astype(jnp.bfloat16)] * 2, axis=1)
        to_ends = jnp.concatenate([by_slot[:, :TILE], by_slot[:, count - TILE:]] * 2, axis=1)
        to_ends = to_ends.astype(jnp.bfloat16)
        by_block = by_slot.T.astype(jnp.bfloat16)
        to_blocks = jnp.concatenate([by_block] * 2, axis=1)
        end_blocks = jnp.concatenate([to_blocks[:TILE], to_blocks[count - TILE:]], axis=0)
        columns = jnp.concatenate([by_block] * 2, axis=0)

        with jax.named_scope("i_waitf4"):
            wait_bytes(recv.at[pl.ds(2, 4)], bulk_rsem.at[0])
        for c in range(2):
            both = dot_rows(to_blocks, recv[2 + c])
            for y in range(2):
                main[CUR_X + c, y] = both[:, y * width:(y + 1) * width]
        with jax.named_scope("i_packmid"):
            pack_rows(1)
            pack_sides(1)
            send_ends(1)
            send_sides(1)
            pack_flank(1)
            send_flank(1)
        for c in range(2):
            both = dot_rows(to_blocks, recv[4 + c])
            for y in range(2):
                main[PUSH_X + c, y] = main[MASS, y] * both[:, y * width:(y + 1) * width]
        for y in range(2):
            share = main[CONC, y] * main[ACTIVE, y]
            back[2, :, pl.ds(y * width, width)] = dot_rows(to_slots, share)

        with jax.named_scope("i_waitf2"):
            wait_bytes(recv.at[pl.ds(0, 2)], bulk_rsem.at[1])
        with jax.named_scope("i_push"):
            for c in range(2):
                both = lax.dot_general(
                    end_blocks, pieces(recv[c], 0), (((1,), (0,)), ((), ())),
                    preferred_element_type=jnp.float32,
                )
                for y in range(2):
                    for k, r in enumerate((top, bottom)):
                        part = both[k * TILE:(k + 1) * TILE, y * width:(y + 1) * width]
                        near_push[c, y, k] = main[ACTIVE, y, r, :] * (
                            main[CONC, y, r, :] * part - main[PUSH_X + c, y, r, :]
                        )
        with jax.named_scope("i_packlate"):
            pack_sides(2)
            send_sides(2)
            pack_rows(2)
            send_ends(2)
        with jax.named_scope("i_push2"):
            for c in range(2):
                both = dot_rows(to_blocks, recv[c])
                for y in range(2):
                    main[PUSH_X + c, y] = main[ACTIVE, y] * (
                        main[CONC, y] * both[:, y * width:(y + 1) * width] - main[PUSH_X + c, y]
                    )
            pack_flank(2)
            send_flank(2)

        def leave(get, u, v):
            dx, dy = u - get(CUR_X), v - get(CUR_Y)
            drag = get(DRAG) * jnp.sqrt(dx * dx + dy * dy + DRAG_FLOOR)
            return drag * dx, drag * dy

        outer = (lane < NSUB) | (lane >= width - NSUB)

        with jax.named_scope("i_vel1"):
            tile_loop(groups, 1, lambda g: sweep_main(g, False, True))
        with jax.named_scope("i_sweeps"):
            tile_loop((NSUB - 1) * groups, 1, lambda k: sweep_main(k % groups, True, True))
        send_rows(0, back, 2, 1, ret, 2, bulk_ssem, bulk_rsem.at[0])

        def returned(t):
            r = pl.ds(pl.multiple_of(t * TILE, TILE), TILE)
            block = sub + t * TILE
            theirs = outer | (block < 2) | (block >= count - 2)
            for y in range(2):
                half = pl.ds(y * width, width)
                u, v = main[U, y, r, :], main[V, y, r, :]
                gone = leave(lambda c: main[c, y, r, :], u, v)
                for c in range(2):
                    forc[c, r, half] = jnp.where(theirs, 0.0, gone[c])

        with jax.named_scope("i_back"):
            tile_loop(tiles, 4, returned)
            for c in range(2):
                back[c] = dot_rows(to_slots, forc[c])
        with jax.named_scope("i_waitmid"):
            when_inside(-1, 3, mid_rsem.at[0])
            when_inside(1, 3, mid_rsem.at[1])
            wait_tiles(2, mid_rsem.at[2])
            wait_tiles(8, mid_rsem.at[3])
        unpack_rows(1)
        unpack_sides(1)
        with jax.named_scope("i_waitlate"):
            when_inside(-1, 3, late_rsem.at[0])
            when_inside(1, 3, late_rsem.at[1])
            wait_tiles(2, late_rsem.at[2])
            wait_tiles(8, late_rsem.at[3])

        def sweep_strips(stress, velocity):
            sweep_flank(stress, velocity)
            sweep_edge(stress, velocity)

        with jax.named_scope("i_edge"):
            unpack_rows(2)
            unpack_sides(2)
            sweep_strips(False, True)
            for _ in range(NSUB - 1):
                sweep_strips(True, True)

        with jax.named_scope("i_fix"):
            for y in range(2):
                for j, far in ((1, 0), (2, count - TILE)):
                    r = pl.ds(j * TILE, TILE)
                    held = (lane >= 2) & (lane < count - 2)
                    held = held & ((sub < NSUB) if j == 1 else (sub >= TILE - NSUB))
                    u, v = flank[U, y, r, :], flank[V, y, r, :]
                    gone = leave(lambda c: flank[c, y, r, :], u, v)
                    for c in range(2):
                        slot = (c * 2 + y) * 2 * TILE + (TILE if j == 1 else 0)
                        flank_back[pl.ds(slot, TILE), :] = jnp.where(held, gone[c], 0.0)
                        flank_vel[c, y, pl.ds(far, TILE), :] = jnp.where(held, (u, v)[c], 0.0)
                for strip in range(2):
                    def get(c):
                        return edge[c, strip, y, :, pl.ds(0, width)]
                    gone = leave(get, get(U), get(V))
                    held = (sub < 2) if strip == 0 else (sub >= TILE - 2)
                    for c in range(2):
                        moved = pltpu.roll(gone[c], TILE - 2 if strip == 0 else 2, 0)
                        ends[c, pl.ds(strip * TILE, TILE), pl.ds(y * width, width)] = jnp.where(
                            held, moved, 0.0
                        )
            across = dot_lanes(to_slots, flank_back[...])
            for c in range(2):
                rest = dot_rows(to_ends, ends[c])
                for y in range(2):
                    slot = (c * 2 + y) * 2 * TILE
                    for t in range(tiles):
                        r, half = pl.ds(t * TILE, TILE), pl.ds(y * width, width)
                        moved = pltpu.roll(across[t * TILE:(t + 1) * TILE], width - TILE - slot, 1)
                        back[c, r, half] += jnp.where(outer, moved, 0.0) + (
                            rest[t * TILE:(t + 1) * TILE, y * width:(y + 1) * width]
                        )
            send_rows(0, back, 0, 2, ret, 0, bulk_ssem, bulk_rsem.at[1], "home")

        same = jnp.where(diag, 1.0, 0.0).astype(jnp.bfloat16)
        same = jnp.concatenate([same] * 2, axis=1)
        for y in range(2):
            for c in range(2):
                half = pl.ds(y * width, width)
                for strip, r in ((0, top), (1, bottom)):
                    end = pltpu.roll(
                        edge[c, strip, y, :, pl.ds(0, width)], TILE - 2 if strip == 0 else 2, 0
                    )
                    held = (sub < 2) if strip == 0 else (sub >= TILE - 2)
                    main[c, y, r, :] = jnp.where(held, end, main[c, y, r, :])
                other = dot_lanes(same, flank_vel[c, y])
                row = lax.broadcasted_iota(jnp.int32, (count, width), 0)
                column = lax.broadcasted_iota(jnp.int32, (count, width), 1)
                theirs = (row >= 2) & (row < count - 2)
                theirs = theirs & ((column < NSUB) | (column >= width - NSUB))
                out[0, c, :, half] = jnp.where(theirs, other, main[c, y])
        wait_bytes(ids.at[pl.ds(0, peers - 1)], ids_ssem)
        wait_bytes(back, bulk_ssem)
        when_inside(-1, 6, halo_ssem.at[0])
        when_inside(1, 6, halo_ssem.at[1])
        wait_tiles(4, halo_ssem.at[2])
        wait_tiles(16, halo_ssem.at[3])


def per_device_kernel(n_lat, n_lon, fields, block_owner, ice_covered, land_mask):
    count, cells = land_mask.shape
    peers = n_lat * n_lon
    f32 = jnp.float32
    anywhere = pl.BlockSpec(memory_space=pl.ANY)
    dma = pltpu.SemaphoreType.DMA
    halos = [pltpu.VMEM((2, num // 2, TILE, BX), f32) for _, num in ROUNDS] * 2
    sides = [pltpu.VMEM((2, TILE, BX), f32) for _ in ROUNDS]
    sides += [pltpu.VMEM((3, 2, TILE, BX), f32) for _ in ROUNDS]
    return pl.pallas_call(
        functools.partial(step_kernel, n_lat, n_lon),
        out_shape=pltpu.VMEM((1, 2, count, cells), f32),
        in_specs=[anywhere, anywhere, anywhere, anywhere],
        out_specs=pl.BlockSpec(memory_space=pltpu.VMEM),
        scratch_shapes=[
            pltpu.VMEM((7, count, cells), f32),
            pltpu.VMEM((2, count, cells), f32),
            pltpu.VMEM((3, count, cells), f32),
            pltpu.VMEM((1, count), jnp.int32),
            pltpu.VMEM((1, count), jnp.int32),
            pltpu.VMEM((peers, 1, count), jnp.int32),
            pltpu.VMEM((6, count, cells), f32),
            pltpu.VMEM((2, count, cells), f32),
            pltpu.VMEM((count, count), f32),
            pltpu.VMEM((3, count, cells), f32),
            pltpu.VMEM((count, cells), jnp.int32),
            pltpu.VMEM((14, 2, count, BX), f32),
            pltpu.VMEM((14, 2, 2, TILE, 2 * BX), f32),
            pltpu.VMEM((14, 2, 4 * TILE, BX), f32),
            pltpu.VMEM((BX, count), f32),
            pltpu.VMEM((2, 2, BX, count), f32),
            pltpu.VMEM((2, 2 * TILE, cells), f32),
            pltpu.VMEM((2, 2, 2, TILE, BX), f32),
            *halos, *sides,
            dma, dma((2,)), dma, dma, dma((4,)), dma((4,)), dma((4,)), dma((4,)),
            pltpu.SemaphoreType.REGULAR,
        ],
        compiler_params=pltpu.CompilerParams(
            collective_id=0, has_side_effects=True, vmem_limit_bytes=63 * 1024 * 1024
        ),
    )(fields, block_owner.reshape(1, count), ice_covered.reshape(1, count), land_mask)


def solution(mesh):
    placed = (
        P("comp", None, ("lat", "lon"), None),
        P(("lat", "lon")),
        P(("lat", "lon")),
        P(("lat", "lon"), None),
    )
    n_lat, n_lon = mesh.shape["lat"], mesh.shape["lon"]

    def body(fields, block_owner, ice_covered, land_mask):
        count = block_owner.shape[0]
        whole_tiles = count % (n_lat * n_lon * TILE) == 0 and count == BX
        if whole_tiles and n_lon > 2:
            return per_device_kernel(n_lat, n_lon, fields, block_owner, ice_covered, land_mask)
        return per_device(fields, block_owner, ice_covered, land_mask)

    return jax.shard_map(
        body,
        mesh=mesh,
        in_specs=placed,
        out_specs=P("comp", None, ("lat", "lon"), None),
        check_vma=False,
    )
```

```python
import functools

import jax
import jax.numpy as jnp
from jax import lax
from jax.experimental import pallas as pl
from jax.experimental.pallas import tpu as pltpu
from jax.sharding import PartitionSpec as P

GX = 1
BY = 2
BX = 128
NSUB = 4


CD_ICE = 0.1
CW = 1.5
CSTAR = 2.0
ECC2 = 4.0
DMIN2 = 0.25
RELAX = 0.5
DTE = 0.5
CORIO = 0.3
MASS_FLOOR = 0.5
DRAG_FLOOR = 0.1


def from_behind(x, axis, by):
    size = lax.axis_size(axis)
    pairs = [(i, i + by) for i in range(size) if 0 <= i + by < size]
    return lax.ppermute(x, axis, pairs)


def with_halo(x, sides, width, wrap):
    for axis, dim in sides:
        size, length = (lax.axis_size(axis), x.shape[dim])
        up = [(i, (i + 1) % size) for i in range(size if wrap else size - 1)]
        down = [(j, i) for i, j in up]
        last = lax.slice_in_dim(x, length - width, length, axis=dim)
        first = lax.slice_in_dim(x, 0, width, axis=dim)
        before = lax.ppermute(last, axis, up)
        after = lax.ppermute(first, axis, down)
        x = jnp.concatenate([before, x, after], axis=dim)
    return x


def air_stress(ocean):
    wind_x, wind_y, current_x, current_y, tilt_x, tilt_y, density = ocean
    speed_ice = jnp.sqrt(wind_x * wind_x + wind_y * wind_y + 1.0)
    scale_ice = density * CD_ICE * speed_ice
    rel_x = wind_x - current_x
    rel_y = wind_y - current_y
    speed_open = jnp.sqrt(rel_x * rel_x + rel_y * rel_y + 1.0)
    scale_open = density * (0.1 + 0.05 * speed_open) * speed_open
    outbound = jnp.stack(
        [scale_ice * wind_x, scale_ice * wind_y, current_x, current_y, tilt_x, tilt_y]
    )
    open_stress = jnp.stack([scale_open * rel_x, scale_open * rel_y])
    return (outbound, open_stress)


def prepare(ice_tile, forcing, active):
    ice_mass = ice_tile[2]
    concentration = ice_tile[3]
    strength = ice_mass * jnp.exp(CSTAR * (concentration - 1.0)) * active
    drag_base = CW * concentration * active
    push_x = active * (concentration * forcing[0] - ice_mass * forcing[4])
    push_y = active * (concentration * forcing[1] - ice_mass * forcing[5])
    return jnp.stack(
        [strength, ice_mass, drag_base, push_x, push_y, forcing[2], forcing[3], active]
    )


def subcycle(ice_state, statics):
    east_vel, north_vel, stress_one, stress_two, stress_three = ice_state
    strength = statics[0]
    east_base = east_vel[:-1, :-1]
    north_base = north_vel[:-1, :-1]
    strain_xx = east_vel[:-1, 1:] - east_base
    strain_yy = north_vel[1:, :-1] - north_base
    shear = east_vel[1:, :-1] - east_base + (north_vel[:-1, 1:] - north_base)
    divergence = strain_xx + strain_yy
    tension = strain_xx - strain_yy
    delta_norm = jnp.sqrt(
        divergence * divergence + (tension * tension + shear * shear) / ECC2 + DMIN2
    )
    viscosity = strength[:-1, :-1] / delta_norm
    stress_sum = (stress_one[:-1, :-1] + RELAX * viscosity * (divergence - delta_norm)) / (
        1.0 + RELAX
    )
    stress_diff = (stress_two[:-1, :-1] + RELAX * viscosity * tension / ECC2) / (1.0 + RELAX)
    stress_shear = (stress_three[:-1, :-1] + RELAX * viscosity * shear / (2.0 * ECC2)) / (
        1.0 + RELAX
    )
    stress_xx = 0.5 * (stress_sum + stress_diff)
    stress_yy = 0.5 * (stress_sum - stress_diff)
    force_x = (
        stress_xx[1:, 1:] - stress_xx[1:, :-1] + (stress_shear[1:, 1:] - stress_shear[:-1, 1:])
    )
    force_y = (
        stress_shear[1:, 1:] - stress_shear[1:, :-1] + (stress_yy[1:, 1:] - stress_yy[:-1, 1:])
    )
    trimmed = statics[:, 1:-1, 1:-1]
    strength, ice_mass, drag_base, push_x, push_y, current_x, current_y, active = trimmed
    east_old = east_vel[1:-1, 1:-1]
    north_old = north_vel[1:-1, 1:-1]
    diff_x = current_x - east_old
    diff_y = current_y - north_old
    drag_coef = drag_base * jnp.sqrt(diff_x * diff_x + diff_y * diff_y + DRAG_FLOOR)
    denominator = jnp.maximum(ice_mass, MASS_FLOOR) / DTE + drag_coef
    east_new = (
        active
        * (
            ice_mass / DTE * east_old
            + force_x
            + push_x
            + drag_coef * current_x
            + CORIO * ice_mass * north_old
        )
        / denominator
    )
    north_new = (
        active
        * (
            ice_mass / DTE * north_old
            + force_y
            + push_y
            + drag_coef * current_y
            - CORIO * ice_mass * east_old
        )
        / denominator
    )
    new_state = jnp.stack(
        [east_new, north_new, stress_sum[1:, 1:], stress_diff[1:, 1:], stress_shear[1:, 1:]]
    )
    return (new_state, trimmed)


def give_back(ice_state, statics):
    east_vel = ice_state[0]
    north_vel = ice_state[1]
    drag_base = statics[2]
    current_x = statics[5]
    current_y = statics[6]
    diff_x = east_vel - current_x
    diff_y = north_vel - current_y
    factor = drag_base * jnp.sqrt(diff_x * diff_x + diff_y * diff_y + DRAG_FLOOR)
    return jnp.stack([factor * diff_x, factor * diff_y, drag_base / CW])


def to_tile(blocks):
    channels, count, cells = blocks.shape
    arranged = blocks.reshape(channels, count // GX, GX, BY, BX).transpose(0, 1, 3, 2, 4)
    return arranged.reshape(channels, count // GX * BY, GX * BX)


def from_tile(values):
    channels, rows, columns = values.shape
    arranged = values.reshape(channels, rows // BY, BY, GX, BX).transpose(0, 1, 3, 2, 4)
    return arranged.reshape(channels, rows // BY * GX, BY * BX)


def per_device(fields, block_owner, ice_covered, land_mask):
    count = block_owner.shape[0]
    is_ocean = lax.axis_index("comp") == 0
    outbound, open_stress = air_stress(fields[0])
    owner_row = block_owner.reshape(1, count)
    crossed = from_behind(outbound, "comp", 1)
    received, anchor = (
        lax.all_to_all(crossed, ("lat", "lon"), split_axis=1, concat_axis=1, tiled=True),
        lax.all_to_all(owner_row, ("lat", "lon"), split_axis=1, concat_axis=1, tiled=True),
    )
    local_ids = anchor[0] % count
    position = jnp.zeros((count,), jnp.int32).at[local_ids].set(jnp.arange(count, dtype=jnp.int32))
    forcing = to_tile(received[:, position])
    ice_tile = to_tile(fields[0])
    covered = ice_covered.astype(jnp.float32)[:, None] * (1 - land_mask).astype(jnp.float32)
    active = to_tile(covered[None])[0]
    statics = prepare(ice_tile, forcing, active)
    ice_state = jnp.stack([ice_tile[0], ice_tile[1], ice_tile[4], ice_tile[5], ice_tile[6]])
    joined = jnp.concatenate([ice_state, statics], 0)
    joined = with_halo(joined, (("lon", 2),), NSUB, True)
    joined = with_halo(joined, (("lat", 1),), NSUB, False)
    ice_state = joined[:5]
    statics = joined[5:]
    for repeat in range(NSUB):
        ice_state, statics = subcycle(ice_state, statics)
    returned = from_tile(give_back(ice_state, statics))
    back_send = returned[:, local_ids]
    regrouped = lax.all_to_all(back_send, ("lat", "lon"), split_axis=1, concat_axis=1, tiled=True)
    received_back = from_behind(regrouped, "comp", -1)
    ocean_out = received_back[:2] + (1.0 - received_back[2]) * open_stress
    ice_out = from_tile(ice_state[:2])
    return jnp.where(is_ocean, ocean_out, ice_out)[None]


TILE = 8
GROUP = 8
MESH = pl.DeviceIdType.MESH
U, V, MASS, CONC, S1, S2, S12, ACTIVE, PUSH_X, PUSH_Y, CUR_X, CUR_Y, STRENGTH, DRAG = range(14)
SIDES = [(a, b) for b in (-1, 1) for a in (-1, 1, 0)]
ROUNDS = ((U, 8), (CUR_X, 2), (PUSH_X, 2))
KEEP = 1.0 / (1.0 + RELAX)


def tile_loop(tiles, together, body):
    def step(k, carry):
        for j in range(together):
            body(k * together + j)
        return carry
    lax.fori_loop(0, tiles // together, step, 0)


def pieces(values, axis):
    high = values.astype(jnp.bfloat16)
    low = (values - high.astype(jnp.float32)).astype(jnp.bfloat16)
    return jnp.concatenate([high, low], axis=axis)


def dot_rows(twice, values):
    return lax.dot_general(
        twice, pieces(values, 0), (((1,), (0,)), ((), ())), preferred_element_type=jnp.float32
    )


def dot_lanes(twice, values):
    return lax.dot_general(
        twice, pieces(values, 1), (((1,), (1,)), ((), ())), preferred_element_type=jnp.float32
    )


def new_stress(strength, s1, s2, s12, u, v, u_east, v_east, u_up, v_up):
    sxx = u_east - u
    syy = v_up - v
    shear = (u_up - u) + (v_east - v)
    div = sxx + syy
    ten = sxx - syy
    square = div * div + (ten * ten + shear * shear) * (1.0 / ECC2) + DMIN2
    inverse = lax.rsqrt(square)
    visc = strength * inverse
    s1 = s1 * KEEP + visc * (div - square * inverse)
    s2 = s2 * KEEP + visc * ten * (1.0 / ECC2)
    s12 = s12 * KEEP + visc * shear * (0.5 / ECC2)
    return s1, s2, s12


def new_velocity(get, u, v, force_x, force_y):
    mass, cx, cy = get(MASS), get(CUR_X), get(CUR_Y)
    dx, dy = cx - u, cy - v
    square = dx * dx + dy * dy + DRAG_FLOOR
    drag = get(DRAG) * (square * lax.rsqrt(square))
    gain = get(ACTIVE) / (jnp.maximum(mass, MASS_FLOOR) * (1.0 / DTE) + drag)
    inertia = mass * (1.0 / DTE)
    turn = CORIO * mass
    return (
        gain * (inertia * u + force_x + get(PUSH_X) + drag * cx + turn * v),
        gain * (inertia * v + force_y + get(PUSH_Y) + drag * cy - turn * u),
    )


def step_kernel(
    n_lat, n_lon,
    fields, owner_hbm, covered_hbm, land, out,
    surf, open_st, ret, owner, covered, ids, recv, forc, one_hot, back, land_v,
    main, edge, flank, flank_back, flank_vel, ends, near_push,
    rows_out0, rows_out1, rows_out2, rows_got0, rows_got1, rows_got2,
    side_out0, side_out1, side_out2, side_got0, side_got1, side_got2,
    bulk_ssem, bulk_rsem, ids_ssem, ids_rsem, halo_ssem, early_rsem, mid_rsem, late_rsem, ready,
):
    comp = lax.axis_index("comp")
    lat = lax.axis_index("lat")
    lon = lax.axis_index("lon")
    peers = n_lat * n_lon
    me = lat * n_lon + lon
    count = owner.shape[1]
    per = count // peers
    width = BX
    barrier = pltpu.get_barrier_semaphore()
    rows_out = (rows_out0, rows_out1, rows_out2)
    rows_got = (rows_got0, rows_got1, rows_got2)
    side_out = (side_out0, side_out1, side_out2)
    side_got = (side_got0, side_got1, side_got2)

    def rows_of(peer):
        return pl.ds(pl.multiple_of(peer * per, per), per)

    planes = [jnp.where(lat < n_lat // 2, n_lat - 1 - j, j) for j in range(n_lat)]
    places = [(lon + i) % n_lon for i in range(n_lon)]

    half_lat = n_lat // 2
    groups_of = {
        "all": ((planes, places),),
        "column": ((planes[:half_lat], places[:1]),),
        "beyond": ((planes[:half_lat], places[1:]),),
        "near": ((planes[half_lat:], places),),
    }

    def each_peer(body, part="all"):
        for chosen, along in groups_of[part]:
            for plane in chosen:
                for place in along:
                    body(plane * n_lon + place, plane, place)

    def home_first(body):
        body(0, 0, 0)
        for plane in range(n_lat):
            for place in places:
                if plane:
                    body(plane * n_lon + place, plane, place)
                else:
                    @pl.when(place > 0)
                    def _():
                        body(place, 0, place)

    def signal_peers(kind, part="all"):
        each_peer(
            lambda p, plane, place: pl.semaphore_signal(
                barrier, inc=1, device_id=(kind, plane, place), device_id_type=MESH
            ),
            part,
        )

    def send_rows(kind, src, lo, num, dst, dlo, ssem, rsem, part="all"):
        def body(p, plane, place):
            pltpu.make_async_remote_copy(
                src_ref=src.at[pl.ds(lo, num), rows_of(p), :],
                dst_ref=dst.at[pl.ds(dlo, num), rows_of(me), :],
                send_sem=ssem, recv_sem=rsem,
                device_id=(kind, plane, place), device_id_type=MESH,
            ).start()
        home_first(body) if part == "home" else each_peer(body, part)

    def wait_bytes(ref, sem):
        pltpu.make_async_copy(ref, ref, sem).wait()

    def wait_tiles(num, sem):
        wait_bytes(main.at[0, 0, pl.ds(0, num * TILE), :], sem)

    @pl.when(comp == 0)
    def _ocean():
        signal_peers(1)
        raw = pltpu.make_async_copy(fields.at[0, pl.ds(2, 4)], surf.at[pl.ds(2, 4)], halo_ssem.at[0])
        wind = pltpu.make_async_copy(fields.at[0, pl.ds(0, 2)], surf.at[pl.ds(0, 2)], halo_ssem.at[1])
        rho = pltpu.make_async_copy(fields.at[0, pl.ds(6, 1)], surf.at[pl.ds(6, 1)], halo_ssem.at[2])
        raw.start()
        wind.start()
        rho.start()
        with jax.named_scope("o_barrier"):
            pl.semaphore_wait(barrier, half_lat)

        def send_four(part):
            send_rows(1, surf, 2, 4, recv, 2, bulk_ssem, bulk_rsem.at[0], part)

        def send_two(part):
            send_rows(1, forc, 0, 2, recv, 0, bulk_ssem, bulk_rsem.at[1], part)

        with jax.named_scope("o_send4"):
            raw.wait()
            send_four("column")
            wind.wait()
            rho.wait()

        def stress(t):
            r = pl.ds(pl.multiple_of(t * TILE, TILE), TILE)
            wx, wy, density = surf[0, r, :], surf[1, r, :], surf[6, r, :]
            scale = density * CD_ICE * jnp.sqrt(wx * wx + wy * wy + 1.0)
            forc[0, r, :] = scale * wx
            forc[1, r, :] = scale * wy

        with jax.named_scope("o_stress"):
            tile_loop(count // TILE, 4, stress)
            send_two("column")
        with jax.named_scope("o_ready"):
            pl.semaphore_wait(ready, 1)
        with jax.named_scope("o_rest"):
            send_four("beyond")
            send_two("beyond")
            send_four("near")
            send_two("near")

        def open_water(t):
            r = pl.ds(pl.multiple_of(t * TILE, TILE), TILE)
            density = surf[6, r, :]
            rel_x = surf[0, r, :] - surf[2, r, :]
            rel_y = surf[1, r, :] - surf[3, r, :]
            speed = jnp.sqrt(rel_x * rel_x + rel_y * rel_y + 1.0)
            scale = density * (0.1 + 0.05 * speed) * speed
            open_st[0, r, :] = scale * rel_x
            open_st[1, r, :] = scale * rel_y

        tile_loop(count // TILE, 2, open_water)
        with jax.named_scope("o_waitret1"):
            wait_bytes(ret.at[pl.ds(2, 1)], bulk_rsem.at[0])

        def water(t):
            r = pl.ds(pl.multiple_of(t * TILE, TILE), TILE)
            share = 1.0 - ret[2, r, :]
            for c in range(2):
                open_st[c, r, :] = share * open_st[c, r, :]

        tile_loop(count // TILE, 4, water)
        with jax.named_scope("o_waitret2"):
            wait_bytes(ret.at[pl.ds(0, 2)], bulk_rsem.at[1])

        def finish(t):
            r = pl.ds(pl.multiple_of(t * TILE, TILE), TILE)
            for c in range(2):
                out[0, c, r, :] = ret[c, r, :] + open_st[c, r, :]

        tile_loop(count // TILE, 4, finish)
        wait_bytes(surf.at[pl.ds(0, 6)], bulk_ssem)

    @pl.when(comp == 1)
    def _ice():
        def inside(a):
            if a == 0:
                return lat >= 0
            return lat + a >= 0 if a < 0 else lat + a < n_lat

        def around(a, b):
            return (1, lat + a, (lon + b + n_lon) % n_lon)

        signal_peers(0, "column")
        for a in range(n_lat):
            for b in range(n_lon):
                if a or b:
                    pl.semaphore_signal(
                        barrier, inc=1, device_id=(1, (lat + a) % n_lat, (lon + b) % n_lon),
                        device_id_type=MESH,
                    )
        for y in range(2):
            pltpu.make_async_copy(
                fields.at[0, :, :, pl.ds(y * width, width)], main.at[pl.ds(0, 7), y], halo_ssem.at[0]
            ).start()
        loads = [
            pltpu.make_async_copy(land, land_v, halo_ssem.at[1]),
            pltpu.make_async_copy(covered_hbm, covered, halo_ssem.at[2]),
        ]
        names = pltpu.make_async_copy(owner_hbm, owner, halo_ssem.at[3])
        names.start()
        for load in loads:
            load.start()
        with jax.named_scope("i_barrier"):
            pl.semaphore_wait(barrier, 2 * peers - 1)
            pl.semaphore_signal(ready, inc=1, device_id=(0, lat, lon), device_id_type=MESH)
            names.wait()
            for a in range(n_lat):
                for b in range(n_lon):
                    if a or b:
                        pltpu.make_async_remote_copy(
                            src_ref=owner, dst_ref=ids.at[me], send_sem=ids_ssem, recv_sem=ids_rsem,
                            device_id=(1, (lat + a) % n_lat, (lon + b) % n_lon),
                            device_id_type=MESH,
                        ).start()
        ids[me] = owner[...]

        tiles = count // TILE
        top, bottom = pl.ds(0, TILE), pl.ds(count - TILE, TILE)
        zero_tile = jnp.zeros((TILE, width), jnp.float32)
        for wall, which in ((lat == 0, 0), (lat == n_lat - 1, 1)):
            @pl.when(wall)
            def _():
                for e in range(3):
                    for k in range(rows_got[e].shape[1]):
                        rows_got[e][which, k] = zero_tile
                    for k in range(2):
                        side_got[e][2 * which, k] = zero_tile

        def clear(t):
            r = pl.ds(pl.multiple_of(t * TILE, TILE), TILE)
            for c in range(2):
                for y in range(2):
                    flank_vel[c, y, r, :] = zero_tile
            flank_back[r, :] = zero_tile

        tile_loop(tiles, 2, clear)
        wait_bytes(main.at[pl.ds(0, 7)], halo_ssem.at[0])
        for load in loads:
            load.wait()
        diag = lax.broadcasted_iota(jnp.int32, (count, count), 0) == lax.broadcasted_iota(
            jnp.int32, (count, count), 1
        )
        wet = jnp.sum(
            jnp.where(diag, covered[...].astype(jnp.float32), 0.0), axis=1, keepdims=True
        )
        sea = wet * (1 - land_v[...]).astype(jnp.float32)
        for y in range(2):
            main[ACTIVE, y] = sea[:, y * width:(y + 1) * width]

        lane = lax.broadcasted_iota(jnp.int32, (TILE, width), 1)
        sub = lax.broadcasted_iota(jnp.int32, (TILE, width), 0)
        pick_row = lax.broadcasted_iota(jnp.int32, (2 * TILE, width), 0)
        pick_col = lax.broadcasted_iota(jnp.int32, (2 * TILE, width), 1)
        picked = jnp.where(pick_row < TILE, pick_row, pick_row + (width - 2 * TILE)) == pick_col
        picker = jnp.where(picked, 1.0, 0.0).astype(jnp.bfloat16)
        picker = jnp.concatenate([picker] * 2, axis=1)

        def end_of(e, c, y, k):
            if e == 2:
                return near_push[c - PUSH_X, y, k]
            return main[c, y, (top, bottom)[k], :]

        def pack_rows(e):
            lo, num = ROUNDS[e]
            for k in range(num // 2):
                ups, downs = zero_tile, zero_tile
                for i in range(4):
                    c, y = lo + 2 * k + i // 2, i % 2
                    head, foot = end_of(e, c, y, 0), end_of(e, c, y, 1)
                    here = (sub >= 2 * i) & (sub < 2 * i + 2)
                    ups = jnp.where(here, pltpu.roll(head, 2 * i, 0) if i else head, ups)
                    downs = jnp.where(here, pltpu.roll(foot, (2 * i + 2) % TILE, 0) if i < 3 else foot, downs)
                rows_out[e][0, k] = ups
                rows_out[e][1, k] = downs

        def pack_sides(e):
            lo, num = ROUNDS[e]
            west, east = zero_tile, zero_tile
            for i in range(2 * num):
                c, y = lo + i // 2, i % 2
                ends = jnp.where(sub < NSUB, end_of(e, c, y, 0), end_of(e, c, y, 1))
                slot = i * NSUB
                mine = (lane >= slot) & (lane < slot + NSUB)
                west = jnp.where(mine, pltpu.roll(ends, slot, 1) if slot else ends, west)
                east = jnp.where(mine, pltpu.roll(ends, (slot + NSUB) % width, 1), east)
            side_out[e][0] = west
            side_out[e][1] = east

        def pack_flank(e):
            lo, num = ROUNDS[e]
            for c in range(lo, lo + num):
                for y in range(2):
                    across = dot_lanes(picker, main[c, y])
                    flank[c, y, pl.ds(TILE, TILE), :] = across[:TILE]
                    flank[c, y, pl.ds(2 * TILE, TILE), :] = across[TILE:]

        def push_on(e, a, b, src, dst, lane_of_sem, recv_lane):
            sems = (early_rsem, mid_rsem, late_rsem)[e]

            @pl.when(inside(a))
            def _():
                pltpu.make_async_remote_copy(
                    src_ref=src, dst_ref=dst,
                    send_sem=halo_ssem.at[lane_of_sem], recv_sem=sems.at[recv_lane],
                    device_id=around(a, b), device_id_type=MESH,
                ).start()

        def send_ends(e):
            for a in (-1, 1):
                k = 1 if a > 0 else 0
                push_on(e, a, 0, rows_out[e].at[k], rows_got[e].at[1 - k], k, 1 - k)

        def send_sides(e):
            for a, b in SIDES:
                k = 1 if b > 0 else 0
                group = {0: 2, -1: 0, 1: 1}[a]
                land_in = {0: 2, -1: 1, 1: 0}[a]
                push_on(e, a, b, side_out[e].at[k], side_got[e].at[1 - a, 1 - k], group, land_in)

        def send_flank(e):
            lo, num = ROUNDS[e]
            for b in (-1, 1):
                src, dst = (2 * TILE, 0) if b > 0 else (TILE, 3 * TILE)
                push_on(
                    e, 0, b,
                    flank.at[pl.ds(lo, num), :, pl.ds(src, TILE), :],
                    flank.at[pl.ds(lo, num), :, pl.ds(dst, TILE), :], 3, 3,
                )

        def when_inside(a, num, sem):
            @pl.when(inside(a))
            def _():
                wait_tiles(num, sem)

        def own_rows():
            for c in range(ROUNDS[0][1]):
                for y in range(2):
                    edge[c, 0, y, :, pl.ds(0, width)] = pltpu.roll(main[c, y, top, :], 2, 0)
                    edge[c, 1, y, :, pl.ds(0, width)] = pltpu.roll(main[c, y, bottom, :], TILE - 2, 0)

        def unpack_rows(e, placed=False):
            lo, num = ROUNDS[e]
            got = rows_got[e]
            for k in range(num // 2):
                for i in range(4):
                    c, y = lo + 2 * k + i // 2, i % 2
                    north = pltpu.roll(got[0, k], (TILE - 2 * i) % TILE, 0) if i else got[0, k]
                    south = pltpu.roll(got[1, k], TILE - 2 - 2 * i, 0) if i < 3 else got[1, k]
                    if placed:
                        head, foot = (edge[c, strip, y, :, pl.ds(0, width)] for strip in range(2))
                    else:
                        head = pltpu.roll(main[c, y, top, :], 2, 0)
                        foot = pltpu.roll(main[c, y, bottom, :], TILE - 2, 0)
                    edge[c, 0, y, :, pl.ds(0, width)] = jnp.where(sub < 2, north, head)
                    edge[c, 1, y, :, pl.ds(0, width)] = jnp.where(sub >= TILE - 2, south, foot)

        def unpack_sides(e):
            lo, num = ROUNDS[e]
            side = side_got[e]
            ends = []
            for k in range(2):
                far, near = side[0, k], side[1, k]
                ends.append(pltpu.roll(jnp.where(sub >= TILE - 2, far, near), 2, 0))
            for k in range(2):
                far, near = side[2, k], side[1, k]
                ends.append(pltpu.roll(jnp.where(sub < 2, far, near), TILE - 2, 0))
            for i in range(2 * num):
                c, y = lo + i // 2, i % 2
                slot = i * NSUB
                for strip in range(2):
                    from_west, from_east = ends[2 * strip], ends[2 * strip + 1]
                    from_east = pltpu.roll(from_east, width - slot, 1) if slot else from_east
                    from_west = pltpu.roll(from_west, width - NSUB - slot, 1)
                    edge[c, strip, y, :, pl.ds(width, width)] = jnp.where(
                        lane < NSUB, from_east, jnp.where(lane >= width - NSUB, from_west, 0.0)
                    )

        def derive(load, store):
            conc, act = load(CONC), load(ACTIVE)
            store(STRENGTH, (RELAX * KEEP) * load(MASS) * jnp.exp(CSTAR * (conc - 1.0)) * act)
            store(DRAG, CW * conc * act)

        def derive_main(t):
            r = pl.ds(pl.multiple_of(t * TILE, TILE), TILE)
            for y in range(2):
                def store(c, x):
                    main[c, y, r, :] = x
                derive(lambda c: main[c, y, r, :], store)

        def derive_flank():
            for y in range(2):
                def store(c, x):
                    flank[c, y] = x
                derive(lambda c: flank[c, y], store)

        def derive_edges():
            for y in range(2):
                for strip in range(2):
                    def store(c, x):
                        edge[c, strip, y] = x
                    derive(lambda c: edge[c, strip, y], store)

        def sweep_main(g, stress, velocity):
            spots = [
                pl.ds(pl.multiple_of((g * GROUP + j) * TILE, TILE), TILE) for j in range(GROUP)
            ]
            behind = pl.ds(pl.multiple_of(jnp.maximum(g * GROUP - 1, 0) * TILE, TILE), TILE)
            ahead = pl.ds(
                pl.multiple_of(jnp.minimum(g * GROUP + GROUP, tiles - 1) * TILE, TILE), TILE
            )
            vels = [[(main[U, y, r, :], main[V, y, r, :]) for y in range(2)] for r in spots]
            stresses = []
            if stress:
                follow = (main[U, 0, ahead, :], main[V, 0, ahead, :])
            for j, r in enumerate(spots):
                old = [tuple(main[c, y, r, :] for c in (S1, S2, S12)) for y in range(2)]
                if not stress:
                    stresses.append(old)
                    continue
                beyond = vels[j + 1][0] if j + 1 < GROUP else follow
                row = []
                for y in range(2):
                    u, v = vels[j][y]
                    if y == 0:
                        u_up, v_up = vels[j][1]
                    else:
                        u_up, v_up = (
                            pltpu.roll(jnp.where(sub == 0, after, x), TILE - 1, 0)
                            for x, after in zip(vels[j][0], beyond)
                        )
                    fresh = new_stress(
                        main[STRENGTH, y, r, :], *old[y], u, v,
                        pltpu.roll(u, width - 1, 1), pltpu.roll(v, width - 1, 1), u_up, v_up,
                    )
                    for c, x in zip((S1, S2, S12), fresh):
                        main[c, y, r, :] = x
                    row.append(fresh)
                stresses.append(row)
            if not velocity:
                return
            yy_before = 0.5 * (main[S1, 1, behind, :] - main[S2, 1, behind, :])
            cross_before = main[S12, 1, behind, :]
            for j, r in enumerate(spots):
                xx = [0.5 * (s1 + s2) for s1, s2, _ in stresses[j]]
                yy = [0.5 * (s1 - s2) for s1, s2, _ in stresses[j]]
                cross = [s12 for _, _, s12 in stresses[j]]
                yy_down, cross_down = (
                    [pltpu.roll(jnp.where(sub == TILE - 1, before, x[1]), 1, 0), x[0]]
                    for x, before in ((yy, yy_before), (cross, cross_before))
                )
                yy_before, cross_before = yy[1], cross[1]
                for y in range(2):
                    force_x = xx[y] - pltpu.roll(xx[y], 1, 1) + (cross[y] - cross_down[y])
                    force_y = cross[y] - pltpu.roll(cross[y], 1, 1) + (yy[y] - yy_down[y])
                    u, v = new_velocity(lambda c: main[c, y, r, :], *vels[j][y], force_x, force_y)
                    main[U, y, r, :] = u
                    main[V, y, r, :] = v

        def sweep_edge(stress, velocity):
            lanes = 2 * width

            for strip in range(2):
                vels = [(edge[U, strip, y], edge[V, strip, y]) for y in range(2)]
                fresh = [tuple(edge[c, strip, y] for c in (S1, S2, S12)) for y in range(2)]
                if stress:
                    ups = [vels[1], tuple(pltpu.roll(x, TILE - 1, 0) for x in vels[0])]
                    for y in range(2):
                        east = [pltpu.roll(x, lanes - 1, 1) for x in vels[y]]
                        fresh[y] = new_stress(
                            edge[STRENGTH, strip, y], *fresh[y], *vels[y], *east, *ups[y]
                        )
                        for c, x in zip((S1, S2, S12), fresh[y]):
                            edge[c, strip, y] = x
                if not velocity:
                    continue
                xx = [0.5 * (s1 + s2) for s1, s2, _ in fresh]
                yy = [0.5 * (s1 - s2) for s1, s2, _ in fresh]
                cross = [s12 for _, _, s12 in fresh]
                yy_down, cross_down = ([pltpu.roll(x[1], 1, 0), x[0]] for x in (yy, cross))
                for y in range(2):
                    force_x = xx[y] - pltpu.roll(xx[y], 1, 1) + (cross[y] - cross_down[y])
                    force_y = cross[y] - pltpu.roll(cross[y], 1, 1) + (yy[y] - yy_down[y])
                    u, v = new_velocity(lambda c: edge[c, strip, y], *vels[y], force_x, force_y)
                    edge[U, strip, y] = u
                    edge[V, strip, y] = v

        def sweep_flank(stress, velocity):
            spots = [pl.ds(j * TILE, TILE) for j in range(4)]
            vels = [[(flank[U, y, r, :], flank[V, y, r, :]) for y in range(2)] for r in spots]
            fresh = [
                [tuple(flank[c, y, r, :] for c in (S1, S2, S12)) for y in range(2)] for r in spots
            ]
            if stress:
                for j, r in enumerate(spots):
                    for y in range(2):
                        after = vels[min(j + 1, 3)][y]
                        east = [
                            pltpu.roll(jnp.where(sub == 0, b, x), TILE - 1, 0)
                            for x, b in zip(vels[j][y], after)
                        ]
                        ups = vels[j][1] if y == 0 else [
                            pltpu.roll(x, width - 1, 1) for x in vels[j][0]
                        ]
                        fresh[j][y] = new_stress(
                            flank[STRENGTH, y, r, :], *fresh[j][y], *vels[j][y], *east, *ups
                        )
                        for c, x in zip((S1, S2, S12), fresh[j][y]):
                            flank[c, y, r, :] = x
            if not velocity:
                return
            xx = [[0.5 * (s1 + s2) for s1, s2, _ in row] for row in fresh]
            yy = [[0.5 * (s1 - s2) for s1, s2, _ in row] for row in fresh]
            cross = [[s12 for _, _, s12 in row] for row in fresh]

            def westward(x, j, y):
                before = x[max(j - 1, 0)][y]
                return pltpu.roll(jnp.where(sub == TILE - 1, before, x[j][y]), 1, 0)

            def downward(x, j, y):
                return x[j][0] if y == 1 else pltpu.roll(x[j][1], 1, 1)

            for j, r in enumerate(spots):
                for y in range(2):
                    force_x = xx[j][y] - westward(xx, j, y) + (cross[j][y] - downward(cross, j, y))
                    force_y = cross[j][y] - westward(cross, j, y) + (yy[j][y] - downward(yy, j, y))
                    u, v = new_velocity(lambda c: flank[c, y, r, :], *vels[j][y], force_x, force_y)
                    flank[U, y, r, :] = u
                    flank[V, y, r, :] = v

        with jax.named_scope("i_pack0"):
            pack_flank(0)
            send_flank(0)
            pack_rows(0)
            pack_sides(0)
        tile_loop(tiles, 2, derive_main)

        with jax.named_scope("i_waitids"):
            wait_bytes(ids.at[pl.ds(0, peers - 1)], ids_rsem)
        wanted = me * per
        row_lane = lax.broadcasted_iota(jnp.int32, (per, count), 1)
        row_sub = lax.broadcasted_iota(jnp.int32, (per, count), 0)
        mine = row_lane == row_sub + wanted
        blocks = lax.broadcasted_iota(jnp.int32, (per, count), 1).astype(jnp.float32)
        base = (me * count).astype(jnp.float32)
        for p in range(peers):
            owned = jnp.broadcast_to(ids[p], (per, count)).astype(jnp.float32)
            local = jnp.sum(jnp.where(mine, owned, 0.0), axis=1, keepdims=True) - base
            one_hot[pl.ds(p * per, per), :] = jnp.where(local == blocks, 1.0, 0.0)

        with jax.named_scope("i_waithalo0"):
            for sems in (halo_ssem, early_rsem):
                wait_bytes(main.at[0], sems.at[3])
        with jax.named_scope("i_unpack0"):
            derive_flank()
            own_rows()
        groups = tiles // GROUP
        with jax.named_scope("i_stress"):
            tile_loop(groups, 1, lambda g: sweep_main(g, True, False))
            sweep_flank(True, False)
        by_slot = one_hot[...]
        to_slots = jnp.concatenate([by_slot.astype(jnp.bfloat16)] * 2, axis=1)
        to_ends = jnp.concatenate([by_slot[:, :TILE], by_slot[:, count - TILE:]] * 2, axis=1)
        to_ends = to_ends.astype(jnp.bfloat16)
        by_block = by_slot.T.astype(jnp.bfloat16)
        to_blocks = jnp.concatenate([by_block] * 2, axis=1)
        end_blocks = jnp.concatenate([to_blocks[:TILE], to_blocks[count - TILE:]], axis=0)
        columns = jnp.concatenate([by_block] * 2, axis=0)

        with jax.named_scope("i_waitf4"):
            wait_bytes(recv.at[pl.ds(2, 4)], bulk_rsem.at[0])
        for c in range(2):
            both = dot_rows(to_blocks, recv[2 + c])
            for y in range(2):
                main[CUR_X + c, y] = both[:, y * width:(y + 1) * width]
        with jax.named_scope("i_packmid"):
            send_sides(0)
            send_ends(0)
            pack_rows(1)
            pack_sides(1)
            send_ends(1)
            send_sides(1)
            pack_flank(1)
            send_flank(1)
        for c in range(2):
            both = dot_rows(to_blocks, recv[4 + c])
            for y in range(2):
                main[PUSH_X + c, y] = main[MASS, y] * both[:, y * width:(y + 1) * width]
        for y in range(2):
            share = main[CONC, y] * main[ACTIVE, y]
            back[2, :, pl.ds(y * width, width)] = dot_rows(to_slots, share)

        with jax.named_scope("i_waitf2"):
            wait_bytes(recv.at[pl.ds(0, 2)], bulk_rsem.at[1])
        with jax.named_scope("i_push"):
            for c in range(2):
                both = lax.dot_general(
                    end_blocks, pieces(recv[c], 0), (((1,), (0,)), ((), ())),
                    preferred_element_type=jnp.float32,
                )
                for y in range(2):
                    for k, r in enumerate((top, bottom)):
                        part = both[k * TILE:(k + 1) * TILE, y * width:(y + 1) * width]
                        near_push[c, y, k] = main[ACTIVE, y, r, :] * (
                            main[CONC, y, r, :] * part - main[PUSH_X + c, y, r, :]
                        )
        with jax.named_scope("i_packlate"):
            pack_sides(2)
            send_sides(2)
            pack_rows(2)
            send_ends(2)
        with jax.named_scope("i_push2"):
            for c in range(2):
                both = dot_rows(to_blocks, recv[c])
                for y in range(2):
                    main[PUSH_X + c, y] = main[ACTIVE, y] * (
                        main[CONC, y] * both[:, y * width:(y + 1) * width] - main[PUSH_X + c, y]
                    )
            pack_flank(2)
            send_flank(2)

        def leave(get, u, v):
            dx, dy = u - get(CUR_X), v - get(CUR_Y)
            drag = get(DRAG) * jnp.sqrt(dx * dx + dy * dy + DRAG_FLOOR)
            return drag * dx, drag * dy

        outer = (lane < NSUB) | (lane >= width - NSUB)

        with jax.named_scope("i_vel1"):
            tile_loop(groups, 1, lambda g: sweep_main(g, False, True))
        with jax.named_scope("i_sweeps"):
            tile_loop((NSUB - 1) * groups, 1, lambda k: sweep_main(k % groups, True, True))
        send_rows(0, back, 2, 1, ret, 2, bulk_ssem, bulk_rsem.at[0])

        def returned(t):
            r = pl.ds(pl.multiple_of(t * TILE, TILE), TILE)
            block = sub + t * TILE
            theirs = outer | (block < 2) | (block >= count - 2)
            for y in range(2):
                half = pl.ds(y * width, width)
                u, v = main[U, y, r, :], main[V, y, r, :]
                gone = leave(lambda c: main[c, y, r, :], u, v)
                for c in range(2):
                    forc[c, r, half] = jnp.where(theirs, 0.0, gone[c])

        with jax.named_scope("i_back"):
            tile_loop(tiles, 4, returned)
            for c in range(2):
                back[c] = dot_rows(to_slots, forc[c])
        with jax.named_scope("i_waitearly"):
            when_inside(-1, 6, early_rsem.at[0])
            when_inside(1, 6, early_rsem.at[1])
            wait_tiles(2, early_rsem.at[2])
        with jax.named_scope("i_early"):
            unpack_rows(0, True)
            unpack_sides(0)
            derive_edges()
            sweep_edge(True, False)
        with jax.named_scope("i_waitmid"):
            when_inside(-1, 3, mid_rsem.at[0])
            when_inside(1, 3, mid_rsem.at[1])
            wait_tiles(2, mid_rsem.at[2])
            wait_tiles(8, mid_rsem.at[3])
        unpack_rows(1)
        unpack_sides(1)
        with jax.named_scope("i_waitlate"):
            when_inside(-1, 3, late_rsem.at[0])
            when_inside(1, 3, late_rsem.at[1])
            wait_tiles(2, late_rsem.at[2])
            wait_tiles(8, late_rsem.at[3])

        def sweep_strips(stress, velocity):
            sweep_flank(stress, velocity)
            sweep_edge(stress, velocity)

        with jax.named_scope("i_edge"):
            unpack_rows(2)
            unpack_sides(2)
            sweep_strips(False, True)
            for _ in range(NSUB - 1):
                sweep_strips(True, True)

        with jax.named_scope("i_fix"):
            for y in range(2):
                for j, far in ((1, 0), (2, count - TILE)):
                    r = pl.ds(j * TILE, TILE)
                    held = (lane >= 2) & (lane < count - 2)
                    held = held & ((sub < NSUB) if j == 1 else (sub >= TILE - NSUB))
                    u, v = flank[U, y, r, :], flank[V, y, r, :]
                    gone = leave(lambda c: flank[c, y, r, :], u, v)
                    for c in range(2):
                        slot = (c * 2 + y) * 2 * TILE + (TILE if j == 1 else 0)
                        flank_back[pl.ds(slot, TILE), :] = jnp.where(held, gone[c], 0.0)
                        flank_vel[c, y, pl.ds(far, TILE), :] = jnp.where(held, (u, v)[c], 0.0)
                for strip in range(2):
                    def get(c):
                        return edge[c, strip, y, :, pl.ds(0, width)]
                    gone = leave(get, get(U), get(V))
                    held = (sub < 2) if strip == 0 else (sub >= TILE - 2)
                    for c in range(2):
                        moved = pltpu.roll(gone[c], TILE - 2 if strip == 0 else 2, 0)
                        ends[c, pl.ds(strip * TILE, TILE), pl.ds(y * width, width)] = jnp.where(
                            held, moved, 0.0
                        )
            across = dot_lanes(to_slots, flank_back[...])
            for c in range(2):
                rest = dot_rows(to_ends, ends[c])
                for y in range(2):
                    slot = (c * 2 + y) * 2 * TILE
                    for t in range(tiles):
                        r, half = pl.ds(t * TILE, TILE), pl.ds(y * width, width)
                        moved = pltpu.roll(across[t * TILE:(t + 1) * TILE], width - TILE - slot, 1)
                        back[c, r, half] += jnp.where(outer, moved, 0.0) + (
                            rest[t * TILE:(t + 1) * TILE, y * width:(y + 1) * width]
                        )
            send_rows(0, back, 0, 2, ret, 0, bulk_ssem, bulk_rsem.at[1], "home")

        same = jnp.where(diag, 1.0, 0.0).astype(jnp.bfloat16)
        same = jnp.concatenate([same] * 2, axis=1)
        for y in range(2):
            for c in range(2):
                half = pl.ds(y * width, width)
                for strip, r in ((0, top), (1, bottom)):
                    end = pltpu.roll(
                        edge[c, strip, y, :, pl.ds(0, width)], TILE - 2 if strip == 0 else 2, 0
                    )
                    held = (sub < 2) if strip == 0 else (sub >= TILE - 2)
                    main[c, y, r, :] = jnp.where(held, end, main[c, y, r, :])
                other = dot_lanes(same, flank_vel[c, y])
                row = lax.broadcasted_iota(jnp.int32, (count, width), 0)
                column = lax.broadcasted_iota(jnp.int32, (count, width), 1)
                theirs = (row >= 2) & (row < count - 2)
                theirs = theirs & ((column < NSUB) | (column >= width - NSUB))
                out[0, c, :, half] = jnp.where(theirs, other, main[c, y])
        wait_bytes(ids.at[pl.ds(0, peers - 1)], ids_ssem)
        wait_bytes(back, bulk_ssem)
        when_inside(-1, 12, halo_ssem.at[0])
        when_inside(1, 12, halo_ssem.at[1])
        wait_tiles(6, halo_ssem.at[2])
        wait_tiles(16, halo_ssem.at[3])


def per_device_kernel(n_lat, n_lon, fields, block_owner, ice_covered, land_mask):
    count, cells = land_mask.shape
    peers = n_lat * n_lon
    f32 = jnp.float32
    anywhere = pl.BlockSpec(memory_space=pl.ANY)
    dma = pltpu.SemaphoreType.DMA
    halos = [pltpu.VMEM((2, num // 2, TILE, BX), f32) for _, num in ROUNDS] * 2
    sides = [pltpu.VMEM((2, TILE, BX), f32) for _ in ROUNDS]
    sides += [pltpu.VMEM((3, 2, TILE, BX), f32) for _ in ROUNDS]
    return pl.pallas_call(
        functools.partial(step_kernel, n_lat, n_lon),
        out_shape=pltpu.VMEM((1, 2, count, cells), f32),
        in_specs=[anywhere, anywhere, anywhere, anywhere],
        out_specs=pl.BlockSpec(memory_space=pltpu.VMEM),
        scratch_shapes=[
            pltpu.VMEM((7, count, cells), f32),
            pltpu.VMEM((2, count, cells), f32),
            pltpu.VMEM((3, count, cells), f32),
            pltpu.VMEM((1, count), jnp.int32),
            pltpu.VMEM((1, count), jnp.int32),
            pltpu.VMEM((peers, 1, count), jnp.int32),
            pltpu.VMEM((6, count, cells), f32),
            pltpu.VMEM((2, count, cells), f32),
            pltpu.VMEM((count, count), f32),
            pltpu.VMEM((3, count, cells), f32),
            pltpu.VMEM((count, cells), jnp.int32),
            pltpu.VMEM((14, 2, count, BX), f32),
            pltpu.VMEM((14, 2, 2, TILE, 2 * BX), f32),
            pltpu.VMEM((14, 2, 4 * TILE, BX), f32),
            pltpu.VMEM((BX, count), f32),
            pltpu.VMEM((2, 2, BX, count), f32),
            pltpu.VMEM((2, 2 * TILE, cells), f32),
            pltpu.VMEM((2, 2, 2, TILE, BX), f32),
            *halos, *sides,
            dma, dma((2,)), dma, dma, dma((4,)), dma((4,)), dma((4,)), dma((4,)),
            pltpu.SemaphoreType.REGULAR,
        ],
        compiler_params=pltpu.CompilerParams(
            collective_id=0, has_side_effects=True, vmem_limit_bytes=63 * 1024 * 1024
        ),
    )(fields, block_owner.reshape(1, count), ice_covered.reshape(1, count), land_mask)


def solution(mesh):
    placed = (
        P("comp", None, ("lat", "lon"), None),
        P(("lat", "lon")),
        P(("lat", "lon")),
        P(("lat", "lon"), None),
    )
    n_lat, n_lon = mesh.shape["lat"], mesh.shape["lon"]

    def body(fields, block_owner, ice_covered, land_mask):
        count = block_owner.shape[0]
        whole_tiles = count % (n_lat * n_lon * TILE) == 0 and count == BX
        if whole_tiles and n_lon > 2:
            return per_device_kernel(n_lat, n_lon, fields, block_owner, ice_covered, land_mask)
        return per_device(fields, block_owner, ice_covered, land_mask)

    return jax.shard_map(
        body,
        mesh=mesh,
        in_specs=placed,
        out_specs=P("comp", None, ("lat", "lon"), None),
        check_vma=False,
    )
```

```python
import functools

import jax
import jax.numpy as jnp
from jax import lax
from jax.experimental import pallas as pl
from jax.experimental.pallas import tpu as pltpu
from jax.sharding import PartitionSpec as P

GX = 1
BY = 2
BX = 128
NSUB = 4


CD_ICE = 0.1
CW = 1.5
CSTAR = 2.0
ECC2 = 4.0
DMIN2 = 0.25
RELAX = 0.5
DTE = 0.5
CORIO = 0.3
MASS_FLOOR = 0.5
DRAG_FLOOR = 0.1


def from_behind(x, axis, by):
    size = lax.axis_size(axis)
    pairs = [(i, i + by) for i in range(size) if 0 <= i + by < size]
    return lax.ppermute(x, axis, pairs)


def with_halo(x, sides, width, wrap):
    for axis, dim in sides:
        size, length = (lax.axis_size(axis), x.shape[dim])
        up = [(i, (i + 1) % size) for i in range(size if wrap else size - 1)]
        down = [(j, i) for i, j in up]
        last = lax.slice_in_dim(x, length - width, length, axis=dim)
        first = lax.slice_in_dim(x, 0, width, axis=dim)
        before = lax.ppermute(last, axis, up)
        after = lax.ppermute(first, axis, down)
        x = jnp.concatenate([before, x, after], axis=dim)
    return x


def air_stress(ocean):
    wind_x, wind_y, current_x, current_y, tilt_x, tilt_y, density = ocean
    speed_ice = jnp.sqrt(wind_x * wind_x + wind_y * wind_y + 1.0)
    scale_ice = density * CD_ICE * speed_ice
    rel_x = wind_x - current_x
    rel_y = wind_y - current_y
    speed_open = jnp.sqrt(rel_x * rel_x + rel_y * rel_y + 1.0)
    scale_open = density * (0.1 + 0.05 * speed_open) * speed_open
    outbound = jnp.stack(
        [scale_ice * wind_x, scale_ice * wind_y, current_x, current_y, tilt_x, tilt_y]
    )
    open_stress = jnp.stack([scale_open * rel_x, scale_open * rel_y])
    return (outbound, open_stress)


def prepare(ice_tile, forcing, active):
    ice_mass = ice_tile[2]
    concentration = ice_tile[3]
    strength = ice_mass * jnp.exp(CSTAR * (concentration - 1.0)) * active
    drag_base = CW * concentration * active
    push_x = active * (concentration * forcing[0] - ice_mass * forcing[4])
    push_y = active * (concentration * forcing[1] - ice_mass * forcing[5])
    return jnp.stack(
        [strength, ice_mass, drag_base, push_x, push_y, forcing[2], forcing[3], active]
    )


def subcycle(ice_state, statics):
    east_vel, north_vel, stress_one, stress_two, stress_three = ice_state
    strength = statics[0]
    east_base = east_vel[:-1, :-1]
    north_base = north_vel[:-1, :-1]
    strain_xx = east_vel[:-1, 1:] - east_base
    strain_yy = north_vel[1:, :-1] - north_base
    shear = east_vel[1:, :-1] - east_base + (north_vel[:-1, 1:] - north_base)
    divergence = strain_xx + strain_yy
    tension = strain_xx - strain_yy
    delta_norm = jnp.sqrt(
        divergence * divergence + (tension * tension + shear * shear) / ECC2 + DMIN2
    )
    viscosity = strength[:-1, :-1] / delta_norm
    stress_sum = (stress_one[:-1, :-1] + RELAX * viscosity * (divergence - delta_norm)) / (
        1.0 + RELAX
    )
    stress_diff = (stress_two[:-1, :-1] + RELAX * viscosity * tension / ECC2) / (1.0 + RELAX)
    stress_shear = (stress_three[:-1, :-1] + RELAX * viscosity * shear / (2.0 * ECC2)) / (
        1.0 + RELAX
    )
    stress_xx = 0.5 * (stress_sum + stress_diff)
    stress_yy = 0.5 * (stress_sum - stress_diff)
    force_x = (
        stress_xx[1:, 1:] - stress_xx[1:, :-1] + (stress_shear[1:, 1:] - stress_shear[:-1, 1:])
    )
    force_y = (
        stress_shear[1:, 1:] - stress_shear[1:, :-1] + (stress_yy[1:, 1:] - stress_yy[:-1, 1:])
    )
    trimmed = statics[:, 1:-1, 1:-1]
    strength, ice_mass, drag_base, push_x, push_y, current_x, current_y, active = trimmed
    east_old = east_vel[1:-1, 1:-1]
    north_old = north_vel[1:-1, 1:-1]
    diff_x = current_x - east_old
    diff_y = current_y - north_old
    drag_coef = drag_base * jnp.sqrt(diff_x * diff_x + diff_y * diff_y + DRAG_FLOOR)
    denominator = jnp.maximum(ice_mass, MASS_FLOOR) / DTE + drag_coef
    east_new = (
        active
        * (
            ice_mass / DTE * east_old
            + force_x
            + push_x
            + drag_coef * current_x
            + CORIO * ice_mass * north_old
        )
        / denominator
    )
    north_new = (
        active
        * (
            ice_mass / DTE * north_old
            + force_y
            + push_y
            + drag_coef * current_y
            - CORIO * ice_mass * east_old
        )
        / denominator
    )
    new_state = jnp.stack(
        [east_new, north_new, stress_sum[1:, 1:], stress_diff[1:, 1:], stress_shear[1:, 1:]]
    )
    return (new_state, trimmed)


def give_back(ice_state, statics):
    east_vel = ice_state[0]
    north_vel = ice_state[1]
    drag_base = statics[2]
    current_x = statics[5]
    current_y = statics[6]
    diff_x = east_vel - current_x
    diff_y = north_vel - current_y
    factor = drag_base * jnp.sqrt(diff_x * diff_x + diff_y * diff_y + DRAG_FLOOR)
    return jnp.stack([factor * diff_x, factor * diff_y, drag_base / CW])


def to_tile(blocks):
    channels, count, cells = blocks.shape
    arranged = blocks.reshape(channels, count // GX, GX, BY, BX).transpose(0, 1, 3, 2, 4)
    return arranged.reshape(channels, count // GX * BY, GX * BX)


def from_tile(values):
    channels, rows, columns = values.shape
    arranged = values.reshape(channels, rows // BY, BY, GX, BX).transpose(0, 1, 3, 2, 4)
    return arranged.reshape(channels, rows // BY * GX, BY * BX)


def per_device(fields, block_owner, ice_covered, land_mask):
    count = block_owner.shape[0]
    is_ocean = lax.axis_index("comp") == 0
    outbound, open_stress = air_stress(fields[0])
    owner_row = block_owner.reshape(1, count)
    crossed = from_behind(outbound, "comp", 1)
    received, anchor = (
        lax.all_to_all(crossed, ("lat", "lon"), split_axis=1, concat_axis=1, tiled=True),
        lax.all_to_all(owner_row, ("lat", "lon"), split_axis=1, concat_axis=1, tiled=True),
    )
    local_ids = anchor[0] % count
    position = jnp.zeros((count,), jnp.int32).at[local_ids].set(jnp.arange(count, dtype=jnp.int32))
    forcing = to_tile(received[:, position])
    ice_tile = to_tile(fields[0])
    covered = ice_covered.astype(jnp.float32)[:, None] * (1 - land_mask).astype(jnp.float32)
    active = to_tile(covered[None])[0]
    statics = prepare(ice_tile, forcing, active)
    ice_state = jnp.stack([ice_tile[0], ice_tile[1], ice_tile[4], ice_tile[5], ice_tile[6]])
    joined = jnp.concatenate([ice_state, statics], 0)
    joined = with_halo(joined, (("lon", 2),), NSUB, True)
    joined = with_halo(joined, (("lat", 1),), NSUB, False)
    ice_state = joined[:5]
    statics = joined[5:]
    for repeat in range(NSUB):
        ice_state, statics = subcycle(ice_state, statics)
    returned = from_tile(give_back(ice_state, statics))
    back_send = returned[:, local_ids]
    regrouped = lax.all_to_all(back_send, ("lat", "lon"), split_axis=1, concat_axis=1, tiled=True)
    received_back = from_behind(regrouped, "comp", -1)
    ocean_out = received_back[:2] + (1.0 - received_back[2]) * open_stress
    ice_out = from_tile(ice_state[:2])
    return jnp.where(is_ocean, ocean_out, ice_out)[None]


TILE = 8
GROUP = 8
MESH = pl.DeviceIdType.MESH
U, V, MASS, CONC, S1, S2, S12, ACTIVE, PUSH_X, PUSH_Y, CUR_X, CUR_Y, STRENGTH, DRAG = range(14)
SIDES = [(a, b) for b in (-1, 1) for a in (-1, 1, 0)]
ROUNDS = ((U, 8), (CUR_X, 2), (PUSH_X, 2))
KEEP = 1.0 / (1.0 + RELAX)


def tile_loop(tiles, together, body):
    def step(k, carry):
        for j in range(together):
            body(k * together + j)
        return carry
    lax.fori_loop(0, tiles // together, step, 0)


def pieces(values, axis):
    high = values.astype(jnp.bfloat16)
    low = (values - high.astype(jnp.float32)).astype(jnp.bfloat16)
    return jnp.concatenate([high, low], axis=axis)


def dot_rows(twice, values):
    return lax.dot_general(
        twice, pieces(values, 0), (((1,), (0,)), ((), ())), preferred_element_type=jnp.float32
    )


def dot_lanes(twice, values):
    return lax.dot_general(
        twice, pieces(values, 1), (((1,), (1,)), ((), ())), preferred_element_type=jnp.float32
    )


def new_stress(strength, s1, s2, s12, u, v, u_east, v_east, u_up, v_up):
    sxx = u_east - u
    syy = v_up - v
    shear = (u_up - u) + (v_east - v)
    div = sxx + syy
    ten = sxx - syy
    square = div * div + (ten * ten + shear * shear) * (1.0 / ECC2) + DMIN2
    inverse = lax.rsqrt(square)
    visc = strength * inverse
    s1 = s1 * KEEP + visc * (div - square * inverse)
    s2 = s2 * KEEP + visc * ten * (1.0 / ECC2)
    s12 = s12 * KEEP + visc * shear * (0.5 / ECC2)
    return s1, s2, s12


def new_velocity(get, u, v, force_x, force_y):
    mass, cx, cy = get(MASS), get(CUR_X), get(CUR_Y)
    dx, dy = cx - u, cy - v
    square = dx * dx + dy * dy + DRAG_FLOOR
    drag = get(DRAG) * (square * lax.rsqrt(square))
    gain = get(ACTIVE) / (jnp.maximum(mass, MASS_FLOOR) * (1.0 / DTE) + drag)
    inertia = mass * (1.0 / DTE)
    turn = CORIO * mass
    return (
        gain * (inertia * u + force_x + get(PUSH_X) + drag * cx + turn * v),
        gain * (inertia * v + force_y + get(PUSH_Y) + drag * cy - turn * u),
    )


def step_kernel(
    n_lat, n_lon,
    fields, owner_hbm, covered_hbm, land, out,
    surf, open_st, ret, owner, covered, ids, recv, forc, one_hot, back, land_v,
    main, edge, flank, flank_back, flank_vel, ends,
    rows_out0, rows_out1, rows_out2, rows_got0, rows_got1, rows_got2,
    side_out0, side_out1, side_out2, side_got0, side_got1, side_got2,
    bulk_ssem, bulk_rsem, ids_ssem, ids_rsem, halo_ssem, early_rsem, mid_rsem, late_rsem, ready,
):
    comp = lax.axis_index("comp")
    lat = lax.axis_index("lat")
    lon = lax.axis_index("lon")
    peers = n_lat * n_lon
    me = lat * n_lon + lon
    count = owner.shape[1]
    per = count // peers
    width = BX
    barrier = pltpu.get_barrier_semaphore()
    rows_out = (rows_out0, rows_out1, rows_out2)
    rows_got = (rows_got0, rows_got1, rows_got2)
    side_out = (side_out0, side_out1, side_out2)
    side_got = (side_got0, side_got1, side_got2)

    def rows_of(peer):
        return pl.ds(pl.multiple_of(peer * per, per), per)

    planes = [jnp.where(lat < n_lat // 2, n_lat - 1 - j, j) for j in range(n_lat)]
    places = [(lon + i) % n_lon for i in range(n_lon)]

    half_lat = n_lat // 2
    groups_of = {
        "all": ((planes, places),),
        "column": ((planes[:half_lat], places[:1]),),
        "beyond": ((planes[:half_lat], places[1:]),),
        "near": ((planes[half_lat:], places),),
    }

    def each_peer(body, part="all"):
        for chosen, along in groups_of[part]:
            for plane in chosen:
                for place in along:
                    body(plane * n_lon + place, plane, place)

    def home_first(body):
        body(0, 0, 0)
        for plane in range(n_lat):
            for place in places:
                if plane:
                    body(plane * n_lon + place, plane, place)
                else:
                    @pl.when(place > 0)
                    def _():
                        body(place, 0, place)

    def signal_peers(kind, part="all"):
        each_peer(
            lambda p, plane, place: pl.semaphore_signal(
                barrier, inc=1, device_id=(kind, plane, place), device_id_type=MESH
            ),
            part,
        )

    def send_rows(kind, src, lo, num, dst, dlo, ssem, rsem, part="all"):
        def body(p, plane, place):
            pltpu.make_async_remote_copy(
                src_ref=src.at[pl.ds(lo, num), rows_of(p), :],
                dst_ref=dst.at[pl.ds(dlo, num), rows_of(me), :],
                send_sem=ssem, recv_sem=rsem,
                device_id=(kind, plane, place), device_id_type=MESH,
            ).start()
        home_first(body) if part == "home" else each_peer(body, part)

    def wait_bytes(ref, sem):
        pltpu.make_async_copy(ref, ref, sem).wait()

    def wait_tiles(num, sem):
        wait_bytes(main.at[0, 0, pl.ds(0, num * TILE), :], sem)

    @pl.when(comp == 0)
    def _ocean():
        signal_peers(1)
        raw = pltpu.make_async_copy(fields.at[0, pl.ds(2, 4)], surf.at[pl.ds(2, 4)], halo_ssem.at[0])
        wind = pltpu.make_async_copy(fields.at[0, pl.ds(0, 2)], surf.at[pl.ds(0, 2)], halo_ssem.at[1])
        rho = pltpu.make_async_copy(fields.at[0, pl.ds(6, 1)], surf.at[pl.ds(6, 1)], halo_ssem.at[2])
        raw.start()
        wind.start()
        rho.start()
        with jax.named_scope("o_barrier"):
            pl.semaphore_wait(barrier, half_lat)

        def send_four(part):
            send_rows(1, surf, 2, 4, recv, 2, bulk_ssem, bulk_rsem.at[0], part)

        def send_two(part):
            send_rows(1, forc, 0, 2, recv, 0, bulk_ssem, bulk_rsem.at[1], part)

        with jax.named_scope("o_send4"):
            raw.wait()
            send_four("column")
            wind.wait()
            rho.wait()

        def stress(t):
            r = pl.ds(pl.multiple_of(t * TILE, TILE), TILE)
            wx, wy, density = surf[0, r, :], surf[1, r, :], surf[6, r, :]
            scale = density * CD_ICE * jnp.sqrt(wx * wx + wy * wy + 1.0)
            forc[0, r, :] = scale * wx
            forc[1, r, :] = scale * wy

        with jax.named_scope("o_stress"):
            tile_loop(count // TILE, 4, stress)
            send_two("column")
        with jax.named_scope("o_ready"):
            pl.semaphore_wait(ready, 1)
        with jax.named_scope("o_rest"):
            send_four("beyond")
            send_two("beyond")
            send_four("near")
            send_two("near")

        def open_water(t):
            r = pl.ds(pl.multiple_of(t * TILE, TILE), TILE)
            density = surf[6, r, :]
            rel_x = surf[0, r, :] - surf[2, r, :]
            rel_y = surf[1, r, :] - surf[3, r, :]
            speed = jnp.sqrt(rel_x * rel_x + rel_y * rel_y + 1.0)
            scale = density * (0.1 + 0.05 * speed) * speed
            open_st[0, r, :] = scale * rel_x
            open_st[1, r, :] = scale * rel_y

        tile_loop(count // TILE, 2, open_water)
        with jax.named_scope("o_waitret1"):
            wait_bytes(ret.at[pl.ds(2, 1)], bulk_rsem.at[0])

        def water(t):
            r = pl.ds(pl.multiple_of(t * TILE, TILE), TILE)
            share = 1.0 - ret[2, r, :]
            for c in range(2):
                open_st[c, r, :] = share * open_st[c, r, :]

        tile_loop(count // TILE, 4, water)
        with jax.named_scope("o_waitret2"):
            wait_bytes(ret.at[pl.ds(0, 2)], bulk_rsem.at[1])

        def finish(t):
            r = pl.ds(pl.multiple_of(t * TILE, TILE), TILE)
            for c in range(2):
                out[0, c, r, :] = ret[c, r, :] + open_st[c, r, :]

        tile_loop(count // TILE, 4, finish)
        wait_bytes(surf.at[pl.ds(0, 6)], bulk_ssem)

    @pl.when(comp == 1)
    def _ice():
        def inside(a):
            if a == 0:
                return lat >= 0
            return lat + a >= 0 if a < 0 else lat + a < n_lat

        def around(a, b):
            return (1, lat + a, (lon + b + n_lon) % n_lon)

        signal_peers(0, "column")
        for a in range(n_lat):
            for b in range(n_lon):
                if a or b:
                    pl.semaphore_signal(
                        barrier, inc=1, device_id=(1, (lat + a) % n_lat, (lon + b) % n_lon),
                        device_id_type=MESH,
                    )
        for y in range(2):
            pltpu.make_async_copy(
                fields.at[0, :, :, pl.ds(y * width, width)], main.at[pl.ds(0, 7), y], halo_ssem.at[0]
            ).start()
        loads = [
            pltpu.make_async_copy(land, land_v, halo_ssem.at[1]),
            pltpu.make_async_copy(covered_hbm, covered, halo_ssem.at[2]),
        ]
        names = pltpu.make_async_copy(owner_hbm, owner, halo_ssem.at[3])
        names.start()
        for load in loads:
            load.start()
        with jax.named_scope("i_barrier"):
            pl.semaphore_wait(barrier, 2 * peers - 1)
            pl.semaphore_signal(ready, inc=1, device_id=(0, lat, lon), device_id_type=MESH)
            names.wait()
            for a in range(n_lat):
                for b in range(n_lon):
                    if a or b:
                        pltpu.make_async_remote_copy(
                            src_ref=owner, dst_ref=ids.at[me], send_sem=ids_ssem, recv_sem=ids_rsem,
                            device_id=(1, (lat + a) % n_lat, (lon + b) % n_lon),
                            device_id_type=MESH,
                        ).start()
        ids[me] = owner[...]

        tiles = count // TILE
        top, bottom = pl.ds(0, TILE), pl.ds(count - TILE, TILE)
        zero_tile = jnp.zeros((TILE, width), jnp.float32)
        for wall, which in ((lat == 0, 0), (lat == n_lat - 1, 1)):
            @pl.when(wall)
            def _():
                for e in range(3):
                    for k in range(rows_got[e].shape[1]):
                        rows_got[e][which, k] = zero_tile
                    for k in range(2):
                        side_got[e][2 * which, k] = zero_tile

        def clear(t):
            r = pl.ds(pl.multiple_of(t * TILE, TILE), TILE)
            for c in range(2):
                for y in range(2):
                    flank_vel[c, y, r, :] = zero_tile
            flank_back[r, :] = zero_tile

        tile_loop(tiles, 2, clear)
        wait_bytes(main.at[pl.ds(0, 7)], halo_ssem.at[0])
        for load in loads:
            load.wait()
        diag = lax.broadcasted_iota(jnp.int32, (count, count), 0) == lax.broadcasted_iota(
            jnp.int32, (count, count), 1
        )
        wet = jnp.sum(
            jnp.where(diag, covered[...].astype(jnp.float32), 0.0), axis=1, keepdims=True
        )
        sea = wet * (1 - land_v[...]).astype(jnp.float32)
        for y in range(2):
            main[ACTIVE, y] = sea[:, y * width:(y + 1) * width]

        lane = lax.broadcasted_iota(jnp.int32, (TILE, width), 1)
        sub = lax.broadcasted_iota(jnp.int32, (TILE, width), 0)
        pick_row = lax.broadcasted_iota(jnp.int32, (2 * TILE, width), 0)
        pick_col = lax.broadcasted_iota(jnp.int32, (2 * TILE, width), 1)
        picked = jnp.where(pick_row < TILE, pick_row, pick_row + (width - 2 * TILE)) == pick_col
        picker = jnp.where(picked, 1.0, 0.0).astype(jnp.bfloat16)
        picker = jnp.concatenate([picker] * 2, axis=1)

        def pack_rows(e):
            lo, num = ROUNDS[e]
            for k in range(num // 2):
                ups, downs = zero_tile, zero_tile
                for i in range(4):
                    c, y = lo + 2 * k + i // 2, i % 2
                    head, foot = main[c, y, top, :], main[c, y, bottom, :]
                    here = (sub >= 2 * i) & (sub < 2 * i + 2)
                    ups = jnp.where(here, pltpu.roll(head, 2 * i, 0) if i else head, ups)
                    downs = jnp.where(here, pltpu.roll(foot, (2 * i + 2) % TILE, 0) if i < 3 else foot, downs)
                rows_out[e][0, k] = ups
                rows_out[e][1, k] = downs

        def pack_sides(e):
            lo, num = ROUNDS[e]
            west, east = zero_tile, zero_tile
            for i in range(2 * num):
                c, y = lo + i // 2, i % 2
                ends = jnp.where(sub < NSUB, main[c, y, top, :], main[c, y, bottom, :])
                slot = i * NSUB
                mine = (lane >= slot) & (lane < slot + NSUB)
                west = jnp.where(mine, pltpu.roll(ends, slot, 1) if slot else ends, west)
                east = jnp.where(mine, pltpu.roll(ends, (slot + NSUB) % width, 1), east)
            side_out[e][0] = west
            side_out[e][1] = east

        def pack_flank(e):
            lo, num = ROUNDS[e]
            for c in range(lo, lo + num):
                for y in range(2):
                    across = dot_lanes(picker, main[c, y])
                    flank[c, y, pl.ds(TILE, TILE), :] = across[:TILE]
                    flank[c, y, pl.ds(2 * TILE, TILE), :] = across[TILE:]

        def push_on(e, a, b, src, dst, lane_of_sem, recv_lane):
            sems = (early_rsem, mid_rsem, late_rsem)[e]

            @pl.when(inside(a))
            def _():
                pltpu.make_async_remote_copy(
                    src_ref=src, dst_ref=dst,
                    send_sem=halo_ssem.at[lane_of_sem], recv_sem=sems.at[recv_lane],
                    device_id=around(a, b), device_id_type=MESH,
                ).start()

        def send_ends(e):
            for a in (-1, 1):
                k = 1 if a > 0 else 0
                push_on(e, a, 0, rows_out[e].at[k], rows_got[e].at[1 - k], k, 1 - k)

        def send_sides(e):
            for a, b in SIDES:
                k = 1 if b > 0 else 0
                group = {0: 2, -1: 0, 1: 1}[a]
                land_in = {0: 2, -1: 1, 1: 0}[a]
                push_on(e, a, b, side_out[e].at[k], side_got[e].at[1 - a, 1 - k], group, land_in)

        def send_flank(e):
            lo, num = ROUNDS[e]
            for b in (-1, 1):
                src, dst = (2 * TILE, 0) if b > 0 else (TILE, 3 * TILE)
                push_on(
                    e, 0, b,
                    flank.at[pl.ds(lo, num), :, pl.ds(src, TILE), :],
                    flank.at[pl.ds(lo, num), :, pl.ds(dst, TILE), :], 3, 3,
                )

        def when_inside(a, num, sem):
            @pl.when(inside(a))
            def _():
                wait_tiles(num, sem)

        def own_rows():
            for c in range(ROUNDS[0][1]):
                for y in range(2):
                    edge[c, 0, y, :, pl.ds(0, width)] = pltpu.roll(main[c, y, top, :], 2, 0)
                    edge[c, 1, y, :, pl.ds(0, width)] = pltpu.roll(main[c, y, bottom, :], TILE - 2, 0)

        def unpack_rows(e, placed=False):
            lo, num = ROUNDS[e]
            got = rows_got[e]
            for k in range(num // 2):
                for i in range(4):
                    c, y = lo + 2 * k + i // 2, i % 2
                    north = pltpu.roll(got[0, k], (TILE - 2 * i) % TILE, 0) if i else got[0, k]
                    south = pltpu.roll(got[1, k], TILE - 2 - 2 * i, 0) if i < 3 else got[1, k]
                    if placed:
                        head, foot = (edge[c, strip, y, :, pl.ds(0, width)] for strip in range(2))
                    else:
                        head = pltpu.roll(main[c, y, top, :], 2, 0)
                        foot = pltpu.roll(main[c, y, bottom, :], TILE - 2, 0)
                    edge[c, 0, y, :, pl.ds(0, width)] = jnp.where(sub < 2, north, head)
                    edge[c, 1, y, :, pl.ds(0, width)] = jnp.where(sub >= TILE - 2, south, foot)

        def unpack_sides(e):
            lo, num = ROUNDS[e]
            side = side_got[e]
            ends = []
            for k in range(2):
                far, near = side[0, k], side[1, k]
                ends.append(pltpu.roll(jnp.where(sub >= TILE - 2, far, near), 2, 0))
            for k in range(2):
                far, near = side[2, k], side[1, k]
                ends.append(pltpu.roll(jnp.where(sub < 2, far, near), TILE - 2, 0))
            for i in range(2 * num):
                c, y = lo + i // 2, i % 2
                slot = i * NSUB
                for strip in range(2):
                    from_west, from_east = ends[2 * strip], ends[2 * strip + 1]
                    from_east = pltpu.roll(from_east, width - slot, 1) if slot else from_east
                    from_west = pltpu.roll(from_west, width - NSUB - slot, 1)
                    edge[c, strip, y, :, pl.ds(width, width)] = jnp.where(
                        lane < NSUB, from_east, jnp.where(lane >= width - NSUB, from_west, 0.0)
                    )

        def derive(load, store):
            conc, act = load(CONC), load(ACTIVE)
            store(STRENGTH, (RELAX * KEEP) * load(MASS) * jnp.exp(CSTAR * (conc - 1.0)) * act)
            store(DRAG, CW * conc * act)

        def derive_main(t):
            r = pl.ds(pl.multiple_of(t * TILE, TILE), TILE)
            for y in range(2):
                def store(c, x):
                    main[c, y, r, :] = x
                derive(lambda c: main[c, y, r, :], store)

        def derive_flank():
            for y in range(2):
                def store(c, x):
                    flank[c, y] = x
                derive(lambda c: flank[c, y], store)

        def derive_edges():
            for y in range(2):
                for strip in range(2):
                    def store(c, x):
                        edge[c, strip, y] = x
                    derive(lambda c: edge[c, strip, y], store)

        def sweep_main(g, stress, velocity):
            spots = [pl.ds((g * GROUP + j) * TILE, TILE) for j in range(GROUP)]
            behind = pl.ds(max(g * GROUP - 1, 0) * TILE, TILE)
            ahead = pl.ds(min(g * GROUP + GROUP, tiles - 1) * TILE, TILE)
            vels = [[(main[U, y, r, :], main[V, y, r, :]) for y in range(2)] for r in spots]
            stresses = []
            if stress:
                follow = (main[U, 0, ahead, :], main[V, 0, ahead, :])
            for j, r in enumerate(spots):
                old = [tuple(main[c, y, r, :] for c in (S1, S2, S12)) for y in range(2)]
                if not stress:
                    stresses.append(old)
                    continue
                beyond = vels[j + 1][0] if j + 1 < GROUP else follow
                row = []
                for y in range(2):
                    u, v = vels[j][y]
                    if y == 0:
                        u_up, v_up = vels[j][1]
                    else:
                        u_up, v_up = (
                            pltpu.roll(jnp.where(sub == 0, after, x), TILE - 1, 0)
                            for x, after in zip(vels[j][0], beyond)
                        )
                    fresh = new_stress(
                        main[STRENGTH, y, r, :], *old[y], u, v,
                        pltpu.roll(u, width - 1, 1), pltpu.roll(v, width - 1, 1), u_up, v_up,
                    )
                    for c, x in zip((S1, S2, S12), fresh):
                        main[c, y, r, :] = x
                    row.append(fresh)
                stresses.append(row)
            if not velocity:
                return
            yy_before = 0.5 * (main[S1, 1, behind, :] - main[S2, 1, behind, :])
            cross_before = main[S12, 1, behind, :]
            for j, r in enumerate(spots):
                xx = [0.5 * (s1 + s2) for s1, s2, _ in stresses[j]]
                yy = [0.5 * (s1 - s2) for s1, s2, _ in stresses[j]]
                cross = [s12 for _, _, s12 in stresses[j]]
                yy_down, cross_down = (
                    [pltpu.roll(jnp.where(sub == TILE - 1, before, x[1]), 1, 0), x[0]]
                    for x, before in ((yy, yy_before), (cross, cross_before))
                )
                yy_before, cross_before = yy[1], cross[1]
                for y in range(2):
                    force_x = xx[y] - pltpu.roll(xx[y], 1, 1) + (cross[y] - cross_down[y])
                    force_y = cross[y] - pltpu.roll(cross[y], 1, 1) + (yy[y] - yy_down[y])
                    u, v = new_velocity(lambda c: main[c, y, r, :], *vels[j][y], force_x, force_y)
                    main[U, y, r, :] = u
                    main[V, y, r, :] = v

        def sweep_edge(stress, velocity):
            lanes = 2 * width

            for strip in range(2):
                vels = [(edge[U, strip, y], edge[V, strip, y]) for y in range(2)]
                fresh = [tuple(edge[c, strip, y] for c in (S1, S2, S12)) for y in range(2)]
                if stress:
                    ups = [vels[1], tuple(pltpu.roll(x, TILE - 1, 0) for x in vels[0])]
                    for y in range(2):
                        east = [pltpu.roll(x, lanes - 1, 1) for x in vels[y]]
                        fresh[y] = new_stress(
                            edge[STRENGTH, strip, y], *fresh[y], *vels[y], *east, *ups[y]
                        )
                        for c, x in zip((S1, S2, S12), fresh[y]):
                            edge[c, strip, y] = x
                if not velocity:
                    continue
                xx = [0.5 * (s1 + s2) for s1, s2, _ in fresh]
                yy = [0.5 * (s1 - s2) for s1, s2, _ in fresh]
                cross = [s12 for _, _, s12 in fresh]
                yy_down, cross_down = ([pltpu.roll(x[1], 1, 0), x[0]] for x in (yy, cross))
                for y in range(2):
                    force_x = xx[y] - pltpu.roll(xx[y], 1, 1) + (cross[y] - cross_down[y])
                    force_y = cross[y] - pltpu.roll(cross[y], 1, 1) + (yy[y] - yy_down[y])
                    u, v = new_velocity(lambda c: edge[c, strip, y], *vels[y], force_x, force_y)
                    edge[U, strip, y] = u
                    edge[V, strip, y] = v

        def sweep_flank(stress, velocity):
            spots = [pl.ds(j * TILE, TILE) for j in range(4)]
            vels = [[(flank[U, y, r, :], flank[V, y, r, :]) for y in range(2)] for r in spots]
            fresh = [
                [tuple(flank[c, y, r, :] for c in (S1, S2, S12)) for y in range(2)] for r in spots
            ]
            if stress:
                for j, r in enumerate(spots):
                    for y in range(2):
                        after = vels[min(j + 1, 3)][y]
                        east = [
                            pltpu.roll(jnp.where(sub == 0, b, x), TILE - 1, 0)
                            for x, b in zip(vels[j][y], after)
                        ]
                        ups = vels[j][1] if y == 0 else [
                            pltpu.roll(x, width - 1, 1) for x in vels[j][0]
                        ]
                        fresh[j][y] = new_stress(
                            flank[STRENGTH, y, r, :], *fresh[j][y], *vels[j][y], *east, *ups
                        )
                        for c, x in zip((S1, S2, S12), fresh[j][y]):
                            flank[c, y, r, :] = x
            if not velocity:
                return
            xx = [[0.5 * (s1 + s2) for s1, s2, _ in row] for row in fresh]
            yy = [[0.5 * (s1 - s2) for s1, s2, _ in row] for row in fresh]
            cross = [[s12 for _, _, s12 in row] for row in fresh]

            def westward(x, j, y):
                before = x[max(j - 1, 0)][y]
                return pltpu.roll(jnp.where(sub == TILE - 1, before, x[j][y]), 1, 0)

            def downward(x, j, y):
                return x[j][0] if y == 1 else pltpu.roll(x[j][1], 1, 1)

            for j, r in enumerate(spots):
                for y in range(2):
                    force_x = xx[j][y] - westward(xx, j, y) + (cross[j][y] - downward(cross, j, y))
                    force_y = cross[j][y] - westward(cross, j, y) + (yy[j][y] - downward(yy, j, y))
                    u, v = new_velocity(lambda c: flank[c, y, r, :], *vels[j][y], force_x, force_y)
                    flank[U, y, r, :] = u
                    flank[V, y, r, :] = v

        with jax.named_scope("i_pack0"):
            pack_flank(0)
            send_flank(0)
            pack_rows(0)
            pack_sides(0)
        tile_loop(tiles, 2, derive_main)

        with jax.named_scope("i_waitids"):
            wait_bytes(ids.at[pl.ds(0, peers - 1)], ids_rsem)
        wanted = me * per
        row_lane = lax.broadcasted_iota(jnp.int32, (per, count), 1)
        row_sub = lax.broadcasted_iota(jnp.int32, (per, count), 0)
        mine = row_lane == row_sub + wanted
        blocks = lax.broadcasted_iota(jnp.int32, (per, count), 1).astype(jnp.float32)
        base = (me * count).astype(jnp.float32)
        for p in range(peers):
            owned = jnp.broadcast_to(ids[p], (per, count)).astype(jnp.float32)
            local = jnp.sum(jnp.where(mine, owned, 0.0), axis=1, keepdims=True) - base
            one_hot[pl.ds(p * per, per), :] = jnp.where(local == blocks, 1.0, 0.0)

        with jax.named_scope("i_waithalo0"):
            for sems in (halo_ssem, early_rsem):
                wait_bytes(main.at[0], sems.at[3])
        with jax.named_scope("i_unpack0"):
            derive_flank()
            own_rows()

        def sweep_all(stress, velocity):
            for g in range(tiles // GROUP):
                sweep_main(g, stress, velocity)

        with jax.named_scope("i_stress"):
            sweep_all(True, False)
            sweep_flank(True, False)
        by_slot = one_hot[...]
        to_slots = jnp.concatenate([by_slot.astype(jnp.bfloat16)] * 2, axis=1)
        to_ends = jnp.concatenate([by_slot[:, :TILE], by_slot[:, count - TILE:]] * 2, axis=1)
        to_ends = to_ends.astype(jnp.bfloat16)
        by_block = by_slot.T.astype(jnp.bfloat16)
        to_blocks = jnp.concatenate([by_block] * 2, axis=1)

        with jax.named_scope("i_waitf4"):
            wait_bytes(recv.at[pl.ds(2, 4)], bulk_rsem.at[0])
        for c in range(2):
            both = dot_rows(to_blocks, recv[2 + c])
            for y in range(2):
                main[CUR_X + c, y] = both[:, y * width:(y + 1) * width]
        with jax.named_scope("i_packmid"):
            send_sides(0)
            send_ends(0)
            pack_rows(1)
            pack_sides(1)
            send_ends(1)
            send_sides(1)
            pack_flank(1)
            send_flank(1)
        for c in range(2):
            both = dot_rows(to_blocks, recv[4 + c])
            for y in range(2):
                main[PUSH_X + c, y] = main[MASS, y] * both[:, y * width:(y + 1) * width]
        for y in range(2):
            share = main[CONC, y] * main[ACTIVE, y]
            back[2, :, pl.ds(y * width, width)] = dot_rows(to_slots, share)

        with jax.named_scope("i_waitf2"):
            wait_bytes(recv.at[pl.ds(0, 2)], bulk_rsem.at[1])
        with jax.named_scope("i_push"):
            for c in range(2):
                both = dot_rows(to_blocks, recv[c])
                for y in range(2):
                    main[PUSH_X + c, y] = main[ACTIVE, y] * (
                        main[CONC, y] * both[:, y * width:(y + 1) * width] - main[PUSH_X + c, y]
                    )
        with jax.named_scope("i_packlate"):
            pack_sides(2)
            send_sides(2)
            pack_flank(2)
            send_flank(2)
            pack_rows(2)
            send_ends(2)

        def leave(get, u, v):
            dx, dy = u - get(CUR_X), v - get(CUR_Y)
            drag = get(DRAG) * jnp.sqrt(dx * dx + dy * dy + DRAG_FLOOR)
            return drag * dx, drag * dy

        outer = (lane < NSUB) | (lane >= width - NSUB)

        with jax.named_scope("i_vel1"):
            sweep_all(False, True)
        with jax.named_scope("i_sweeps"):
            tile_loop(NSUB - 1, 1, lambda k: sweep_all(True, True))
        send_rows(0, back, 2, 1, ret, 2, bulk_ssem, bulk_rsem.at[0])

        def returned(t):
            r = pl.ds(pl.multiple_of(t * TILE, TILE), TILE)
            block = sub + t * TILE
            theirs = outer | (block < 2) | (block >= count - 2)
            for y in range(2):
                half = pl.ds(y * width, width)
                u, v = main[U, y, r, :], main[V, y, r, :]
                gone = leave(lambda c: main[c, y, r, :], u, v)
                for c in range(2):
                    forc[c, r, half] = jnp.where(theirs, 0.0, gone[c])

        with jax.named_scope("i_back"):
            tile_loop(tiles, 4, returned)
            for c in range(2):
                back[c] = dot_rows(to_slots, forc[c])
        with jax.named_scope("i_waitearly"):
            when_inside(-1, 6, early_rsem.at[0])
            when_inside(1, 6, early_rsem.at[1])
            wait_tiles(2, early_rsem.at[2])
        with jax.named_scope("i_early"):
            unpack_rows(0, True)
            unpack_sides(0)
            derive_edges()
            sweep_edge(True, False)
        with jax.named_scope("i_waitmid"):
            when_inside(-1, 3, mid_rsem.at[0])
            when_inside(1, 3, mid_rsem.at[1])
            wait_tiles(2, mid_rsem.at[2])
            wait_tiles(8, mid_rsem.at[3])
        unpack_rows(1)
        unpack_sides(1)
        with jax.named_scope("i_waitlate"):
            when_inside(-1, 3, late_rsem.at[0])
            when_inside(1, 3, late_rsem.at[1])
            wait_tiles(2, late_rsem.at[2])
            wait_tiles(8, late_rsem.at[3])

        def sweep_strips(stress, velocity):
            sweep_flank(stress, velocity)
            sweep_edge(stress, velocity)

        with jax.named_scope("i_edge"):
            unpack_rows(2)
            unpack_sides(2)
            sweep_strips(False, True)
            for _ in range(NSUB - 1):
                sweep_strips(True, True)

        with jax.named_scope("i_fix"):
            for y in range(2):
                for j, far in ((1, 0), (2, count - TILE)):
                    r = pl.ds(j * TILE, TILE)
                    held = (lane >= 2) & (lane < count - 2)
                    held = held & ((sub < NSUB) if j == 1 else (sub >= TILE - NSUB))
                    u, v = flank[U, y, r, :], flank[V, y, r, :]
                    gone = leave(lambda c: flank[c, y, r, :], u, v)
                    for c in range(2):
                        slot = (c * 2 + y) * 2 * TILE + (TILE if j == 1 else 0)
                        flank_back[pl.ds(slot, TILE), :] = jnp.where(held, gone[c], 0.0)
                        flank_vel[c, y, pl.ds(far, TILE), :] = jnp.where(held, (u, v)[c], 0.0)
                for strip in range(2):
                    def get(c):
                        return edge[c, strip, y, :, pl.ds(0, width)]
                    gone = leave(get, get(U), get(V))
                    held = (sub < 2) if strip == 0 else (sub >= TILE - 2)
                    for c in range(2):
                        moved = pltpu.roll(gone[c], TILE - 2 if strip == 0 else 2, 0)
                        ends[c, pl.ds(strip * TILE, TILE), pl.ds(y * width, width)] = jnp.where(
                            held, moved, 0.0
                        )
            across = dot_lanes(to_slots, flank_back[...])
            for c in range(2):
                rest = dot_rows(to_ends, ends[c])
                for y in range(2):
                    slot = (c * 2 + y) * 2 * TILE
                    for t in range(tiles):
                        r, half = pl.ds(t * TILE, TILE), pl.ds(y * width, width)
                        moved = pltpu.roll(across[t * TILE:(t + 1) * TILE], width - TILE - slot, 1)
                        back[c, r, half] += jnp.where(outer, moved, 0.0) + (
                            rest[t * TILE:(t + 1) * TILE, y * width:(y + 1) * width]
                        )
            send_rows(0, back, 0, 2, ret, 0, bulk_ssem, bulk_rsem.at[1], "home")

        same = jnp.where(diag, 1.0, 0.0).astype(jnp.bfloat16)
        same = jnp.concatenate([same] * 2, axis=1)
        for y in range(2):
            for c in range(2):
                half = pl.ds(y * width, width)
                for strip, r in ((0, top), (1, bottom)):
                    end = pltpu.roll(
                        edge[c, strip, y, :, pl.ds(0, width)], TILE - 2 if strip == 0 else 2, 0
                    )
                    held = (sub < 2) if strip == 0 else (sub >= TILE - 2)
                    main[c, y, r, :] = jnp.where(held, end, main[c, y, r, :])
                other = dot_lanes(same, flank_vel[c, y])
                row = lax.broadcasted_iota(jnp.int32, (count, width), 0)
                column = lax.broadcasted_iota(jnp.int32, (count, width), 1)
                theirs = (row >= 2) & (row < count - 2)
                theirs = theirs & ((column < NSUB) | (column >= width - NSUB))
                out[0, c, :, half] = jnp.where(theirs, other, main[c, y])
        wait_bytes(ids.at[pl.ds(0, peers - 1)], ids_ssem)
        wait_bytes(back, bulk_ssem)
        when_inside(-1, 12, halo_ssem.at[0])
        when_inside(1, 12, halo_ssem.at[1])
        wait_tiles(6, halo_ssem.at[2])
        wait_tiles(16, halo_ssem.at[3])


def per_device_kernel(n_lat, n_lon, fields, block_owner, ice_covered, land_mask):
    count, cells = land_mask.shape
    peers = n_lat * n_lon
    f32 = jnp.float32
    anywhere = pl.BlockSpec(memory_space=pl.ANY)
    dma = pltpu.SemaphoreType.DMA
    halos = [pltpu.VMEM((2, num // 2, TILE, BX), f32) for _, num in ROUNDS] * 2
    sides = [pltpu.VMEM((2, TILE, BX), f32) for _ in ROUNDS]
    sides += [pltpu.VMEM((3, 2, TILE, BX), f32) for _ in ROUNDS]
    return pl.pallas_call(
        functools.partial(step_kernel, n_lat, n_lon),
        out_shape=pltpu.VMEM((1, 2, count, cells), f32),
        in_specs=[anywhere, anywhere, anywhere, anywhere],
        out_specs=pl.BlockSpec(memory_space=pltpu.VMEM),
        scratch_shapes=[
            pltpu.VMEM((7, count, cells), f32),
            pltpu.VMEM((2, count, cells), f32),
            pltpu.VMEM((3, count, cells), f32),
            pltpu.VMEM((1, count), jnp.int32),
            pltpu.VMEM((1, count), jnp.int32),
            pltpu.VMEM((peers, 1, count), jnp.int32),
            pltpu.VMEM((6, count, cells), f32),
            pltpu.VMEM((2, count, cells), f32),
            pltpu.VMEM((count, count), f32),
            pltpu.VMEM((3, count, cells), f32),
            pltpu.VMEM((count, cells), jnp.int32),
            pltpu.VMEM((14, 2, count, BX), f32),
            pltpu.VMEM((14, 2, 2, TILE, 2 * BX), f32),
            pltpu.VMEM((14, 2, 4 * TILE, BX), f32),
            pltpu.VMEM((BX, count), f32),
            pltpu.VMEM((2, 2, BX, count), f32),
            pltpu.VMEM((2, 2 * TILE, cells), f32),
            *halos, *sides,
            dma, dma((2,)), dma, dma, dma((4,)), dma((4,)), dma((4,)), dma((4,)),
            pltpu.SemaphoreType.REGULAR,
        ],
        compiler_params=pltpu.CompilerParams(
            collective_id=0, has_side_effects=True, vmem_limit_bytes=63 * 1024 * 1024
        ),
    )(fields, block_owner.reshape(1, count), ice_covered.reshape(1, count), land_mask)


def solution(mesh):
    placed = (
        P("comp", None, ("lat", "lon"), None),
        P(("lat", "lon")),
        P(("lat", "lon")),
        P(("lat", "lon"), None),
    )
    n_lat, n_lon = mesh.shape["lat"], mesh.shape["lon"]

    def body(fields, block_owner, ice_covered, land_mask):
        count = block_owner.shape[0]
        whole_tiles = count % (n_lat * n_lon * TILE) == 0 and count == BX
        if whole_tiles and n_lon > 2:
            return per_device_kernel(n_lat, n_lon, fields, block_owner, ice_covered, land_mask)
        return per_device(fields, block_owner, ice_covered, land_mask)

    return jax.shard_map(
        body,
        mesh=mesh,
        in_specs=placed,
        out_specs=P("comp", None, ("lat", "lon"), None),
        check_vma=False,
    )
```

```python
import functools

import jax
import jax.numpy as jnp
from jax import lax
from jax.experimental import pallas as pl
from jax.experimental.pallas import tpu as pltpu
from jax.sharding import PartitionSpec as P

GX = 1
BY = 2
BX = 128
NSUB = 4


CD_ICE = 0.1
CW = 1.5
CSTAR = 2.0
ECC2 = 4.0
DMIN2 = 0.25
RELAX = 0.5
DTE = 0.5
CORIO = 0.3
MASS_FLOOR = 0.5
DRAG_FLOOR = 0.1


def from_behind(x, axis, by):
    size = lax.axis_size(axis)
    pairs = [(i, i + by) for i in range(size) if 0 <= i + by < size]
    return lax.ppermute(x, axis, pairs)


def with_halo(x, sides, width, wrap):
    for axis, dim in sides:
        size, length = (lax.axis_size(axis), x.shape[dim])
        up = [(i, (i + 1) % size) for i in range(size if wrap else size - 1)]
        down = [(j, i) for i, j in up]
        last = lax.slice_in_dim(x, length - width, length, axis=dim)
        first = lax.slice_in_dim(x, 0, width, axis=dim)
        before = lax.ppermute(last, axis, up)
        after = lax.ppermute(first, axis, down)
        x = jnp.concatenate([before, x, after], axis=dim)
    return x


def air_stress(ocean):
    wind_x, wind_y, current_x, current_y, tilt_x, tilt_y, density = ocean
    speed_ice = jnp.sqrt(wind_x * wind_x + wind_y * wind_y + 1.0)
    scale_ice = density * CD_ICE * speed_ice
    rel_x = wind_x - current_x
    rel_y = wind_y - current_y
    speed_open = jnp.sqrt(rel_x * rel_x + rel_y * rel_y + 1.0)
    scale_open = density * (0.1 + 0.05 * speed_open) * speed_open
    outbound = jnp.stack(
        [scale_ice * wind_x, scale_ice * wind_y, current_x, current_y, tilt_x, tilt_y]
    )
    open_stress = jnp.stack([scale_open * rel_x, scale_open * rel_y])
    return (outbound, open_stress)


def prepare(ice_tile, forcing, active):
    ice_mass = ice_tile[2]
    concentration = ice_tile[3]
    strength = ice_mass * jnp.exp(CSTAR * (concentration - 1.0)) * active
    drag_base = CW * concentration * active
    push_x = active * (concentration * forcing[0] - ice_mass * forcing[4])
    push_y = active * (concentration * forcing[1] - ice_mass * forcing[5])
    return jnp.stack(
        [strength, ice_mass, drag_base, push_x, push_y, forcing[2], forcing[3], active]
    )


def subcycle(ice_state, statics):
    east_vel, north_vel, stress_one, stress_two, stress_three = ice_state
    strength = statics[0]
    east_base = east_vel[:-1, :-1]
    north_base = north_vel[:-1, :-1]
    strain_xx = east_vel[:-1, 1:] - east_base
    strain_yy = north_vel[1:, :-1] - north_base
    shear = east_vel[1:, :-1] - east_base + (north_vel[:-1, 1:] - north_base)
    divergence = strain_xx + strain_yy
    tension = strain_xx - strain_yy
    delta_norm = jnp.sqrt(
        divergence * divergence + (tension * tension + shear * shear) / ECC2 + DMIN2
    )
    viscosity = strength[:-1, :-1] / delta_norm
    stress_sum = (stress_one[:-1, :-1] + RELAX * viscosity * (divergence - delta_norm)) / (
        1.0 + RELAX
    )
    stress_diff = (stress_two[:-1, :-1] + RELAX * viscosity * tension / ECC2) / (1.0 + RELAX)
    stress_shear = (stress_three[:-1, :-1] + RELAX * viscosity * shear / (2.0 * ECC2)) / (
        1.0 + RELAX
    )
    stress_xx = 0.5 * (stress_sum + stress_diff)
    stress_yy = 0.5 * (stress_sum - stress_diff)
    force_x = (
        stress_xx[1:, 1:] - stress_xx[1:, :-1] + (stress_shear[1:, 1:] - stress_shear[:-1, 1:])
    )
    force_y = (
        stress_shear[1:, 1:] - stress_shear[1:, :-1] + (stress_yy[1:, 1:] - stress_yy[:-1, 1:])
    )
    trimmed = statics[:, 1:-1, 1:-1]
    strength, ice_mass, drag_base, push_x, push_y, current_x, current_y, active = trimmed
    east_old = east_vel[1:-1, 1:-1]
    north_old = north_vel[1:-1, 1:-1]
    diff_x = current_x - east_old
    diff_y = current_y - north_old
    drag_coef = drag_base * jnp.sqrt(diff_x * diff_x + diff_y * diff_y + DRAG_FLOOR)
    denominator = jnp.maximum(ice_mass, MASS_FLOOR) / DTE + drag_coef
    east_new = (
        active
        * (
            ice_mass / DTE * east_old
            + force_x
            + push_x
            + drag_coef * current_x
            + CORIO * ice_mass * north_old
        )
        / denominator
    )
    north_new = (
        active
        * (
            ice_mass / DTE * north_old
            + force_y
            + push_y
            + drag_coef * current_y
            - CORIO * ice_mass * east_old
        )
        / denominator
    )
    new_state = jnp.stack(
        [east_new, north_new, stress_sum[1:, 1:], stress_diff[1:, 1:], stress_shear[1:, 1:]]
    )
    return (new_state, trimmed)


def give_back(ice_state, statics):
    east_vel = ice_state[0]
    north_vel = ice_state[1]
    drag_base = statics[2]
    current_x = statics[5]
    current_y = statics[6]
    diff_x = east_vel - current_x
    diff_y = north_vel - current_y
    factor = drag_base * jnp.sqrt(diff_x * diff_x + diff_y * diff_y + DRAG_FLOOR)
    return jnp.stack([factor * diff_x, factor * diff_y, drag_base / CW])


def to_tile(blocks):
    channels, count, cells = blocks.shape
    arranged = blocks.reshape(channels, count // GX, GX, BY, BX).transpose(0, 1, 3, 2, 4)
    return arranged.reshape(channels, count // GX * BY, GX * BX)


def from_tile(values):
    channels, rows, columns = values.shape
    arranged = values.reshape(channels, rows // BY, BY, GX, BX).transpose(0, 1, 3, 2, 4)
    return arranged.reshape(channels, rows // BY * GX, BY * BX)


def per_device(fields, block_owner, ice_covered, land_mask):
    count = block_owner.shape[0]
    is_ocean = lax.axis_index("comp") == 0
    outbound, open_stress = air_stress(fields[0])
    owner_row = block_owner.reshape(1, count)
    crossed = from_behind(outbound, "comp", 1)
    received, anchor = (
        lax.all_to_all(crossed, ("lat", "lon"), split_axis=1, concat_axis=1, tiled=True),
        lax.all_to_all(owner_row, ("lat", "lon"), split_axis=1, concat_axis=1, tiled=True),
    )
    local_ids = anchor[0] % count
    position = jnp.zeros((count,), jnp.int32).at[local_ids].set(jnp.arange(count, dtype=jnp.int32))
    forcing = to_tile(received[:, position])
    ice_tile = to_tile(fields[0])
    covered = ice_covered.astype(jnp.float32)[:, None] * (1 - land_mask).astype(jnp.float32)
    active = to_tile(covered[None])[0]
    statics = prepare(ice_tile, forcing, active)
    ice_state = jnp.stack([ice_tile[0], ice_tile[1], ice_tile[4], ice_tile[5], ice_tile[6]])
    joined = jnp.concatenate([ice_state, statics], 0)
    joined = with_halo(joined, (("lon", 2),), NSUB, True)
    joined = with_halo(joined, (("lat", 1),), NSUB, False)
    ice_state = joined[:5]
    statics = joined[5:]
    for repeat in range(NSUB):
        ice_state, statics = subcycle(ice_state, statics)
    returned = from_tile(give_back(ice_state, statics))
    back_send = returned[:, local_ids]
    regrouped = lax.all_to_all(back_send, ("lat", "lon"), split_axis=1, concat_axis=1, tiled=True)
    received_back = from_behind(regrouped, "comp", -1)
    ocean_out = received_back[:2] + (1.0 - received_back[2]) * open_stress
    ice_out = from_tile(ice_state[:2])
    return jnp.where(is_ocean, ocean_out, ice_out)[None]


TILE = 8
GROUP = 8
MESH = pl.DeviceIdType.MESH
U, V, MASS, CONC, S1, S2, S12, ACTIVE, PUSH_X, PUSH_Y, CUR_X, CUR_Y, STRENGTH, DRAG = range(14)
SIDES = [(a, b) for b in (-1, 1) for a in (-1, 1, 0)]
ROUNDS = ((U, 8), (CUR_X, 2), (PUSH_X, 2))
KEEP = 1.0 / (1.0 + RELAX)


def tile_loop(tiles, together, body):
    def step(k, carry):
        for j in range(together):
            body(k * together + j)
        return carry
    lax.fori_loop(0, tiles // together, step, 0)


def pieces(values, axis):
    high = values.astype(jnp.bfloat16)
    low = (values - high.astype(jnp.float32)).astype(jnp.bfloat16)
    return jnp.concatenate([high, low], axis=axis)


def dot_rows(twice, values):
    return lax.dot_general(
        twice, pieces(values, 0), (((1,), (0,)), ((), ())), preferred_element_type=jnp.float32
    )


def dot_lanes(twice, values):
    return lax.dot_general(
        twice, pieces(values, 1), (((1,), (1,)), ((), ())), preferred_element_type=jnp.float32
    )


def new_stress(strength, s1, s2, s12, u, v, u_east, v_east, u_up, v_up):
    sxx = u_east - u
    syy = v_up - v
    shear = (u_up - u) + (v_east - v)
    div = sxx + syy
    ten = sxx - syy
    square = div * div + (ten * ten + shear * shear) * (1.0 / ECC2) + DMIN2
    inverse = lax.rsqrt(square)
    visc = strength * inverse
    s1 = s1 * KEEP + visc * (div - square * inverse)
    s2 = s2 * KEEP + visc * ten * (1.0 / ECC2)
    s12 = s12 * KEEP + visc * shear * (0.5 / ECC2)
    return s1, s2, s12


def new_velocity(get, u, v, force_x, force_y):
    mass, cx, cy = get(MASS), get(CUR_X), get(CUR_Y)
    dx, dy = cx - u, cy - v
    square = dx * dx + dy * dy + DRAG_FLOOR
    drag = get(DRAG) * (square * lax.rsqrt(square))
    gain = get(ACTIVE) / (jnp.maximum(mass, MASS_FLOOR) * (1.0 / DTE) + drag)
    inertia = mass * (1.0 / DTE)
    turn = CORIO * mass
    return (
        gain * (inertia * u + force_x + get(PUSH_X) + drag * cx + turn * v),
        gain * (inertia * v + force_y + get(PUSH_Y) + drag * cy - turn * u),
    )


def step_kernel(
    n_lat, n_lon,
    fields, owner_hbm, covered_hbm, land, out,
    surf, open_st, ret, owner, covered, ids, recv, forc, one_hot, back, land_v,
    main, edge, flank, flank_back, flank_vel, ends,
    rows_out0, rows_out1, rows_out2, rows_got0, rows_got1, rows_got2,
    side_out0, side_out1, side_out2, side_got0, side_got1, side_got2,
    bulk_ssem, bulk_rsem, ids_ssem, ids_rsem, halo_ssem, early_rsem, mid_rsem, late_rsem, ready,
):
    comp = lax.axis_index("comp")
    lat = lax.axis_index("lat")
    lon = lax.axis_index("lon")
    peers = n_lat * n_lon
    me = lat * n_lon + lon
    count = owner.shape[1]
    per = count // peers
    width = BX
    barrier = pltpu.get_barrier_semaphore()
    rows_out = (rows_out0, rows_out1, rows_out2)
    rows_got = (rows_got0, rows_got1, rows_got2)
    side_out = (side_out0, side_out1, side_out2)
    side_got = (side_got0, side_got1, side_got2)

    def rows_of(peer):
        return pl.ds(pl.multiple_of(peer * per, per), per)

    planes = [jnp.where(lat < n_lat // 2, n_lat - 1 - j, j) for j in range(n_lat)]
    places = [(lon + i) % n_lon for i in range(n_lon)]

    half_lat = n_lat // 2
    groups_of = {
        "all": ((planes, places),),
        "column": ((planes[:half_lat], places[:1]),),
        "beyond": ((planes[:half_lat], places[1:]),),
        "near": ((planes[half_lat:], places),),
    }

    def each_peer(body, part="all"):
        for chosen, along in groups_of[part]:
            for plane in chosen:
                for place in along:
                    body(plane * n_lon + place, plane, place)

    def away(body):
        for plane in range(n_lat):
            for place in places:
                if plane:
                    body(plane * n_lon + place, plane, place)
                else:
                    @pl.when(place > 0)
                    def _():
                        body(place, 0, place)

    def signal_peers(kind, part="all"):
        each_peer(
            lambda p, plane, place: pl.semaphore_signal(
                barrier, inc=1, device_id=(kind, plane, place), device_id_type=MESH
            ),
            part,
        )

    def send_rows(kind, src, lo, num, dst, dlo, ssem, rsem, part="all"):
        def body(p, plane, place):
            pltpu.make_async_remote_copy(
                src_ref=src.at[pl.ds(lo, num), rows_of(p), :],
                dst_ref=dst.at[pl.ds(dlo, num), rows_of(me), :],
                send_sem=ssem, recv_sem=rsem,
                device_id=(kind, plane, place), device_id_type=MESH,
            ).start()
        if part == "home":
            body(0, 0, 0)
        elif part == "away":
            away(body)
        else:
            each_peer(body, part)

    def wait_bytes(ref, sem):
        pltpu.make_async_copy(ref, ref, sem).wait()

    def wait_tiles(num, sem):
        wait_bytes(main.at[0, 0, pl.ds(0, num * TILE), :], sem)

    @pl.when(comp == 0)
    def _ocean():
        signal_peers(1)
        raw = pltpu.make_async_copy(fields.at[0, pl.ds(2, 4)], surf.at[pl.ds(2, 4)], halo_ssem.at[0])
        wind = pltpu.make_async_copy(fields.at[0, pl.ds(0, 2)], surf.at[pl.ds(0, 2)], halo_ssem.at[1])
        rho = pltpu.make_async_copy(fields.at[0, pl.ds(6, 1)], surf.at[pl.ds(6, 1)], halo_ssem.at[2])
        raw.start()
        wind.start()
        rho.start()
        with jax.named_scope("o_barrier"):
            pl.semaphore_wait(barrier, half_lat)

        def send_four(part):
            send_rows(1, surf, 2, 4, recv, 2, bulk_ssem, bulk_rsem.at[0], part)

        def send_two(part):
            send_rows(1, forc, 0, 2, recv, 0, bulk_ssem, bulk_rsem.at[1], part)

        with jax.named_scope("o_send4"):
            raw.wait()
            send_four("column")
            wind.wait()
            rho.wait()

        def stress(t):
            r = pl.ds(pl.multiple_of(t * TILE, TILE), TILE)
            wx, wy, density = surf[0, r, :], surf[1, r, :], surf[6, r, :]
            scale = density * CD_ICE * jnp.sqrt(wx * wx + wy * wy + 1.0)
            forc[0, r, :] = scale * wx
            forc[1, r, :] = scale * wy

        with jax.named_scope("o_stress"):
            tile_loop(count // TILE, 4, stress)
            send_two("column")
        with jax.named_scope("o_ready"):
            pl.semaphore_wait(ready, 1)
        with jax.named_scope("o_rest"):
            send_four("beyond")
            send_two("beyond")
            send_four("near")
            send_two("near")

        def open_water(t):
            r = pl.ds(pl.multiple_of(t * TILE, TILE), TILE)
            density = surf[6, r, :]
            rel_x = surf[0, r, :] - surf[2, r, :]
            rel_y = surf[1, r, :] - surf[3, r, :]
            speed = jnp.sqrt(rel_x * rel_x + rel_y * rel_y + 1.0)
            scale = density * (0.1 + 0.05 * speed) * speed
            open_st[0, r, :] = scale * rel_x
            open_st[1, r, :] = scale * rel_y

        tile_loop(count // TILE, 2, open_water)
        with jax.named_scope("o_waitret1"):
            wait_bytes(ret.at[pl.ds(2, 1)], bulk_rsem.at[0])

        def water(t):
            r = pl.ds(pl.multiple_of(t * TILE, TILE), TILE)
            share = 1.0 - ret[2, r, :]
            for c in range(2):
                open_st[c, r, :] = share * open_st[c, r, :]

        tile_loop(count // TILE, 4, water)
        with jax.named_scope("o_waitret2"):
            wait_bytes(ret.at[pl.ds(0, 2)], bulk_rsem.at[1])

        def finish(t):
            r = pl.ds(pl.multiple_of(t * TILE, TILE), TILE)
            for c in range(2):
                out[0, c, r, :] = ret[c, r, :] + open_st[c, r, :]

        tile_loop(count // TILE, 4, finish)
        wait_bytes(surf.at[pl.ds(0, 6)], bulk_ssem)

    @pl.when(comp == 1)
    def _ice():
        def inside(a):
            if a == 0:
                return lat >= 0
            return lat + a >= 0 if a < 0 else lat + a < n_lat

        def around(a, b):
            return (1, lat + a, (lon + b + n_lon) % n_lon)

        signal_peers(0, "column")
        for a in range(n_lat):
            for b in range(n_lon):
                if a or b:
                    pl.semaphore_signal(
                        barrier, inc=1, device_id=(1, (lat + a) % n_lat, (lon + b) % n_lon),
                        device_id_type=MESH,
                    )
        for y in range(2):
            pltpu.make_async_copy(
                fields.at[0, :, :, pl.ds(y * width, width)], main.at[pl.ds(0, 7), y], halo_ssem.at[0]
            ).start()
        loads = [
            pltpu.make_async_copy(land, land_v, halo_ssem.at[1]),
            pltpu.make_async_copy(covered_hbm, covered, halo_ssem.at[2]),
        ]
        names = pltpu.make_async_copy(owner_hbm, owner, halo_ssem.at[3])
        names.start()
        for load in loads:
            load.start()
        with jax.named_scope("i_barrier"):
            pl.semaphore_wait(barrier, 2 * peers - 1)
            pl.semaphore_signal(ready, inc=1, device_id=(0, lat, lon), device_id_type=MESH)
            names.wait()
            for a in range(n_lat):
                for b in range(n_lon):
                    if a or b:
                        pltpu.make_async_remote_copy(
                            src_ref=owner, dst_ref=ids.at[me], send_sem=ids_ssem, recv_sem=ids_rsem,
                            device_id=(1, (lat + a) % n_lat, (lon + b) % n_lon),
                            device_id_type=MESH,
                        ).start()
        ids[me] = owner[...]

        tiles = count // TILE
        top, bottom = pl.ds(0, TILE), pl.ds(count - TILE, TILE)
        zero_tile = jnp.zeros((TILE, width), jnp.float32)
        for wall, which in ((lat == 0, 0), (lat == n_lat - 1, 1)):
            @pl.when(wall)
            def _():
                for e in range(3):
                    for k in range(rows_got[e].shape[1]):
                        rows_got[e][which, k] = zero_tile
                    for k in range(2):
                        side_got[e][2 * which, k] = zero_tile

        def clear(t):
            r = pl.ds(pl.multiple_of(t * TILE, TILE), TILE)
            for c in range(2):
                for y in range(2):
                    flank_vel[c, y, r, :] = zero_tile
            flank_back[r, :] = zero_tile

        tile_loop(tiles, 2, clear)
        wait_bytes(main.at[pl.ds(0, 7)], halo_ssem.at[0])
        for load in loads:
            load.wait()
        diag = lax.broadcasted_iota(jnp.int32, (count, count), 0) == lax.broadcasted_iota(
            jnp.int32, (count, count), 1
        )
        wet = jnp.sum(
            jnp.where(diag, covered[...].astype(jnp.float32), 0.0), axis=1, keepdims=True
        )
        sea = wet * (1 - land_v[...]).astype(jnp.float32)
        for y in range(2):
            main[ACTIVE, y] = sea[:, y * width:(y + 1) * width]

        lane = lax.broadcasted_iota(jnp.int32, (TILE, width), 1)
        sub = lax.broadcasted_iota(jnp.int32, (TILE, width), 0)
        pick_row = lax.broadcasted_iota(jnp.int32, (2 * TILE, width), 0)
        pick_col = lax.broadcasted_iota(jnp.int32, (2 * TILE, width), 1)
        picked = jnp.where(pick_row < TILE, pick_row, pick_row + (width - 2 * TILE)) == pick_col
        picker = jnp.where(picked, 1.0, 0.0).astype(jnp.bfloat16)
        picker = jnp.concatenate([picker] * 2, axis=1)

        def pack_rows(e):
            lo, num = ROUNDS[e]
            for k in range(num // 2):
                ups, downs = zero_tile, zero_tile
                for i in range(4):
                    c, y = lo + 2 * k + i // 2, i % 2
                    head, foot = main[c, y, top, :], main[c, y, bottom, :]
                    here = (sub >= 2 * i) & (sub < 2 * i + 2)
                    ups = jnp.where(here, pltpu.roll(head, 2 * i, 0) if i else head, ups)
                    downs = jnp.where(here, pltpu.roll(foot, (2 * i + 2) % TILE, 0) if i < 3 else foot, downs)
                rows_out[e][0, k] = ups
                rows_out[e][1, k] = downs

        def pack_sides(e):
            lo, num = ROUNDS[e]
            west, east = zero_tile, zero_tile
            for i in range(2 * num):
                c, y = lo + i // 2, i % 2
                ends = jnp.where(sub < NSUB, main[c, y, top, :], main[c, y, bottom, :])
                slot = i * NSUB
                mine = (lane >= slot) & (lane < slot + NSUB)
                west = jnp.where(mine, pltpu.roll(ends, slot, 1) if slot else ends, west)
                east = jnp.where(mine, pltpu.roll(ends, (slot + NSUB) % width, 1), east)
            side_out[e][0] = west
            side_out[e][1] = east

        def pack_flank(e):
            lo, num = ROUNDS[e]
            for c in range(lo, lo + num):
                for y in range(2):
                    across = dot_lanes(picker, main[c, y])
                    flank[c, y, pl.ds(TILE, TILE), :] = across[:TILE]
                    flank[c, y, pl.ds(2 * TILE, TILE), :] = across[TILE:]

        def push_on(e, a, b, src, dst, lane_of_sem, recv_lane):
            sems = (early_rsem, mid_rsem, late_rsem)[e]

            @pl.when(inside(a))
            def _():
                pltpu.make_async_remote_copy(
                    src_ref=src, dst_ref=dst,
                    send_sem=halo_ssem.at[lane_of_sem], recv_sem=sems.at[recv_lane],
                    device_id=around(a, b), device_id_type=MESH,
                ).start()

        def send_ends(e):
            for a in (-1, 1):
                k = 1 if a > 0 else 0
                push_on(e, a, 0, rows_out[e].at[k], rows_got[e].at[1 - k], k, 1 - k)

        def send_sides(e):
            for a, b in SIDES:
                k = 1 if b > 0 else 0
                group = {0: 2, -1: 0, 1: 1}[a]
                land_in = {0: 2, -1: 1, 1: 0}[a]
                push_on(e, a, b, side_out[e].at[k], side_got[e].at[1 - a, 1 - k], group, land_in)

        def send_flank(e):
            lo, num = ROUNDS[e]
            for b in (-1, 1):
                src, dst = (2 * TILE, 0) if b > 0 else (TILE, 3 * TILE)
                push_on(
                    e, 0, b,
                    flank.at[pl.ds(lo, num), :, pl.ds(src, TILE), :],
                    flank.at[pl.ds(lo, num), :, pl.ds(dst, TILE), :], 3, 3,
                )

        def when_inside(a, num, sem):
            @pl.when(inside(a))
            def _():
                wait_tiles(num, sem)

        def own_rows():
            for c in range(ROUNDS[0][1]):
                for y in range(2):
                    edge[c, 0, y, :, pl.ds(0, width)] = pltpu.roll(main[c, y, top, :], 2, 0)
                    edge[c, 1, y, :, pl.ds(0, width)] = pltpu.roll(main[c, y, bottom, :], TILE - 2, 0)

        def unpack_rows(e, placed=False):
            lo, num = ROUNDS[e]
            got = rows_got[e]
            for k in range(num // 2):
                for i in range(4):
                    c, y = lo + 2 * k + i // 2, i % 2
                    north = pltpu.roll(got[0, k], (TILE - 2 * i) % TILE, 0) if i else got[0, k]
                    south = pltpu.roll(got[1, k], TILE - 2 - 2 * i, 0) if i < 3 else got[1, k]
                    if placed:
                        head, foot = (edge[c, strip, y, :, pl.ds(0, width)] for strip in range(2))
                    else:
                        head = pltpu.roll(main[c, y, top, :], 2, 0)
                        foot = pltpu.roll(main[c, y, bottom, :], TILE - 2, 0)
                    edge[c, 0, y, :, pl.ds(0, width)] = jnp.where(sub < 2, north, head)
                    edge[c, 1, y, :, pl.ds(0, width)] = jnp.where(sub >= TILE - 2, south, foot)

        def unpack_sides(e):
            lo, num = ROUNDS[e]
            side = side_got[e]
            ends = []
            for k in range(2):
                far, near = side[0, k], side[1, k]
                ends.append(pltpu.roll(jnp.where(sub >= TILE - 2, far, near), 2, 0))
            for k in range(2):
                far, near = side[2, k], side[1, k]
                ends.append(pltpu.roll(jnp.where(sub < 2, far, near), TILE - 2, 0))
            for i in range(2 * num):
                c, y = lo + i // 2, i % 2
                slot = i * NSUB
                for strip in range(2):
                    from_west, from_east = ends[2 * strip], ends[2 * strip + 1]
                    from_east = pltpu.roll(from_east, width - slot, 1) if slot else from_east
                    from_west = pltpu.roll(from_west, width - NSUB - slot, 1)
                    edge[c, strip, y, :, pl.ds(width, width)] = jnp.where(
                        lane < NSUB, from_east, jnp.where(lane >= width - NSUB, from_west, 0.0)
                    )

        def derive(load, store):
            conc, act = load(CONC), load(ACTIVE)
            store(STRENGTH, (RELAX * KEEP) * load(MASS) * jnp.exp(CSTAR * (conc - 1.0)) * act)
            store(DRAG, CW * conc * act)

        def derive_main(t):
            r = pl.ds(pl.multiple_of(t * TILE, TILE), TILE)
            for y in range(2):
                def store(c, x):
                    main[c, y, r, :] = x
                derive(lambda c: main[c, y, r, :], store)

        def derive_flank():
            for y in range(2):
                def store(c, x):
                    flank[c, y] = x
                derive(lambda c: flank[c, y], store)

        def derive_edges():
            for y in range(2):
                for strip in range(2):
                    def store(c, x):
                        edge[c, strip, y] = x
                    derive(lambda c: edge[c, strip, y], store)

        def sweep_main(g, stress, velocity):
            spots = [pl.ds((g * GROUP + j) * TILE, TILE) for j in range(GROUP)]
            behind = pl.ds(max(g * GROUP - 1, 0) * TILE, TILE)
            ahead = pl.ds(min(g * GROUP + GROUP, tiles - 1) * TILE, TILE)
            vels = [[(main[U, y, r, :], main[V, y, r, :]) for y in range(2)] for r in spots]
            stresses = []
            if stress:
                follow = (main[U, 0, ahead, :], main[V, 0, ahead, :])
            for j, r in enumerate(spots):
                old = [tuple(main[c, y, r, :] for c in (S1, S2, S12)) for y in range(2)]
                if not stress:
                    stresses.append(old)
                    continue
                beyond = vels[j + 1][0] if j + 1 < GROUP else follow
                row = []
                for y in range(2):
                    u, v = vels[j][y]
                    if y == 0:
                        u_up, v_up = vels[j][1]
                    else:
                        u_up, v_up = (
                            pltpu.roll(jnp.where(sub == 0, after, x), TILE - 1, 0)
                            for x, after in zip(vels[j][0], beyond)
                        )
                    fresh = new_stress(
                        main[STRENGTH, y, r, :], *old[y], u, v,
                        pltpu.roll(u, width - 1, 1), pltpu.roll(v, width - 1, 1), u_up, v_up,
                    )
                    for c, x in zip((S1, S2, S12), fresh):
                        main[c, y, r, :] = x
                    row.append(fresh)
                stresses.append(row)
            if not velocity:
                return
            yy_before = 0.5 * (main[S1, 1, behind, :] - main[S2, 1, behind, :])
            cross_before = main[S12, 1, behind, :]
            for j, r in enumerate(spots):
                xx = [0.5 * (s1 + s2) for s1, s2, _ in stresses[j]]
                yy = [0.5 * (s1 - s2) for s1, s2, _ in stresses[j]]
                cross = [s12 for _, _, s12 in stresses[j]]
                yy_down, cross_down = (
                    [pltpu.roll(jnp.where(sub == TILE - 1, before, x[1]), 1, 0), x[0]]
                    for x, before in ((yy, yy_before), (cross, cross_before))
                )
                yy_before, cross_before = yy[1], cross[1]
                for y in range(2):
                    force_x = xx[y] - pltpu.roll(xx[y], 1, 1) + (cross[y] - cross_down[y])
                    force_y = cross[y] - pltpu.roll(cross[y], 1, 1) + (yy[y] - yy_down[y])
                    u, v = new_velocity(lambda c: main[c, y, r, :], *vels[j][y], force_x, force_y)
                    main[U, y, r, :] = u
                    main[V, y, r, :] = v

        def sweep_edge(stress, velocity):
            lanes = 2 * width

            for strip in range(2):
                vels = [(edge[U, strip, y], edge[V, strip, y]) for y in range(2)]
                fresh = [tuple(edge[c, strip, y] for c in (S1, S2, S12)) for y in range(2)]
                if stress:
                    ups = [vels[1], tuple(pltpu.roll(x, TILE - 1, 0) for x in vels[0])]
                    for y in range(2):
                        east = [pltpu.roll(x, lanes - 1, 1) for x in vels[y]]
                        fresh[y] = new_stress(
                            edge[STRENGTH, strip, y], *fresh[y], *vels[y], *east, *ups[y]
                        )
                        for c, x in zip((S1, S2, S12), fresh[y]):
                            edge[c, strip, y] = x
                if not velocity:
                    continue
                xx = [0.5 * (s1 + s2) for s1, s2, _ in fresh]
                yy = [0.5 * (s1 - s2) for s1, s2, _ in fresh]
                cross = [s12 for _, _, s12 in fresh]
                yy_down, cross_down = ([pltpu.roll(x[1], 1, 0), x[0]] for x in (yy, cross))
                for y in range(2):
                    force_x = xx[y] - pltpu.roll(xx[y], 1, 1) + (cross[y] - cross_down[y])
                    force_y = cross[y] - pltpu.roll(cross[y], 1, 1) + (yy[y] - yy_down[y])
                    u, v = new_velocity(lambda c: edge[c, strip, y], *vels[y], force_x, force_y)
                    edge[U, strip, y] = u
                    edge[V, strip, y] = v

        def sweep_flank(stress, velocity):
            spots = [pl.ds(j * TILE, TILE) for j in range(4)]
            vels = [[(flank[U, y, r, :], flank[V, y, r, :]) for y in range(2)] for r in spots]
            fresh = [
                [tuple(flank[c, y, r, :] for c in (S1, S2, S12)) for y in range(2)] for r in spots
            ]
            if stress:
                for j, r in enumerate(spots):
                    for y in range(2):
                        after = vels[min(j + 1, 3)][y]
                        east = [
                            pltpu.roll(jnp.where(sub == 0, b, x), TILE - 1, 0)
                            for x, b in zip(vels[j][y], after)
                        ]
                        ups = vels[j][1] if y == 0 else [
                            pltpu.roll(x, width - 1, 1) for x in vels[j][0]
                        ]
                        fresh[j][y] = new_stress(
                            flank[STRENGTH, y, r, :], *fresh[j][y], *vels[j][y], *east, *ups
                        )
                        for c, x in zip((S1, S2, S12), fresh[j][y]):
                            flank[c, y, r, :] = x
            if not velocity:
                return
            xx = [[0.5 * (s1 + s2) for s1, s2, _ in row] for row in fresh]
            yy = [[0.5 * (s1 - s2) for s1, s2, _ in row] for row in fresh]
            cross = [[s12 for _, _, s12 in row] for row in fresh]

            def westward(x, j, y):
                before = x[max(j - 1, 0)][y]
                return pltpu.roll(jnp.where(sub == TILE - 1, before, x[j][y]), 1, 0)

            def downward(x, j, y):
                return x[j][0] if y == 1 else pltpu.roll(x[j][1], 1, 1)

            for j, r in enumerate(spots):
                for y in range(2):
                    force_x = xx[j][y] - westward(xx, j, y) + (cross[j][y] - downward(cross, j, y))
                    force_y = cross[j][y] - westward(cross, j, y) + (yy[j][y] - downward(yy, j, y))
                    u, v = new_velocity(lambda c: flank[c, y, r, :], *vels[j][y], force_x, force_y)
                    flank[U, y, r, :] = u
                    flank[V, y, r, :] = v

        with jax.named_scope("i_pack0"):
            pack_flank(0)
            send_flank(0)
            pack_rows(0)
            pack_sides(0)
        tile_loop(tiles, 2, derive_main)

        with jax.named_scope("i_waitids"):
            wait_bytes(ids.at[pl.ds(0, peers - 1)], ids_rsem)
        wanted = me * per
        row_lane = lax.broadcasted_iota(jnp.int32, (per, count), 1)
        row_sub = lax.broadcasted_iota(jnp.int32, (per, count), 0)
        mine = row_lane == row_sub + wanted
        blocks = lax.broadcasted_iota(jnp.int32, (per, count), 1).astype(jnp.float32)
        base = (me * count).astype(jnp.float32)
        for p in range(peers):
            owned = jnp.broadcast_to(ids[p], (per, count)).astype(jnp.float32)
            local = jnp.sum(jnp.where(mine, owned, 0.0), axis=1, keepdims=True) - base
            one_hot[pl.ds(p * per, per), :] = jnp.where(local == blocks, 1.0, 0.0)

        with jax.named_scope("i_waithalo0"):
            for sems in (halo_ssem, early_rsem):
                wait_bytes(main.at[0], sems.at[3])
        with jax.named_scope("i_unpack0"):
            derive_flank()
            own_rows()

        def sweep_all(stress, velocity):
            for g in range(tiles // GROUP):
                sweep_main(g, stress, velocity)

        with jax.named_scope("i_stress"):
            sweep_all(True, False)
            sweep_flank(True, False)
        by_slot = one_hot[...]
        to_slots = jnp.concatenate([by_slot.astype(jnp.bfloat16)] * 2, axis=1)
        to_ends = jnp.concatenate([by_slot[:, :TILE], by_slot[:, count - TILE:]] * 2, axis=1)
        to_ends = to_ends.astype(jnp.bfloat16)
        by_block = by_slot.T.astype(jnp.bfloat16)
        to_blocks = jnp.concatenate([by_block] * 2, axis=1)

        with jax.named_scope("i_waitf4"):
            wait_bytes(recv.at[pl.ds(2, 4)], bulk_rsem.at[0])
        for c in range(2):
            both = dot_rows(to_blocks, recv[2 + c])
            for y in range(2):
                main[CUR_X + c, y] = both[:, y * width:(y + 1) * width]
        with jax.named_scope("i_packmid"):
            send_sides(0)
            send_ends(0)
            pack_rows(1)
            pack_sides(1)
            send_ends(1)
            send_sides(1)
            pack_flank(1)
            send_flank(1)
        for c in range(2):
            both = dot_rows(to_blocks, recv[4 + c])
            for y in range(2):
                main[PUSH_X + c, y] = main[MASS, y] * both[:, y * width:(y + 1) * width]
        for y in range(2):
            share = main[CONC, y] * main[ACTIVE, y]
            back[2, :, pl.ds(y * width, width)] = dot_rows(to_slots, share)

        with jax.named_scope("i_waitf2"):
            wait_bytes(recv.at[pl.ds(0, 2)], bulk_rsem.at[1])
        with jax.named_scope("i_push"):
            for c in range(2):
                both = dot_rows(to_blocks, recv[c])
                for y in range(2):
                    main[PUSH_X + c, y] = main[ACTIVE, y] * (
                        main[CONC, y] * both[:, y * width:(y + 1) * width] - main[PUSH_X + c, y]
                    )
        with jax.named_scope("i_packlate"):
            pack_sides(2)
            send_sides(2)
            pack_flank(2)
            send_flank(2)
            pack_rows(2)
            send_ends(2)

        def leave(get, u, v):
            dx, dy = u - get(CUR_X), v - get(CUR_Y)
            drag = get(DRAG) * jnp.sqrt(dx * dx + dy * dy + DRAG_FLOOR)
            return drag * dx, drag * dy

        outer = (lane < NSUB) | (lane >= width - NSUB)

        with jax.named_scope("i_vel1"):
            sweep_all(False, True)
        with jax.named_scope("i_sweeps"):
            tile_loop(NSUB - 1, 1, lambda k: sweep_all(True, True))
        send_rows(0, back, 2, 1, ret, 2, bulk_ssem, bulk_rsem.at[0])

        def returned(t):
            r = pl.ds(pl.multiple_of(t * TILE, TILE), TILE)
            block = sub + t * TILE
            theirs = outer | (block < 2) | (block >= count - 2)
            for y in range(2):
                half = pl.ds(y * width, width)
                u, v = main[U, y, r, :], main[V, y, r, :]
                gone = leave(lambda c: main[c, y, r, :], u, v)
                for c in range(2):
                    forc[c, r, half] = jnp.where(theirs, 0.0, gone[c])

        with jax.named_scope("i_back"):
            tile_loop(tiles, 4, returned)
            for c in range(2):
                back[c] = dot_rows(to_slots, forc[c])
        with jax.named_scope("i_waitearly"):
            when_inside(-1, 6, early_rsem.at[0])
            when_inside(1, 6, early_rsem.at[1])
            wait_tiles(2, early_rsem.at[2])
        with jax.named_scope("i_early"):
            unpack_rows(0, True)
            unpack_sides(0)
            derive_edges()
            sweep_edge(True, False)
        with jax.named_scope("i_waitmid"):
            when_inside(-1, 3, mid_rsem.at[0])
            when_inside(1, 3, mid_rsem.at[1])
            wait_tiles(2, mid_rsem.at[2])
            wait_tiles(8, mid_rsem.at[3])
        unpack_rows(1)
        unpack_sides(1)
        with jax.named_scope("i_waitlate"):
            when_inside(-1, 3, late_rsem.at[0])
            when_inside(1, 3, late_rsem.at[1])
            wait_tiles(2, late_rsem.at[2])
            wait_tiles(8, late_rsem.at[3])

        def sweep_strips(stress, velocity):
            sweep_flank(stress, velocity)
            sweep_edge(stress, velocity)

        with jax.named_scope("i_edge"):
            unpack_rows(2)
            unpack_sides(2)
            sweep_strips(False, True)
            for _ in range(NSUB - 1):
                sweep_strips(True, True)

        with jax.named_scope("i_fix"):
            for y in range(2):
                for j, far in ((1, 0), (2, count - TILE)):
                    r = pl.ds(j * TILE, TILE)
                    held = (lane >= 2) & (lane < count - 2)
                    held = held & ((sub < NSUB) if j == 1 else (sub >= TILE - NSUB))
                    u, v = flank[U, y, r, :], flank[V, y, r, :]
                    gone = leave(lambda c: flank[c, y, r, :], u, v)
                    for c in range(2):
                        slot = (c * 2 + y) * 2 * TILE + (TILE if j == 1 else 0)
                        flank_back[pl.ds(slot, TILE), :] = jnp.where(held, gone[c], 0.0)
                        flank_vel[c, y, pl.ds(far, TILE), :] = jnp.where(held, (u, v)[c], 0.0)
                for strip in range(2):
                    def get(c):
                        return edge[c, strip, y, :, pl.ds(0, width)]
                    gone = leave(get, get(U), get(V))
                    held = (sub < 2) if strip == 0 else (sub >= TILE - 2)
                    for c in range(2):
                        moved = pltpu.roll(gone[c], TILE - 2 if strip == 0 else 2, 0)
                        ends[c, pl.ds(strip * TILE, TILE), pl.ds(y * width, width)] = jnp.where(
                            held, moved, 0.0
                        )
            across = dot_lanes(to_slots, flank_back[...])
            for c in range(2):
                rest = dot_rows(to_ends, ends[c])
                for y in range(2):
                    slot = (c * 2 + y) * 2 * TILE
                    for t in range(tiles):
                        r, half = pl.ds(t * TILE, TILE), pl.ds(y * width, width)
                        moved = pltpu.roll(across[t * TILE:(t + 1) * TILE], width - TILE - slot, 1)
                        back[c, r, half] += jnp.where(outer, moved, 0.0) + (
                            rest[t * TILE:(t + 1) * TILE, y * width:(y + 1) * width]
                        )
                send_rows(0, back, c, 1, ret, c, bulk_ssem, bulk_rsem.at[1], "home")
            send_rows(0, back, 0, 2, ret, 0, bulk_ssem, bulk_rsem.at[1], "away")

        same = jnp.where(diag, 1.0, 0.0).astype(jnp.bfloat16)
        same = jnp.concatenate([same] * 2, axis=1)
        for y in range(2):
            for c in range(2):
                half = pl.ds(y * width, width)
                for strip, r in ((0, top), (1, bottom)):
                    end = pltpu.roll(
                        edge[c, strip, y, :, pl.ds(0, width)], TILE - 2 if strip == 0 else 2, 0
                    )
                    held = (sub < 2) if strip == 0 else (sub >= TILE - 2)
                    main[c, y, r, :] = jnp.where(held, end, main[c, y, r, :])
                other = dot_lanes(same, flank_vel[c, y])
                row = lax.broadcasted_iota(jnp.int32, (count, width), 0)
                column = lax.broadcasted_iota(jnp.int32, (count, width), 1)
                theirs = (row >= 2) & (row < count - 2)
                theirs = theirs & ((column < NSUB) | (column >= width - NSUB))
                out[0, c, :, half] = jnp.where(theirs, other, main[c, y])
        wait_bytes(ids.at[pl.ds(0, peers - 1)], ids_ssem)
        wait_bytes(back, bulk_ssem)
        when_inside(-1, 12, halo_ssem.at[0])
        when_inside(1, 12, halo_ssem.at[1])
        wait_tiles(6, halo_ssem.at[2])
        wait_tiles(16, halo_ssem.at[3])


def per_device_kernel(n_lat, n_lon, fields, block_owner, ice_covered, land_mask):
    count, cells = land_mask.shape
    peers = n_lat * n_lon
    f32 = jnp.float32
    anywhere = pl.BlockSpec(memory_space=pl.ANY)
    dma = pltpu.SemaphoreType.DMA
    halos = [pltpu.VMEM((2, num // 2, TILE, BX), f32) for _, num in ROUNDS] * 2
    sides = [pltpu.VMEM((2, TILE, BX), f32) for _ in ROUNDS]
    sides += [pltpu.VMEM((3, 2, TILE, BX), f32) for _ in ROUNDS]
    return pl.pallas_call(
        functools.partial(step_kernel, n_lat, n_lon),
        out_shape=pltpu.VMEM((1, 2, count, cells), f32),
        in_specs=[anywhere, anywhere, anywhere, anywhere],
        out_specs=pl.BlockSpec(memory_space=pltpu.VMEM),
        scratch_shapes=[
            pltpu.VMEM((7, count, cells), f32),
            pltpu.VMEM((2, count, cells), f32),
            pltpu.VMEM((3, count, cells), f32),
            pltpu.VMEM((1, count), jnp.int32),
            pltpu.VMEM((1, count), jnp.int32),
            pltpu.VMEM((peers, 1, count), jnp.int32),
            pltpu.VMEM((6, count, cells), f32),
            pltpu.VMEM((2, count, cells), f32),
            pltpu.VMEM((count, count), f32),
            pltpu.VMEM((3, count, cells), f32),
            pltpu.VMEM((count, cells), jnp.int32),
            pltpu.VMEM((14, 2, count, BX), f32),
            pltpu.VMEM((14, 2, 2, TILE, 2 * BX), f32),
            pltpu.VMEM((14, 2, 4 * TILE, BX), f32),
            pltpu.VMEM((BX, count), f32),
            pltpu.VMEM((2, 2, BX, count), f32),
            pltpu.VMEM((2, 2 * TILE, cells), f32),
            *halos, *sides,
            dma, dma((2,)), dma, dma, dma((4,)), dma((4,)), dma((4,)), dma((4,)),
            pltpu.SemaphoreType.REGULAR,
        ],
        compiler_params=pltpu.CompilerParams(
            collective_id=0, has_side_effects=True, vmem_limit_bytes=63 * 1024 * 1024
        ),
    )(fields, block_owner.reshape(1, count), ice_covered.reshape(1, count), land_mask)


def solution(mesh):
    placed = (
        P("comp", None, ("lat", "lon"), None),
        P(("lat", "lon")),
        P(("lat", "lon")),
        P(("lat", "lon"), None),
    )
    n_lat, n_lon = mesh.shape["lat"], mesh.shape["lon"]

    def body(fields, block_owner, ice_covered, land_mask):
        count = block_owner.shape[0]
        whole_tiles = count % (n_lat * n_lon * TILE) == 0 and count == BX
        if whole_tiles and n_lon > 2:
            return per_device_kernel(n_lat, n_lon, fields, block_owner, ice_covered, land_mask)
        return per_device(fields, block_owner, ice_covered, land_mask)

    return jax.shard_map(
        body,
        mesh=mesh,
        in_specs=placed,
        out_specs=P("comp", None, ("lat", "lon"), None),
        check_vma=False,
    )
```
